32 devices in a mesh: dp: 2 (over core), row: 4 (over y, x), col: 4 (over z).
Axes of the slice: x: 2, y: 2, z: 4, core: 2. Of those that a mesh axis runs over, the one named last changes fastest.
Arguments:
- tokens: bfloat16 [4, 768, 2048], P('dp', 'row', 'col'), may hold values from -6 to 6
- segments: int32 [4, 2048], P('dp'), may hold values from 0 to 5, never falling along the last dimension, each value on 1 to 800 neighbouring positions
- labels: int32 [4, 6], P('dp'), may hold values from 0 to 13
- cotangent: bfloat16 [4, 768, 2048], P('dp', 'row', 'col'), may hold values from -6 to 6
- w_qkv: bfloat16 [768, 2304], P('row', 'col'), may hold values from -0.21875 to 0.21875
- b_qkv: float32 [2, 768], P(None, 'col'), may hold values from -0.75 to 0.75
- w_out: bfloat16 [768, 768], P('col', 'row'), may hold values from -2.5 to 2.5
- b_out: float32 [768], P('row'), may hold values from -4 to 4
- ln1_gain: float32 [768], P('row'), may hold values from 0.5 to 1.5
- ln1_bias: float32 [768], P('row'), may hold values from -4 to 4
- w_in: bfloat16 [768, 3072], P('row', 'col'), may hold values from -0.21875 to 0.21875
- b_in: float32 [3072], P('col'), may hold values from -4 to 4
- w_back: bfloat16 [768, 3072], P('row', 'col'), may hold values from -0.109375 to 0.109375
- b_back: float32 [768], P('row'), may hold values from -4 to 4
- ln2_gain: float32 [768], P('row'), may hold values from 0.5 to 1.5
- ln2_bias: float32 [768], P('row'), may hold values from -4 to 4
- s_proj: bfloat16 [768, 128], P('row'), may hold values from -0.21875 to 0.21875
- s_bias: float32 [128], replicated, may hold values from -4 to 4
- s_query: float32 [128], replicated, may hold values from -4 to 4
- s_mid: float32 [128, 128], replicated, may hold values from -0.5 to 0.5
- s_mid_bias: float32 [128], replicated, may hold values from -4 to 4
- s_cls: float32 [128, 14], replicated, may hold values from -0.5 to 0.5
- s_cls_bias: float32 [14], replicated, may hold values from -6 to 6
Outputs:
- out: bfloat16 [4, 768, 2048], P('dp', 'row', 'col')
- logits: float32 [4, 6, 14], P('dp')
- tokens_grad: float32 [4, 768, 2048], P('dp', 'row', 'col')
- w_qkv_grad: float32 [768, 2304], P('row', 'col')
- b_qkv_grad: float32 [2, 768], P(None, 'col')
- w_out_grad: float32 [768, 768], P('col', 'row')
- b_out_grad: float32 [768], P('row')
- ln1_gain_grad: float32 [768], P('row')
- ln1_bias_grad: float32 [768], P('row')
- w_in_grad: float32 [768, 3072], P('row', 'col')
- b_in_grad: float32 [3072], P('col')
- w_back_grad: float32 [768, 3072], P('row', 'col')
- b_back_grad: float32 [768], P('row')
- ln2_gain_grad: float32 [768], P('row')
- ln2_bias_grad: float32 [768], P('row')
- s_proj_grad: float32 [768, 128], P('row')
- s_bias_grad: float32 [128], replicated
- s_query_grad: float32 [128], replicated
- s_mid_grad: float32 [128, 128], replicated
- s_mid_bias_grad: float32 [128], replicated
- s_cls_grad: float32 [128, 14], replicated
- s_cls_bias_grad: float32 [14], replicated
The draws below stay inside these ranges and needn't reach their ends.
Inputs may be any that keep to these rules, and one draw needn't show every extreme that they name: `segments`: in each sequence the ids never fall, every id from 0 to 5 is present, every document has 1 to 800 tokens, and some document has exactly 800.
All inputs are finite; a program needn't handle non-finite values.
Results may differ from the reference program's by a relative error of at most 0.015.
Values may be sent and summed in bfloat16 or wider, within the bound.
A program may use at most 192 MiB of HBM per device.

```python
import math
import jax
import jax.numpy as jnp
import numpy as np
from jax import lax

D = 768
HEADS = 12
HD = 64
FF = 3072
SH = 2
SHD = 64
SW = 128
CLASSES = 14
L = 2048
DOCS = 6
MOST = 800
SEQS = 4


def touch_ends(values, rng, low, high):
    extent = values.shape
    index_at = [jax.random.randint(jax.random.fold_in(rng, axis), (), 0, extent[axis]) for axis in range(len(extent))]
    values = values.at[tuple(index_at)].set(low)
    longest = extent.index(max(extent))
    index_at[longest] = (index_at[longest] + 1) % extent[longest]
    return values.at[tuple(index_at)].set(high)


def block_levels(rng, dims, split, smallest, largest):
    def one(axis_at, parts):
        draws = jax.random.uniform(jax.random.fold_in(jax.random.fold_in(rng, 6), axis_at), (parts,), jnp.float32, smallest / len(split), largest / len(split))
        return jnp.repeat(jnp.exp(draws), dims[axis_at] // parts).reshape((-1,) + (1,) * (len(dims) - axis_at - 1))

    loudness = one(*split[0])
    for cut in split[1:]:
        loudness = loudness * one(*cut)
    return loudness


def split_up(count, total, bound, lean):
    loads = [(1 << 20) // math.isqrt(grade ** lean) + 1 for grade in range(2, count + 1)]
    surplus, holding = total - bound - (count - 1), [1] * (count - 1)
    while surplus > 0:
        free = [i for i in range(count - 1) if holding[i] < bound]
        mass, remaining = sum([loads[i] for i in free]), surplus
        for i in free:
            more = min(bound - holding[i], max(1, remaining * loads[i] // mass), surplus)
            holding[i] = holding[i] + more
            surplus = surplus - more
    return np.array([bound] + holding)


def ragged_sizes(stream_key, number_of, total, reach, slope):
    if number_of == 2:
        one = jax.random.randint(stream_key, (), max(1, total - reach), min(reach, total - 1) + 1)
        return jnp.stack([one, total - one])
    sizes = jnp.asarray(split_up(number_of, total, reach, slope), jnp.int32)
    pairs = (number_of - 1) // 2
    donor, receiver = sizes[1:1 + 2 * pairs:2], sizes[2:2 + 2 * pairs:2]
    slack = jnp.minimum(donor - 1, reach - receiver)
    passed = jax.random.randint(jax.random.fold_in(stream_key, 1), (pairs,), 0, 1 << 20) % (slack + 1)
    sizes = sizes.at[1:1 + 2 * pairs:2].set(donor - passed).at[2:2 + 2 * pairs:2].set(receiver + passed)
    return sizes[jax.random.permutation(jax.random.fold_in(stream_key, 2), number_of)]


def normal_values(key, dims, scale, most, split=(), kind=jnp.bfloat16):
    drawn = scale * jax.random.normal(key, dims, jnp.float32)
    if split:
        drawn = drawn * block_levels(key, dims, split, -0.22, 0.18)
    return jnp.clip(drawn, -most, most).astype(kind)


def setup_inputs(seed: int = 0) -> dict:
    key_of = jax.random.split(jax.random.key(seed), 24)
    tokens = normal_values(key_of[0], (SEQS, D, L), 1.0, 6.0, ((0, 2), (1, 4), (2, 4)))
    segments = jax.vmap(lambda own: jnp.searchsorted(jnp.cumsum(ragged_sizes(own, DOCS, L, MOST, 1)), jnp.arange(L), side="right"))(jax.random.split(key_of[1], SEQS)).reshape((SEQS, L)).astype(jnp.int32)
    labels = touch_ends(jax.random.randint(key_of[2], (SEQS, DOCS), 0, CLASSES), jax.random.fold_in(key_of[2], 1), 0, CLASSES - 1).astype(jnp.int32)
    cotangent = normal_values(key_of[3], (SEQS, D, L), 1.0, 6.0, ((0, 2), (1, 4), (2, 4)))
    w_qkv = normal_values(key_of[4], (D, 3 * D), D ** -0.5, 0.21875, ((0, 4), (1, 4)))
    b_qkv = normal_values(key_of[5], (2, D), 0.05, 0.75, ((1, 4),), jnp.float32)
    w_out = normal_values(key_of[6], (D, D), (max(D // 128, 1)) ** -0.5, 2.5, ((0, 4), (1, 4)))
    b_out = normal_values(key_of[7], (D,), 0.3, 4.0, ((0, 4),), jnp.float32)
    ln1_gain = jnp.clip(1.0 + 0.1 * jax.random.normal(key_of[8], (D,), jnp.float32), 0.5, 1.5)
    ln1_bias = normal_values(key_of[9], (D,), 0.3, 4.0, ((0, 4),), jnp.float32)
    w_in = normal_values(key_of[10], (D, FF), D ** -0.5, 0.21875, ((0, 4), (1, 4)))
    b_in = normal_values(key_of[11], (FF,), 0.3, 4.0, ((0, 4),), jnp.float32)
    w_back = normal_values(key_of[12], (D, FF), FF ** -0.5, 0.109375, ((0, 4), (1, 4)))
    b_back = normal_values(key_of[13], (D,), 0.3, 4.0, ((0, 4),), jnp.float32)
    ln2_gain = jnp.clip(1.0 + 0.1 * jax.random.normal(key_of[14], (D,), jnp.float32), 0.5, 1.5)
    ln2_bias = normal_values(key_of[15], (D,), 0.3, 4.0, ((0, 4),), jnp.float32)
    s_proj = normal_values(key_of[16], (D, SW), D ** -0.5, 0.21875, ((0, 4),))
    s_bias = normal_values(key_of[17], (SW,), 0.3, 4.0, (), jnp.float32)
    s_query = normal_values(key_of[18], (SW,), 1.0, 4.0, (), jnp.float32)
    s_mid = normal_values(key_of[19], (SW, SW), SW ** -0.5, 0.5, (), jnp.float32)
    s_mid_bias = normal_values(key_of[20], (SW,), 0.3, 4.0, (), jnp.float32)
    s_cls = normal_values(key_of[21], (SW, CLASSES), SW ** -0.5, 0.5, (), jnp.float32)
    s_cls_bias = normal_values(key_of[22], (CLASSES,), 0.5, 6.0, (), jnp.float32)
    return {"tokens": tokens, "segments": segments, "labels": labels, "cotangent": cotangent, "w_qkv": w_qkv, "b_qkv": b_qkv, "w_out": w_out, "b_out": b_out, "ln1_gain": ln1_gain, "ln1_bias": ln1_bias, "w_in": w_in, "b_in": b_in, "w_back": w_back, "b_back": b_back, "ln2_gain": ln2_gain, "ln2_bias": ln2_bias, "s_proj": s_proj, "s_bias": s_bias, "s_query": s_query, "s_mid": s_mid, "s_mid_bias": s_mid_bias, "s_cls": s_cls, "s_cls_bias": s_cls_bias}


norm_eps = 1e-06
masked_value = -1e+30

@jax.custom_vjp
def low(v):
    return lax.optimization_barrier(v.astype(jnp.bfloat16)).astype(jnp.float32)

@jax.custom_vjp
def low_back(v):
    return v

def low_keep(v):
    return (low(v), None)

def low_pass(kept, grad):
    return (grad,)

def back_keep(v):
    return (v, None)

def back_low(kept, grad):
    return (low(grad),)
low.defvjp(low_keep, low_pass)
low_back.defvjp(back_keep, back_low)

def round_both(values):
    return low(low_back(values))

def matmul_hi(first_op, second_op):
    return jnp.dot(first_op, second_op, precision=lax.Precision.HIGHEST)

def layer_norm(values, gain_vec, bias_vec):
    center = values - lax.optimization_barrier(jnp.mean(values, axis=-1, keepdims=True))
    spread = lax.optimization_barrier(jnp.mean(center * center, axis=-1, keepdims=True))
    return center * lax.rsqrt(spread + norm_eps) * gain_vec + bias_vec

def block_forward(params, inputs, seg_ids):
    w_qkv, b_qkv, w_out, b_out, gain_one, bias_one, w_in, b_in, w_back, b_back, gain_two, bias_two = params
    w_three = w_qkv.reshape(D, HEADS, 3, HD).transpose(0, 2, 1, 3).reshape(D, 3, D)
    qkv_all = jnp.einsum('td,dkf->tkf', inputs, w_three, precision=lax.Precision.HIGHEST)
    offsets = jnp.stack([b_qkv[0], jnp.zeros_like(b_qkv[0]), b_qkv[1]])
    qkv_all = round_both(qkv_all + offsets[None])
    queries = qkv_all[:, 0].reshape(L, HEADS, HD)
    key_rows = qkv_all[:, 1].reshape(L, HEADS, HD)
    value_rows = qkv_all[:, 2].reshape(L, HEADS, HD)
    q_block = min(512, L)

    def attend(pieces):
        query_rows, query_segs = pieces
        scores = jnp.einsum('qhd,khd->hqk', query_rows, key_rows, precision=lax.Precision.HIGHEST) * HD ** (-0.5)
        scores = low_back(scores)
        same_doc = query_segs[:, None] == seg_ids[None, :]
        scores = jnp.where(same_doc[None], scores, masked_value)
        row_top = lax.optimization_barrier(jnp.max(scores, axis=-1, keepdims=True))
        exp_scores = jnp.exp(scores - row_top)
        probs_f = exp_scores / lax.optimization_barrier(jnp.sum(exp_scores, axis=-1, keepdims=True))
        return jnp.einsum('hqk,khd->qhd', low(probs_f), value_rows, precision=lax.Precision.HIGHEST)
    blocks = L // q_block
    context = lax.map(jax.checkpoint(attend), (queries.reshape(blocks, q_block, HEADS, HD), seg_ids.reshape(blocks, q_block)))
    context = round_both(context.reshape(L, D))
    attn_out = low_back(matmul_hi(context, w_out) + b_out)
    hidden_one = layer_norm(inputs + attn_out, gain_one, bias_one)
    pre_act = low_back(matmul_hi(low(hidden_one), w_in) + b_in)
    activation = low(jax.nn.gelu(pre_act, approximate=False))
    ffn_out = low_back(matmul_hi(activation, w_back.T) + b_back)
    return layer_norm(hidden_one + ffn_out, gain_two, bias_two)

def student_logits(sparams, layer_out, seg_ids):
    s_proj, s_bias, s_query, s_mid, s_mid_bias, s_cls, s_cls_bias = sparams
    hidden_s = matmul_hi(layer_out, s_proj) + s_bias
    head_parts = hidden_s.reshape(L, SH, SHD)
    pool_logit = lax.optimization_barrier(jnp.sum(head_parts * s_query.reshape(SH, SHD), axis=-1)) * SHD ** (-0.5)
    member = seg_ids[:, None] == jnp.arange(DOCS, dtype=jnp.int32)[None, :]
    masked = jnp.where(member[:, :, None], pool_logit[:, None, :], masked_value)
    doc_top = lax.optimization_barrier(jnp.max(masked, axis=0))
    weights_e = jnp.where(member[:, :, None], jnp.exp(masked - doc_top[None]), 0.0)
    shares = weights_e / lax.optimization_barrier(jnp.sum(weights_e, axis=0))[None]
    pooled = jnp.einsum('tdh,thk->dhk', shares, head_parts, precision=lax.Precision.HIGHEST).reshape(DOCS, SW)
    middle = jnp.tanh(matmul_hi(pooled, s_mid) + s_mid_bias)
    return matmul_hi(middle, s_cls) + s_cls_bias

def student_loss(sparams, layer_out, seg_ids, label_ids):
    logit_rows = student_logits(sparams, layer_out, seg_ids)
    row_top = lax.optimization_barrier(jnp.max(logit_rows, axis=-1, keepdims=True))
    log_total = row_top[:, 0] + jnp.log(lax.optimization_barrier(jnp.sum(jnp.exp(logit_rows - row_top), axis=-1)))
    chosen = label_ids[:, None] == jnp.arange(CLASSES, dtype=jnp.int32)[None, :]
    picked = lax.optimization_barrier(jnp.sum(jnp.where(chosen, logit_rows, 0.0), axis=-1))
    return (jnp.sum(log_total - picked), logit_rows)

def reference(tokens, segments, labels, cotangent, w_qkv, b_qkv, w_out, b_out, ln1_gain, ln1_bias, w_in, b_in, w_back, b_back, ln2_gain, ln2_bias, s_proj, s_bias, s_query, s_mid, s_mid_bias, s_cls, s_cls_bias):
    layer_params = (w_qkv.astype(jnp.float32), b_qkv, w_out.astype(jnp.float32), b_out, ln1_gain, ln1_bias, w_in.astype(jnp.float32), b_in, w_back.astype(jnp.float32), b_back, ln2_gain, ln2_bias)
    student_params = (s_proj.astype(jnp.float32), s_bias, s_query, s_mid, s_mid_bias, s_cls, s_cls_bias)
    zero_grads = jax.tree.map(jnp.zeros_like, (layer_params, student_params))

    def one_sequence(carry, inputs):
        tok_seq, seg_seq, lab_seq, cot_seq = inputs

        def forward_fn(params, values):
            return block_forward(params, values, seg_seq)
        layer_out, back_fn = jax.vjp(forward_fn, layer_params, tok_seq.astype(jnp.float32).T)
        grad_layer, grad_tokens = back_fn(cot_seq.astype(jnp.float32).T)
        out_low = layer_out.astype(jnp.bfloat16)

        def loss_fn(sparams):
            return student_loss(sparams, out_low.astype(jnp.float32), seg_seq, lab_seq)
        loss_value, student_back, logit_rows = jax.vjp(loss_fn, student_params, has_aux=True)
        grad_student, = student_back(jnp.ones_like(loss_value))
        carry = jax.tree.map(jnp.add, carry, (grad_layer, grad_student))
        return (carry, (out_low.T, logit_rows, grad_tokens.T))
    (grad_layer, grad_student), (outs, logit_all, grad_tokens) = lax.scan(one_sequence, zero_grads, (tokens, segments, labels, cotangent))
    return (outs, logit_all, grad_tokens, grad_layer[0], grad_layer[1], grad_layer[2], grad_layer[3], grad_layer[4], grad_layer[5], grad_layer[6], grad_layer[7], grad_layer[8], grad_layer[9], grad_layer[10], grad_layer[11], grad_student[0], grad_student[1], grad_student[2], grad_student[3], grad_student[4], grad_student[5], grad_student[6])
```

```python
import jax
import jax.numpy as jnp
from jax import lax
from jax.sharding import PartitionSpec as P

HD = 64
SH = 2
SHD = 64

norm_eps = 1e-06
masked_value = -1e30
highest = lax.Precision.HIGHEST
f32 = jnp.float32
bf16 = jnp.bfloat16
WORLD = ("col", "row", "dp")


def sizes(seqs_local):
    parts = lax.axis_size("dp")
    rows = lax.axis_size("row")
    seqs = seqs_local * parts
    return parts, rows, lax.axis_size("col"), seqs, rows // seqs


def row_groups(rows, sub):
    return [list(range(at, at + sub)) for at in range(0, rows, sub)]


def take_in(values):
    parts, rows, _, seqs, sub = sizes(values.shape[0])
    held = lax.all_to_all(values, "dp", 2, 0, tiled=True)
    feats, half = held.shape[1:]
    held = held.reshape(seqs, feats, sub, half // sub).transpose(0, 2, 1, 3)
    held = held.reshape(rows, feats, half // sub)
    held = lax.all_to_all(held, "row", 0, 0, tiled=True)
    return held.reshape(rows * feats, half // sub)


def give_back(values, seqs_local):
    parts, rows, _, seqs, sub = sizes(seqs_local)
    width, own = values.shape
    feats = width // rows
    held = lax.all_to_all(values.reshape(rows, feats, own), "row", 0, 0, tiled=True)
    held = held.reshape(seqs, sub, feats, own).transpose(0, 2, 1, 3).reshape(seqs, feats, sub * own)
    return lax.all_to_all(held, "dp", 0, 2, tiled=True)


def gather_world(shard):
    cols, rows = lax.axis_size("col"), lax.axis_size("row")
    out = lax.all_gather(shard, WORLD, axis=0, tiled=True)
    return out.reshape(cols, rows, -1, shard.shape[1])


def own_half(block):
    parts = lax.axis_size("dp")
    amount = block.shape[0] // parts
    return lax.dynamic_slice_in_dim(block, lax.axis_index("dp") * amount, amount)


def scatter_world(full):
    flat = full.reshape(-1, full.shape[-1])
    mine = lax.psum_scatter(flat, WORLD, scatter_dimension=0, tiled=True)
    return lax.all_gather(mine, "dp", axis=0, tiled=True)


def swap_cols(values):
    return lax.all_to_all(values, "col", 0, 0, tiled=True)


def gather_sequence(values, sub):
    cols, own, width = values.shape
    held = values[:, None]
    if sub > 1:
        groups = row_groups(lax.axis_size("row"), sub)
        held = lax.all_gather(held, "row", axis=1, tiled=True, axis_index_groups=groups)
    held = lax.all_gather(held[:, None], "dp", axis=1, tiled=True)
    return held.reshape(-1, width)


def scatter_sequence(values, cols, sub):
    parts = lax.axis_size("dp")
    width = values.shape[-1]
    held = values.reshape(cols, parts, sub, -1, width)
    held = lax.psum_scatter(held, "dp", scatter_dimension=1, tiled=True)[:, 0]
    if sub > 1:
        groups = row_groups(lax.axis_size("row"), sub)
        held = lax.psum_scatter(
            held, "row", scatter_dimension=1, tiled=True, axis_index_groups=groups
        )
    return held[:, 0]


def normalize(values):
    mean_v = jnp.mean(values, axis=-1, keepdims=True)
    center = values - mean_v
    inv_std = lax.rsqrt(jnp.mean(center * center, axis=-1, keepdims=True) + norm_eps)
    return center * inv_std, inv_std


def normalize_back(grad_hat, normed, inv_std):
    return inv_std * (
        grad_hat
        - jnp.mean(grad_hat, axis=-1, keepdims=True)
        - normed * jnp.mean(grad_hat * normed, axis=-1, keepdims=True)
    )


def gelu_exact(values):
    return jax.nn.gelu(values, approximate=False)


def mm(a, b, contract):
    return lax.dot_general(a, b, (contract, ((), ())), preferred_element_type=f32)


def combine_pool(part_one, part_two):
    top_a, total_a, sum_a = part_one
    top_b, total_b, sum_b = part_two
    row_top = jnp.maximum(top_a, top_b)
    factor_a = jnp.exp(top_a - row_top)
    factor_b = jnp.exp(top_b - row_top)
    return (
        row_top,
        total_a * factor_a + total_b * factor_b,
        sum_a * factor_a[:, :, None] + sum_b * factor_b[:, :, None],
    )


def attend(q, k, v, q_seg, k_seg, scale):
    scores = jnp.einsum("qhd,khd->hqk", q, k, preferred_element_type=f32) * scale
    scores = jnp.where((q_seg[:, None] == k_seg[None, :])[None], scores, masked_value)
    top = jnp.max(scores, axis=-1, keepdims=True)
    exp_scores = jnp.exp(scores - top)
    total = jnp.sum(exp_scores, axis=-1, keepdims=True)
    probs = exp_scores / total
    context = jnp.einsum("hqk,khd->qhd", probs.astype(bf16), v, preferred_element_type=f32)
    return context.astype(bf16), probs


def attend_back(q, k, v, probs, d_ctx, scale):
    d_probs = jnp.einsum("qhd,khd->hqk", d_ctx, v, preferred_element_type=f32)
    delta = jnp.sum(probs * d_probs, axis=-1, keepdims=True)
    d_scores = (probs * (d_probs - delta)).astype(bf16)
    d_q = jnp.einsum("hqk,khd->qhd", d_scores, k, preferred_element_type=f32) * scale
    d_k = jnp.einsum("hqk,qhd->khd", d_scores, q, preferred_element_type=f32) * scale
    d_v = jnp.einsum("hqk,qhd->khd", probs.astype(bf16), d_ctx, preferred_element_type=f32)
    return d_q, d_k, d_v


def local(
    tokens,
    segments,
    labels,
    cotangent,
    w_qkv,
    b_qkv,
    w_out,
    b_out,
    ln1_gain,
    ln1_bias,
    w_in,
    b_in,
    w_back,
    b_back,
    ln2_gain,
    ln2_bias,
    s_proj,
    s_bias,
    s_query,
    s_mid,
    s_mid_bias,
    s_cls,
    s_cls_bias,
):
    seqs_local, width_row, cols_local = tokens.shape
    parts, rows, cols, seqs, sub = sizes(seqs_local)
    width = width_row * rows
    own = cols_local // (parts * sub)
    width_col = b_qkv.shape[1]
    heads_dev = width_col // HD
    hidden_col = b_in.shape[0]
    docs_count = labels.shape[1]
    class_count = s_cls.shape[1]
    student_width = s_proj.shape[1]
    row_index = lax.axis_index("row")
    col_index = lax.axis_index("col")
    dp_index = lax.axis_index("dp")
    seq_index = row_index // sub
    sub_index = row_index % sub
    score_scale = HD ** (-0.5)
    pool_scale = SHD ** (-0.5)
    query_heads = s_query.reshape(SH, SHD)
    doc_ids = jnp.arange(docs_count, dtype=jnp.int32)
    class_ids = jnp.arange(class_count, dtype=jnp.int32)

    w_qkv_all = gather_world(own_half(w_qkv)).reshape(cols, width, 3 * width_col)
    x_t = take_in(tokens)
    rest = jnp.concatenate([own_half(w_in), own_half(w_back), own_half(w_out).reshape(-1, width_col)], axis=1)
    rest_all = gather_world(rest)
    w_in_all = rest_all[..., :hidden_col].reshape(cols, width, hidden_col)
    w_back_all = rest_all[..., hidden_col : 2 * hidden_col].reshape(cols, width, hidden_col)
    w_out_all = rest_all[..., 2 * hidden_col :].reshape(cols, rows, width_col, width_row)
    w_out_all = w_out_all.transpose(0, 2, 1, 3).reshape(width, width)
    row_vectors = lax.all_gather(
        jnp.stack([b_out, ln1_gain, ln1_bias, b_back, ln2_gain, ln2_bias]), "row", axis=1, tiled=True
    )
    b_out_a, gain_one, bias_one, b_back_a, gain_two, bias_two = [row_vectors[i] for i in range(6)]
    b_qkv_all = lax.all_gather(b_qkv, "col")
    b_in_all = lax.all_gather(b_in, "col")
    s_proj_all = lax.all_gather(s_proj, "row", axis=0, tiled=True)
    whole_ints = lax.all_gather(jnp.concatenate([segments, labels], axis=1), "dp", axis=0, tiled=True)
    ints = lax.dynamic_index_in_dim(whole_ints, seq_index, 0, False)
    seq_len = segments.shape[1]
    seg_all, label_seq = ints[:seq_len], ints[seq_len:]
    seg_blocks = seg_all.reshape(cols, parts, sub, own)
    seg_q = lax.dynamic_index_in_dim(seg_blocks, dp_index, 1, False)
    seg_q = lax.dynamic_index_in_dim(seg_q, sub_index, 1, False)
    seg_own = lax.dynamic_index_in_dim(seg_q, col_index, 0, False)
    seg_q = seg_q.reshape(-1)

    x = x_t.T
    offsets = jnp.stack([b_qkv_all[:, 0], jnp.zeros_like(b_qkv_all[:, 0]), b_qkv_all[:, 1]], axis=1)
    offsets = offsets.reshape(cols, 3, heads_dev, HD).transpose(0, 2, 1, 3).reshape(cols, 1, -1)
    qkv = jnp.einsum("td,cdn->ctn", x, w_qkv_all, preferred_element_type=f32) + offsets
    qkv = swap_cols(qkv.astype(bf16)).reshape(cols, own, heads_dev, 3, HD)
    queries = qkv[:, :, :, 0].reshape(cols * own, heads_dev, HD)
    kv = gather_sequence(qkv[:, :, :, 1:].reshape(cols, own, -1), sub)
    kv = kv.reshape(seq_len, heads_dev, 2, HD)
    key_rows, value_rows = kv[:, :, 0], kv[:, :, 1]
    context, probs = attend(queries, key_rows, value_rows, seg_q, seg_all, score_scale)
    ctx = swap_cols(context.reshape(cols, own, width_col))
    ctx = ctx.transpose(1, 0, 2).reshape(own, width)

    attn_out = mm(ctx, w_out_all, ((1,), (0,))) + b_out_a
    normed_one, inv_one = normalize(x.astype(f32) + attn_out)
    hidden_one = normed_one * gain_one + bias_one
    hidden_low = hidden_one.astype(bf16)
    pre_act = jnp.einsum("td,cdn->ctn", hidden_low, w_in_all, preferred_element_type=f32)
    pre_act = pre_act + b_in_all[:, None, :]
    act = gelu_exact(pre_act).astype(bf16)
    ffn_out = jnp.einsum("ctn,cdn->td", act, w_back_all, preferred_element_type=f32) + b_back_a
    normed_two, inv_two = normalize(hidden_one + ffn_out)
    layer_out = (normed_two * gain_two + bias_two).astype(bf16)
    out = give_back(layer_out.T, seqs_local)

    student_h = mm(layer_out, s_proj_all, ((1,), (0,))) + s_bias
    head_parts = student_h.reshape(own, SH, SHD)
    pool_logit = jnp.sum(head_parts * query_heads, axis=-1) * pool_scale
    member = (seg_own[:, None] == doc_ids[None, :])[:, :, None]
    masked = jnp.where(member, pool_logit[:, None, :], masked_value)
    local_top = jnp.max(masked, axis=0)
    local_exp = jnp.where(member, jnp.exp(masked - local_top[None]), 0.0)
    local_total = jnp.sum(local_exp, axis=0)
    local_sum = jnp.einsum("tdh,thk->dhk", local_exp, head_parts, precision=highest)
    stats = jnp.concatenate([local_top[..., None], local_total[..., None], local_sum], axis=-1)
    stats = lax.all_gather(stats, ("dp", "col"))
    if sub > 1:
        stats = lax.all_gather(stats, "row", axis=0, tiled=True, axis_index_groups=row_groups(rows, sub))
    tops, totals, sums = stats[..., 0], stats[..., 1], stats[..., 2:]
    doc_top = jnp.max(tops, axis=0)
    factors = jnp.exp(tops - doc_top[None])
    doc_total = jnp.sum(totals * factors, axis=0)
    pooled_heads = jnp.sum(sums * factors[..., None], axis=0) / doc_total[:, :, None]
    pooled = pooled_heads.reshape(docs_count, student_width)
    middle = jnp.tanh(jnp.dot(pooled, s_mid, precision=highest) + s_mid_bias)
    logit_rows = jnp.dot(middle, s_cls, precision=highest) + s_cls_bias
    logits = lax.all_gather(logit_rows, "row")[::sub]
    logits = lax.dynamic_slice_in_dim(logits, dp_index * seqs_local, seqs_local)
    logit_top = jnp.max(logit_rows, axis=-1, keepdims=True)
    logit_exp = jnp.exp(logit_rows - logit_top)
    one_hot = (label_seq[:, None] == class_ids[None, :]).astype(f32)
    d_logits = logit_exp / jnp.sum(logit_exp, axis=-1, keepdims=True) - one_hot
    g_cls = jnp.dot(middle.T, d_logits, precision=highest)
    g_cls_bias = jnp.sum(d_logits, axis=0)
    d_middle = jnp.dot(d_logits, s_cls.T, precision=highest) * (1.0 - middle * middle)
    g_mid = jnp.dot(pooled.T, d_middle, precision=highest)
    g_mid_bias = jnp.sum(d_middle, axis=0)
    d_pooled = jnp.dot(d_middle, s_mid.T, precision=highest).reshape(docs_count, SH, SHD)
    shares = jnp.where(member, jnp.exp(masked - doc_top[None]), 0.0) / doc_total[None]
    d_share = jnp.einsum("dhk,thk->tdh", d_pooled, head_parts, precision=highest)
    base_term = jnp.sum(d_pooled * pooled_heads, axis=-1)
    d_pool_logit = jnp.sum(shares * (d_share - base_term[None]), axis=1)
    d_heads = jnp.einsum("tdh,dhk->thk", shares, d_pooled, precision=highest)
    d_heads = d_heads + d_pool_logit[:, :, None] * query_heads[None] * pool_scale
    g_query = (jnp.sum(d_pool_logit[:, :, None] * head_parts, axis=0) * pool_scale).reshape(-1)
    d_student = d_heads.reshape(own, student_width)
    g_sbias = jnp.sum(d_student, axis=0)
    g_sproj = jnp.dot(layer_out.astype(f32).T, d_student, precision=highest)

    d_out = take_in(cotangent).T.astype(f32)
    g_ln2_gain = jnp.sum(d_out * normed_two, axis=0)
    g_ln2_bias = jnp.sum(d_out, axis=0)
    d_resid_two = normalize_back(d_out * gain_two, normed_two, inv_two)
    d_ffn = d_resid_two.astype(bf16)
    g_back_bias = jnp.sum(d_ffn.astype(f32), axis=0)
    g_back = jnp.einsum("td,ctn->cdn", d_ffn, act, preferred_element_type=f32)
    d_act = jnp.einsum("td,cdn->ctn", d_ffn, w_back_all, preferred_element_type=f32)
    _, gelu_fn = jax.vjp(gelu_exact, pre_act)
    d_pre = gelu_fn(d_act)[0].astype(bf16)
    g_in_bias = jnp.sum(d_pre.astype(f32), axis=1)
    g_in = jnp.einsum("td,ctn->cdn", hidden_low, d_pre, preferred_element_type=f32)
    d_hidden_one = d_resid_two + jnp.einsum(
        "ctn,cdn->td", d_pre, w_in_all, preferred_element_type=f32
    )
    g_ln1_gain = jnp.sum(d_hidden_one * normed_one, axis=0)
    g_ln1_bias = jnp.sum(d_hidden_one, axis=0)
    d_resid_one = normalize_back(d_hidden_one * gain_one, normed_one, inv_one)
    d_attn = d_resid_one.astype(bf16)
    g_out_bias = jnp.sum(d_attn.astype(f32), axis=0)
    g_out = mm(ctx, d_attn, ((0,), (0,)))
    d_ctx = mm(d_attn, w_out_all, ((1,), (1,))).astype(bf16)
    d_ctx = swap_cols(d_ctx.reshape(own, cols, width_col).transpose(1, 0, 2))
    d_ctx = d_ctx.reshape(cols * own, heads_dev, HD)
    d_q, d_k, d_v = attend_back(queries, key_rows, value_rows, probs, d_ctx, score_scale)
    d_kv = jnp.stack([d_k, d_v], axis=2).astype(bf16).reshape(seq_len, -1)
    d_kv = scatter_sequence(d_kv, cols, sub).reshape(cols, own, heads_dev, 2, HD)
    d_q = d_q.astype(bf16).reshape(cols, own, heads_dev, 1, HD)
    d_qkv = jnp.concatenate([d_q, d_kv], axis=3).reshape(cols, own, 3 * width_col)
    d_qkv = swap_cols(d_qkv)
    g_qkv_bias = jnp.sum(d_qkv.astype(f32), axis=1).reshape(cols, heads_dev, 3, HD)
    g_qkv = jnp.einsum("td,ctn->cdn", x, d_qkv, preferred_element_type=f32)
    d_tokens = d_resid_one + jnp.einsum("ctn,cdn->td", d_qkv, w_qkv_all, preferred_element_type=f32)
    grad_tokens = give_back(d_tokens.astype(bf16).T, seqs_local).astype(f32)

    g_out = g_out.reshape(cols, width_col, rows, width_row).transpose(0, 2, 1, 3)
    g_out = g_out.reshape(cols, rows, width_row, width_col)
    model = jnp.concatenate(
        [
            g_in.reshape(cols, rows, width_row, hidden_col).astype(bf16),
            g_back.reshape(cols, rows, width_row, hidden_col).astype(bf16),
            g_out.astype(bf16),
        ],
        axis=-1,
    )
    model = scatter_world(model).astype(f32)
    g_qkv = scatter_world(g_qkv.reshape(cols, rows, width_row, 3 * width_col).astype(bf16)).astype(f32)
    once = 1.0 / (parts * cols * sub)
    small = (
        g_qkv_bias[:, :, 0].reshape(cols, width_col),
        g_qkv_bias[:, :, 2].reshape(cols, width_col),
        g_in_bias,
        g_out_bias,
        g_ln1_gain,
        g_ln1_bias,
        g_back_bias,
        g_ln2_gain,
        g_ln2_bias,
        g_sproj,
        g_sbias,
        g_query,
        g_mid * once,
        g_mid_bias * once,
        g_cls * once,
        g_cls_bias * once,
    )
    small = lax.psum(small, WORLD)

    def at_col(part):
        return lax.dynamic_index_in_dim(part, col_index, 0, False)

    def at_row(part):
        return lax.dynamic_slice_in_dim(part, row_index * width_row, width_row)

    return (
        out,
        logits,
        grad_tokens,
        g_qkv,
        jnp.stack([at_col(small[0]), at_col(small[1])]),
        model[:, 2 * hidden_col :].reshape(width_col, width_row),
        at_row(small[3]),
        at_row(small[4]),
        at_row(small[5]),
        model[:, :hidden_col],
        at_col(small[2]),
        model[:, hidden_col : 2 * hidden_col],
        at_row(small[6]),
        at_row(small[7]),
        at_row(small[8]),
        at_row(small[9]),
        small[10],
        small[11],
        small[12],
        small[13],
        small[14],
        small[15],
    )


def solution(mesh):
    row, col = P("row"), P("col")
    grid, whole = P("row", "col"), P("dp", "row", "col")
    placed = (
        (whole, P("dp", None), P("dp", None), whole, grid, P(None, "col"), P("col", "row"))
        + (row, row, row, grid, col, grid, row, row, row, P("row", None))
        + (P(),) * 6
    )
    results = (
        (whole, P("dp", None, None), whole, grid, P(None, "col"), P("col", "row"))
        + (row, row, row, grid, col, grid, row, row, row, P("row", None))
        + (P(),) * 6
    )
    return jax.shard_map(local, mesh=mesh, in_specs=placed, out_specs=results, check_vma=False)
```

```python
import functools
import jax
import jax.numpy as jnp
from jax import lax
from jax.experimental import pallas as pl
from jax.experimental.pallas import tpu as pltpu
from jax.sharding import PartitionSpec as P

HD = 64
SH = 2
SHD = 64

norm_eps = 1e-06
masked_value = -1e30
highest = lax.Precision.HIGHEST
f32 = jnp.float32
bf16 = jnp.bfloat16
WORLD = ("col", "row", "dp")


def sizes(seqs_local):
    parts = lax.axis_size("dp")
    rows = lax.axis_size("row")
    seqs = seqs_local * parts
    return parts, rows, lax.axis_size("col"), seqs, rows // seqs


def row_groups(rows, sub):
    return [list(range(at, at + sub)) for at in range(0, rows, sub)]


def take_in(values):
    parts, rows, _, seqs, sub = sizes(values.shape[0])
    held = lax.all_to_all(values, "dp", 2, 0, tiled=True)
    feats, half = held.shape[1:]
    held = held.reshape(seqs, feats, sub, half // sub).transpose(0, 2, 1, 3)
    held = held.reshape(rows, feats, half // sub)
    held = lax.all_to_all(held, "row", 0, 0, tiled=True)
    return held.reshape(rows * feats, half // sub)


def give_back(values, seqs_local):
    parts, rows, _, seqs, sub = sizes(seqs_local)
    width, own = values.shape
    feats = width // rows
    held = lax.all_to_all(values.reshape(rows, feats, own), "row", 0, 0, tiled=True)
    held = held.reshape(seqs, sub, feats, own).transpose(0, 2, 1, 3).reshape(seqs, feats, sub * own)
    return lax.all_to_all(held, "dp", 0, 2, tiled=True)


def gather_world(shard):
    cols, rows = lax.axis_size("col"), lax.axis_size("row")
    out = lax.all_gather(shard, WORLD, axis=0, tiled=True)
    return out.reshape(cols, rows, -1, shard.shape[1])


def own_half(block):
    parts = lax.axis_size("dp")
    amount = block.shape[0] // parts
    return lax.dynamic_slice_in_dim(block, lax.axis_index("dp") * amount, amount)


def scatter_world(full):
    flat = full.reshape(-1, full.shape[-1])
    mine = lax.psum_scatter(flat, WORLD, scatter_dimension=0, tiled=True)
    return lax.all_gather(mine, "dp", axis=0, tiled=True)


def swap_cols(values):
    return lax.all_to_all(values, "col", 0, 0, tiled=True)


def gather_sequence(values, sub):
    cols, own, width = values.shape
    held = values[:, None]
    if sub > 1:
        groups = row_groups(lax.axis_size("row"), sub)
        held = lax.all_gather(held, "row", axis=1, tiled=True, axis_index_groups=groups)
    held = lax.all_gather(held[:, None], "dp", axis=1, tiled=True)
    return held.reshape(-1, width)


def scatter_sequence(values, cols, sub):
    parts = lax.axis_size("dp")
    width = values.shape[-1]
    held = values.reshape(cols, parts, sub, -1, width)
    held = lax.psum_scatter(held, "dp", scatter_dimension=1, tiled=True)[:, 0]
    if sub > 1:
        groups = row_groups(lax.axis_size("row"), sub)
        held = lax.psum_scatter(
            held, "row", scatter_dimension=1, tiled=True, axis_index_groups=groups
        )
    return held[:, 0]


def normalize(values):
    mean_v = jnp.mean(values, axis=-1, keepdims=True)
    center = values - mean_v
    inv_std = lax.rsqrt(jnp.mean(center * center, axis=-1, keepdims=True) + norm_eps)
    return center * inv_std, inv_std


def normalize_back(grad_hat, normed, inv_std):
    return inv_std * (
        grad_hat
        - jnp.mean(grad_hat, axis=-1, keepdims=True)
        - normed * jnp.mean(grad_hat * normed, axis=-1, keepdims=True)
    )


def gelu_exact(values):
    return jax.nn.gelu(values, approximate=False)


def mm(a, b, contract):
    return lax.dot_general(a, b, (contract, ((), ())), preferred_element_type=f32)


def combine_pool(part_one, part_two):
    top_a, total_a, sum_a = part_one
    top_b, total_b, sum_b = part_two
    row_top = jnp.maximum(top_a, top_b)
    factor_a = jnp.exp(top_a - row_top)
    factor_b = jnp.exp(top_b - row_top)
    return (
        row_top,
        total_a * factor_a + total_b * factor_b,
        sum_a * factor_a[:, :, None] + sum_b * factor_b[:, :, None],
    )


def attend(q, k, v, q_seg, k_seg, scale):
    scores = jnp.einsum("qhd,khd->hqk", q, k, preferred_element_type=f32) * scale
    scores = jnp.where((q_seg[:, None] == k_seg[None, :])[None], scores, masked_value)
    top = jnp.max(scores, axis=-1, keepdims=True)
    exp_scores = jnp.exp(scores - top)
    total = jnp.sum(exp_scores, axis=-1, keepdims=True)
    probs = exp_scores / total
    context = jnp.einsum("hqk,khd->qhd", probs.astype(bf16), v, preferred_element_type=f32)
    return context.astype(bf16), probs


def attend_back(q, k, v, probs, d_ctx, scale):
    d_probs = jnp.einsum("qhd,khd->hqk", d_ctx, v, preferred_element_type=f32)
    delta = jnp.sum(probs * d_probs, axis=-1, keepdims=True)
    d_scores = (probs * (d_probs - delta)).astype(bf16)
    d_q = jnp.einsum("hqk,khd->qhd", d_scores, k, preferred_element_type=f32) * scale
    d_k = jnp.einsum("hqk,qhd->khd", d_scores, q, preferred_element_type=f32) * scale
    d_v = jnp.einsum("hqk,qhd->khd", probs.astype(bf16), d_ctx, preferred_element_type=f32)
    return d_q, d_k, d_v


def general_local(
    tokens,
    segments,
    labels,
    cotangent,
    w_qkv,
    b_qkv,
    w_out,
    b_out,
    ln1_gain,
    ln1_bias,
    w_in,
    b_in,
    w_back,
    b_back,
    ln2_gain,
    ln2_bias,
    s_proj,
    s_bias,
    s_query,
    s_mid,
    s_mid_bias,
    s_cls,
    s_cls_bias,
):
    seqs_local, width_row, cols_local = tokens.shape
    parts, rows, cols, seqs, sub = sizes(seqs_local)
    width = width_row * rows
    own = cols_local // (parts * sub)
    width_col = b_qkv.shape[1]
    heads_dev = width_col // HD
    hidden_col = b_in.shape[0]
    docs_count = labels.shape[1]
    class_count = s_cls.shape[1]
    student_width = s_proj.shape[1]
    row_index = lax.axis_index("row")
    col_index = lax.axis_index("col")
    dp_index = lax.axis_index("dp")
    seq_index = row_index // sub
    sub_index = row_index % sub
    score_scale = HD ** (-0.5)
    pool_scale = SHD ** (-0.5)
    query_heads = s_query.reshape(SH, SHD)
    doc_ids = jnp.arange(docs_count, dtype=jnp.int32)
    class_ids = jnp.arange(class_count, dtype=jnp.int32)

    w_qkv_all = gather_world(own_half(w_qkv)).reshape(cols, width, 3 * width_col)
    x_t = take_in(tokens)
    rest = jnp.concatenate([own_half(w_in), own_half(w_back), own_half(w_out).reshape(-1, width_col)], axis=1)
    rest_all = gather_world(rest)
    w_in_all = rest_all[..., :hidden_col].reshape(cols, width, hidden_col)
    w_back_all = rest_all[..., hidden_col : 2 * hidden_col].reshape(cols, width, hidden_col)
    w_out_all = rest_all[..., 2 * hidden_col :].reshape(cols, rows, width_col, width_row)
    w_out_all = w_out_all.transpose(0, 2, 1, 3).reshape(width, width)
    row_vectors = lax.all_gather(
        jnp.stack([b_out, ln1_gain, ln1_bias, b_back, ln2_gain, ln2_bias]), "row", axis=1, tiled=True
    )
    b_out_a, gain_one, bias_one, b_back_a, gain_two, bias_two = [row_vectors[i] for i in range(6)]
    b_qkv_all = lax.all_gather(b_qkv, "col")
    b_in_all = lax.all_gather(b_in, "col")
    s_proj_all = lax.all_gather(s_proj, "row", axis=0, tiled=True)
    whole_ints = lax.all_gather(jnp.concatenate([segments, labels], axis=1), "dp", axis=0, tiled=True)
    ints = lax.dynamic_index_in_dim(whole_ints, seq_index, 0, False)
    seq_len = segments.shape[1]
    seg_all, label_seq = ints[:seq_len], ints[seq_len:]
    seg_blocks = seg_all.reshape(cols, parts, sub, own)
    seg_q = lax.dynamic_index_in_dim(seg_blocks, dp_index, 1, False)
    seg_q = lax.dynamic_index_in_dim(seg_q, sub_index, 1, False)
    seg_own = lax.dynamic_index_in_dim(seg_q, col_index, 0, False)
    seg_q = seg_q.reshape(-1)

    x = x_t.T
    offsets = jnp.stack([b_qkv_all[:, 0], jnp.zeros_like(b_qkv_all[:, 0]), b_qkv_all[:, 1]], axis=1)
    offsets = offsets.reshape(cols, 3, heads_dev, HD).transpose(0, 2, 1, 3).reshape(cols, 1, -1)
    qkv = jnp.einsum("td,cdn->ctn", x, w_qkv_all, preferred_element_type=f32) + offsets
    qkv = swap_cols(qkv.astype(bf16)).reshape(cols, own, heads_dev, 3, HD)
    queries = qkv[:, :, :, 0].reshape(cols * own, heads_dev, HD)
    kv = gather_sequence(qkv[:, :, :, 1:].reshape(cols, own, -1), sub)
    kv = kv.reshape(seq_len, heads_dev, 2, HD)
    key_rows, value_rows = kv[:, :, 0], kv[:, :, 1]
    context, probs = attend(queries, key_rows, value_rows, seg_q, seg_all, score_scale)
    ctx = swap_cols(context.reshape(cols, own, width_col))
    ctx = ctx.transpose(1, 0, 2).reshape(own, width)

    attn_out = mm(ctx, w_out_all, ((1,), (0,))) + b_out_a
    normed_one, inv_one = normalize(x.astype(f32) + attn_out)
    hidden_one = normed_one * gain_one + bias_one
    hidden_low = hidden_one.astype(bf16)
    pre_act = jnp.einsum("td,cdn->ctn", hidden_low, w_in_all, preferred_element_type=f32)
    pre_act = pre_act + b_in_all[:, None, :]
    act = gelu_exact(pre_act).astype(bf16)
    ffn_out = jnp.einsum("ctn,cdn->td", act, w_back_all, preferred_element_type=f32) + b_back_a
    normed_two, inv_two = normalize(hidden_one + ffn_out)
    layer_out = (normed_two * gain_two + bias_two).astype(bf16)
    out = give_back(layer_out.T, seqs_local)

    student_h = mm(layer_out, s_proj_all, ((1,), (0,))) + s_bias
    head_parts = student_h.reshape(own, SH, SHD)
    pool_logit = jnp.sum(head_parts * query_heads, axis=-1) * pool_scale
    member = (seg_own[:, None] == doc_ids[None, :])[:, :, None]
    masked = jnp.where(member, pool_logit[:, None, :], masked_value)
    local_top = jnp.max(masked, axis=0)
    local_exp = jnp.where(member, jnp.exp(masked - local_top[None]), 0.0)
    local_total = jnp.sum(local_exp, axis=0)
    local_sum = jnp.einsum("tdh,thk->dhk", local_exp, head_parts, precision=highest)
    stats = jnp.concatenate([local_top[..., None], local_total[..., None], local_sum], axis=-1)
    stats = lax.all_gather(stats, ("dp", "col"))
    if sub > 1:
        stats = lax.all_gather(stats, "row", axis=0, tiled=True, axis_index_groups=row_groups(rows, sub))
    tops, totals, sums = stats[..., 0], stats[..., 1], stats[..., 2:]
    doc_top = jnp.max(tops, axis=0)
    factors = jnp.exp(tops - doc_top[None])
    doc_total = jnp.sum(totals * factors, axis=0)
    pooled_heads = jnp.sum(sums * factors[..., None], axis=0) / doc_total[:, :, None]
    pooled = pooled_heads.reshape(docs_count, student_width)
    middle = jnp.tanh(jnp.dot(pooled, s_mid, precision=highest) + s_mid_bias)
    logit_rows = jnp.dot(middle, s_cls, precision=highest) + s_cls_bias
    logits = lax.all_gather(logit_rows, "row")[::sub]
    logits = lax.dynamic_slice_in_dim(logits, dp_index * seqs_local, seqs_local)
    logit_top = jnp.max(logit_rows, axis=-1, keepdims=True)
    logit_exp = jnp.exp(logit_rows - logit_top)
    one_hot = (label_seq[:, None] == class_ids[None, :]).astype(f32)
    d_logits = logit_exp / jnp.sum(logit_exp, axis=-1, keepdims=True) - one_hot
    g_cls = jnp.dot(middle.T, d_logits, precision=highest)
    g_cls_bias = jnp.sum(d_logits, axis=0)
    d_middle = jnp.dot(d_logits, s_cls.T, precision=highest) * (1.0 - middle * middle)
    g_mid = jnp.dot(pooled.T, d_middle, precision=highest)
    g_mid_bias = jnp.sum(d_middle, axis=0)
    d_pooled = jnp.dot(d_middle, s_mid.T, precision=highest).reshape(docs_count, SH, SHD)
    shares = jnp.where(member, jnp.exp(masked - doc_top[None]), 0.0) / doc_total[None]
    d_share = jnp.einsum("dhk,thk->tdh", d_pooled, head_parts, precision=highest)
    base_term = jnp.sum(d_pooled * pooled_heads, axis=-1)
    d_pool_logit = jnp.sum(shares * (d_share - base_term[None]), axis=1)
    d_heads = jnp.einsum("tdh,dhk->thk", shares, d_pooled, precision=highest)
    d_heads = d_heads + d_pool_logit[:, :, None] * query_heads[None] * pool_scale
    g_query = (jnp.sum(d_pool_logit[:, :, None] * head_parts, axis=0) * pool_scale).reshape(-1)
    d_student = d_heads.reshape(own, student_width)
    g_sbias = jnp.sum(d_student, axis=0)
    g_sproj = jnp.dot(layer_out.astype(f32).T, d_student, precision=highest)

    d_out = take_in(cotangent).T.astype(f32)
    g_ln2_gain = jnp.sum(d_out * normed_two, axis=0)
    g_ln2_bias = jnp.sum(d_out, axis=0)
    d_resid_two = normalize_back(d_out * gain_two, normed_two, inv_two)
    d_ffn = d_resid_two.astype(bf16)
    g_back_bias = jnp.sum(d_ffn.astype(f32), axis=0)
    g_back = jnp.einsum("td,ctn->cdn", d_ffn, act, preferred_element_type=f32)
    d_act = jnp.einsum("td,cdn->ctn", d_ffn, w_back_all, preferred_element_type=f32)
    _, gelu_fn = jax.vjp(gelu_exact, pre_act)
    d_pre = gelu_fn(d_act)[0].astype(bf16)
    g_in_bias = jnp.sum(d_pre.astype(f32), axis=1)
    g_in = jnp.einsum("td,ctn->cdn", hidden_low, d_pre, preferred_element_type=f32)
    d_hidden_one = d_resid_two + jnp.einsum(
        "ctn,cdn->td", d_pre, w_in_all, preferred_element_type=f32
    )
    g_ln1_gain = jnp.sum(d_hidden_one * normed_one, axis=0)
    g_ln1_bias = jnp.sum(d_hidden_one, axis=0)
    d_resid_one = normalize_back(d_hidden_one * gain_one, normed_one, inv_one)
    d_attn = d_resid_one.astype(bf16)
    g_out_bias = jnp.sum(d_attn.astype(f32), axis=0)
    g_out = mm(ctx, d_attn, ((0,), (0,)))
    d_ctx = mm(d_attn, w_out_all, ((1,), (1,))).astype(bf16)
    d_ctx = swap_cols(d_ctx.reshape(own, cols, width_col).transpose(1, 0, 2))
    d_ctx = d_ctx.reshape(cols * own, heads_dev, HD)
    d_q, d_k, d_v = attend_back(queries, key_rows, value_rows, probs, d_ctx, score_scale)
    d_kv = jnp.stack([d_k, d_v], axis=2).astype(bf16).reshape(seq_len, -1)
    d_kv = scatter_sequence(d_kv, cols, sub).reshape(cols, own, heads_dev, 2, HD)
    d_q = d_q.astype(bf16).reshape(cols, own, heads_dev, 1, HD)
    d_qkv = jnp.concatenate([d_q, d_kv], axis=3).reshape(cols, own, 3 * width_col)
    d_qkv = swap_cols(d_qkv)
    g_qkv_bias = jnp.sum(d_qkv.astype(f32), axis=1).reshape(cols, heads_dev, 3, HD)
    g_qkv = jnp.einsum("td,ctn->cdn", x, d_qkv, preferred_element_type=f32)
    d_tokens = d_resid_one + jnp.einsum("ctn,cdn->td", d_qkv, w_qkv_all, preferred_element_type=f32)
    grad_tokens = give_back(d_tokens.astype(bf16).T, seqs_local).astype(f32)

    g_out = g_out.reshape(cols, width_col, rows, width_row).transpose(0, 2, 1, 3)
    g_out = g_out.reshape(cols, rows, width_row, width_col)
    model = jnp.concatenate(
        [
            g_in.reshape(cols, rows, width_row, hidden_col).astype(bf16),
            g_back.reshape(cols, rows, width_row, hidden_col).astype(bf16),
            g_out.astype(bf16),
        ],
        axis=-1,
    )
    model = scatter_world(model).astype(f32)
    g_qkv = scatter_world(g_qkv.reshape(cols, rows, width_row, 3 * width_col).astype(bf16)).astype(f32)
    once = 1.0 / (parts * cols * sub)
    small = (
        g_qkv_bias[:, :, 0].reshape(cols, width_col),
        g_qkv_bias[:, :, 2].reshape(cols, width_col),
        g_in_bias,
        g_out_bias,
        g_ln1_gain,
        g_ln1_bias,
        g_back_bias,
        g_ln2_gain,
        g_ln2_bias,
        g_sproj,
        g_sbias,
        g_query,
        g_mid * once,
        g_mid_bias * once,
        g_cls * once,
        g_cls_bias * once,
    )
    small = lax.psum(small, WORLD)

    def at_col(part):
        return lax.dynamic_index_in_dim(part, col_index, 0, False)

    def at_row(part):
        return lax.dynamic_slice_in_dim(part, row_index * width_row, width_row)

    return (
        out,
        logits,
        grad_tokens,
        g_qkv,
        jnp.stack([at_col(small[0]), at_col(small[1])]),
        model[:, 2 * hidden_col :].reshape(width_col, width_row),
        at_row(small[3]),
        at_row(small[4]),
        at_row(small[5]),
        model[:, :hidden_col],
        at_col(small[2]),
        model[:, hidden_col : 2 * hidden_col],
        at_row(small[6]),
        at_row(small[7]),
        at_row(small[8]),
        at_row(small[9]),
        small[10],
        small[11],
        small[12],
        small[13],
        small[14],
        small[15],
    )


MESH = pl.DeviceIdType.MESH
HBM = pl.BlockSpec(memory_space=pl.ANY)


def place():
    return lax.axis_index("dp"), lax.axis_index("row"), lax.axis_index("col")


def greet(peers, guarded=()):
    barrier = pltpu.get_barrier_semaphore()
    for peer in peers:
        pl.semaphore_signal(barrier, inc=1, device_id=peer, device_id_type=MESH)
    for there, peer in guarded:

        @pl.when(there)
        def _():
            pl.semaphore_signal(barrier, inc=1, device_id=peer, device_id_type=MESH)

    amount = len(peers)
    for there, _ in guarded:
        amount = amount + there.astype(jnp.int32)
    pl.semaphore_wait(barrier, amount)


def rcopy(src, dst, send, recv, peer):
    return pltpu.make_async_remote_copy(
        src_ref=src, dst_ref=dst, send_sem=send, recv_sem=recv, device_id=peer, device_id_type=MESH
    )


def take_copies(src, out, local, send, recv):
    d, r, c = place()
    own = out.shape[2]
    moves = []
    for i in range(2):
        for far in range(2):
            row, core = 2 * d + i, d ^ far
            piece = src.at[i, :, pl.ds(pl.multiple_of(core * own, own), own)]
            here = (row == r) if far == 0 else None

            def start(piece=piece, row=row, core=core, slot=2 * i + far, here=here):
                def away():
                    rcopy(piece, out.at[r], send.at[slot], recv.at[r], (core, row, c)).start()

                if here is None:
                    away()
                else:
                    pl.when(jnp.logical_not(here))(away)

                    @pl.when(here)
                    def _():
                        pltpu.make_async_copy(piece, out.at[r], local).start()

            def wait(piece=piece, row=row, core=core, slot=2 * i + far, here=here):
                def away():
                    rcopy(piece, out.at[r], send.at[slot], recv.at[r], (core, row, c)).wait_send()

                if here is None:
                    away()
                else:
                    pl.when(jnp.logical_not(here))(away)

                    @pl.when(here)
                    def _():
                        pltpu.make_async_copy(piece, out.at[r], local).wait()

            moves.append((start, wait))
    for row in range(4):

        def arrive(row=row):
            @pl.when(jnp.logical_not((row == r) & (r // 2 == d)))
            def _():
                piece = src.at[0, :, pl.ds(0, own)]
                rcopy(piece, out.at[row], send.at[0], recv.at[row], (d, r, c)).wait_recv()

        moves.append((lambda: None, arrive))
    return moves


def gather_kernel(kinds, *refs):
    shards, refs = refs[:kinds], refs[kinds:]
    (tok, cot, ints), refs = refs[:3], refs[3:]
    outs, refs = refs[:kinds], refs[kinds:]
    (tok_out, cot_out, ints_out), refs = refs[:3], refs[3:]
    own_sem, zs, zr, xs, xr, ys, yr, cs, cr, ps, pr, tl, ts, tr, il = refs
    d, r, c = place()
    cols = 4
    xn, yn, pn = (d, r ^ 1, c), (d, r ^ 2, c), (1 - d, r, c)
    up, down = (d, r, c + 1), (d, r, c - 1)
    has_up, has_down = c < cols - 1, c > 0
    plane = [(d ^ (j // 4), r ^ (j % 4), c) for j in range(1, 8)]
    greet(plane, [(has_up, up), (has_down, down)])
    ahead = [take_copies(tok, tok_out, tl.at[0], ts.at[0], tr.at[0])]
    for start, _ in ahead[0]:
        start()
    pltpu.make_async_copy(ints, ints_out.at[d], il.at[0]).start()
    rcopy(ints, ints_out.at[d], il.at[1], il.at[2], pn).start()
    halves = [shard.shape[0] // 2 for shard in shards]

    def z_send(k, at, way, hop):
        src = shards[k] if hop == 1 else outs[k].at[at, r, d]
        return rcopy(
            src, outs[k].at[at, r, d], zs.at[k, way, hop - 1], zr.at[k, way, hop - 1], up if way == 0 else down
        )

    def src_of(k, at, own):
        return shards[k] if own else outs[k].at[at, r, d]

    def to_x(k, at, own):
        return rcopy(src_of(k, at, own), outs[k].at[at, r, d], xs.at[k, at], xr.at[k, at], xn)

    def to_y(k, at, own):
        return rcopy(src_of(k, at, own), outs[k].at[at, r, d], ys.at[k, at], yr.at[k, at], yn)

    def to_p(k, at, own):
        return rcopy(src_of(k, at, own), outs[k].at[at, r, d], ps.at[k, at, 0], pr.at[k, at, 0], pn)

    def relay(k, at, which):
        row = r ^ 1 if which == 0 else r ^ 2
        ref = outs[k].at[at, row, d, pl.ds(which * halves[k], halves[k])]
        return rcopy(ref, ref, cs.at[k, at, which], cr.at[k, at, which], yn if which == 0 else xn)

    def pass_p(k, at, bit):
        ref = outs[k].at[at, r ^ bit, d]
        return rcopy(ref, ref, ps.at[k, at, bit], pr.at[k, at, bit], pn)

    def got_x(k, at):
        ref = outs[k].at[at, r ^ 1, d]
        rcopy(ref, ref, xs.at[k, at], xr.at[k, at], xn).wait_recv()

    def got_y(k, at):
        ref = outs[k].at[at, r ^ 2, d]
        rcopy(ref, ref, ys.at[k, at], yr.at[k, at], yn).wait_recv()

    def got_corner(k, at):
        for which in range(2):
            ref = outs[k].at[at, r ^ 3, d, pl.ds(which * halves[k], halves[k])]
            rcopy(ref, ref, cs.at[k, at, which], cr.at[k, at, which], xn).wait_recv()

    def got_p(k, at, bit):
        ref = outs[k].at[at, r ^ bit, 1 - d]
        rcopy(ref, ref, ps.at[k, at, bit], pr.at[k, at, bit], pn).wait_recv()

    for k in range(kinds):
        pltpu.make_async_copy(shards[k], outs[k].at[c, r, d], own_sem.at[k]).start()

        @pl.when(has_up)
        def _():
            z_send(k, c, 0, 1).start()

        @pl.when(has_down)
        def _():
            z_send(k, c, 1, 1).start()

    def spread(k, at, own):
        to_x(k, at, own).start()
        to_y(k, at, own).start()
        to_p(k, at, own).start()

    def onward(k, at):
        got_x(k, at)
        relay(k, at, 0).start()
        pass_p(k, at, 1).start()
        got_y(k, at)
        relay(k, at, 1).start()
        pass_p(k, at, 2).start()

    steps = [(0, 0)] + [(way, hop) for hop in (1, 2, 3) for way in (0, 1)]
    jobs = [(k, way, hop) for k in range(kinds) for way, hop in steps]

    def at_of(way, hop):
        return c - hop if way == 0 else c + hop

    def valid(way, hop):
        return c >= hop if way == 0 else c + hop < cols

    def guard(way, hop, body):
        if hop == 0:
            body()
        else:
            pl.when(valid(way, hop))(body)

    def first(k, way, hop):
        def body():
            at = at_of(way, hop)
            if hop:
                z_send(k, at, way, hop).wait_recv()
                if hop < 3:
                    can = has_up if way == 0 else has_down

                    @pl.when(can)
                    def _():
                        z_send(k, at, way, hop + 1).start()

            spread(k, at, hop == 0)

        guard(way, hop, body)

    def second(k, way, hop):
        guard(way, hop, lambda: onward(k, at_of(way, hop)))

    def third(k, way, hop):
        def body():
            at = at_of(way, hop)
            got_corner(k, at)
            pass_p(k, at, 3).start()

        guard(way, hop, body)

    lag = 3
    for i in range(len(jobs) + 2 * lag):
        if i < len(jobs):
            first(*jobs[i])
        if 0 <= i - lag < len(jobs):
            second(*jobs[i - lag])
        if 0 <= i - 2 * lag < len(jobs):
            third(*jobs[i - 2 * lag])

    ahead.append(take_copies(cot, cot_out, tl.at[1], ts.at[1], tr.at[1]))
    for start, _ in ahead[1]:
        start()
    for k in range(kinds):
        pltpu.make_async_copy(shards[k], outs[k].at[c, r, d], own_sem.at[k]).wait()
        for way, hop in steps:

            def body():
                at = at_of(way, hop)
                own = hop == 0
                to_x(k, at, own).wait_send()
                to_y(k, at, own).wait_send()
                to_p(k, at, own).wait_send()
                for which in range(2):
                    relay(k, at, which).wait_send()
                for bit in (1, 2, 3):
                    pass_p(k, at, bit).wait_send()
                for bit in range(4):
                    got_p(k, at, bit)
                if hop < 3:
                    if own:

                        @pl.when(has_up)
                        def _():
                            z_send(k, c, 0, 1).wait_send()

                        @pl.when(has_down)
                        def _():
                            z_send(k, c, 1, 1).wait_send()
                    else:
                        can = has_up if way == 0 else has_down

                        @pl.when(can)
                        def _():
                            z_send(k, at, way, hop + 1).wait_send()

            guard(way, hop, body)
    for moves in ahead:
        for _, wait in moves:
            wait()
    pltpu.make_async_copy(ints, ints_out.at[d], il.at[0]).wait()
    rcopy(ints, ints_out.at[1 - d], il.at[1], il.at[2], pn).wait()


def gather_fast(shards, tokens, cotangent, ints, cid):
    kinds = len(shards)
    dma = pltpu.SemaphoreType.DMA
    _, feats, cols = tokens.shape
    taken = jax.ShapeDtypeStruct((4, feats, cols // 2), tokens.dtype)
    return pl.pallas_call(
        functools.partial(gather_kernel, kinds),
        out_shape=[jax.ShapeDtypeStruct((4, 4, 2) + s.shape, s.dtype) for s in shards]
        + [taken, taken, jax.ShapeDtypeStruct((2,) + ints.shape, ints.dtype)],
        in_specs=[HBM] * (kinds + 3),
        out_specs=[HBM] * (kinds + 3),
        scratch_shapes=[
            dma((kinds,)),
            dma((kinds, 2, 3)), dma((kinds, 2, 3)),
            dma((kinds, 4)), dma((kinds, 4)),
            dma((kinds, 4)), dma((kinds, 4)),
            dma((kinds, 4, 2)), dma((kinds, 4, 2)),
            dma((kinds, 4, 4)), dma((kinds, 4, 4)),
            dma((2,)), dma((2, 4)), dma((2, 4)), dma((3,)),
        ],
        compiler_params=pltpu.CompilerParams(collective_id=cid, has_side_effects=True),
        name="gather_all",
    )(*shards, tokens, cotangent, ints)


def scatter_kernel(kinds, *refs):
    grads, outs = refs[:kinds], refs[kinds : 2 * kinds]
    (acc, precv, xr1, yr1, xr2, yr2, zup, zdn, fin) = refs[2 * kinds : 2 * kinds + 9]
    (ls, ps, pr, xs1, xm1, ys1, ym1, xs2, xm2, ys2, ym2, us, um, ds, dm, fs, fm, os) = refs[2 * kinds + 9 :]
    d, r, c = place()
    cols = 4
    chunks = kinds * cols
    xn, yn, pn = (d, r ^ 1, c), (d, r ^ 2, c), (1 - d, r, c)
    up, down = (d, r, c + 1), (d, r, c - 1)
    greet([xn, yn, pn], [(c < cols - 1, up), (c > 0, down)])
    half = acc.shape[2] // 2
    first, last = pl.ds(0, half), pl.ds(half, half)

    def split(i):
        k = i // cols
        j = i - k * cols
        at = jnp.where(j == 0, 0, jnp.where(j == 1, 3, j - 1))
        return k, at

    def at_static(i):
        return i // cols, (0, 3, 1, 2)[i % cols]

    def load(i):
        k, at = at_static(i)
        return pltpu.make_async_copy(grads[k].at[at, :, d], acc.at[i], ls.at[i])

    def pair(i):
        k, at = at_static(i)
        return rcopy(grads[k].at[at, :, 1 - d], precv.at[i], ps.at[i], pr.at[i], pn)

    for i in range(chunks):
        pair(i).start()
        load(i).start()

    def x1(i, j):
        return rcopy(acc.at[i, r ^ 1 ^ (2 * j), first], xr1.at[i, j], xs1.at[i, j], xm1.at[i, j], xn)

    def y1(i, j):
        return rcopy(acc.at[i, r ^ 2 ^ j, last], yr1.at[i, j], ys1.at[i, j], ym1.at[i, j], yn)

    def y2(i):
        return rcopy(acc.at[i, r ^ 2, first], yr2.at[i], ys2.at[i], ym2.at[i], yn)

    def x2(i):
        return rcopy(acc.at[i, r ^ 1, last], xr2.at[i], xs2.at[i], xm2.at[i], xn)

    def to_up(i):
        return rcopy(acc.at[i, r], zup.at[i], us.at[i], um.at[i], up)

    def to_down(i):
        return rcopy(acc.at[i, r], zdn.at[i], ds.at[i], dm.at[i], down)

    def stage1(i):
        pltpu.make_async_copy(precv.at[i], acc.at[i], ls.at[i]).wait()
        rcopy(acc.at[i], precv.at[i], ps.at[i], pr.at[i], pn).wait_recv()

        @pl.loop(0, 4)
        def _(row):
            acc[i, row] = acc[i, row] + precv[i, row]

        x1(i, 1).start()
        y1(i, 1).start()
        x1(i, 0).start()
        y1(i, 0).start()

    def stage2(i):
        x1(i, 1).wait_recv()
        acc[i, r ^ 2, first] = acc[i, r ^ 2, first] + xr1[i, 1]
        y2(i).start()
        y1(i, 1).wait_recv()
        acc[i, r ^ 1, last] = acc[i, r ^ 1, last] + yr1[i, 1]
        x2(i).start()
        x1(i, 0).wait_recv()
        acc[i, r, first] = acc[i, r, first] + xr1[i, 0]
        y1(i, 0).wait_recv()
        acc[i, r, last] = acc[i, r, last] + yr1[i, 0]

    def stage3(i):
        y2(i).wait_recv()
        acc[i, r, first] = acc[i, r, first] + yr2[i]
        x2(i).wait_recv()
        acc[i, r, last] = acc[i, r, last] + xr2[i]

    def stage4(i, hops):
        k, at = split(i)

        @pl.when((at > c) & (c == hops))
        def _():
            @pl.when(c > 0)
            def _():
                to_up(i).wait_recv()
                acc[i, r] = acc[i, r] + zup[i]

            to_up(i).start()

        @pl.when((at < c) & (cols - 1 - c == hops))
        def _():
            @pl.when(c < cols - 1)
            def _():
                to_down(i).wait_recv()
                acc[i, r] = acc[i, r] + zdn[i]

            to_down(i).start()

        @pl.when((at == c) & (jnp.maximum(c, cols - 1 - c) == hops))
        def _():
            @pl.when(c > 0)
            def _():
                to_up(i).wait_recv()
                acc[i, r] = acc[i, r] + zup[i]

            @pl.when(c < cols - 1)
            def _():
                to_down(i).wait_recv()
                acc[i, r] = acc[i, r] + zdn[i]

            fin[k, d] = acc[i, r]
            rcopy(fin.at[k, d], fin.at[k, d], fs.at[k], fm.at[k], pn).start()

    stages = [(0, stage1), (2, stage2), (4, stage3)]
    stages += [(5 + h, functools.partial(lambda h, i: stage4(i, h), h)) for h in range(cols)]
    ending = stages[-1][0]

    @pl.loop(0, chunks + ending)
    def _(step):
        for lag, stage in stages:

            @pl.when((step >= lag) & (step - lag < chunks))
            def _():
                stage(step - lag)

    @pl.loop(0, chunks)
    def _(i):
        k, at = split(i)
        rcopy(acc.at[i], precv.at[i], ps.at[i], pr.at[i], pn).wait_send()
        for j in range(2):
            x1(i, j).wait_send()
            y1(i, j).wait_send()
        y2(i).wait_send()
        x2(i).wait_send()

        @pl.when(at > c)
        def _():
            to_up(i).wait_send()

        @pl.when(at < c)
        def _():
            to_down(i).wait_send()

    for k in range(kinds):
        rcopy(fin.at[k, 1 - d], fin.at[k, 1 - d], fs.at[k], fm.at[k], pn).wait()
        pltpu.make_async_copy(fin.at[k], outs[k], os.at[k]).start()
    for k in range(kinds):
        pltpu.make_async_copy(fin.at[k], outs[k], os.at[k]).wait()


def scatter_fast(grads, cid):
    kinds = len(grads)
    chunks = kinds * 4
    n, w = grads[0].shape[3:]
    dma = pltpu.SemaphoreType.DMA
    dt = grads[0].dtype
    return pl.pallas_call(
        functools.partial(scatter_kernel, kinds),
        out_shape=[jax.ShapeDtypeStruct((2, n, w), dt)] * kinds,
        in_specs=[HBM] * kinds,
        out_specs=[HBM] * kinds,
        scratch_shapes=[
            pltpu.VMEM((chunks, 4, n, w), dt),
            pltpu.VMEM((chunks, 4, n, w), dt),
            pltpu.VMEM((chunks, 2, n // 2, w), dt),
            pltpu.VMEM((chunks, 2, n // 2, w), dt),
            pltpu.VMEM((chunks, n // 2, w), dt),
            pltpu.VMEM((chunks, n // 2, w), dt),
            pltpu.VMEM((chunks, n, w), dt),
            pltpu.VMEM((chunks, n, w), dt),
            pltpu.VMEM((kinds, 2, n, w), dt),
            dma((chunks,)), dma((chunks,)), dma((chunks,)),
            dma((chunks, 2)), dma((chunks, 2)), dma((chunks, 2)), dma((chunks, 2)),
            dma((chunks,)), dma((chunks,)), dma((chunks,)), dma((chunks,)),
            dma((chunks,)), dma((chunks,)), dma((chunks,)), dma((chunks,)),
            dma((kinds,)), dma((kinds,)), dma((kinds,)),
        ],
        compiler_params=pltpu.CompilerParams(
            collective_id=cid, has_side_effects=True, vmem_limit_bytes=48 * 1024 * 1024
        ),
        name="scatter_all",
    )(*grads)


def give_kernel(src_ref, out_ref, local, send, recv):
    d, r, c = place()
    own = src_ref.shape[2]
    greet([(d ^ (j // 4), r ^ (j % 4), c) for j in range(1, 8)])
    home = r // 2

    def slot(i, core):
        return out_ref.at[i, :, pl.ds(pl.multiple_of(core * own, own), own)]

    def move(row):
        return rcopy(src_ref.at[row], slot(r % 2, d), send.at[row], recv.at[r % 2, d], (home, row, c))

    def stay():
        return pltpu.make_async_copy(src_ref.at[r], slot(r % 2, d), local)

    for row in range(4):
        here = (row == r) & (home == d)

        @pl.when(jnp.logical_not(here))
        def _():
            move(row).start()

    @pl.when(home == d)
    def _():
        stay().start()

    for row in range(4):
        here = (row == r) & (home == d)

        @pl.when(jnp.logical_not(here))
        def _():
            move(row).wait_send()

    @pl.when(home == d)
    def _():
        stay().wait()

    for i in range(2):
        for core in range(2):

            @pl.when(jnp.logical_not((2 * d + i == r) & (core == d)))
            def _():
                rcopy(src_ref.at[0], slot(i, core), send.at[0], recv.at[i, core], (d, r, c)).wait_recv()


def give_fast(values, cid):
    width, own = values.shape
    dma = pltpu.SemaphoreType.DMA
    return pl.pallas_call(
        give_kernel,
        out_shape=jax.ShapeDtypeStruct((2, width // 4, 2 * own), values.dtype),
        in_specs=[HBM],
        out_specs=HBM,
        scratch_shapes=[dma, dma((4,)), dma((2, 2))],
        compiler_params=pltpu.CompilerParams(collective_id=cid, has_side_effects=True),
        name="give_back",
    )(values.reshape(4, width // 4, own))


VM = pl.BlockSpec(memory_space=pltpu.VMEM)


def swap_kernel(count, *refs):
    srcs, outs = refs[:count], refs[count : 2 * count]
    send, recv = refs[2 * count :]
    d, r, c = place()
    greet([(d, r, c ^ j) for j in (1, 2, 3)])

    def move(k, j):
        return rcopy(srcs[k].at[c ^ j], outs[k].at[c], send.at[k, j], recv.at[k, j], (d, r, c ^ j))

    for j in (3, 2, 1):
        for k in range(count):
            move(k, j).start()
    for k in range(count):
        outs[k][c] = srcs[k][c]
    for j in (1, 2, 3):
        for k in range(count):
            move(k, j).wait()


def swap_fast(arrays, cid):
    count = len(arrays)
    dma = pltpu.SemaphoreType.DMA
    return pl.pallas_call(
        functools.partial(swap_kernel, count),
        out_shape=[jax.ShapeDtypeStruct(a.shape, a.dtype) for a in arrays],
        in_specs=[VM] * count,
        out_specs=[VM] * count,
        scratch_shapes=[dma((count, 4)), dma((count, 4))],
        compiler_params=pltpu.CompilerParams(collective_id=cid, has_side_effects=True),
        name="swap_cols",
    )(*arrays)


def heads_kernel(q_ref, kv_ref, q_out, kv_out, send, recv, psend, precv):
    d, r, c = place()
    pn = (1 - d, r, c)
    greet([(d, r, c ^ j) for j in (1, 2, 3)] + [pn])

    def kv(j):
        return rcopy(kv_ref.at[c ^ j], kv_out.at[c, d], send.at[0, j], recv.at[0, j], (d, r, c ^ j))

    def q(j):
        return rcopy(q_ref.at[c ^ j], q_out.at[c], send.at[1, j], recv.at[1, j], (d, r, c ^ j))

    def pair(j):
        src = kv_ref.at[c] if j == 0 else kv_out.at[c ^ j, d]
        return rcopy(src, kv_out.at[c ^ j, d], psend.at[j], precv.at[j], pn)

    for j in (3, 2, 1):
        kv(j).start()
    pair(0).start()
    for j in (3, 2, 1):
        q(j).start()
    kv_out[c, d] = kv_ref[c]
    q_out[c] = q_ref[c]
    for j in (1, 2, 3):
        kv(j).wait_recv()
        pair(j).start()
    for j in (1, 2, 3):
        q(j).wait()
        kv(j).wait_send()
    for j in range(4):
        pair(j).wait()


def heads_fast(q, kv, cid):
    cols, own, wide = kv.shape
    dma = pltpu.SemaphoreType.DMA
    return pl.pallas_call(
        heads_kernel,
        out_shape=[
            jax.ShapeDtypeStruct(q.shape, q.dtype),
            jax.ShapeDtypeStruct((cols, 2, own, wide), kv.dtype),
        ],
        in_specs=[VM] * 2,
        out_specs=[VM] * 2,
        scratch_shapes=[dma((2, 4)), dma((2, 4)), dma((4,)), dma((4,))],
        compiler_params=pltpu.CompilerParams(collective_id=cid, has_side_effects=True),
        name="to_heads",
    )(q, kv)


def tokens_kernel(q_ref, kv_ref, q_out, kv_out, total, theirs, send, recv, psend, precv):
    d, r, c = place()
    pn = (1 - d, r, c)
    greet([(d, r, c ^ j) for j in (1, 2, 3)] + [pn])

    def pair(j):
        return rcopy(kv_ref.at[c ^ j, 1 - d], theirs.at[c ^ j], psend.at[j], precv.at[j], pn)

    def kv(j):
        return rcopy(total.at[c ^ j], kv_out.at[c], send.at[0, j], recv.at[0, j], (d, r, c ^ j))

    def q(j):
        return rcopy(q_ref.at[c ^ j], q_out.at[c], send.at[1, j], recv.at[1, j], (d, r, c ^ j))

    for j in (3, 2, 1, 0):
        pair(j).start()
    for j in (3, 2, 1):
        q(j).start()
    q_out[c] = q_ref[c]
    for j in (3, 2, 1):
        pair(j).wait_recv()
        total[c ^ j] = kv_ref[c ^ j, d] + theirs[c ^ j]
        kv(j).start()
    pair(0).wait_recv()
    kv_out[c] = kv_ref[c, d] + theirs[c]
    for j in range(4):
        pair(j).wait_send()
    for j in (1, 2, 3):
        q(j).wait()
        kv(j).wait()


def tokens_fast(q, kv, cid):
    cols, _, own, wide = kv.shape
    dma = pltpu.SemaphoreType.DMA
    piece = jax.ShapeDtypeStruct((cols, own, wide), kv.dtype)
    return pl.pallas_call(
        tokens_kernel,
        out_shape=[jax.ShapeDtypeStruct(q.shape, q.dtype), piece],
        in_specs=[VM] * 2,
        out_specs=[VM] * 2,
        scratch_shapes=[
            pltpu.VMEM((cols, own, wide), kv.dtype),
            pltpu.VMEM((cols, own, wide), kv.dtype),
            dma((2, 4)), dma((2, 4)), dma((4,)), dma((4,)),
        ],
        compiler_params=pltpu.CompilerParams(collective_id=cid, has_side_effects=True),
        name="to_tokens",
    )(q, kv)


def dot(a, b, contract=((1,), (0,))):
    return lax.dot_general(a, b, (contract, ((), ())), preferred_element_type=f32)


def block_rows(ref, heads, scale, out):
    own = ref.shape[-1]
    for h in range(heads):
        for g in range(heads):
            spot = (pl.ds(h * HD, HD), pl.ds(g * own, own))
            if h == g:
                out[spot] = ref[0, pl.ds(h * HD, HD)] * jnp.asarray(scale, out.dtype)
            else:
                out[spot] = jnp.zeros((HD, own), out.dtype)


def attn_fwd_kernel(heads, scale, bounds, q_ref, kv_ref, qseg_ref, kseg_ref, ctx_ref, lse_ref, kn, q3, s_scr, o_scr):
    step = pl.program_id(0)
    tiles, _, tile = kv_ref.shape
    wide = heads * HD
    own = q_ref.shape[-1]

    @pl.when(step == 0)
    def _():
        @pl.loop(0, tiles)
        def _(j):
            kn[j] = kv_ref[j, pl.ds(0, wide)].astype(f32).T.astype(bf16)

    block_rows(q_ref, heads, scale, q3)
    low, high = bounds[step, 0], bounds[step, 1]
    qseg = jnp.concatenate([qseg_ref[0]] * heads, axis=1)

    def one(j, top):
        s = dot(kn[j], q3[...])
        s = jnp.where(kseg_ref[j] == qseg, s, masked_value)
        s_scr[j] = s
        return jnp.maximum(top, jnp.max(s, axis=0, keepdims=True))

    top = lax.fori_loop(low, high, one, jnp.full((1, heads * own), masked_value, f32))
    o_scr[...] = jnp.zeros_like(o_scr)

    def two(j, total):
        p = jnp.exp(s_scr[j] - top)
        low_p = p.astype(bf16)
        for h in range(heads):
            rows = pl.ds(h * HD, HD)
            v = kv_ref[j, pl.ds(wide + h * HD, HD)]
            o_scr[rows] += dot(v, low_p[:, h * own : (h + 1) * own])
        return total + jnp.sum(p, axis=0, keepdims=True)

    total = lax.fori_loop(low, high, two, jnp.zeros((1, heads * own), f32))
    for h in range(heads):
        rows = pl.ds(h * HD, HD)
        ctx_ref[0, rows] = (o_scr[rows] / total[:, h * own : (h + 1) * own]).astype(bf16)
    lse_ref[0] = top + jnp.log(total)


def attn_fwd(bounds, q, kv, qseg, kseg, scale):
    blocks, wide, own = q.shape
    tiles, _, tile = kv.shape
    heads = wide // HD
    return pl.pallas_call(
        functools.partial(attn_fwd_kernel, heads, scale),
        out_shape=[
            jax.ShapeDtypeStruct(q.shape, bf16),
            jax.ShapeDtypeStruct((blocks, 1, heads * own), f32),
        ],
        grid_spec=pltpu.PrefetchScalarGridSpec(
            num_scalar_prefetch=1,
            grid=(blocks,),
            in_specs=[
                pl.BlockSpec((1, wide, own), lambda i, b: (i, 0, 0)),
                pl.BlockSpec(kv.shape, lambda i, b: (0, 0, 0)),
                pl.BlockSpec((1, 1, own), lambda i, b: (i, 0, 0)),
                pl.BlockSpec(kseg.shape, lambda i, b: (0, 0, 0)),
            ],
            out_specs=[
                pl.BlockSpec((1, wide, own), lambda i, b: (i, 0, 0)),
                pl.BlockSpec((1, 1, heads * own), lambda i, b: (i, 0, 0)),
            ],
            scratch_shapes=[
                pltpu.VMEM((tiles, tile, wide), bf16),
                pltpu.VMEM((wide, heads * own), bf16),
                pltpu.VMEM((tiles, tile, heads * own), f32),
                pltpu.VMEM((wide, own), f32),
            ],
        ),
        compiler_params=pltpu.CompilerParams(
            dimension_semantics=("arbitrary",), vmem_limit_bytes=48 * 1024 * 1024
        ),
        name="attn_fwd",
    )(bounds, q, kv, qseg, kseg)


def attn_bwd_kernel(
    heads, scale, bounds, q_ref, kv_ref, qseg_ref, kseg_ref, lse_ref, ctx_ref, dctx_ref,
    dq_ref, dkv_ref, kn, vn, q3, dc3, dq_scr, dkv_scr,
):
    step = pl.program_id(0)
    tiles, _, tile = kv_ref.shape
    wide = heads * HD
    own = q_ref.shape[-1]

    @pl.when(step == 0)
    def _():
        @pl.loop(0, tiles)
        def _(j):
            kn[j] = kv_ref[j, pl.ds(0, wide)].astype(f32).T.astype(bf16)
            vn[j] = kv_ref[j, pl.ds(wide, wide)].astype(f32).T.astype(bf16)
            dkv_scr[j] = jnp.zeros((2 * wide, tile), f32)

    block_rows(q_ref, heads, scale, q3)
    block_rows(dctx_ref, heads, 1.0, dc3)
    low, high = bounds[step, 0], bounds[step, 1]
    qseg = jnp.concatenate([qseg_ref[0]] * heads, axis=1)
    lse = lse_ref[0]
    product = ctx_ref[0].astype(f32) * dctx_ref[0].astype(f32)
    delta = jnp.concatenate(
        [jnp.sum(product[h * HD : (h + 1) * HD], axis=0, keepdims=True) for h in range(heads)], axis=1
    )
    dq_scr[...] = jnp.zeros_like(dq_scr)

    @pl.loop(low, high)
    def _(j):
        s = dot(kn[j], q3[...])
        s = jnp.where(kseg_ref[j] == qseg, s, masked_value)
        p = jnp.exp(s - lse)
        d_p = dot(vn[j], dc3[...])
        d_s = (p * (d_p - delta)).astype(bf16)
        p = p.astype(bf16)
        for h in range(heads):
            rows, lanes = pl.ds(h * HD, HD), slice(h * own, (h + 1) * own)
            dq_scr[rows] += dot(kv_ref[j, rows], d_s[:, lanes])
            dkv_scr[j, rows] += dot(q3[rows, lanes], d_s[:, lanes], ((1,), (1,)))
            deep = pl.ds(wide + h * HD, HD)
            dkv_scr[j, deep] += dot(dctx_ref[0, rows], p[:, lanes], ((1,), (1,)))

    dq_ref[0] = (dq_scr[...] * scale).astype(bf16)

    @pl.when(step == pl.num_programs(0) - 1)
    def _():
        @pl.loop(0, tiles)
        def _(j):
            dkv_ref[j] = dkv_scr[j].astype(bf16)


def attn_bwd(bounds, q, kv, qseg, kseg, lse, ctx, dctx, scale):
    blocks, wide, own = q.shape
    tiles, _, tile = kv.shape
    heads = wide // HD
    rowed = pl.BlockSpec((1, wide, own), lambda i, b: (i, 0, 0))
    return pl.pallas_call(
        functools.partial(attn_bwd_kernel, heads, scale),
        out_shape=[jax.ShapeDtypeStruct(q.shape, bf16), jax.ShapeDtypeStruct(kv.shape, bf16)],
        grid_spec=pltpu.PrefetchScalarGridSpec(
            num_scalar_prefetch=1,
            grid=(blocks,),
            in_specs=[
                rowed,
                pl.BlockSpec(kv.shape, lambda i, b: (0, 0, 0)),
                pl.BlockSpec((1, 1, own), lambda i, b: (i, 0, 0)),
                pl.BlockSpec(kseg.shape, lambda i, b: (0, 0, 0)),
                pl.BlockSpec((1, 1, heads * own), lambda i, b: (i, 0, 0)),
                rowed,
                rowed,
            ],
            out_specs=[rowed, pl.BlockSpec(kv.shape, lambda i, b: (0, 0, 0))],
            scratch_shapes=[
                pltpu.VMEM((tiles, tile, wide), bf16),
                pltpu.VMEM((tiles, tile, wide), bf16),
                pltpu.VMEM((wide, heads * own), bf16),
                pltpu.VMEM((wide, heads * own), bf16),
                pltpu.VMEM((wide, own), f32),
                pltpu.VMEM((tiles, 2 * wide, tile), f32),
            ],
        ),
        compiler_params=pltpu.CompilerParams(
            dimension_semantics=("arbitrary",), vmem_limit_bytes=48 * 1024 * 1024
        ),
        name="attn_bwd",
    )(bounds, q, kv, qseg, kseg, lse, ctx, dctx)


def fast_local(
    tokens,
    segments,
    labels,
    cotangent,
    w_qkv,
    b_qkv,
    w_out,
    b_out,
    ln1_gain,
    ln1_bias,
    w_in,
    b_in,
    w_back,
    b_back,
    ln2_gain,
    ln2_bias,
    s_proj,
    s_bias,
    s_query,
    s_mid,
    s_mid_bias,
    s_cls,
    s_cls_bias,
):
    _, width_row, cols_local = tokens.shape
    parts, rows, cols, seqs, _ = sizes(tokens.shape[0])
    width = width_row * rows
    own = cols_local // parts
    width_col = b_qkv.shape[1]
    heads_dev = width_col // HD
    hidden_col = b_in.shape[0]
    docs_count = labels.shape[1]
    class_count = s_cls.shape[1]
    student_width = s_proj.shape[1]
    seq_len = segments.shape[1]
    row_index = lax.axis_index("row")
    col_index = lax.axis_index("col")
    dp_index = lax.axis_index("dp")
    score_scale = HD ** (-0.5)
    pool_scale = SHD ** (-0.5)
    query_heads = s_query.reshape(SH, SHD)
    doc_ids = jnp.arange(docs_count, dtype=jnp.int32)
    class_ids = jnp.arange(class_count, dtype=jnp.int32)

    w_three = w_qkv.reshape(width_row, heads_dev, 3, HD).transpose(0, 2, 1, 3)
    w_three = jnp.concatenate([w_three[:, 1], w_three[:, 2], w_three[:, 0]], axis=1)
    shard_attn = own_half(jnp.concatenate([w_three.reshape(width_row, -1), w_out], axis=1))
    proj_rows = width_row // cols
    vectors = [b_out, ln1_gain, ln1_bias, b_back, ln2_gain, ln2_bias, b_qkv.reshape(-1), b_in]
    vectors.append(lax.dynamic_slice_in_dim(s_proj, col_index * proj_rows, proj_rows).astype(f32).reshape(-1))
    flat = jnp.concatenate(vectors)
    flat = jnp.pad(flat, (0, 96 * 128 - flat.shape[0])).reshape(96, 128)
    w_attn, vec, w_in_all, w_back_all, x_parts, c_parts, ints = gather_fast(
        [shard_attn, own_half(flat), own_half(w_in), own_half(w_back)],
        tokens,
        cotangent,
        jnp.concatenate([segments, labels], axis=1),
        1,
    )
    w_attn = w_attn.reshape(cols, rows, width_row, 4 * width_col)
    w_qkv_all = w_attn[..., : 3 * width_col].reshape(cols, width, 3 * width_col)
    w_out_all = w_attn[..., 3 * width_col :].transpose(0, 2, 1, 3).reshape(width, width)
    w_in_all = w_in_all.reshape(cols, width, hidden_col)
    w_back_all = w_back_all.reshape(cols, width, hidden_col)
    vec = vec.reshape(cols, rows, -1)
    at = 6 * width_row
    row_vectors = vec[0, :, :at].reshape(rows, 6, width_row).transpose(1, 0, 2).reshape(6, width)
    b_out_a, gain_one, bias_one, b_back_a, gain_two, bias_two = [row_vectors[i] for i in range(6)]
    b_qkv_all = vec[:, 0, at : at + 2 * width_col].reshape(cols, 2, width_col)
    at += 2 * width_col
    b_in_all = vec[:, 0, at : at + hidden_col]
    at += hidden_col
    s_proj_all = vec[:, :, at : at + proj_rows * student_width].astype(bf16)
    s_proj_all = s_proj_all.reshape(cols, rows, proj_rows, student_width).transpose(1, 0, 2, 3)
    s_proj_all = s_proj_all.reshape(width, student_width)
    x_t = x_parts.reshape(width, own)
    ints = lax.dynamic_index_in_dim(ints.reshape(seqs, -1), row_index, 0, False)
    seg_all, label_seq = ints[:seq_len], ints[seq_len:]
    seg_blocks = seg_all.reshape(cols, parts, own)
    seg_q = lax.dynamic_index_in_dim(seg_blocks, dp_index, 1, False)
    seg_own = lax.dynamic_index_in_dim(seg_q, col_index, 0, False)
    lows = jnp.sum(seg_all[None, :] < seg_q[:, :1], axis=1) // own
    highs = (jnp.sum(seg_all[None, :] <= seg_q[:, -1:], axis=1) + own - 1) // own
    bounds = jnp.stack([lows, highs], axis=1).astype(jnp.int32)

    offsets = jnp.concatenate([jnp.zeros_like(b_qkv_all[:, 0]), b_qkv_all[:, 1], b_qkv_all[:, 0]], axis=1)
    qkv = jnp.einsum("cdn,dt->cnt", w_qkv_all, x_t, preferred_element_type=f32) + offsets[:, :, None]
    qkv = qkv.astype(bf16)
    queries, kv = heads_fast(qkv[:, 2 * width_col :], qkv[:, : 2 * width_col], 2)
    kv = kv.reshape(cols * parts, 2 * width_col, own)
    q_rows, k_rows = seg_q[:, None, :], seg_all.reshape(cols * parts, own, 1)
    context, lse = attn_fwd(bounds, queries, kv, q_rows, k_rows, score_scale)
    (ctx_t,) = swap_fast([context], 3)
    ctx_t = ctx_t.reshape(width, own)

    x = x_t.T
    attn_out = mm(ctx_t, w_out_all, ((0,), (0,))) + b_out_a
    normed_one, inv_one = normalize(x.astype(f32) + attn_out)
    hidden_one = normed_one * gain_one + bias_one
    hidden_low = hidden_one.astype(bf16)
    pre_act = jnp.einsum("td,cdn->ctn", hidden_low, w_in_all, preferred_element_type=f32)
    pre_act = pre_act + b_in_all[:, None, :]
    act = gelu_exact(pre_act).astype(bf16)
    ffn_out = jnp.einsum("ctn,cdn->td", act, w_back_all, preferred_element_type=f32) + b_back_a
    normed_two, inv_two = normalize(hidden_one + ffn_out)
    layer_out = (normed_two * gain_two + bias_two).astype(bf16)
    out = give_fast(layer_out.T, 4)

    student_h = mm(layer_out, s_proj_all, ((1,), (0,))) + s_bias
    head_parts = student_h.reshape(own, SH, SHD)
    pool_logit = jnp.sum(head_parts * query_heads, axis=-1) * pool_scale
    member = (seg_own[:, None] == doc_ids[None, :])[:, :, None]
    masked = jnp.where(member, pool_logit[:, None, :], masked_value)
    local_top = jnp.max(masked, axis=0)
    local_exp = jnp.where(member, jnp.exp(masked - local_top[None]), 0.0)
    local_total = jnp.sum(local_exp, axis=0)
    local_sum = jnp.einsum("tdh,thk->dhk", local_exp, head_parts, precision=highest)
    stats = jnp.concatenate([local_top[..., None], local_total[..., None], local_sum], axis=-1)
    stats = lax.all_gather(stats, ("dp", "col"))
    tops, totals, sums = stats[..., 0], stats[..., 1], stats[..., 2:]
    doc_top = jnp.max(tops, axis=0)
    factors = jnp.exp(tops - doc_top[None])
    doc_total = jnp.sum(totals * factors, axis=0)
    pooled_heads = jnp.sum(sums * factors[..., None], axis=0) / doc_total[:, :, None]
    pooled = pooled_heads.reshape(docs_count, student_width)
    middle = jnp.tanh(jnp.dot(pooled, s_mid, precision=highest) + s_mid_bias)
    logit_rows = jnp.dot(middle, s_cls, precision=highest) + s_cls_bias
    logits = lax.all_gather(logit_rows, "row")
    logits = lax.dynamic_slice_in_dim(logits, dp_index * (seqs // parts), seqs // parts)
    logit_top = jnp.max(logit_rows, axis=-1, keepdims=True)
    logit_exp = jnp.exp(logit_rows - logit_top)
    one_hot = (label_seq[:, None] == class_ids[None, :]).astype(f32)
    d_logits = logit_exp / jnp.sum(logit_exp, axis=-1, keepdims=True) - one_hot
    g_cls = jnp.dot(middle.T, d_logits, precision=highest)
    g_cls_bias = jnp.sum(d_logits, axis=0)
    d_middle = jnp.dot(d_logits, s_cls.T, precision=highest) * (1.0 - middle * middle)
    g_mid = jnp.dot(pooled.T, d_middle, precision=highest)
    g_mid_bias = jnp.sum(d_middle, axis=0)
    d_pooled = jnp.dot(d_middle, s_mid.T, precision=highest).reshape(docs_count, SH, SHD)
    shares = jnp.where(member, jnp.exp(masked - doc_top[None]), 0.0) / doc_total[None]
    d_share = jnp.einsum("dhk,thk->tdh", d_pooled, head_parts, precision=highest)
    base_term = jnp.sum(d_pooled * pooled_heads, axis=-1)
    d_pool_logit = jnp.sum(shares * (d_share - base_term[None]), axis=1)
    d_heads = jnp.einsum("tdh,dhk->thk", shares, d_pooled, precision=highest)
    d_heads = d_heads + d_pool_logit[:, :, None] * query_heads[None] * pool_scale
    g_query = (jnp.sum(d_pool_logit[:, :, None] * head_parts, axis=0) * pool_scale).reshape(-1)
    d_student = d_heads.reshape(own, student_width)
    g_sbias = jnp.sum(d_student, axis=0)
    g_sproj = jnp.dot(layer_out.astype(f32).T, d_student, precision=highest)

    d_out = c_parts.reshape(width, own).T.astype(f32)
    g_ln2_gain = jnp.sum(d_out * normed_two, axis=0)
    g_ln2_bias = jnp.sum(d_out, axis=0)
    d_resid_two = normalize_back(d_out * gain_two, normed_two, inv_two)
    d_ffn = d_resid_two.astype(bf16)
    g_back_bias = jnp.sum(d_ffn.astype(f32), axis=0)
    g_back = jnp.einsum("td,ctn->cdn", d_ffn, act, preferred_element_type=f32)
    d_act = jnp.einsum("td,cdn->ctn", d_ffn, w_back_all, preferred_element_type=f32)
    _, gelu_fn = jax.vjp(gelu_exact, pre_act)
    d_pre = gelu_fn(d_act)[0].astype(bf16)
    g_in_bias = jnp.sum(d_pre.astype(f32), axis=1)
    g_in = jnp.einsum("td,ctn->cdn", hidden_low, d_pre, preferred_element_type=f32)
    d_hidden_one = d_resid_two + jnp.einsum(
        "ctn,cdn->td", d_pre, w_in_all, preferred_element_type=f32
    )
    g_ln1_gain = jnp.sum(d_hidden_one * normed_one, axis=0)
    g_ln1_bias = jnp.sum(d_hidden_one, axis=0)
    d_resid_one = normalize_back(d_hidden_one * gain_one, normed_one, inv_one)
    d_attn = d_resid_one.astype(bf16)
    g_out_bias = jnp.sum(d_attn.astype(f32), axis=0)
    d_ctx = mm(w_out_all, d_attn, ((1,), (1,))).astype(bf16)
    (d_ctx,) = swap_fast([d_ctx.reshape(cols, width_col, own)], 5)
    once = 1.0 / (parts * cols)
    small = (
        g_in_bias,
        g_out_bias,
        g_ln1_gain,
        g_ln1_bias,
        g_back_bias,
        g_ln2_gain,
        g_ln2_bias,
        g_sproj,
        g_sbias,
        g_query,
        g_mid * once,
        g_mid_bias * once,
        g_cls * once,
        g_cls_bias * once,
    )
    small = lax.psum(small, WORLD)
    d_q, d_kv = attn_bwd(bounds, queries, kv, q_rows, k_rows, lse, context, d_ctx, score_scale)
    d_q, d_kv = tokens_fast(d_q, d_kv.reshape(cols, parts, 2 * width_col, own), 6)
    d_qkv = jnp.concatenate([d_kv, d_q], axis=1)
    g_qkv_bias = jnp.sum(d_qkv.astype(f32), axis=2)
    g_qkv_bias, small = lax.optimization_barrier((g_qkv_bias, small))
    g_qkv_bias = lax.psum(g_qkv_bias[:, width_col:], WORLD)
    g_qkv = jnp.einsum("dt,cnt->cdn", x_t, d_qkv, preferred_element_type=f32)
    d_tokens = jnp.einsum("cdn,cnt->dt", w_qkv_all, d_qkv, preferred_element_type=f32)
    d_tokens = (d_tokens + d_resid_one.T).astype(bf16)
    grad_tokens = give_fast(d_tokens, 7).astype(f32)

    g_out = mm(ctx_t, d_attn, ((1,), (0,)))
    g_out = g_out.reshape(cols, width_col, rows, width_row).transpose(0, 2, 1, 3)
    g_attn = jnp.concatenate(
        [g_qkv.astype(bf16).reshape(cols, rows, width_row, 3 * width_col), g_out.astype(bf16)], axis=-1
    )
    blocked = (cols, rows, parts, width_row // parts, -1)
    g_in, g_back, g_attn = [
        part.reshape(width_row, -1).astype(f32)
        for part in scatter_fast(
            [g_in.astype(bf16).reshape(blocked), g_back.astype(bf16).reshape(blocked), g_attn.reshape(blocked)],
            8,
        )
    ]
    g_qkv = g_attn[:, : 3 * width_col].reshape(width_row, 3, heads_dev, HD)
    g_qkv = jnp.stack([g_qkv[:, 2], g_qkv[:, 0], g_qkv[:, 1]], axis=2).reshape(width_row, -1)

    def at_col(part):
        return lax.dynamic_index_in_dim(part, col_index, 0, False)

    def at_row(part):
        return lax.dynamic_slice_in_dim(part, row_index * width_row, width_row)

    bias_grad = at_col(g_qkv_bias)
    return (
        out,
        logits,
        grad_tokens,
        g_qkv,
        jnp.stack([bias_grad[width_col:], bias_grad[:width_col]]),
        g_attn[:, 3 * width_col :],
        at_row(small[1]),
        at_row(small[2]),
        at_row(small[3]),
        g_in,
        at_col(small[0]),
        g_back,
        at_row(small[4]),
        at_row(small[5]),
        at_row(small[6]),
        at_row(small[7]),
    ) + tuple(small[8:])


def solution(mesh):
    row, col = P("row"), P("col")
    grid, whole = P("row", "col"), P("dp", "row", "col")
    placed = (
        (whole, P("dp", None), P("dp", None), whole, grid, P(None, "col"), P("col", "row"))
        + (row, row, row, grid, col, grid, row, row, row, P("row", None))
        + (P(),) * 6
    )
    results = (
        (whole, P("dp", None, None), whole, grid, P(None, "col"), P("col", "row"))
        + (row, row, row, grid, col, grid, row, row, row, P("row", None))
        + (P(),) * 6
    )
    quick = dict(mesh.shape) == {"dp": 2, "row": 4, "col": 4}
    local = fast_local if quick else general_local
    return jax.shard_map(local, mesh=mesh, in_specs=placed, out_specs=results, check_vma=False)
```

```python
import functools
import jax
import jax.numpy as jnp
from jax import lax
from jax.experimental import pallas as pl
from jax.experimental.pallas import tpu as pltpu
from jax.sharding import PartitionSpec as P

HD = 64
SH = 2
SHD = 64

norm_eps = 1e-06
masked_value = -1e30
highest = lax.Precision.HIGHEST
f32 = jnp.float32
bf16 = jnp.bfloat16
WORLD = ("col", "row", "dp")


def sizes(seqs_local):
    parts = lax.axis_size("dp")
    rows = lax.axis_size("row")
    seqs = seqs_local * parts
    return parts, rows, lax.axis_size("col"), seqs, rows // seqs


def row_groups(rows, sub):
    return [list(range(at, at + sub)) for at in range(0, rows, sub)]


def take_in(values):
    parts, rows, _, seqs, sub = sizes(values.shape[0])
    held = lax.all_to_all(values, "dp", 2, 0, tiled=True)
    feats, half = held.shape[1:]
    held = held.reshape(seqs, feats, sub, half // sub).transpose(0, 2, 1, 3)
    held = held.reshape(rows, feats, half // sub)
    held = lax.all_to_all(held, "row", 0, 0, tiled=True)
    return held.reshape(rows * feats, half // sub)


def give_back(values, seqs_local):
    parts, rows, _, seqs, sub = sizes(seqs_local)
    width, own = values.shape
    feats = width // rows
    held = lax.all_to_all(values.reshape(rows, feats, own), "row", 0, 0, tiled=True)
    held = held.reshape(seqs, sub, feats, own).transpose(0, 2, 1, 3).reshape(seqs, feats, sub * own)
    return lax.all_to_all(held, "dp", 0, 2, tiled=True)


def gather_world(shard):
    cols, rows = lax.axis_size("col"), lax.axis_size("row")
    out = lax.all_gather(shard, WORLD, axis=0, tiled=True)
    return out.reshape(cols, rows, -1, shard.shape[1])


def own_half(block):
    parts = lax.axis_size("dp")
    amount = block.shape[0] // parts
    return lax.dynamic_slice_in_dim(block, lax.axis_index("dp") * amount, amount)


def scatter_world(full):
    flat = full.reshape(-1, full.shape[-1])
    mine = lax.psum_scatter(flat, WORLD, scatter_dimension=0, tiled=True)
    return lax.all_gather(mine, "dp", axis=0, tiled=True)


def swap_cols(values):
    return lax.all_to_all(values, "col", 0, 0, tiled=True)


def gather_sequence(values, sub):
    cols, own, width = values.shape
    held = values[:, None]
    if sub > 1:
        groups = row_groups(lax.axis_size("row"), sub)
        held = lax.all_gather(held, "row", axis=1, tiled=True, axis_index_groups=groups)
    held = lax.all_gather(held[:, None], "dp", axis=1, tiled=True)
    return held.reshape(-1, width)


def scatter_sequence(values, cols, sub):
    parts = lax.axis_size("dp")
    width = values.shape[-1]
    held = values.reshape(cols, parts, sub, -1, width)
    held = lax.psum_scatter(held, "dp", scatter_dimension=1, tiled=True)[:, 0]
    if sub > 1:
        groups = row_groups(lax.axis_size("row"), sub)
        held = lax.psum_scatter(
            held, "row", scatter_dimension=1, tiled=True, axis_index_groups=groups
        )
    return held[:, 0]


def normalize(values):
    mean_v = jnp.mean(values, axis=-1, keepdims=True)
    center = values - mean_v
    inv_std = lax.rsqrt(jnp.mean(center * center, axis=-1, keepdims=True) + norm_eps)
    return center * inv_std, inv_std


def normalize_back(grad_hat, normed, inv_std):
    return inv_std * (
        grad_hat
        - jnp.mean(grad_hat, axis=-1, keepdims=True)
        - normed * jnp.mean(grad_hat * normed, axis=-1, keepdims=True)
    )


def gelu_exact(values):
    return jax.nn.gelu(values, approximate=False)


def mm(a, b, contract):
    return lax.dot_general(a, b, (contract, ((), ())), preferred_element_type=f32)


def combine_pool(part_one, part_two):
    top_a, total_a, sum_a = part_one
    top_b, total_b, sum_b = part_two
    row_top = jnp.maximum(top_a, top_b)
    factor_a = jnp.exp(top_a - row_top)
    factor_b = jnp.exp(top_b - row_top)
    return (
        row_top,
        total_a * factor_a + total_b * factor_b,
        sum_a * factor_a[:, :, None] + sum_b * factor_b[:, :, None],
    )


def attend(q, k, v, q_seg, k_seg, scale):
    scores = jnp.einsum("qhd,khd->hqk", q, k, preferred_element_type=f32) * scale
    scores = jnp.where((q_seg[:, None] == k_seg[None, :])[None], scores, masked_value)
    top = jnp.max(scores, axis=-1, keepdims=True)
    exp_scores = jnp.exp(scores - top)
    total = jnp.sum(exp_scores, axis=-1, keepdims=True)
    probs = exp_scores / total
    context = jnp.einsum("hqk,khd->qhd", probs.astype(bf16), v, preferred_element_type=f32)
    return context.astype(bf16), probs


def attend_back(q, k, v, probs, d_ctx, scale):
    d_probs = jnp.einsum("qhd,khd->hqk", d_ctx, v, preferred_element_type=f32)
    delta = jnp.sum(probs * d_probs, axis=-1, keepdims=True)
    d_scores = (probs * (d_probs - delta)).astype(bf16)
    d_q = jnp.einsum("hqk,khd->qhd", d_scores, k, preferred_element_type=f32) * scale
    d_k = jnp.einsum("hqk,qhd->khd", d_scores, q, preferred_element_type=f32) * scale
    d_v = jnp.einsum("hqk,qhd->khd", probs.astype(bf16), d_ctx, preferred_element_type=f32)
    return d_q, d_k, d_v


def general_local(
    tokens,
    segments,
    labels,
    cotangent,
    w_qkv,
    b_qkv,
    w_out,
    b_out,
    ln1_gain,
    ln1_bias,
    w_in,
    b_in,
    w_back,
    b_back,
    ln2_gain,
    ln2_bias,
    s_proj,
    s_bias,
    s_query,
    s_mid,
    s_mid_bias,
    s_cls,
    s_cls_bias,
):
    seqs_local, width_row, cols_local = tokens.shape
    parts, rows, cols, seqs, sub = sizes(seqs_local)
    width = width_row * rows
    own = cols_local // (parts * sub)
    width_col = b_qkv.shape[1]
    heads_dev = width_col // HD
    hidden_col = b_in.shape[0]
    docs_count = labels.shape[1]
    class_count = s_cls.shape[1]
    student_width = s_proj.shape[1]
    row_index = lax.axis_index("row")
    col_index = lax.axis_index("col")
    dp_index = lax.axis_index("dp")
    seq_index = row_index // sub
    sub_index = row_index % sub
    score_scale = HD ** (-0.5)
    pool_scale = SHD ** (-0.5)
    query_heads = s_query.reshape(SH, SHD)
    doc_ids = jnp.arange(docs_count, dtype=jnp.int32)
    class_ids = jnp.arange(class_count, dtype=jnp.int32)

    w_qkv_all = gather_world(own_half(w_qkv)).reshape(cols, width, 3 * width_col)
    x_t = take_in(tokens)
    rest = jnp.concatenate([own_half(w_in), own_half(w_back), own_half(w_out).reshape(-1, width_col)], axis=1)
    rest_all = gather_world(rest)
    w_in_all = rest_all[..., :hidden_col].reshape(cols, width, hidden_col)
    w_back_all = rest_all[..., hidden_col : 2 * hidden_col].reshape(cols, width, hidden_col)
    w_out_all = rest_all[..., 2 * hidden_col :].reshape(cols, rows, width_col, width_row)
    w_out_all = w_out_all.transpose(0, 2, 1, 3).reshape(width, width)
    row_vectors = lax.all_gather(
        jnp.stack([b_out, ln1_gain, ln1_bias, b_back, ln2_gain, ln2_bias]), "row", axis=1, tiled=True
    )
    b_out_a, gain_one, bias_one, b_back_a, gain_two, bias_two = [row_vectors[i] for i in range(6)]
    b_qkv_all = lax.all_gather(b_qkv, "col")
    b_in_all = lax.all_gather(b_in, "col")
    s_proj_all = lax.all_gather(s_proj, "row", axis=0, tiled=True)
    whole_ints = lax.all_gather(jnp.concatenate([segments, labels], axis=1), "dp", axis=0, tiled=True)
    ints = lax.dynamic_index_in_dim(whole_ints, seq_index, 0, False)
    seq_len = segments.shape[1]
    seg_all, label_seq = ints[:seq_len], ints[seq_len:]
    seg_blocks = seg_all.reshape(cols, parts, sub, own)
    seg_q = lax.dynamic_index_in_dim(seg_blocks, dp_index, 1, False)
    seg_q = lax.dynamic_index_in_dim(seg_q, sub_index, 1, False)
    seg_own = lax.dynamic_index_in_dim(seg_q, col_index, 0, False)
    seg_q = seg_q.reshape(-1)

    x = x_t.T
    offsets = jnp.stack([b_qkv_all[:, 0], jnp.zeros_like(b_qkv_all[:, 0]), b_qkv_all[:, 1]], axis=1)
    offsets = offsets.reshape(cols, 3, heads_dev, HD).transpose(0, 2, 1, 3).reshape(cols, 1, -1)
    qkv = jnp.einsum("td,cdn->ctn", x, w_qkv_all, preferred_element_type=f32) + offsets
    qkv = swap_cols(qkv.astype(bf16)).reshape(cols, own, heads_dev, 3, HD)
    queries = qkv[:, :, :, 0].reshape(cols * own, heads_dev, HD)
    kv = gather_sequence(qkv[:, :, :, 1:].reshape(cols, own, -1), sub)
    kv = kv.reshape(seq_len, heads_dev, 2, HD)
    key_rows, value_rows = kv[:, :, 0], kv[:, :, 1]
    context, probs = attend(queries, key_rows, value_rows, seg_q, seg_all, score_scale)
    ctx = swap_cols(context.reshape(cols, own, width_col))
    ctx = ctx.transpose(1, 0, 2).reshape(own, width)

    attn_out = mm(ctx, w_out_all, ((1,), (0,))) + b_out_a
    normed_one, inv_one = normalize(x.astype(f32) + attn_out)
    hidden_one = normed_one * gain_one + bias_one
    hidden_low = hidden_one.astype(bf16)
    pre_act = jnp.einsum("td,cdn->ctn", hidden_low, w_in_all, preferred_element_type=f32)
    pre_act = pre_act + b_in_all[:, None, :]
    act = gelu_exact(pre_act).astype(bf16)
    ffn_out = jnp.einsum("ctn,cdn->td", act, w_back_all, preferred_element_type=f32) + b_back_a
    normed_two, inv_two = normalize(hidden_one + ffn_out)
    layer_out = (normed_two * gain_two + bias_two).astype(bf16)
    out = give_back(layer_out.T, seqs_local)

    student_h = mm(layer_out, s_proj_all, ((1,), (0,))) + s_bias
    head_parts = student_h.reshape(own, SH, SHD)
    pool_logit = jnp.sum(head_parts * query_heads, axis=-1) * pool_scale
    member = (seg_own[:, None] == doc_ids[None, :])[:, :, None]
    masked = jnp.where(member, pool_logit[:, None, :], masked_value)
    local_top = jnp.max(masked, axis=0)
    local_exp = jnp.where(member, jnp.exp(masked - local_top[None]), 0.0)
    local_total = jnp.sum(local_exp, axis=0)
    local_sum = jnp.einsum("tdh,thk->dhk", local_exp, head_parts, precision=highest)
    stats = jnp.concatenate([local_top[..., None], local_total[..., None], local_sum], axis=-1)
    stats = lax.all_gather(stats, ("dp", "col"))
    if sub > 1:
        stats = lax.all_gather(stats, "row", axis=0, tiled=True, axis_index_groups=row_groups(rows, sub))
    tops, totals, sums = stats[..., 0], stats[..., 1], stats[..., 2:]
    doc_top = jnp.max(tops, axis=0)
    factors = jnp.exp(tops - doc_top[None])
    doc_total = jnp.sum(totals * factors, axis=0)
    pooled_heads = jnp.sum(sums * factors[..., None], axis=0) / doc_total[:, :, None]
    pooled = pooled_heads.reshape(docs_count, student_width)
    middle = jnp.tanh(jnp.dot(pooled, s_mid, precision=highest) + s_mid_bias)
    logit_rows = jnp.dot(middle, s_cls, precision=highest) + s_cls_bias
    logits = lax.all_gather(logit_rows, "row")[::sub]
    logits = lax.dynamic_slice_in_dim(logits, dp_index * seqs_local, seqs_local)
    logit_top = jnp.max(logit_rows, axis=-1, keepdims=True)
    logit_exp = jnp.exp(logit_rows - logit_top)
    one_hot = (label_seq[:, None] == class_ids[None, :]).astype(f32)
    d_logits = logit_exp / jnp.sum(logit_exp, axis=-1, keepdims=True) - one_hot
    g_cls = jnp.dot(middle.T, d_logits, precision=highest)
    g_cls_bias = jnp.sum(d_logits, axis=0)
    d_middle = jnp.dot(d_logits, s_cls.T, precision=highest) * (1.0 - middle * middle)
    g_mid = jnp.dot(pooled.T, d_middle, precision=highest)
    g_mid_bias = jnp.sum(d_middle, axis=0)
    d_pooled = jnp.dot(d_middle, s_mid.T, precision=highest).reshape(docs_count, SH, SHD)
    shares = jnp.where(member, jnp.exp(masked - doc_top[None]), 0.0) / doc_total[None]
    d_share = jnp.einsum("dhk,thk->tdh", d_pooled, head_parts, precision=highest)
    base_term = jnp.sum(d_pooled * pooled_heads, axis=-1)
    d_pool_logit = jnp.sum(shares * (d_share - base_term[None]), axis=1)
    d_heads = jnp.einsum("tdh,dhk->thk", shares, d_pooled, precision=highest)
    d_heads = d_heads + d_pool_logit[:, :, None] * query_heads[None] * pool_scale
    g_query = (jnp.sum(d_pool_logit[:, :, None] * head_parts, axis=0) * pool_scale).reshape(-1)
    d_student = d_heads.reshape(own, student_width)
    g_sbias = jnp.sum(d_student, axis=0)
    g_sproj = jnp.dot(layer_out.astype(f32).T, d_student, precision=highest)

    d_out = take_in(cotangent).T.astype(f32)
    g_ln2_gain = jnp.sum(d_out * normed_two, axis=0)
    g_ln2_bias = jnp.sum(d_out, axis=0)
    d_resid_two = normalize_back(d_out * gain_two, normed_two, inv_two)
    d_ffn = d_resid_two.astype(bf16)
    g_back_bias = jnp.sum(d_ffn.astype(f32), axis=0)
    g_back = jnp.einsum("td,ctn->cdn", d_ffn, act, preferred_element_type=f32)
    d_act = jnp.einsum("td,cdn->ctn", d_ffn, w_back_all, preferred_element_type=f32)
    _, gelu_fn = jax.vjp(gelu_exact, pre_act)
    d_pre = gelu_fn(d_act)[0].astype(bf16)
    g_in_bias = jnp.sum(d_pre.astype(f32), axis=1)
    g_in = jnp.einsum("td,ctn->cdn", hidden_low, d_pre, preferred_element_type=f32)
    d_hidden_one = d_resid_two + jnp.einsum(
        "ctn,cdn->td", d_pre, w_in_all, preferred_element_type=f32
    )
    g_ln1_gain = jnp.sum(d_hidden_one * normed_one, axis=0)
    g_ln1_bias = jnp.sum(d_hidden_one, axis=0)
    d_resid_one = normalize_back(d_hidden_one * gain_one, normed_one, inv_one)
    d_attn = d_resid_one.astype(bf16)
    g_out_bias = jnp.sum(d_attn.astype(f32), axis=0)
    g_out = mm(ctx, d_attn, ((0,), (0,)))
    d_ctx = mm(d_attn, w_out_all, ((1,), (1,))).astype(bf16)
    d_ctx = swap_cols(d_ctx.reshape(own, cols, width_col).transpose(1, 0, 2))
    d_ctx = d_ctx.reshape(cols * own, heads_dev, HD)
    d_q, d_k, d_v = attend_back(queries, key_rows, value_rows, probs, d_ctx, score_scale)
    d_kv = jnp.stack([d_k, d_v], axis=2).astype(bf16).reshape(seq_len, -1)
    d_kv = scatter_sequence(d_kv, cols, sub).reshape(cols, own, heads_dev, 2, HD)
    d_q = d_q.astype(bf16).reshape(cols, own, heads_dev, 1, HD)
    d_qkv = jnp.concatenate([d_q, d_kv], axis=3).reshape(cols, own, 3 * width_col)
    d_qkv = swap_cols(d_qkv)
    g_qkv_bias = jnp.sum(d_qkv.astype(f32), axis=1).reshape(cols, heads_dev, 3, HD)
    g_qkv = jnp.einsum("td,ctn->cdn", x, d_qkv, preferred_element_type=f32)
    d_tokens = d_resid_one + jnp.einsum("ctn,cdn->td", d_qkv, w_qkv_all, preferred_element_type=f32)
    grad_tokens = give_back(d_tokens.astype(bf16).T, seqs_local).astype(f32)

    g_out = g_out.reshape(cols, width_col, rows, width_row).transpose(0, 2, 1, 3)
    g_out = g_out.reshape(cols, rows, width_row, width_col)
    model = jnp.concatenate(
        [
            g_in.reshape(cols, rows, width_row, hidden_col).astype(bf16),
            g_back.reshape(cols, rows, width_row, hidden_col).astype(bf16),
            g_out.astype(bf16),
        ],
        axis=-1,
    )
    model = scatter_world(model).astype(f32)
    g_qkv = scatter_world(g_qkv.reshape(cols, rows, width_row, 3 * width_col).astype(bf16)).astype(f32)
    once = 1.0 / (parts * cols * sub)
    small = (
        g_qkv_bias[:, :, 0].reshape(cols, width_col),
        g_qkv_bias[:, :, 2].reshape(cols, width_col),
        g_in_bias,
        g_out_bias,
        g_ln1_gain,
        g_ln1_bias,
        g_back_bias,
        g_ln2_gain,
        g_ln2_bias,
        g_sproj,
        g_sbias,
        g_query,
        g_mid * once,
        g_mid_bias * once,
        g_cls * once,
        g_cls_bias * once,
    )
    small = lax.psum(small, WORLD)

    def at_col(part):
        return lax.dynamic_index_in_dim(part, col_index, 0, False)

    def at_row(part):
        return lax.dynamic_slice_in_dim(part, row_index * width_row, width_row)

    return (
        out,
        logits,
        grad_tokens,
        g_qkv,
        jnp.stack([at_col(small[0]), at_col(small[1])]),
        model[:, 2 * hidden_col :].reshape(width_col, width_row),
        at_row(small[3]),
        at_row(small[4]),
        at_row(small[5]),
        model[:, :hidden_col],
        at_col(small[2]),
        model[:, hidden_col : 2 * hidden_col],
        at_row(small[6]),
        at_row(small[7]),
        at_row(small[8]),
        at_row(small[9]),
        small[10],
        small[11],
        small[12],
        small[13],
        small[14],
        small[15],
    )


MESH = pl.DeviceIdType.MESH
HBM = pl.BlockSpec(memory_space=pl.ANY)


def place():
    return lax.axis_index("dp"), lax.axis_index("row"), lax.axis_index("col")


def greet(peers, guarded=()):
    barrier = pltpu.get_barrier_semaphore()
    for peer in peers:
        pl.semaphore_signal(barrier, inc=1, device_id=peer, device_id_type=MESH)
    for there, peer in guarded:

        @pl.when(there)
        def _():
            pl.semaphore_signal(barrier, inc=1, device_id=peer, device_id_type=MESH)

    amount = len(peers)
    for there, _ in guarded:
        amount = amount + there.astype(jnp.int32)
    pl.semaphore_wait(barrier, amount)


def rcopy(src, dst, send, recv, peer):
    return pltpu.make_async_remote_copy(
        src_ref=src, dst_ref=dst, send_sem=send, recv_sem=recv, device_id=peer, device_id_type=MESH
    )


def take_copies(src, out, local, send, recv):
    d, r, c = place()
    own = out.shape[2]
    moves = []
    for i in range(2):
        for far in range(2):
            row, core = 2 * d + i, d ^ far
            piece = src.at[i, :, pl.ds(pl.multiple_of(core * own, own), own)]
            here = (row == r) if far == 0 else None

            def start(piece=piece, row=row, core=core, slot=2 * i + far, here=here):
                def away():
                    rcopy(piece, out.at[r], send.at[slot], recv.at[r], (core, row, c)).start()

                if here is None:
                    away()
                else:
                    pl.when(jnp.logical_not(here))(away)

                    @pl.when(here)
                    def _():
                        pltpu.make_async_copy(piece, out.at[r], local).start()

            def wait(piece=piece, row=row, core=core, slot=2 * i + far, here=here):
                def away():
                    rcopy(piece, out.at[r], send.at[slot], recv.at[r], (core, row, c)).wait_send()

                if here is None:
                    away()
                else:
                    pl.when(jnp.logical_not(here))(away)

                    @pl.when(here)
                    def _():
                        pltpu.make_async_copy(piece, out.at[r], local).wait()

            moves.append((start, wait))
    for row in range(4):

        def arrive(row=row):
            @pl.when(jnp.logical_not((row == r) & (r // 2 == d)))
            def _():
                piece = src.at[0, :, pl.ds(0, own)]
                rcopy(piece, out.at[row], send.at[0], recv.at[row], (d, r, c)).wait_recv()

        moves.append((lambda: None, arrive))
    return moves


def gather_kernel(kinds, *refs):
    shards, refs = refs[:kinds], refs[kinds:]
    (tok, cot, ints), refs = refs[:3], refs[3:]
    outs, refs = refs[:kinds], refs[kinds:]
    (tok_out, cot_out, ints_out), refs = refs[:3], refs[3:]
    own_sem, zs, zr, xs, xr, ys, yr, cs, cr, ps, pr, tl, ts, tr, il = refs
    d, r, c = place()
    cols = 4
    xn, yn, pn = (d, r ^ 1, c), (d, r ^ 2, c), (1 - d, r, c)
    up, down = (d, r, c + 1), (d, r, c - 1)
    has_up, has_down = c < cols - 1, c > 0
    plane = [(d ^ (j // 4), r ^ (j % 4), c) for j in range(1, 8)]
    greet(plane, [(has_up, up), (has_down, down)])
    ahead = [take_copies(tok, tok_out, tl.at[0], ts.at[0], tr.at[0])]
    for start, _ in ahead[0]:
        start()
    pltpu.make_async_copy(ints, ints_out.at[d], il.at[0]).start()
    rcopy(ints, ints_out.at[d], il.at[1], il.at[2], pn).start()
    halves = [shard.shape[0] // 2 for shard in shards]

    def z_send(k, at, way, hop):
        src = shards[k] if hop == 1 else outs[k].at[at, r, d]
        return rcopy(
            src, outs[k].at[at, r, d], zs.at[k, way, hop - 1], zr.at[k, way, hop - 1], up if way == 0 else down
        )

    def src_of(k, at, own):
        return shards[k] if own else outs[k].at[at, r, d]

    def to_x(k, at, own):
        return rcopy(src_of(k, at, own), outs[k].at[at, r, d], xs.at[k, at], xr.at[k, at], xn)

    def to_y(k, at, own):
        return rcopy(src_of(k, at, own), outs[k].at[at, r, d], ys.at[k, at], yr.at[k, at], yn)

    def to_p(k, at, own):
        return rcopy(src_of(k, at, own), outs[k].at[at, r, d], ps.at[k, at, 0], pr.at[k, at, 0], pn)

    def relay(k, at, which):
        row = r ^ 1 if which == 0 else r ^ 2
        ref = outs[k].at[at, row, d, pl.ds(which * halves[k], halves[k])]
        return rcopy(ref, ref, cs.at[k, at, which], cr.at[k, at, which], yn if which == 0 else xn)

    def pass_p(k, at, bit):
        ref = outs[k].at[at, r ^ bit, d]
        return rcopy(ref, ref, ps.at[k, at, bit], pr.at[k, at, bit], pn)

    def got_x(k, at):
        ref = outs[k].at[at, r ^ 1, d]
        rcopy(ref, ref, xs.at[k, at], xr.at[k, at], xn).wait_recv()

    def got_y(k, at):
        ref = outs[k].at[at, r ^ 2, d]
        rcopy(ref, ref, ys.at[k, at], yr.at[k, at], yn).wait_recv()

    def got_corner(k, at):
        for which in range(2):
            ref = outs[k].at[at, r ^ 3, d, pl.ds(which * halves[k], halves[k])]
            rcopy(ref, ref, cs.at[k, at, which], cr.at[k, at, which], xn).wait_recv()

    def got_p(k, at, bit):
        ref = outs[k].at[at, r ^ bit, 1 - d]
        rcopy(ref, ref, ps.at[k, at, bit], pr.at[k, at, bit], pn).wait_recv()

    for k in range(kinds):
        pltpu.make_async_copy(shards[k], outs[k].at[c, r, d], own_sem.at[k]).start()

        @pl.when(has_up)
        def _():
            z_send(k, c, 0, 1).start()

        @pl.when(has_down)
        def _():
            z_send(k, c, 1, 1).start()

    def spread(k, at, own):
        to_x(k, at, own).start()
        to_y(k, at, own).start()
        to_p(k, at, own).start()

    def onward(k, at):
        got_x(k, at)
        relay(k, at, 0).start()
        pass_p(k, at, 1).start()
        got_y(k, at)
        relay(k, at, 1).start()
        pass_p(k, at, 2).start()

    steps = [(0, 0)] + [(way, hop) for hop in (1, 2, 3) for way in (0, 1)]
    jobs = [(k, way, hop) for k in range(kinds) for way, hop in steps]

    def at_of(way, hop):
        return c - hop if way == 0 else c + hop

    def valid(way, hop):
        return c >= hop if way == 0 else c + hop < cols

    def guard(way, hop, body):
        if hop == 0:
            body()
        else:
            pl.when(valid(way, hop))(body)

    def first(k, way, hop):
        def body():
            at = at_of(way, hop)
            if hop:
                z_send(k, at, way, hop).wait_recv()
                if hop < 3:
                    can = has_up if way == 0 else has_down

                    @pl.when(can)
                    def _():
                        z_send(k, at, way, hop + 1).start()

            spread(k, at, hop == 0)

        guard(way, hop, body)

    def second(k, way, hop):
        guard(way, hop, lambda: onward(k, at_of(way, hop)))

    def third(k, way, hop):
        def body():
            at = at_of(way, hop)
            got_corner(k, at)
            pass_p(k, at, 3).start()

        guard(way, hop, body)

    lag = 3
    for i in range(len(jobs) + 2 * lag):
        if i < len(jobs):
            first(*jobs[i])
        if 0 <= i - lag < len(jobs):
            second(*jobs[i - lag])
        if 0 <= i - 2 * lag < len(jobs):
            third(*jobs[i - 2 * lag])

    ahead.append(take_copies(cot, cot_out, tl.at[1], ts.at[1], tr.at[1]))
    for start, _ in ahead[1]:
        start()
    for k in range(kinds):
        pltpu.make_async_copy(shards[k], outs[k].at[c, r, d], own_sem.at[k]).wait()
        for way, hop in steps:

            def body():
                at = at_of(way, hop)
                own = hop == 0
                to_x(k, at, own).wait_send()
                to_y(k, at, own).wait_send()
                to_p(k, at, own).wait_send()
                for which in range(2):
                    relay(k, at, which).wait_send()
                for bit in (1, 2, 3):
                    pass_p(k, at, bit).wait_send()
                for bit in range(4):
                    got_p(k, at, bit)
                if hop < 3:
                    if own:

                        @pl.when(has_up)
                        def _():
                            z_send(k, c, 0, 1).wait_send()

                        @pl.when(has_down)
                        def _():
                            z_send(k, c, 1, 1).wait_send()
                    else:
                        can = has_up if way == 0 else has_down

                        @pl.when(can)
                        def _():
                            z_send(k, at, way, hop + 1).wait_send()

            guard(way, hop, body)
    for moves in ahead:
        for _, wait in moves:
            wait()
    pltpu.make_async_copy(ints, ints_out.at[d], il.at[0]).wait()
    rcopy(ints, ints_out.at[1 - d], il.at[1], il.at[2], pn).wait()


def gather_fast(shards, tokens, cotangent, ints, cid):
    kinds = len(shards)
    dma = pltpu.SemaphoreType.DMA
    _, feats, cols = tokens.shape
    taken = jax.ShapeDtypeStruct((4, feats, cols // 2), tokens.dtype)
    return pl.pallas_call(
        functools.partial(gather_kernel, kinds),
        out_shape=[jax.ShapeDtypeStruct((4, 4, 2) + s.shape, s.dtype) for s in shards]
        + [taken, taken, jax.ShapeDtypeStruct((2,) + ints.shape, ints.dtype)],
        in_specs=[HBM] * (kinds + 3),
        out_specs=[HBM] * (kinds + 3),
        scratch_shapes=[
            dma((kinds,)),
            dma((kinds, 2, 3)), dma((kinds, 2, 3)),
            dma((kinds, 4)), dma((kinds, 4)),
            dma((kinds, 4)), dma((kinds, 4)),
            dma((kinds, 4, 2)), dma((kinds, 4, 2)),
            dma((kinds, 4, 4)), dma((kinds, 4, 4)),
            dma((2,)), dma((2, 4)), dma((2, 4)), dma((3,)),
        ],
        compiler_params=pltpu.CompilerParams(collective_id=cid, has_side_effects=True),
        name="gather_all",
    )(*shards, tokens, cotangent, ints)


def scatter_core(grads, outs, scratch, begin, during):
    kinds = len(grads)
    (acc, precv, xr1, yr1, xr2, yr2, zup, zdn, fin) = scratch[:9]
    (ls, ps, pr, xs1, xm1, ys1, ym1, xs2, xm2, ys2, ym2, us, um, ds, dm, fs, fm, os) = scratch[9:]
    d, r, c = place()
    cols = 4
    chunks = kinds * cols
    xn, yn, pn = (d, r ^ 1, c), (d, r ^ 2, c), (1 - d, r, c)
    up, down = (d, r, c + 1), (d, r, c - 1)
    half = acc.shape[2] // 2
    first, last = pl.ds(0, half), pl.ds(half, half)

    def split(i):
        k = i // cols
        j = i - k * cols
        at = jnp.where(j == 0, 0, jnp.where(j == 1, 3, j - 1))
        return k, at

    def at_static(i):
        return i // cols, (0, 3, 1, 2)[i % cols]

    def load(i):
        k, at = at_static(i)
        return pltpu.make_async_copy(grads[k].at[at, :, d], acc.at[i], ls.at[i])

    def pair(i):
        k, at = at_static(i)
        return rcopy(grads[k].at[at, :, 1 - d], precv.at[i], ps.at[i], pr.at[i], pn)

    for i in range(chunks):
        pair(i).start()
        load(i).start()
    begin()

    def x1(i, j):
        return rcopy(acc.at[i, r ^ 1 ^ (2 * j), first], xr1.at[i, j], xs1.at[i, j], xm1.at[i, j], xn)

    def y1(i, j):
        return rcopy(acc.at[i, r ^ 2 ^ j, last], yr1.at[i, j], ys1.at[i, j], ym1.at[i, j], yn)

    def y2(i):
        return rcopy(acc.at[i, r ^ 2, first], yr2.at[i], ys2.at[i], ym2.at[i], yn)

    def x2(i):
        return rcopy(acc.at[i, r ^ 1, last], xr2.at[i], xs2.at[i], xm2.at[i], xn)

    def to_up(i):
        return rcopy(acc.at[i, r], zup.at[i], us.at[i], um.at[i], up)

    def to_down(i):
        return rcopy(acc.at[i, r], zdn.at[i], ds.at[i], dm.at[i], down)

    def stage1(i):
        pltpu.make_async_copy(precv.at[i], acc.at[i], ls.at[i]).wait()
        rcopy(acc.at[i], precv.at[i], ps.at[i], pr.at[i], pn).wait_recv()

        @pl.loop(0, 4)
        def _(row):
            acc[i, row] = acc[i, row] + precv[i, row]

        x1(i, 1).start()
        y1(i, 1).start()
        x1(i, 0).start()
        y1(i, 0).start()

    def stage2(i):
        x1(i, 1).wait_recv()
        acc[i, r ^ 2, first] = acc[i, r ^ 2, first] + xr1[i, 1]
        y2(i).start()
        y1(i, 1).wait_recv()
        acc[i, r ^ 1, last] = acc[i, r ^ 1, last] + yr1[i, 1]
        x2(i).start()
        x1(i, 0).wait_recv()
        acc[i, r, first] = acc[i, r, first] + xr1[i, 0]
        y1(i, 0).wait_recv()
        acc[i, r, last] = acc[i, r, last] + yr1[i, 0]

    def stage3(i):
        y2(i).wait_recv()
        acc[i, r, first] = acc[i, r, first] + yr2[i]
        x2(i).wait_recv()
        acc[i, r, last] = acc[i, r, last] + xr2[i]

    def stage4(i, hops):
        k, at = split(i)

        @pl.when((at > c) & (c == hops))
        def _():
            @pl.when(c > 0)
            def _():
                to_up(i).wait_recv()
                acc[i, r] = acc[i, r] + zup[i]

            to_up(i).start()

        @pl.when((at < c) & (cols - 1 - c == hops))
        def _():
            @pl.when(c < cols - 1)
            def _():
                to_down(i).wait_recv()
                acc[i, r] = acc[i, r] + zdn[i]

            to_down(i).start()

        @pl.when((at == c) & (jnp.maximum(c, cols - 1 - c) == hops))
        def _():
            @pl.when(c > 0)
            def _():
                to_up(i).wait_recv()
                acc[i, r] = acc[i, r] + zup[i]

            @pl.when(c < cols - 1)
            def _():
                to_down(i).wait_recv()
                acc[i, r] = acc[i, r] + zdn[i]

            fin[k, d] = acc[i, r]
            rcopy(fin.at[k, d], fin.at[k, d], fs.at[k], fm.at[k], pn).start()

    stages = [(0, stage1), (2, stage2), (4, stage3)]
    stages += [(5 + h, functools.partial(lambda h, i: stage4(i, h), h)) for h in range(cols)]
    ending = stages[-1][0]

    assert len(during) <= chunks + ending

    @pl.loop(0, chunks + ending)
    def _(step):
        for i, extra in enumerate(during):
            pl.when(step == i)(extra)

        for lag, stage in stages:

            @pl.when((step >= lag) & (step - lag < chunks))
            def _():
                stage(step - lag)

    @pl.loop(0, chunks)
    def _(i):
        k, at = split(i)
        rcopy(acc.at[i], precv.at[i], ps.at[i], pr.at[i], pn).wait_send()
        for j in range(2):
            x1(i, j).wait_send()
            y1(i, j).wait_send()
        y2(i).wait_send()
        x2(i).wait_send()

        @pl.when(at > c)
        def _():
            to_up(i).wait_send()

        @pl.when(at < c)
        def _():
            to_down(i).wait_send()

    for k in range(kinds):
        rcopy(fin.at[k, 1 - d], fin.at[k, 1 - d], fs.at[k], fm.at[k], pn).wait()
        pltpu.make_async_copy(fin.at[k], outs[k], os.at[k]).start()
    for k in range(kinds):
        pltpu.make_async_copy(fin.at[k], outs[k], os.at[k]).wait()

def scatter_scratch(kinds, n, w, dt):
    dma = pltpu.SemaphoreType.DMA
    chunks = kinds * 4
    return [
        pltpu.VMEM((chunks, 4, n, w), dt),
        pltpu.VMEM((chunks, 4, n, w), dt),
        pltpu.VMEM((chunks, 2, n // 2, w), dt),
        pltpu.VMEM((chunks, 2, n // 2, w), dt),
        pltpu.VMEM((chunks, n // 2, w), dt),
        pltpu.VMEM((chunks, n // 2, w), dt),
        pltpu.VMEM((chunks, n, w), dt),
        pltpu.VMEM((chunks, n, w), dt),
        pltpu.VMEM((kinds, 2, n, w), dt),
        dma((chunks,)), dma((chunks,)), dma((chunks,)),
        dma((chunks, 2)), dma((chunks, 2)), dma((chunks, 2)), dma((chunks, 2)),
        dma((chunks,)), dma((chunks,)), dma((chunks,)), dma((chunks,)),
        dma((chunks,)), dma((chunks,)), dma((chunks,)), dma((chunks,)),
        dma((kinds,)), dma((kinds,)), dma((kinds,)),
    ]


def give_moves(src_ref, out_ref, local, send, recv):
    d, r, c = place()
    own = src_ref.shape[2]
    home = r // 2

    def slot(i, core):
        return out_ref.at[i, :, pl.ds(pl.multiple_of(core * own, own), own)]

    def move(row):
        return rcopy(src_ref.at[row], slot(r % 2, d), send.at[row], recv.at[r % 2, d], (home, row, c))

    def stay():
        return pltpu.make_async_copy(src_ref.at[r], slot(r % 2, d), local)

    def start():
        for row in range(4):

            @pl.when(jnp.logical_not((row == r) & (home == d)))
            def _():
                move(row).start()

        @pl.when(home == d)
        def _():
            stay().start()

    def finish():
        for row in range(4):

            @pl.when(jnp.logical_not((row == r) & (home == d)))
            def _():
                move(row).wait_send()

        @pl.when(home == d)
        def _():
            stay().wait()

        for i in range(2):
            for core in range(2):

                @pl.when(jnp.logical_not((2 * d + i == r) & (core == d)))
                def _():
                    rcopy(src_ref.at[0], slot(i, core), send.at[0], recv.at[i, core], (d, r, c)).wait_recv()

    return start, finish


def plane_peers():
    d, r, c = place()
    return [(d ^ (j // 4), r ^ (j % 4), c) for j in range(1, 8)]


def line_peers():
    d, r, c = place()
    return [(d ^ (j // 4), r, c ^ (j % 4)) for j in range(1, 8)]


VM = pl.BlockSpec(memory_space=pltpu.VMEM)


def swap_kernel(count, *refs):
    srcs, outs = refs[:count], refs[count : 2 * count]
    send, recv = refs[2 * count :]
    d, r, c = place()
    greet([(d, r, c ^ j) for j in (1, 2, 3)])

    def move(k, j):
        return rcopy(srcs[k].at[c ^ j], outs[k].at[c], send.at[k, j], recv.at[k, j], (d, r, c ^ j))

    for j in (3, 2, 1):
        for k in range(count):
            move(k, j).start()
    for k in range(count):
        outs[k][c] = srcs[k][c]
    for j in (1, 2, 3):
        for k in range(count):
            move(k, j).wait()


def swap_fast(arrays, cid):
    count = len(arrays)
    dma = pltpu.SemaphoreType.DMA
    return pl.pallas_call(
        functools.partial(swap_kernel, count),
        out_shape=[jax.ShapeDtypeStruct(a.shape, a.dtype) for a in arrays],
        in_specs=[VM] * count,
        out_specs=[VM] * count,
        scratch_shapes=[dma((count, 4)), dma((count, 4))],
        compiler_params=pltpu.CompilerParams(collective_id=cid, has_side_effects=True),
        name="swap_cols",
    )(*arrays)


def heads_kernel(q_ref, kv_ref, q_out, kv_out, send, recv, psend, precv):
    d, r, c = place()
    pn = (1 - d, r, c)
    greet([(d, r, c ^ j) for j in (1, 2, 3)] + [pn])

    def kv(j):
        return rcopy(kv_ref.at[c ^ j], kv_out.at[c, d], send.at[0, j], recv.at[0, j], (d, r, c ^ j))

    def q(j):
        return rcopy(q_ref.at[c ^ j], q_out.at[c], send.at[1, j], recv.at[1, j], (d, r, c ^ j))

    def pair(j):
        src = kv_ref.at[c] if j == 0 else kv_out.at[c ^ j, d]
        return rcopy(src, kv_out.at[c ^ j, d], psend.at[j], precv.at[j], pn)

    for j in (3, 2, 1):
        kv(j).start()
    pair(0).start()
    for j in (3, 2, 1):
        q(j).start()
    kv_out[c, d] = kv_ref[c]
    q_out[c] = q_ref[c]
    for j in (1, 2, 3):
        kv(j).wait_recv()
        pair(j).start()
    for j in (1, 2, 3):
        q(j).wait()
        kv(j).wait_send()
    for j in range(4):
        pair(j).wait()


def heads_fast(q, kv, cid):
    cols, own, wide = kv.shape
    dma = pltpu.SemaphoreType.DMA
    return pl.pallas_call(
        heads_kernel,
        out_shape=[
            jax.ShapeDtypeStruct(q.shape, q.dtype),
            jax.ShapeDtypeStruct((cols, 2, own, wide), kv.dtype),
        ],
        in_specs=[VM] * 2,
        out_specs=[VM] * 2,
        scratch_shapes=[dma((2, 4)), dma((2, 4)), dma((4,)), dma((4,))],
        compiler_params=pltpu.CompilerParams(collective_id=cid, has_side_effects=True),
        name="to_heads",
    )(q, kv)


def turn_kernel(ctx_ref, stats_ref, give_ref, ctx_out, stats_out, give_out, send, recv, ssend, srecv, gl, gs, gr):
    d, r, c = place()
    peers = line_peers()
    greet(plane_peers() + peers[:3] + peers[4:])

    def move(j):
        return rcopy(ctx_ref.at[c ^ j], ctx_out.at[c], send.at[j], recv.at[j], (d, r, c ^ j))

    def tell(j):
        return rcopy(stats_ref, stats_out.at[d, c], ssend.at[j - 1], srecv.at[j - 1], peers[j - 1])

    for j in range(1, 8):
        tell(j).start()
    for j in (3, 2, 1):
        move(j).start()
    start, finish = give_moves(give_ref, give_out, gl, gs, gr)
    start()
    ctx_out[c] = ctx_ref[c]
    stats_out[d, c] = stats_ref[...]
    for j in range(1, 8):
        tell(j).wait()
    for j in (1, 2, 3):
        move(j).wait()
    finish()


def turn_fast(d_ctx, stats, out_t, cid):
    width, own = out_t.shape
    dma = pltpu.SemaphoreType.DMA
    return pl.pallas_call(
        turn_kernel,
        out_shape=[
            jax.ShapeDtypeStruct(d_ctx.shape, d_ctx.dtype),
            jax.ShapeDtypeStruct((2, 4) + stats.shape, stats.dtype),
            jax.ShapeDtypeStruct((2, width // 4, 2 * own), out_t.dtype),
        ],
        in_specs=[VM, VM, HBM],
        out_specs=[VM, VM, HBM],
        scratch_shapes=[dma((4,)), dma((4,)), dma((7,)), dma((7,)), dma, dma((4,)), dma((2, 2))],
        compiler_params=pltpu.CompilerParams(collective_id=cid, has_side_effects=True),
        name="turn",
    )(d_ctx, stats, out_t.reshape(4, width // 4, own))


def sum_steps(src, total, parts, sems):
    d, r, c = place()
    peers = [(1 - d, r, c), (d, r ^ 1, c), (d, r ^ 2, c), (d, r, c ^ 1), (d, r, c ^ 2)]
    bits = [d, r % 2, r // 2, c % 2, c // 2]
    rs, rr, gs, gr = sems
    count = len(peers)
    size = [src.shape[0] >> (i + 1) for i in range(count)]
    offset = [jnp.int32(0)]
    for i in range(count):
        offset.append(offset[i] + bits[i] * size[i])

    def rows(at, amount):
        return pl.ds(pl.multiple_of(at, 8), amount)

    def down(i):
        other = offset[i] + (1 - bits[i]) * size[i]
        held = src if i == 0 else parts[i - 1]
        at = other if i == 0 else other - offset[i]
        return rcopy(held.at[rows(at, size[i])], parts[count + i], rs.at[i], rr.at[i], peers[i])

    def fold(i):
        down(i).wait_recv()
        held = src if i == 0 else parts[i - 1]
        at = offset[i + 1] if i == 0 else offset[i + 1] - offset[i]
        parts[i][...] = held[rows(at, size[i])] + parts[count + i][...]

    def back(i):
        spot = total.at[rows(offset[i + 1], size[i])]
        return rcopy(spot, spot, gs.at[i], gr.at[i], peers[i])

    def back_recv(i):
        spot = total.at[rows(offset[i] + (1 - bits[i]) * size[i], size[i])]
        rcopy(spot, spot, gs.at[i], gr.at[i], peers[i]).wait_recv()

    steps = [lambda: down(0).start()]
    for i in range(1, count):

        def step(i=i):
            fold(i - 1)
            down(i).start()

        steps.append(step)

    def middle():
        fold(count - 1)
        total[rows(offset[count], size[-1])] = parts[count - 1][...]
        back(count - 1).start()

    steps.append(middle)
    for i in range(count - 2, -1, -1):

        def step(i=i):
            back_recv(i + 1)
            back(i).start()

        steps.append(step)

    def end():
        back_recv(0)
        for i in range(count):
            down(i).wait_send()
            back(i).wait_send()

    return steps, end


def tail_kernel(kinds, *refs):
    grads, refs = refs[:kinds], refs[kinds:]
    (q_ref, kv_ref, small_ref), refs = refs[:3], refs[3:]
    outs, refs = refs[:kinds], refs[kinds:]
    (q_out, kv_out, small_out), refs = refs[:3], refs[3:]
    (total, theirs), refs = refs[:2], refs[2:]
    parts, refs = refs[:10], refs[10:]
    (send, recv, psend, precv), sems, scratch = refs[:4], refs[4:8], refs[8:]
    d, r, c = place()
    pn = (1 - d, r, c)
    greet([(d, r, c ^ j) for j in (1, 2, 3)] + [pn, (d, r ^ 1, c), (d, r ^ 2, c)])

    def pair(j):
        return rcopy(kv_ref.at[c ^ j, 1 - d], theirs.at[c ^ j], psend.at[j], precv.at[j], pn)

    def kv(j):
        return rcopy(total.at[c ^ j], kv_out.at[c], send.at[0, j], recv.at[0, j], (d, r, c ^ j))

    def q(j):
        return rcopy(q_ref.at[c ^ j], q_out.at[c], send.at[1, j], recv.at[1, j], (d, r, c ^ j))

    for j in (3, 2, 1, 0):
        pair(j).start()
    for j in (3, 2, 1):
        q(j).start()
    q_out[c] = q_ref[c]
    steps, end = sum_steps(small_ref, small_out, parts, sems)

    def begin():
        for j in (3, 2, 1):
            pair(j).wait_recv()
            total[c ^ j] = kv_ref[c ^ j, d] + theirs[c ^ j]
            kv(j).start()
        pair(0).wait_recv()
        kv_out[c] = kv_ref[c, d] + theirs[c]

    scatter_core(grads, outs, scratch, begin, steps)
    end()
    for j in range(4):
        pair(j).wait_send()
    for j in (1, 2, 3):
        q(j).wait()
        kv(j).wait()


def tail_fast(grads, q, kv, small, cid):
    kinds = len(grads)
    n, w = grads[0].shape[3:]
    dma = pltpu.SemaphoreType.DMA
    cols, _, wide, own = kv.shape
    parts = [pltpu.VMEM((small.shape[0] >> (i + 1), small.shape[1]), f32) for i in range(5)]
    return pl.pallas_call(
        functools.partial(tail_kernel, kinds),
        out_shape=[jax.ShapeDtypeStruct((2, n, w), bf16)] * kinds
        + [
            jax.ShapeDtypeStruct(q.shape, q.dtype),
            jax.ShapeDtypeStruct((cols, wide, own), kv.dtype),
            jax.ShapeDtypeStruct(small.shape, f32),
        ],
        in_specs=[HBM] * kinds + [VM] * 3,
        out_specs=[HBM] * kinds + [VM] * 3,
        scratch_shapes=[pltpu.VMEM((cols, wide, own), kv.dtype)] * 2
        + parts * 2
        + [dma((2, 4)), dma((2, 4)), dma((4,)), dma((4,)), dma((5,)), dma((5,)), dma((5,)), dma((5,))]
        + scatter_scratch(kinds, n, w, bf16),
        compiler_params=pltpu.CompilerParams(
            collective_id=cid, has_side_effects=True, vmem_limit_bytes=48 * 1024 * 1024
        ),
        name="tail",
    )(*grads, q, kv, small)


def last_kernel(kinds, *refs):
    grads, refs = refs[:kinds], refs[kinds:]
    give_ref, refs = refs[0], refs[1:]
    outs, refs = refs[:kinds], refs[kinds:]
    give_out, gl, gs, gr = refs[:4]
    d, r, c = place()
    greet(plane_peers(), [(c < 3, (d, r, c + 1)), (c > 0, (d, r, c - 1))])
    start, finish = give_moves(give_ref, give_out, gl, gs, gr)
    scatter_core(grads, outs, refs[4:], start, [])
    finish()


def last_fast(grads, grad_t, cid):
    kinds = len(grads)
    n, w = grads[0].shape[3:]
    width, own = grad_t.shape
    dma = pltpu.SemaphoreType.DMA
    return pl.pallas_call(
        functools.partial(last_kernel, kinds),
        out_shape=[jax.ShapeDtypeStruct((2, n, w), bf16)] * kinds
        + [jax.ShapeDtypeStruct((2, width // 4, 2 * own), bf16)],
        in_specs=[HBM] * (kinds + 1),
        out_specs=[HBM] * (kinds + 1),
        scratch_shapes=[dma, dma((4,)), dma((2, 2))] + scatter_scratch(kinds, n, w, bf16),
        compiler_params=pltpu.CompilerParams(
            collective_id=cid, has_side_effects=True, vmem_limit_bytes=48 * 1024 * 1024
        ),
        name="last_sums",
    )(*grads, grad_t.reshape(4, width // 4, own))


def dot(a, b, contract=((1,), (0,))):
    return lax.dot_general(a, b, (contract, ((), ())), preferred_element_type=f32)


def block_rows(ref, heads, scale, out):
    own = ref.shape[-1]
    for h in range(heads):
        for g in range(heads):
            spot = (pl.ds(h * HD, HD), pl.ds(g * own, own))
            if h == g:
                out[spot] = ref[0, pl.ds(h * HD, HD)] * jnp.asarray(scale, out.dtype)
            else:
                out[spot] = jnp.zeros((HD, own), out.dtype)


def attn_fwd_kernel(heads, scale, bounds, q_ref, kv_ref, qseg_ref, kseg_ref, ctx_ref, lse_ref, kn, q3, s_scr, o_scr):
    step = pl.program_id(0)
    tiles, _, tile = kv_ref.shape
    wide = heads * HD
    own = q_ref.shape[-1]

    @pl.when(step == 0)
    def _():
        @pl.loop(0, tiles)
        def _(j):
            kn[j] = kv_ref[j, pl.ds(0, wide)].astype(f32).T.astype(bf16)

    block_rows(q_ref, heads, scale, q3)
    low, high = bounds[step, 0], bounds[step, 1]
    qseg = jnp.concatenate([qseg_ref[0]] * heads, axis=1)

    def one(j, top):
        s = dot(kn[j], q3[...])
        s = jnp.where(kseg_ref[j] == qseg, s, masked_value)
        s_scr[j] = s
        return jnp.maximum(top, jnp.max(s, axis=0, keepdims=True))

    top = lax.fori_loop(low, high, one, jnp.full((1, heads * own), masked_value, f32))
    o_scr[...] = jnp.zeros_like(o_scr)

    def two(j, total):
        p = jnp.exp(s_scr[j] - top)
        low_p = p.astype(bf16)
        for h in range(heads):
            rows = pl.ds(h * HD, HD)
            v = kv_ref[j, pl.ds(wide + h * HD, HD)]
            o_scr[rows] += dot(v, low_p[:, h * own : (h + 1) * own])
        return total + jnp.sum(p, axis=0, keepdims=True)

    total = lax.fori_loop(low, high, two, jnp.zeros((1, heads * own), f32))
    for h in range(heads):
        rows = pl.ds(h * HD, HD)
        ctx_ref[0, rows] = (o_scr[rows] / total[:, h * own : (h + 1) * own]).astype(bf16)
    lse_ref[0] = top + jnp.log(total)


def attn_fwd(bounds, q, kv, qseg, kseg, scale):
    blocks, wide, own = q.shape
    tiles, _, tile = kv.shape
    heads = wide // HD
    return pl.pallas_call(
        functools.partial(attn_fwd_kernel, heads, scale),
        out_shape=[
            jax.ShapeDtypeStruct(q.shape, bf16),
            jax.ShapeDtypeStruct((blocks, 1, heads * own), f32),
        ],
        grid_spec=pltpu.PrefetchScalarGridSpec(
            num_scalar_prefetch=1,
            grid=(blocks,),
            in_specs=[
                pl.BlockSpec((1, wide, own), lambda i, b: (i, 0, 0)),
                pl.BlockSpec(kv.shape, lambda i, b: (0, 0, 0)),
                pl.BlockSpec((1, 1, own), lambda i, b: (i, 0, 0)),
                pl.BlockSpec(kseg.shape, lambda i, b: (0, 0, 0)),
            ],
            out_specs=[
                pl.BlockSpec((1, wide, own), lambda i, b: (i, 0, 0)),
                pl.BlockSpec((1, 1, heads * own), lambda i, b: (i, 0, 0)),
            ],
            scratch_shapes=[
                pltpu.VMEM((tiles, tile, wide), bf16),
                pltpu.VMEM((wide, heads * own), bf16),
                pltpu.VMEM((tiles, tile, heads * own), f32),
                pltpu.VMEM((wide, own), f32),
            ],
        ),
        compiler_params=pltpu.CompilerParams(
            dimension_semantics=("arbitrary",), vmem_limit_bytes=48 * 1024 * 1024
        ),
        name="attn_fwd",
    )(bounds, q, kv, qseg, kseg)


def attn_bwd_kernel(
    heads, scale, bounds, q_ref, kv_ref, qseg_ref, kseg_ref, lse_ref, ctx_ref, dctx_ref,
    dq_ref, dkv_ref, kn, vn, q3, dc3, dq_scr, dkv_scr,
):
    step = pl.program_id(0)
    tiles, _, tile = kv_ref.shape
    wide = heads * HD
    own = q_ref.shape[-1]

    @pl.when(step == 0)
    def _():
        @pl.loop(0, tiles)
        def _(j):
            kn[j] = kv_ref[j, pl.ds(0, wide)].astype(f32).T.astype(bf16)
            vn[j] = kv_ref[j, pl.ds(wide, wide)].astype(f32).T.astype(bf16)
            dkv_scr[j] = jnp.zeros((2 * wide, tile), f32)

    block_rows(q_ref, heads, scale, q3)
    block_rows(dctx_ref, heads, 1.0, dc3)
    low, high = bounds[step, 0], bounds[step, 1]
    qseg = jnp.concatenate([qseg_ref[0]] * heads, axis=1)
    lse = lse_ref[0]
    product = ctx_ref[0].astype(f32) * dctx_ref[0].astype(f32)
    delta = jnp.concatenate(
        [jnp.sum(product[h * HD : (h + 1) * HD], axis=0, keepdims=True) for h in range(heads)], axis=1
    )
    dq_scr[...] = jnp.zeros_like(dq_scr)

    @pl.loop(low, high)
    def _(j):
        s = dot(kn[j], q3[...])
        s = jnp.where(kseg_ref[j] == qseg, s, masked_value)
        p = jnp.exp(s - lse)
        d_p = dot(vn[j], dc3[...])
        d_s = (p * (d_p - delta)).astype(bf16)
        p = p.astype(bf16)
        for h in range(heads):
            rows, lanes = pl.ds(h * HD, HD), slice(h * own, (h + 1) * own)
            dq_scr[rows] += dot(kv_ref[j, rows], d_s[:, lanes])
            dkv_scr[j, rows] += dot(q3[rows, lanes], d_s[:, lanes], ((1,), (1,)))
            deep = pl.ds(wide + h * HD, HD)
            dkv_scr[j, deep] += dot(dctx_ref[0, rows], p[:, lanes], ((1,), (1,)))

    dq_ref[0] = (dq_scr[...] * scale).astype(bf16)

    @pl.when(step == pl.num_programs(0) - 1)
    def _():
        @pl.loop(0, tiles)
        def _(j):
            dkv_ref[j] = dkv_scr[j].astype(bf16)


def attn_bwd(bounds, q, kv, qseg, kseg, lse, ctx, dctx, scale):
    blocks, wide, own = q.shape
    tiles, _, tile = kv.shape
    heads = wide // HD
    rowed = pl.BlockSpec((1, wide, own), lambda i, b: (i, 0, 0))
    return pl.pallas_call(
        functools.partial(attn_bwd_kernel, heads, scale),
        out_shape=[jax.ShapeDtypeStruct(q.shape, bf16), jax.ShapeDtypeStruct(kv.shape, bf16)],
        grid_spec=pltpu.PrefetchScalarGridSpec(
            num_scalar_prefetch=1,
            grid=(blocks,),
            in_specs=[
                rowed,
                pl.BlockSpec(kv.shape, lambda i, b: (0, 0, 0)),
                pl.BlockSpec((1, 1, own), lambda i, b: (i, 0, 0)),
                pl.BlockSpec(kseg.shape, lambda i, b: (0, 0, 0)),
                pl.BlockSpec((1, 1, heads * own), lambda i, b: (i, 0, 0)),
                rowed,
                rowed,
            ],
            out_specs=[rowed, pl.BlockSpec(kv.shape, lambda i, b: (0, 0, 0))],
            scratch_shapes=[
                pltpu.VMEM((tiles, tile, wide), bf16),
                pltpu.VMEM((tiles, tile, wide), bf16),
                pltpu.VMEM((wide, heads * own), bf16),
                pltpu.VMEM((wide, heads * own), bf16),
                pltpu.VMEM((wide, own), f32),
                pltpu.VMEM((tiles, 2 * wide, tile), f32),
            ],
        ),
        compiler_params=pltpu.CompilerParams(
            dimension_semantics=("arbitrary",), vmem_limit_bytes=48 * 1024 * 1024
        ),
        name="attn_bwd",
    )(bounds, q, kv, qseg, kseg, lse, ctx, dctx)


def fast_local(
    tokens,
    segments,
    labels,
    cotangent,
    w_qkv,
    b_qkv,
    w_out,
    b_out,
    ln1_gain,
    ln1_bias,
    w_in,
    b_in,
    w_back,
    b_back,
    ln2_gain,
    ln2_bias,
    s_proj,
    s_bias,
    s_query,
    s_mid,
    s_mid_bias,
    s_cls,
    s_cls_bias,
):
    _, width_row, cols_local = tokens.shape
    parts, rows, cols, seqs, _ = sizes(tokens.shape[0])
    width = width_row * rows
    own = cols_local // parts
    width_col = b_qkv.shape[1]
    heads_dev = width_col // HD
    hidden_col = b_in.shape[0]
    docs_count = labels.shape[1]
    class_count = s_cls.shape[1]
    student_width = s_proj.shape[1]
    seq_len = segments.shape[1]
    row_index = lax.axis_index("row")
    col_index = lax.axis_index("col")
    dp_index = lax.axis_index("dp")
    score_scale = HD ** (-0.5)
    pool_scale = SHD ** (-0.5)
    query_heads = s_query.reshape(SH, SHD)
    doc_ids = jnp.arange(docs_count, dtype=jnp.int32)
    class_ids = jnp.arange(class_count, dtype=jnp.int32)

    w_three = w_qkv.reshape(width_row, heads_dev, 3, HD).transpose(0, 2, 1, 3)
    w_three = jnp.concatenate([w_three[:, 1], w_three[:, 2], w_three[:, 0]], axis=1)
    shard_attn = own_half(jnp.concatenate([w_three.reshape(width_row, -1), w_out], axis=1))
    proj_rows = width_row // cols
    vectors = [b_out, ln1_gain, ln1_bias, b_back, ln2_gain, ln2_bias, b_qkv.reshape(-1), b_in]
    vectors.append(lax.dynamic_slice_in_dim(s_proj, col_index * proj_rows, proj_rows).astype(f32).reshape(-1))
    flat = jnp.concatenate(vectors)
    flat = jnp.pad(flat, (0, 96 * 128 - flat.shape[0])).reshape(96, 128)
    w_attn, vec, w_in_all, w_back_all, x_parts, c_parts, ints = gather_fast(
        [shard_attn, own_half(flat), own_half(w_in), own_half(w_back)],
        tokens,
        cotangent,
        jnp.concatenate([segments, labels], axis=1),
        1,
    )
    w_attn = w_attn.reshape(cols, rows, width_row, 4 * width_col)
    w_qkv_all = w_attn[..., : 3 * width_col].reshape(cols, width, 3 * width_col)
    w_out_all = w_attn[..., 3 * width_col :].transpose(0, 2, 1, 3).reshape(width, width)
    w_in_all = w_in_all.reshape(cols, width, hidden_col)
    w_back_all = w_back_all.reshape(cols, width, hidden_col)
    vec = vec.reshape(cols, rows, -1)
    at = 6 * width_row
    row_vectors = vec[0, :, :at].reshape(rows, 6, width_row).transpose(1, 0, 2).reshape(6, width)
    b_out_a, gain_one, bias_one, b_back_a, gain_two, bias_two = [row_vectors[i] for i in range(6)]
    b_qkv_all = vec[:, 0, at : at + 2 * width_col].reshape(cols, 2, width_col)
    at += 2 * width_col
    b_in_all = vec[:, 0, at : at + hidden_col]
    at += hidden_col
    s_proj_all = vec[:, :, at : at + proj_rows * student_width].astype(bf16)
    s_proj_all = s_proj_all.reshape(cols, rows, proj_rows, student_width).transpose(1, 0, 2, 3)
    s_proj_all = s_proj_all.reshape(width, student_width)
    x_t = x_parts.reshape(width, own)
    ints = lax.dynamic_index_in_dim(ints.reshape(seqs, -1), row_index, 0, False)
    seg_all, label_seq = ints[:seq_len], ints[seq_len:]
    seg_blocks = seg_all.reshape(cols, parts, own)
    seg_q = lax.dynamic_index_in_dim(seg_blocks, dp_index, 1, False)
    seg_own = lax.dynamic_index_in_dim(seg_q, col_index, 0, False)
    lows = jnp.sum(seg_all[None, :] < seg_q[:, :1], axis=1) // own
    highs = (jnp.sum(seg_all[None, :] <= seg_q[:, -1:], axis=1) + own - 1) // own
    bounds = jnp.stack([lows, highs], axis=1).astype(jnp.int32)

    offsets = jnp.concatenate([jnp.zeros_like(b_qkv_all[:, 0]), b_qkv_all[:, 1], b_qkv_all[:, 0]], axis=1)
    qkv = jnp.einsum("cdn,dt->cnt", w_qkv_all, x_t, preferred_element_type=f32) + offsets[:, :, None]
    qkv = qkv.astype(bf16)
    queries, kv = heads_fast(qkv[:, 2 * width_col :], qkv[:, : 2 * width_col], 2)
    kv = kv.reshape(cols * parts, 2 * width_col, own)
    q_rows, k_rows = seg_q[:, None, :], seg_all.reshape(cols * parts, own, 1)
    context, lse = attn_fwd(bounds, queries, kv, q_rows, k_rows, score_scale)
    (ctx_t,) = swap_fast([context], 3)
    ctx_t = ctx_t.reshape(width, own)

    x = x_t.T
    attn_out = mm(ctx_t, w_out_all, ((0,), (0,))) + b_out_a
    normed_one, inv_one = normalize(x.astype(f32) + attn_out)
    hidden_one = normed_one * gain_one + bias_one
    hidden_low = hidden_one.astype(bf16)
    pre_act = jnp.einsum("td,cdn->ctn", hidden_low, w_in_all, preferred_element_type=f32)
    pre_act = pre_act + b_in_all[:, None, :]
    act = gelu_exact(pre_act).astype(bf16)
    ffn_out = jnp.einsum("ctn,cdn->td", act, w_back_all, preferred_element_type=f32) + b_back_a
    normed_two, inv_two = normalize(hidden_one + ffn_out)
    layer_out = (normed_two * gain_two + bias_two).astype(bf16)

    student_h = mm(layer_out, s_proj_all, ((1,), (0,))) + s_bias
    head_parts = student_h.reshape(own, SH, SHD)
    pool_logit = jnp.sum(head_parts * query_heads, axis=-1) * pool_scale
    member = (seg_own[:, None] == doc_ids[None, :])[:, :, None]
    masked = jnp.where(member, pool_logit[:, None, :], masked_value)
    local_top = jnp.max(masked, axis=0)
    local_exp = jnp.where(member, jnp.exp(masked - local_top[None]), 0.0)
    local_total = jnp.sum(local_exp, axis=0)
    local_sum = jnp.einsum("tdh,thk->dhk", local_exp, head_parts, precision=highest)
    stats = jnp.concatenate([local_top[..., None], local_total[..., None], local_sum], axis=-1)
    stats = jnp.pad(stats.reshape(-1), (0, 8 * 128 - stats.size)).reshape(8, 128)

    d_out = c_parts.reshape(width, own).T.astype(f32)
    g_ln2_gain = jnp.sum(d_out * normed_two, axis=0)
    g_ln2_bias = jnp.sum(d_out, axis=0)
    d_resid_two = normalize_back(d_out * gain_two, normed_two, inv_two)
    d_ffn = d_resid_two.astype(bf16)
    g_back_bias = jnp.sum(d_ffn.astype(f32), axis=0)
    g_back = jnp.einsum("td,ctn->cdn", d_ffn, act, preferred_element_type=f32)
    d_act = jnp.einsum("td,cdn->ctn", d_ffn, w_back_all, preferred_element_type=f32)
    _, gelu_fn = jax.vjp(gelu_exact, pre_act)
    d_pre = gelu_fn(d_act)[0].astype(bf16)
    g_in_bias = jnp.sum(d_pre.astype(f32), axis=1)
    g_in = jnp.einsum("td,ctn->cdn", hidden_low, d_pre, preferred_element_type=f32)
    d_hidden_one = d_resid_two + jnp.einsum(
        "ctn,cdn->td", d_pre, w_in_all, preferred_element_type=f32
    )
    g_ln1_gain = jnp.sum(d_hidden_one * normed_one, axis=0)
    g_ln1_bias = jnp.sum(d_hidden_one, axis=0)
    d_resid_one = normalize_back(d_hidden_one * gain_one, normed_one, inv_one)
    d_attn = d_resid_one.astype(bf16)
    g_out_bias = jnp.sum(d_attn.astype(f32), axis=0)
    d_ctx = mm(w_out_all, d_attn, ((1,), (1,))).astype(bf16)
    d_ctx, stats, out = turn_fast(d_ctx.reshape(cols, width_col, own), stats, layer_out.T, 4)

    stats = stats.reshape(cols * parts, -1)[:, : docs_count * SH * (SHD + 2)]
    stats = stats.reshape(cols * parts, docs_count, SH, SHD + 2)
    tops, totals, sums = stats[..., 0], stats[..., 1], stats[..., 2:]
    doc_top = jnp.max(tops, axis=0)
    factors = jnp.exp(tops - doc_top[None])
    doc_total = jnp.sum(totals * factors, axis=0)
    pooled_heads = jnp.sum(sums * factors[..., None], axis=0) / doc_total[:, :, None]
    pooled = pooled_heads.reshape(docs_count, student_width)
    middle = jnp.tanh(jnp.dot(pooled, s_mid, precision=highest) + s_mid_bias)
    logit_rows = jnp.dot(middle, s_cls, precision=highest) + s_cls_bias
    logit_top = jnp.max(logit_rows, axis=-1, keepdims=True)
    logit_exp = jnp.exp(logit_rows - logit_top)
    one_hot = (label_seq[:, None] == class_ids[None, :]).astype(f32)
    d_logits = logit_exp / jnp.sum(logit_exp, axis=-1, keepdims=True) - one_hot
    g_cls = jnp.dot(middle.T, d_logits, precision=highest)
    g_cls_bias = jnp.sum(d_logits, axis=0)
    d_middle = jnp.dot(d_logits, s_cls.T, precision=highest) * (1.0 - middle * middle)
    g_mid = jnp.dot(pooled.T, d_middle, precision=highest)
    g_mid_bias = jnp.sum(d_middle, axis=0)
    d_pooled = jnp.dot(d_middle, s_mid.T, precision=highest).reshape(docs_count, SH, SHD)
    shares = jnp.where(member, jnp.exp(masked - doc_top[None]), 0.0) / doc_total[None]
    d_share = jnp.einsum("dhk,thk->tdh", d_pooled, head_parts, precision=highest)
    base_term = jnp.sum(d_pooled * pooled_heads, axis=-1)
    d_pool_logit = jnp.sum(shares * (d_share - base_term[None]), axis=1)
    d_heads = jnp.einsum("tdh,dhk->thk", shares, d_pooled, precision=highest)
    d_heads = d_heads + d_pool_logit[:, :, None] * query_heads[None] * pool_scale
    g_query = (jnp.sum(d_pool_logit[:, :, None] * head_parts, axis=0) * pool_scale).reshape(-1)
    d_student = d_heads.reshape(own, student_width)
    g_sbias = jnp.sum(d_student, axis=0)
    g_sproj = jnp.dot(layer_out.astype(f32).T, d_student, precision=highest)

    d_q, d_kv = attn_bwd(bounds, queries, kv, q_rows, k_rows, lse, context, d_ctx, score_scale)
    at_seq = (jnp.arange(seqs) == row_index).astype(f32)[:, None]
    at_heads = (jnp.arange(cols) == col_index).astype(f32)[:, None, None]
    g_q_bias = jnp.sum(d_q.astype(f32), axis=(0, 2))
    g_v_bias = jnp.sum(d_kv[:, width_col:].astype(f32), axis=(0, 2))
    once = 1.0 / (parts * cols)
    small = (
        g_sproj,
        jnp.stack([g_q_bias, g_v_bias])[None] * at_heads,
        g_in_bias,
        g_out_bias,
        g_ln1_gain,
        g_ln1_bias,
        g_back_bias,
        g_ln2_gain,
        g_ln2_bias,
        g_sbias,
        g_query,
        g_mid * once,
        g_mid_bias * once,
        g_cls * once,
        logit_rows.reshape(1, -1) * (at_seq * once),
        g_cls_bias * once,
    )
    flat = jnp.concatenate([part.reshape(-1) for part in small])
    tall = -(-flat.shape[0] // (128 * 256)) * 256
    flat = jnp.pad(flat, (0, tall * 128 - flat.shape[0])).reshape(tall, 128)
    blocked = (cols, rows, parts, width_row // parts, -1)
    g_in, g_back, d_q, d_kv, flat = tail_fast(
        [g_in.astype(bf16).reshape(blocked), g_back.astype(bf16).reshape(blocked)],
        d_q,
        d_kv.reshape(cols, parts, 2 * width_col, own),
        flat,
        5,
    )
    flat = flat.reshape(-1)
    sums_all, at = [], 0
    for part in small:
        sums_all.append(flat[at : at + part.size].reshape(part.shape))
        at += part.size
    d_qkv = jnp.concatenate([d_kv, d_q], axis=1)
    g_qkv = jnp.einsum("dt,cnt->cdn", x_t, d_qkv, preferred_element_type=f32)
    d_tokens = jnp.einsum("cdn,cnt->dt", w_qkv_all, d_qkv, preferred_element_type=f32)
    d_tokens = (d_tokens + d_resid_one.T).astype(bf16)
    g_out = mm(ctx_t, d_attn, ((1,), (0,)))
    g_out = g_out.reshape(cols, width_col, rows, width_row).transpose(0, 2, 1, 3)
    g_attn = jnp.concatenate(
        [g_qkv.astype(bf16).reshape(cols, rows, width_row, 3 * width_col), g_out.astype(bf16)], axis=-1
    )
    g_attn, grad_tokens = last_fast([g_attn.reshape(blocked)], d_tokens, 6)
    g_in, g_back, g_attn = [part.reshape(width_row, -1).astype(f32) for part in (g_in, g_back, g_attn)]
    g_qkv = g_attn[:, : 3 * width_col].reshape(width_row, 3, heads_dev, HD)
    g_qkv = jnp.stack([g_qkv[:, 2], g_qkv[:, 0], g_qkv[:, 1]], axis=2).reshape(width_row, -1)

    def at_col(part):
        return lax.dynamic_index_in_dim(part, col_index, 0, False)

    def at_row(part):
        return lax.dynamic_slice_in_dim(part, row_index * width_row, width_row)

    (
        g_sproj, g_qkv_bias, g_in_bias, g_out_bias, g_ln1_gain, g_ln1_bias, g_back_bias, g_ln2_gain,
        g_ln2_bias, g_sbias, g_query, g_mid, g_mid_bias, g_cls, logits, g_cls_bias,
    ) = sums_all
    logits = lax.dynamic_slice_in_dim(logits, dp_index * (seqs // parts), seqs // parts)
    return (
        out,
        logits.reshape(seqs // parts, docs_count, class_count),
        grad_tokens.astype(f32),
        g_qkv,
        at_col(g_qkv_bias),
        g_attn[:, 3 * width_col :],
        at_row(g_out_bias),
        at_row(g_ln1_gain),
        at_row(g_ln1_bias),
        g_in,
        at_col(g_in_bias),
        g_back,
        at_row(g_back_bias),
        at_row(g_ln2_gain),
        at_row(g_ln2_bias),
        at_row(g_sproj),
        g_sbias,
        g_query,
        g_mid,
        g_mid_bias,
        g_cls,
        g_cls_bias,
    )


def solution(mesh):
    row, col = P("row"), P("col")
    grid, whole = P("row", "col"), P("dp", "row", "col")
    placed = (
        (whole, P("dp", None), P("dp", None), whole, grid, P(None, "col"), P("col", "row"))
        + (row, row, row, grid, col, grid, row, row, row, P("row", None))
        + (P(),) * 6
    )
    results = (
        (whole, P("dp", None, None), whole, grid, P(None, "col"), P("col", "row"))
        + (row, row, row, grid, col, grid, row, row, row, P("row", None))
        + (P(),) * 6
    )
    quick = dict(mesh.shape) == {"dp": 2, "row": 4, "col": 4}
    local = fast_local if quick else general_local
    return jax.shard_map(local, mesh=mesh, in_specs=placed, out_specs=results, check_vma=False)
```

```python
import functools
import jax
import jax.numpy as jnp
from jax import lax
from jax.experimental import pallas as pl
from jax.experimental.pallas import tpu as pltpu
from jax.sharding import PartitionSpec as P

HD = 64
SH = 2
SHD = 64

norm_eps = 1e-06
masked_value = -1e30
highest = lax.Precision.HIGHEST
f32 = jnp.float32
bf16 = jnp.bfloat16
WORLD = ("col", "row", "dp")


def sizes(seqs_local):
    parts = lax.axis_size("dp")
    rows = lax.axis_size("row")
    seqs = seqs_local * parts
    return parts, rows, lax.axis_size("col"), seqs, rows // seqs


def row_groups(rows, sub):
    return [list(range(at, at + sub)) for at in range(0, rows, sub)]


def take_in(values):
    parts, rows, _, seqs, sub = sizes(values.shape[0])
    held = lax.all_to_all(values, "dp", 2, 0, tiled=True)
    feats, half = held.shape[1:]
    held = held.reshape(seqs, feats, sub, half // sub).transpose(0, 2, 1, 3)
    held = held.reshape(rows, feats, half // sub)
    held = lax.all_to_all(held, "row", 0, 0, tiled=True)
    return held.reshape(rows * feats, half // sub)


def give_back(values, seqs_local):
    parts, rows, _, seqs, sub = sizes(seqs_local)
    width, own = values.shape
    feats = width // rows
    held = lax.all_to_all(values.reshape(rows, feats, own), "row", 0, 0, tiled=True)
    held = held.reshape(seqs, sub, feats, own).transpose(0, 2, 1, 3).reshape(seqs, feats, sub * own)
    return lax.all_to_all(held, "dp", 0, 2, tiled=True)


def gather_world(shard):
    cols, rows = lax.axis_size("col"), lax.axis_size("row")
    out = lax.all_gather(shard, WORLD, axis=0, tiled=True)
    return out.reshape(cols, rows, -1, shard.shape[1])


def own_half(block):
    parts = lax.axis_size("dp")
    amount = block.shape[0] // parts
    return lax.dynamic_slice_in_dim(block, lax.axis_index("dp") * amount, amount)


def scatter_world(full):
    flat = full.reshape(-1, full.shape[-1])
    mine = lax.psum_scatter(flat, WORLD, scatter_dimension=0, tiled=True)
    return lax.all_gather(mine, "dp", axis=0, tiled=True)


def swap_cols(values):
    return lax.all_to_all(values, "col", 0, 0, tiled=True)


def gather_sequence(values, sub):
    cols, own, width = values.shape
    held = values[:, None]
    if sub > 1:
        groups = row_groups(lax.axis_size("row"), sub)
        held = lax.all_gather(held, "row", axis=1, tiled=True, axis_index_groups=groups)
    held = lax.all_gather(held[:, None], "dp", axis=1, tiled=True)
    return held.reshape(-1, width)


def scatter_sequence(values, cols, sub):
    parts = lax.axis_size("dp")
    width = values.shape[-1]
    held = values.reshape(cols, parts, sub, -1, width)
    held = lax.psum_scatter(held, "dp", scatter_dimension=1, tiled=True)[:, 0]
    if sub > 1:
        groups = row_groups(lax.axis_size("row"), sub)
        held = lax.psum_scatter(
            held, "row", scatter_dimension=1, tiled=True, axis_index_groups=groups
        )
    return held[:, 0]


def normalize(values):
    mean_v = jnp.mean(values, axis=-1, keepdims=True)
    center = values - mean_v
    inv_std = lax.rsqrt(jnp.mean(center * center, axis=-1, keepdims=True) + norm_eps)
    return center * inv_std, inv_std


def normalize_back(grad_hat, normed, inv_std):
    return inv_std * (
        grad_hat
        - jnp.mean(grad_hat, axis=-1, keepdims=True)
        - normed * jnp.mean(grad_hat * normed, axis=-1, keepdims=True)
    )


def gelu_exact(values):
    return jax.nn.gelu(values, approximate=False)


def mm(a, b, contract):
    return lax.dot_general(a, b, (contract, ((), ())), preferred_element_type=f32)


def combine_pool(part_one, part_two):
    top_a, total_a, sum_a = part_one
    top_b, total_b, sum_b = part_two
    row_top = jnp.maximum(top_a, top_b)
    factor_a = jnp.exp(top_a - row_top)
    factor_b = jnp.exp(top_b - row_top)
    return (
        row_top,
        total_a * factor_a + total_b * factor_b,
        sum_a * factor_a[:, :, None] + sum_b * factor_b[:, :, None],
    )


def attend(q, k, v, q_seg, k_seg, scale):
    scores = jnp.einsum("qhd,khd->hqk", q, k, preferred_element_type=f32) * scale
    scores = jnp.where((q_seg[:, None] == k_seg[None, :])[None], scores, masked_value)
    top = jnp.max(scores, axis=-1, keepdims=True)
    exp_scores = jnp.exp(scores - top)
    total = jnp.sum(exp_scores, axis=-1, keepdims=True)
    probs = exp_scores / total
    context = jnp.einsum("hqk,khd->qhd", probs.astype(bf16), v, preferred_element_type=f32)
    return context.astype(bf16), probs


def attend_back(q, k, v, probs, d_ctx, scale):
    d_probs = jnp.einsum("qhd,khd->hqk", d_ctx, v, preferred_element_type=f32)
    delta = jnp.sum(probs * d_probs, axis=-1, keepdims=True)
    d_scores = (probs * (d_probs - delta)).astype(bf16)
    d_q = jnp.einsum("hqk,khd->qhd", d_scores, k, preferred_element_type=f32) * scale
    d_k = jnp.einsum("hqk,qhd->khd", d_scores, q, preferred_element_type=f32) * scale
    d_v = jnp.einsum("hqk,qhd->khd", probs.astype(bf16), d_ctx, preferred_element_type=f32)
    return d_q, d_k, d_v


def general_local(
    tokens,
    segments,
    labels,
    cotangent,
    w_qkv,
    b_qkv,
    w_out,
    b_out,
    ln1_gain,
    ln1_bias,
    w_in,
    b_in,
    w_back,
    b_back,
    ln2_gain,
    ln2_bias,
    s_proj,
    s_bias,
    s_query,
    s_mid,
    s_mid_bias,
    s_cls,
    s_cls_bias,
):
    seqs_local, width_row, cols_local = tokens.shape
    parts, rows, cols, seqs, sub = sizes(seqs_local)
    width = width_row * rows
    own = cols_local // (parts * sub)
    width_col = b_qkv.shape[1]
    heads_dev = width_col // HD
    hidden_col = b_in.shape[0]
    docs_count = labels.shape[1]
    class_count = s_cls.shape[1]
    student_width = s_proj.shape[1]
    row_index = lax.axis_index("row")
    col_index = lax.axis_index("col")
    dp_index = lax.axis_index("dp")
    seq_index = row_index // sub
    sub_index = row_index % sub
    score_scale = HD ** (-0.5)
    pool_scale = SHD ** (-0.5)
    query_heads = s_query.reshape(SH, SHD)
    doc_ids = jnp.arange(docs_count, dtype=jnp.int32)
    class_ids = jnp.arange(class_count, dtype=jnp.int32)

    w_qkv_all = gather_world(own_half(w_qkv)).reshape(cols, width, 3 * width_col)
    x_t = take_in(tokens)
    rest = jnp.concatenate([own_half(w_in), own_half(w_back), own_half(w_out).reshape(-1, width_col)], axis=1)
    rest_all = gather_world(rest)
    w_in_all = rest_all[..., :hidden_col].reshape(cols, width, hidden_col)
    w_back_all = rest_all[..., hidden_col : 2 * hidden_col].reshape(cols, width, hidden_col)
    w_out_all = rest_all[..., 2 * hidden_col :].reshape(cols, rows, width_col, width_row)
    w_out_all = w_out_all.transpose(0, 2, 1, 3).reshape(width, width)
    row_vectors = lax.all_gather(
        jnp.stack([b_out, ln1_gain, ln1_bias, b_back, ln2_gain, ln2_bias]), "row", axis=1, tiled=True
    )
    b_out_a, gain_one, bias_one, b_back_a, gain_two, bias_two = [row_vectors[i] for i in range(6)]
    b_qkv_all = lax.all_gather(b_qkv, "col")
    b_in_all = lax.all_gather(b_in, "col")
    s_proj_all = lax.all_gather(s_proj, "row", axis=0, tiled=True)
    whole_ints = lax.all_gather(jnp.concatenate([segments, labels], axis=1), "dp", axis=0, tiled=True)
    ints = lax.dynamic_index_in_dim(whole_ints, seq_index, 0, False)
    seq_len = segments.shape[1]
    seg_all, label_seq = ints[:seq_len], ints[seq_len:]
    seg_blocks = seg_all.reshape(cols, parts, sub, own)
    seg_q = lax.dynamic_index_in_dim(seg_blocks, dp_index, 1, False)
    seg_q = lax.dynamic_index_in_dim(seg_q, sub_index, 1, False)
    seg_own = lax.dynamic_index_in_dim(seg_q, col_index, 0, False)
    seg_q = seg_q.reshape(-1)

    x = x_t.T
    offsets = jnp.stack([b_qkv_all[:, 0], jnp.zeros_like(b_qkv_all[:, 0]), b_qkv_all[:, 1]], axis=1)
    offsets = offsets.reshape(cols, 3, heads_dev, HD).transpose(0, 2, 1, 3).reshape(cols, 1, -1)
    qkv = jnp.einsum("td,cdn->ctn", x, w_qkv_all, preferred_element_type=f32) + offsets
    qkv = swap_cols(qkv.astype(bf16)).reshape(cols, own, heads_dev, 3, HD)
    queries = qkv[:, :, :, 0].reshape(cols * own, heads_dev, HD)
    kv = gather_sequence(qkv[:, :, :, 1:].reshape(cols, own, -1), sub)
    kv = kv.reshape(seq_len, heads_dev, 2, HD)
    key_rows, value_rows = kv[:, :, 0], kv[:, :, 1]
    context, probs = attend(queries, key_rows, value_rows, seg_q, seg_all, score_scale)
    ctx = swap_cols(context.reshape(cols, own, width_col))
    ctx = ctx.transpose(1, 0, 2).reshape(own, width)

    attn_out = mm(ctx, w_out_all, ((1,), (0,))) + b_out_a
    normed_one, inv_one = normalize(x.astype(f32) + attn_out)
    hidden_one = normed_one * gain_one + bias_one
    hidden_low = hidden_one.astype(bf16)
    pre_act = jnp.einsum("td,cdn->ctn", hidden_low, w_in_all, preferred_element_type=f32)
    pre_act = pre_act + b_in_all[:, None, :]
    act = gelu_exact(pre_act).astype(bf16)
    ffn_out = jnp.einsum("ctn,cdn->td", act, w_back_all, preferred_element_type=f32) + b_back_a
    normed_two, inv_two = normalize(hidden_one + ffn_out)
    layer_out = (normed_two * gain_two + bias_two).astype(bf16)
    out = give_back(layer_out.T, seqs_local)

    student_h = mm(layer_out, s_proj_all, ((1,), (0,))) + s_bias
    head_parts = student_h.reshape(own, SH, SHD)
    pool_logit = jnp.sum(head_parts * query_heads, axis=-1) * pool_scale
    member = (seg_own[:, None] == doc_ids[None, :])[:, :, None]
    masked = jnp.where(member, pool_logit[:, None, :], masked_value)
    local_top = jnp.max(masked, axis=0)
    local_exp = jnp.where(member, jnp.exp(masked - local_top[None]), 0.0)
    local_total = jnp.sum(local_exp, axis=0)
    local_sum = jnp.einsum("tdh,thk->dhk", local_exp, head_parts, precision=highest)
    stats = jnp.concatenate([local_top[..., None], local_total[..., None], local_sum], axis=-1)
    stats = lax.all_gather(stats, ("dp", "col"))
    if sub > 1:
        stats = lax.all_gather(stats, "row", axis=0, tiled=True, axis_index_groups=row_groups(rows, sub))
    tops, totals, sums = stats[..., 0], stats[..., 1], stats[..., 2:]
    doc_top = jnp.max(tops, axis=0)
    factors = jnp.exp(tops - doc_top[None])
    doc_total = jnp.sum(totals * factors, axis=0)
    pooled_heads = jnp.sum(sums * factors[..., None], axis=0) / doc_total[:, :, None]
    pooled = pooled_heads.reshape(docs_count, student_width)
    middle = jnp.tanh(jnp.dot(pooled, s_mid, precision=highest) + s_mid_bias)
    logit_rows = jnp.dot(middle, s_cls, precision=highest) + s_cls_bias
    logits = lax.all_gather(logit_rows, "row")[::sub]
    logits = lax.dynamic_slice_in_dim(logits, dp_index * seqs_local, seqs_local)
    logit_top = jnp.max(logit_rows, axis=-1, keepdims=True)
    logit_exp = jnp.exp(logit_rows - logit_top)
    one_hot = (label_seq[:, None] == class_ids[None, :]).astype(f32)
    d_logits = logit_exp / jnp.sum(logit_exp, axis=-1, keepdims=True) - one_hot
    g_cls = jnp.dot(middle.T, d_logits, precision=highest)
    g_cls_bias = jnp.sum(d_logits, axis=0)
    d_middle = jnp.dot(d_logits, s_cls.T, precision=highest) * (1.0 - middle * middle)
    g_mid = jnp.dot(pooled.T, d_middle, precision=highest)
    g_mid_bias = jnp.sum(d_middle, axis=0)
    d_pooled = jnp.dot(d_middle, s_mid.T, precision=highest).reshape(docs_count, SH, SHD)
    shares = jnp.where(member, jnp.exp(masked - doc_top[None]), 0.0) / doc_total[None]
    d_share = jnp.einsum("dhk,thk->tdh", d_pooled, head_parts, precision=highest)
    base_term = jnp.sum(d_pooled * pooled_heads, axis=-1)
    d_pool_logit = jnp.sum(shares * (d_share - base_term[None]), axis=1)
    d_heads = jnp.einsum("tdh,dhk->thk", shares, d_pooled, precision=highest)
    d_heads = d_heads + d_pool_logit[:, :, None] * query_heads[None] * pool_scale
    g_query = (jnp.sum(d_pool_logit[:, :, None] * head_parts, axis=0) * pool_scale).reshape(-1)
    d_student = d_heads.reshape(own, student_width)
    g_sbias = jnp.sum(d_student, axis=0)
    g_sproj = jnp.dot(layer_out.astype(f32).T, d_student, precision=highest)

    d_out = take_in(cotangent).T.astype(f32)
    g_ln2_gain = jnp.sum(d_out * normed_two, axis=0)
    g_ln2_bias = jnp.sum(d_out, axis=0)
    d_resid_two = normalize_back(d_out * gain_two, normed_two, inv_two)
    d_ffn = d_resid_two.astype(bf16)
    g_back_bias = jnp.sum(d_ffn.astype(f32), axis=0)
    g_back = jnp.einsum("td,ctn->cdn", d_ffn, act, preferred_element_type=f32)
    d_act = jnp.einsum("td,cdn->ctn", d_ffn, w_back_all, preferred_element_type=f32)
    _, gelu_fn = jax.vjp(gelu_exact, pre_act)
    d_pre = gelu_fn(d_act)[0].astype(bf16)
    g_in_bias = jnp.sum(d_pre.astype(f32), axis=1)
    g_in = jnp.einsum("td,ctn->cdn", hidden_low, d_pre, preferred_element_type=f32)
    d_hidden_one = d_resid_two + jnp.einsum(
        "ctn,cdn->td", d_pre, w_in_all, preferred_element_type=f32
    )
    g_ln1_gain = jnp.sum(d_hidden_one * normed_one, axis=0)
    g_ln1_bias = jnp.sum(d_hidden_one, axis=0)
    d_resid_one = normalize_back(d_hidden_one * gain_one, normed_one, inv_one)
    d_attn = d_resid_one.astype(bf16)
    g_out_bias = jnp.sum(d_attn.astype(f32), axis=0)
    g_out = mm(ctx, d_attn, ((0,), (0,)))
    d_ctx = mm(d_attn, w_out_all, ((1,), (1,))).astype(bf16)
    d_ctx = swap_cols(d_ctx.reshape(own, cols, width_col).transpose(1, 0, 2))
    d_ctx = d_ctx.reshape(cols * own, heads_dev, HD)
    d_q, d_k, d_v = attend_back(queries, key_rows, value_rows, probs, d_ctx, score_scale)
    d_kv = jnp.stack([d_k, d_v], axis=2).astype(bf16).reshape(seq_len, -1)
    d_kv = scatter_sequence(d_kv, cols, sub).reshape(cols, own, heads_dev, 2, HD)
    d_q = d_q.astype(bf16).reshape(cols, own, heads_dev, 1, HD)
    d_qkv = jnp.concatenate([d_q, d_kv], axis=3).reshape(cols, own, 3 * width_col)
    d_qkv = swap_cols(d_qkv)
    g_qkv_bias = jnp.sum(d_qkv.astype(f32), axis=1).reshape(cols, heads_dev, 3, HD)
    g_qkv = jnp.einsum("td,ctn->cdn", x, d_qkv, preferred_element_type=f32)
    d_tokens = d_resid_one + jnp.einsum("ctn,cdn->td", d_qkv, w_qkv_all, preferred_element_type=f32)
    grad_tokens = give_back(d_tokens.astype(bf16).T, seqs_local).astype(f32)

    g_out = g_out.reshape(cols, width_col, rows, width_row).transpose(0, 2, 1, 3)
    g_out = g_out.reshape(cols, rows, width_row, width_col)
    model = jnp.concatenate(
        [
            g_in.reshape(cols, rows, width_row, hidden_col).astype(bf16),
            g_back.reshape(cols, rows, width_row, hidden_col).astype(bf16),
            g_out.astype(bf16),
        ],
        axis=-1,
    )
    model = scatter_world(model).astype(f32)
    g_qkv = scatter_world(g_qkv.reshape(cols, rows, width_row, 3 * width_col).astype(bf16)).astype(f32)
    once = 1.0 / (parts * cols * sub)
    small = (
        g_qkv_bias[:, :, 0].reshape(cols, width_col),
        g_qkv_bias[:, :, 2].reshape(cols, width_col),
        g_in_bias,
        g_out_bias,
        g_ln1_gain,
        g_ln1_bias,
        g_back_bias,
        g_ln2_gain,
        g_ln2_bias,
        g_sproj,
        g_sbias,
        g_query,
        g_mid * once,
        g_mid_bias * once,
        g_cls * once,
        g_cls_bias * once,
    )
    small = lax.psum(small, WORLD)

    def at_col(part):
        return lax.dynamic_index_in_dim(part, col_index, 0, False)

    def at_row(part):
        return lax.dynamic_slice_in_dim(part, row_index * width_row, width_row)

    return (
        out,
        logits,
        grad_tokens,
        g_qkv,
        jnp.stack([at_col(small[0]), at_col(small[1])]),
        model[:, 2 * hidden_col :].reshape(width_col, width_row),
        at_row(small[3]),
        at_row(small[4]),
        at_row(small[5]),
        model[:, :hidden_col],
        at_col(small[2]),
        model[:, hidden_col : 2 * hidden_col],
        at_row(small[6]),
        at_row(small[7]),
        at_row(small[8]),
        at_row(small[9]),
        small[10],
        small[11],
        small[12],
        small[13],
        small[14],
        small[15],
    )


MESH = pl.DeviceIdType.MESH
HBM = pl.BlockSpec(memory_space=pl.ANY)


def place():
    return lax.axis_index("dp"), lax.axis_index("row"), lax.axis_index("col")


def greet(peers, guarded=()):
    barrier = pltpu.get_barrier_semaphore()
    for peer in peers:
        pl.semaphore_signal(barrier, inc=1, device_id=peer, device_id_type=MESH)
    for there, peer in guarded:

        @pl.when(there)
        def _():
            pl.semaphore_signal(barrier, inc=1, device_id=peer, device_id_type=MESH)

    amount = len(peers)
    for there, _ in guarded:
        amount = amount + there.astype(jnp.int32)
    pl.semaphore_wait(barrier, amount)


def rcopy(src, dst, send, recv, peer):
    return pltpu.make_async_remote_copy(
        src_ref=src, dst_ref=dst, send_sem=send, recv_sem=recv, device_id=peer, device_id_type=MESH
    )


def take_copies(src, out, local, send, recv):
    d, r, c = place()
    own = out.shape[2]
    moves = []
    for i in range(2):
        for far in range(2):
            row, core = 2 * d + i, d ^ far
            piece = src.at[i, :, pl.ds(pl.multiple_of(core * own, own), own)]
            here = (row == r) if far == 0 else None

            def start(piece=piece, row=row, core=core, slot=2 * i + far, here=here):
                def away():
                    rcopy(piece, out.at[r], send.at[slot], recv.at[r], (core, row, c)).start()

                if here is None:
                    away()
                else:
                    pl.when(jnp.logical_not(here))(away)

                    @pl.when(here)
                    def _():
                        pltpu.make_async_copy(piece, out.at[r], local).start()

            def wait(piece=piece, row=row, core=core, slot=2 * i + far, here=here):
                def away():
                    rcopy(piece, out.at[r], send.at[slot], recv.at[r], (core, row, c)).wait_send()

                if here is None:
                    away()
                else:
                    pl.when(jnp.logical_not(here))(away)

                    @pl.when(here)
                    def _():
                        pltpu.make_async_copy(piece, out.at[r], local).wait()

            moves.append((start, wait))
    for row in range(4):

        def arrive(row=row):
            @pl.when(jnp.logical_not((row == r) & (r // 2 == d)))
            def _():
                piece = src.at[0, :, pl.ds(0, own)]
                rcopy(piece, out.at[row], send.at[0], recv.at[row], (d, r, c)).wait_recv()

        moves.append((lambda: None, arrive))
    return moves


def gather_kernel(kinds, *refs):
    shards, refs = refs[:kinds], refs[kinds:]
    (tok, ints), refs = refs[:2], refs[2:]
    outs, refs = refs[:kinds], refs[kinds:]
    (tok_out, ints_out, q_out, kv_out), refs = refs[:4], refs[4:]
    (x_nat, q_src, kv_src), refs = refs[:3], refs[3:]
    own_sem, zs, zr, xs, xr, ys, yr, cs, cr, ps, pr, tl, ts, tr, il, hs, hr, hps, hpr = refs
    d, r, c = place()
    cols = 4
    xn, yn, pn = (d, r ^ 1, c), (d, r ^ 2, c), (1 - d, r, c)
    up, down = (d, r, c + 1), (d, r, c - 1)
    has_up, has_down = c < cols - 1, c > 0
    greet(plane_peers() + [(d, r, c ^ j) for j in (1, 2, 3)])
    moves = take_copies(tok, tok_out, tl, ts, tr)
    for start, _ in moves:
        start()
    pltpu.make_async_copy(ints, ints_out.at[d], il.at[0]).start()
    rcopy(ints, ints_out.at[d], il.at[1], il.at[2], pn).start()
    halves = [shard.shape[0] // 2 for shard in shards]

    def z_send(k, at, way, hop):
        src = shards[k] if hop == 1 else outs[k].at[at, r, d]
        return rcopy(
            src, outs[k].at[at, r, d], zs.at[k, way, hop - 1], zr.at[k, way, hop - 1], up if way == 0 else down
        )

    def src_of(k, at, own):
        return shards[k] if own else outs[k].at[at, r, d]

    def to_x(k, at, own):
        return rcopy(src_of(k, at, own), outs[k].at[at, r, d], xs.at[k, at], xr.at[k, at], xn)

    def to_y(k, at, own):
        return rcopy(src_of(k, at, own), outs[k].at[at, r, d], ys.at[k, at], yr.at[k, at], yn)

    def to_p(k, at, own):
        return rcopy(src_of(k, at, own), outs[k].at[at, r, d], ps.at[k, at, 0], pr.at[k, at, 0], pn)

    def relay(k, at, which):
        row = r ^ 1 if which == 0 else r ^ 2
        ref = outs[k].at[at, row, d, pl.ds(which * halves[k], halves[k])]
        return rcopy(ref, ref, cs.at[k, at, which], cr.at[k, at, which], yn if which == 0 else xn)

    def pass_p(k, at, bit):
        ref = outs[k].at[at, r ^ bit, d]
        return rcopy(ref, ref, ps.at[k, at, bit], pr.at[k, at, bit], pn)

    def got_x(k, at):
        ref = outs[k].at[at, r ^ 1, d]
        rcopy(ref, ref, xs.at[k, at], xr.at[k, at], xn).wait_recv()

    def got_y(k, at):
        ref = outs[k].at[at, r ^ 2, d]
        rcopy(ref, ref, ys.at[k, at], yr.at[k, at], yn).wait_recv()

    def got_corner(k, at):
        for which in range(2):
            ref = outs[k].at[at, r ^ 3, d, pl.ds(which * halves[k], halves[k])]
            rcopy(ref, ref, cs.at[k, at, which], cr.at[k, at, which], xn).wait_recv()

    def got_p(k, at, bit):
        ref = outs[k].at[at, r ^ bit, 1 - d]
        rcopy(ref, ref, ps.at[k, at, bit], pr.at[k, at, bit], pn).wait_recv()

    for k in range(kinds):
        pltpu.make_async_copy(shards[k], outs[k].at[c, r, d], own_sem.at[k]).start()

        @pl.when(has_up)
        def _():
            z_send(k, c, 0, 1).start()

        @pl.when(has_down)
        def _():
            z_send(k, c, 1, 1).start()

    def spread(k, at, own):
        to_x(k, at, own).start()
        to_y(k, at, own).start()
        to_p(k, at, own).start()

    def onward(k, at):
        got_x(k, at)
        relay(k, at, 0).start()
        pass_p(k, at, 1).start()
        got_y(k, at)
        relay(k, at, 1).start()
        pass_p(k, at, 2).start()

    steps = [(0, 0)] + [(way, hop) for hop in (1, 2, 3) for way in (0, 1)]
    jobs = [(k, way, hop) for k in range(kinds) for way, hop in steps]

    def at_of(way, hop):
        return c - hop if way == 0 else c + hop

    def valid(way, hop):
        return c >= hop if way == 0 else c + hop < cols

    def guard(way, hop, body):
        if hop == 0:
            body()
        else:
            pl.when(valid(way, hop))(body)

    def first(k, way, hop):
        def body():
            at = at_of(way, hop)
            if hop:
                z_send(k, at, way, hop).wait_recv()
                if hop < 3:
                    can = has_up if way == 0 else has_down

                    @pl.when(can)
                    def _():
                        z_send(k, at, way, hop + 1).start()

            spread(k, at, hop == 0)

        guard(way, hop, body)

    def second(k, way, hop):
        guard(way, hop, lambda: onward(k, at_of(way, hop)))

    def third(k, way, hop):
        def body():
            at = at_of(way, hop)
            got_corner(k, at)
            pass_p(k, at, 3).start()

        guard(way, hop, body)

    def settle(k):
        pltpu.make_async_copy(shards[k], outs[k].at[c, r, d], own_sem.at[k]).wait()
        for way, hop in steps:

            def body():
                for bit in range(4):
                    got_p(k, at_of(way, hop), bit)

            guard(way, hop, body)

    def kv(j):
        return rcopy(kv_src.at[c ^ j], kv_out.at[c, d], hs.at[0, j], hr.at[0, j], (d, r, c ^ j))

    def q(j):
        return rcopy(q_src.at[c ^ j], q_out.at[c], hs.at[1, j], hr.at[1, j], (d, r, c ^ j))

    def pair(j):
        src = kv_src.at[c] if j == 0 else kv_out.at[c ^ j, d]
        return rcopy(src, kv_out.at[c ^ j, d], hps.at[j], hpr.at[j], pn)

    deep = kv_src.shape[1]
    out_cols = deep + q_src.shape[1]
    lanes = -(-out_cols // 128) * 128

    def prepare():
        for _, wait in moves:
            wait()
        feats = tok_out.shape[1]
        x_nat[...] = tok_out[...].reshape(4 * feats, -1).astype(f32).T.astype(bf16)

    def project(j):
        to = c ^ j
        weights = outs[0][to, :, :, :, :lanes].reshape(-1, lanes)
        bias = outs[1][to, r, 0, pl.ds(0, 8)]
        bias = jnp.concatenate([bias[i : i + 1] for i in range(lanes // 128)], axis=1)
        made = jnp.dot(x_nat[...], weights, preferred_element_type=f32) + bias
        made = made.T.astype(bf16)
        kv_src[to] = made[:deep]
        q_src[to] = made[deep:out_cols]
        if j:
            kv(j).start()
            q(j).start()
        else:
            pair(0).start()
            kv_out[c, d] = kv_src[c]
            q_out[c] = q_src[c]

    lag = 3
    ready = 2 * len(steps) + 2 * lag
    for i in range(len(jobs) + 2 * lag):
        if i == ready:
            prepare()
            settle(0)
            settle(1)
        if ready <= i < ready + 4:
            project((3, 2, 1, 0)[i - ready])
        if i < len(jobs):
            first(*jobs[i])
        if 0 <= i - lag < len(jobs):
            second(*jobs[i - lag])
        if 0 <= i - 2 * lag < len(jobs):
            third(*jobs[i - 2 * lag])

    for j in (1, 2, 3):
        kv(j).wait_recv()
        pair(j).start()
    for k in range(kinds):
        if k > 1:
            settle(k)
        for way, hop in steps:

            def body():
                at = at_of(way, hop)
                own = hop == 0
                to_x(k, at, own).wait_send()
                to_y(k, at, own).wait_send()
                to_p(k, at, own).wait_send()
                for which in range(2):
                    relay(k, at, which).wait_send()
                for bit in (1, 2, 3):
                    pass_p(k, at, bit).wait_send()
                if hop < 3:
                    if own:

                        @pl.when(has_up)
                        def _():
                            z_send(k, c, 0, 1).wait_send()

                        @pl.when(has_down)
                        def _():
                            z_send(k, c, 1, 1).wait_send()
                    else:
                        can = has_up if way == 0 else has_down

                        @pl.when(can)
                        def _():
                            z_send(k, at, way, hop + 1).wait_send()

            guard(way, hop, body)
    for j in (1, 2, 3):
        q(j).wait()
        kv(j).wait_send()
    for j in range(4):
        pair(j).wait()
    pltpu.make_async_copy(ints, ints_out.at[d], il.at[0]).wait()
    rcopy(ints, ints_out.at[1 - d], il.at[1], il.at[2], pn).wait()


VM = pl.BlockSpec(memory_space=pltpu.VMEM)


def gather_fast(shards, tokens, ints, wide, cid):
    kinds = len(shards)
    dma = pltpu.SemaphoreType.DMA
    _, feats, cols = tokens.shape
    own = cols // 2
    piece = jax.ShapeDtypeStruct((4, wide, own), bf16)
    return pl.pallas_call(
        functools.partial(gather_kernel, kinds),
        out_shape=[jax.ShapeDtypeStruct((4, 4, 2) + s.shape, s.dtype) for s in shards]
        + [
            jax.ShapeDtypeStruct((4, feats, own), tokens.dtype),
            jax.ShapeDtypeStruct((2,) + ints.shape, ints.dtype),
            piece,
            jax.ShapeDtypeStruct((4, 2, 2 * wide, own), bf16),
        ],
        in_specs=[HBM] * (kinds + 2),
        out_specs=[VM, VM] + [HBM] * (kinds - 2) + [VM, HBM, VM, VM],
        scratch_shapes=[
            pltpu.VMEM((own, 4 * feats), bf16),
            pltpu.VMEM((4, wide, own), bf16),
            pltpu.VMEM((4, 2 * wide, own), bf16),
            dma((kinds,)),
            dma((kinds, 2, 3)), dma((kinds, 2, 3)),
            dma((kinds, 4)), dma((kinds, 4)),
            dma((kinds, 4)), dma((kinds, 4)),
            dma((kinds, 4, 2)), dma((kinds, 4, 2)),
            dma((kinds, 4, 4)), dma((kinds, 4, 4)),
            dma, dma((4,)), dma((4,)), dma((3,)),
            dma((2, 4)), dma((2, 4)), dma((4,)), dma((4,)),
        ],
        compiler_params=pltpu.CompilerParams(
            collective_id=cid, has_side_effects=True, vmem_limit_bytes=40 * 1024 * 1024
        ),
        name="head",
    )(*shards, tokens, ints)


def scatter_core(grads, outs, scratch, begin, during):
    kinds = len(grads)
    (acc, precv, xr1, yr1, xr2, yr2, zup, zdn, fin) = scratch[:9]
    (ls, ps, pr, xs1, xm1, ys1, ym1, xs2, xm2, ys2, ym2, us, um, ds, dm, fs, fm, os) = scratch[9:]
    d, r, c = place()
    cols = 4
    chunks = kinds * cols
    xn, yn, pn = (d, r ^ 1, c), (d, r ^ 2, c), (1 - d, r, c)
    up, down = (d, r, c + 1), (d, r, c - 1)
    half = acc.shape[2] // 2
    first, last = pl.ds(0, half), pl.ds(half, half)

    def split(i):
        k = i // cols
        j = i - k * cols
        at = jnp.where(j == 0, 0, jnp.where(j == 1, 3, j - 1))
        return k, at

    def at_static(i):
        return i // cols, (0, 3, 1, 2)[i % cols]

    def load(i):
        k, at = at_static(i)
        return pltpu.make_async_copy(grads[k].at[at, :, d], acc.at[i], ls.at[i])

    def pair(i):
        k, at = at_static(i)
        return rcopy(grads[k].at[at, :, 1 - d], precv.at[i], ps.at[i], pr.at[i], pn)

    for i in range(chunks):
        pair(i).start()
        load(i).start()
    begin()

    def x1(i, j):
        return rcopy(acc.at[i, r ^ 1 ^ (2 * j), first], xr1.at[i, j], xs1.at[i, j], xm1.at[i, j], xn)

    def y1(i, j):
        return rcopy(acc.at[i, r ^ 2 ^ j, last], yr1.at[i, j], ys1.at[i, j], ym1.at[i, j], yn)

    def y2(i):
        return rcopy(acc.at[i, r ^ 2, first], yr2.at[i], ys2.at[i], ym2.at[i], yn)

    def x2(i):
        return rcopy(acc.at[i, r ^ 1, last], xr2.at[i], xs2.at[i], xm2.at[i], xn)

    def to_up(i):
        return rcopy(acc.at[i, r], zup.at[i], us.at[i], um.at[i], up)

    def to_down(i):
        return rcopy(acc.at[i, r], zdn.at[i], ds.at[i], dm.at[i], down)

    def stage1(i):
        pltpu.make_async_copy(precv.at[i], acc.at[i], ls.at[i]).wait()
        rcopy(acc.at[i], precv.at[i], ps.at[i], pr.at[i], pn).wait_recv()

        @pl.loop(0, 4)
        def _(row):
            acc[i, row] = acc[i, row] + precv[i, row]

        x1(i, 1).start()
        y1(i, 1).start()
        x1(i, 0).start()
        y1(i, 0).start()

    def stage2(i):
        x1(i, 1).wait_recv()
        acc[i, r ^ 2, first] = acc[i, r ^ 2, first] + xr1[i, 1]
        y2(i).start()
        y1(i, 1).wait_recv()
        acc[i, r ^ 1, last] = acc[i, r ^ 1, last] + yr1[i, 1]
        x2(i).start()
        x1(i, 0).wait_recv()
        acc[i, r, first] = acc[i, r, first] + xr1[i, 0]
        y1(i, 0).wait_recv()
        acc[i, r, last] = acc[i, r, last] + yr1[i, 0]

    def stage3(i):
        y2(i).wait_recv()
        acc[i, r, first] = acc[i, r, first] + yr2[i]
        x2(i).wait_recv()
        acc[i, r, last] = acc[i, r, last] + xr2[i]

    def stage4(i, hops):
        k, at = split(i)

        @pl.when((at > c) & (c == hops))
        def _():
            @pl.when(c > 0)
            def _():
                to_up(i).wait_recv()
                acc[i, r] = acc[i, r] + zup[i]

            to_up(i).start()

        @pl.when((at < c) & (cols - 1 - c == hops))
        def _():
            @pl.when(c < cols - 1)
            def _():
                to_down(i).wait_recv()
                acc[i, r] = acc[i, r] + zdn[i]

            to_down(i).start()

        @pl.when((at == c) & (jnp.maximum(c, cols - 1 - c) == hops))
        def _():
            @pl.when(c > 0)
            def _():
                to_up(i).wait_recv()
                acc[i, r] = acc[i, r] + zup[i]

            @pl.when(c < cols - 1)
            def _():
                to_down(i).wait_recv()
                acc[i, r] = acc[i, r] + zdn[i]

            fin[k, d] = acc[i, r]
            rcopy(fin.at[k, d], fin.at[k, d], fs.at[k], fm.at[k], pn).start()

    stages = [(0, stage1), (2, stage2), (4, stage3)]
    stages += [(5 + h, functools.partial(lambda h, i: stage4(i, h), h)) for h in range(cols)]
    ending = stages[-1][0]

    assert len(during) <= chunks + ending

    @pl.loop(0, chunks + ending)
    def _(step):
        for i, extra in enumerate(during):
            pl.when(step == i)(extra)

        for lag, stage in stages:

            @pl.when((step >= lag) & (step - lag < chunks))
            def _():
                stage(step - lag)

    @pl.loop(0, chunks)
    def _(i):
        k, at = split(i)
        rcopy(acc.at[i], precv.at[i], ps.at[i], pr.at[i], pn).wait_send()
        for j in range(2):
            x1(i, j).wait_send()
            y1(i, j).wait_send()
        y2(i).wait_send()
        x2(i).wait_send()

        @pl.when(at > c)
        def _():
            to_up(i).wait_send()

        @pl.when(at < c)
        def _():
            to_down(i).wait_send()

    for k in range(kinds):
        rcopy(fin.at[k, 1 - d], fin.at[k, 1 - d], fs.at[k], fm.at[k], pn).wait()
        pltpu.make_async_copy(fin.at[k], outs[k], os.at[k]).start()
    for k in range(kinds):
        pltpu.make_async_copy(fin.at[k], outs[k], os.at[k]).wait()

def scatter_scratch(kinds, n, w, dt):
    dma = pltpu.SemaphoreType.DMA
    chunks = kinds * 4
    return [
        pltpu.VMEM((chunks, 4, n, w), dt),
        pltpu.VMEM((chunks, 4, n, w), dt),
        pltpu.VMEM((chunks, 2, n // 2, w), dt),
        pltpu.VMEM((chunks, 2, n // 2, w), dt),
        pltpu.VMEM((chunks, n // 2, w), dt),
        pltpu.VMEM((chunks, n // 2, w), dt),
        pltpu.VMEM((chunks, n, w), dt),
        pltpu.VMEM((chunks, n, w), dt),
        pltpu.VMEM((kinds, 2, n, w), dt),
        dma((chunks,)), dma((chunks,)), dma((chunks,)),
        dma((chunks, 2)), dma((chunks, 2)), dma((chunks, 2)), dma((chunks, 2)),
        dma((chunks,)), dma((chunks,)), dma((chunks,)), dma((chunks,)),
        dma((chunks,)), dma((chunks,)), dma((chunks,)), dma((chunks,)),
        dma((kinds,)), dma((kinds,)), dma((kinds,)),
    ]


def give_moves(src_ref, out_ref, local, send, recv):
    d, r, c = place()
    own = src_ref.shape[2]
    home = r // 2

    def slot(i, core):
        return out_ref.at[i, :, pl.ds(pl.multiple_of(core * own, own), own)]

    def move(row):
        return rcopy(src_ref.at[row], slot(r % 2, d), send.at[row], recv.at[r % 2, d], (home, row, c))

    def stay():
        return pltpu.make_async_copy(src_ref.at[r], slot(r % 2, d), local)

    def start():
        for row in range(4):

            @pl.when(jnp.logical_not((row == r) & (home == d)))
            def _():
                move(row).start()

        @pl.when(home == d)
        def _():
            stay().start()

    def finish():
        for row in range(4):

            @pl.when(jnp.logical_not((row == r) & (home == d)))
            def _():
                move(row).wait_send()

        @pl.when(home == d)
        def _():
            stay().wait()

        for i in range(2):
            for core in range(2):

                @pl.when(jnp.logical_not((2 * d + i == r) & (core == d)))
                def _():
                    rcopy(src_ref.at[0], slot(i, core), send.at[0], recv.at[i, core], (d, r, c)).wait_recv()

    return start, finish


def plane_peers():
    d, r, c = place()
    return [(d ^ (j // 4), r ^ (j % 4), c) for j in range(1, 8)]


def line_peers():
    d, r, c = place()
    return [(d ^ (j // 4), r, c ^ (j % 4)) for j in range(1, 8)]


def swap_kernel(src, cot, out, cot_out, send, recv, tl, ts, tr):
    d, r, c = place()
    greet(plane_peers() + [(d, r, c ^ j) for j in (1, 2, 3)])

    def move(j):
        return rcopy(src.at[c ^ j], out.at[c], send.at[j], recv.at[j], (d, r, c ^ j))

    for j in (3, 2, 1):
        move(j).start()
    moves = take_copies(cot, cot_out, tl, ts, tr)
    for start, _ in moves:
        start()
    out[c] = src[c]
    for j in (1, 2, 3):
        move(j).wait()
    for _, wait in moves:
        wait()


def swap_fast(values, cotangent, cid):
    dma = pltpu.SemaphoreType.DMA
    _, feats, cols = cotangent.shape
    return pl.pallas_call(
        swap_kernel,
        out_shape=[
            jax.ShapeDtypeStruct(values.shape, values.dtype),
            jax.ShapeDtypeStruct((4, feats, cols // 2), cotangent.dtype),
        ],
        in_specs=[VM, HBM],
        out_specs=[VM, VM],
        scratch_shapes=[dma((4,)), dma((4,)), dma, dma((4,)), dma((4,))],
        compiler_params=pltpu.CompilerParams(collective_id=cid, has_side_effects=True),
        name="swap",
    )(values, cotangent)


def turn_kernel(ctx_ref, stats_ref, give_ref, ctx_out, stats_out, give_out, send, recv, ssend, srecv, gl, gs, gr):
    d, r, c = place()
    peers = line_peers()
    greet(plane_peers() + peers[:3] + peers[4:])

    def move(j):
        return rcopy(ctx_ref.at[c ^ j], ctx_out.at[c], send.at[j], recv.at[j], (d, r, c ^ j))

    def tell(j):
        return rcopy(stats_ref, stats_out.at[d, c], ssend.at[j - 1], srecv.at[j - 1], peers[j - 1])

    for j in range(1, 8):
        tell(j).start()
    for j in (3, 2, 1):
        move(j).start()
    start, finish = give_moves(give_ref, give_out, gl, gs, gr)
    start()
    ctx_out[c] = ctx_ref[c]
    stats_out[d, c] = stats_ref[...]
    for j in range(1, 8):
        tell(j).wait()
    for j in (1, 2, 3):
        move(j).wait()
    finish()


def turn_fast(d_ctx, stats, out_t, cid):
    width, own = out_t.shape
    dma = pltpu.SemaphoreType.DMA
    return pl.pallas_call(
        turn_kernel,
        out_shape=[
            jax.ShapeDtypeStruct(d_ctx.shape, d_ctx.dtype),
            jax.ShapeDtypeStruct((2, 4) + stats.shape, stats.dtype),
            jax.ShapeDtypeStruct((2, width // 4, 2 * own), out_t.dtype),
        ],
        in_specs=[VM, VM, HBM],
        out_specs=[VM, VM, HBM],
        scratch_shapes=[dma((4,)), dma((4,)), dma((7,)), dma((7,)), dma, dma((4,)), dma((2, 2))],
        compiler_params=pltpu.CompilerParams(collective_id=cid, has_side_effects=True),
        name="turn",
    )(d_ctx, stats, out_t.reshape(4, width // 4, own))


def sum_steps(src, total, parts, sems):
    d, r, c = place()
    peers = [(1 - d, r, c), (d, r ^ 1, c), (d, r ^ 2, c), (d, r, c ^ 1), (d, r, c ^ 2)]
    bits = [d, r % 2, r // 2, c % 2, c // 2]
    rs, rr, gs, gr = sems
    count = len(peers)
    size = [src.shape[0] >> (i + 1) for i in range(count)]
    offset = [jnp.int32(0)]
    for i in range(count):
        offset.append(offset[i] + bits[i] * size[i])

    def rows(at, amount):
        return pl.ds(pl.multiple_of(at, 8), amount)

    def down(i):
        other = offset[i] + (1 - bits[i]) * size[i]
        held = src if i == 0 else parts[i - 1]
        at = other if i == 0 else other - offset[i]
        return rcopy(held.at[rows(at, size[i])], parts[count + i], rs.at[i], rr.at[i], peers[i])

    def fold(i):
        down(i).wait_recv()
        held = src if i == 0 else parts[i - 1]
        at = offset[i + 1] if i == 0 else offset[i + 1] - offset[i]
        parts[i][...] = held[rows(at, size[i])] + parts[count + i][...]

    def back(i):
        spot = total.at[rows(offset[i + 1], size[i])]
        return rcopy(spot, spot, gs.at[i], gr.at[i], peers[i])

    def back_recv(i):
        spot = total.at[rows(offset[i] + (1 - bits[i]) * size[i], size[i])]
        rcopy(spot, spot, gs.at[i], gr.at[i], peers[i]).wait_recv()

    steps = [lambda: down(0).start()]
    for i in range(1, count):

        def step(i=i):
            fold(i - 1)
            down(i).start()

        steps.append(step)

    def middle():
        fold(count - 1)
        total[rows(offset[count], size[-1])] = parts[count - 1][...]
        back(count - 1).start()

    steps.append(middle)
    for i in range(count - 2, -1, -1):

        def step(i=i):
            back_recv(i + 1)
            back(i).start()

        steps.append(step)

    def end():
        back_recv(0)
        for i in range(count):
            down(i).wait_send()
            back(i).wait_send()

    return steps, end


def tail_kernel(kinds, *refs):
    grads, refs = refs[:kinds], refs[kinds:]
    (q_ref, kv_ref, small_ref), refs = refs[:3], refs[3:]
    outs, refs = refs[:kinds], refs[kinds:]
    (q_out, kv_out, small_out), refs = refs[:3], refs[3:]
    (total, theirs), refs = refs[:2], refs[2:]
    parts, refs = refs[:10], refs[10:]
    (send, recv, psend, precv), sems, scratch = refs[:4], refs[4:8], refs[8:]
    d, r, c = place()
    pn = (1 - d, r, c)
    greet([(d, r, c ^ j) for j in (1, 2, 3)] + [pn, (d, r ^ 1, c), (d, r ^ 2, c)])

    def pair(j):
        return rcopy(kv_ref.at[c ^ j, 1 - d], theirs.at[c ^ j], psend.at[j], precv.at[j], pn)

    def kv(j):
        return rcopy(total.at[c ^ j], kv_out.at[c], send.at[0, j], recv.at[0, j], (d, r, c ^ j))

    def q(j):
        return rcopy(q_ref.at[c ^ j], q_out.at[c], send.at[1, j], recv.at[1, j], (d, r, c ^ j))

    for j in (3, 2, 1, 0):
        pair(j).start()
    for j in (3, 2, 1):
        q(j).start()
    q_out[c] = q_ref[c]
    steps, end = sum_steps(small_ref, small_out, parts, sems)

    def begin():
        for j in (3, 2, 1):
            pair(j).wait_recv()
            total[c ^ j] = kv_ref[c ^ j, d] + theirs[c ^ j]
            kv(j).start()
        pair(0).wait_recv()
        kv_out[c] = kv_ref[c, d] + theirs[c]

    scatter_core(grads, outs, scratch, begin, steps)
    end()
    for j in range(4):
        pair(j).wait_send()
    for j in (1, 2, 3):
        q(j).wait()
        kv(j).wait()


def tail_fast(grads, q, kv, small, cid):
    kinds = len(grads)
    n, w = grads[0].shape[3:]
    dma = pltpu.SemaphoreType.DMA
    cols, _, wide, own = kv.shape
    parts = [pltpu.VMEM((small.shape[0] >> (i + 1), small.shape[1]), f32) for i in range(5)]
    return pl.pallas_call(
        functools.partial(tail_kernel, kinds),
        out_shape=[jax.ShapeDtypeStruct((2, n, w), bf16)] * kinds
        + [
            jax.ShapeDtypeStruct(q.shape, q.dtype),
            jax.ShapeDtypeStruct((cols, wide, own), kv.dtype),
            jax.ShapeDtypeStruct(small.shape, f32),
        ],
        in_specs=[HBM] * kinds + [VM] * 3,
        out_specs=[HBM] * kinds + [VM] * 3,
        scratch_shapes=[pltpu.VMEM((cols, wide, own), kv.dtype)] * 2
        + parts * 2
        + [dma((2, 4)), dma((2, 4)), dma((4,)), dma((4,)), dma((5,)), dma((5,)), dma((5,)), dma((5,))]
        + scatter_scratch(kinds, n, w, bf16),
        compiler_params=pltpu.CompilerParams(
            collective_id=cid, has_side_effects=True, vmem_limit_bytes=48 * 1024 * 1024
        ),
        name="tail",
    )(*grads, q, kv, small)


def last_kernel(kinds, *refs):
    grads, refs = refs[:kinds], refs[kinds:]
    give_ref, refs = refs[0], refs[1:]
    outs, refs = refs[:kinds], refs[kinds:]
    give_out, gl, gs, gr = refs[:4]
    d, r, c = place()
    greet(plane_peers(), [(c < 3, (d, r, c + 1)), (c > 0, (d, r, c - 1))])
    start, finish = give_moves(give_ref, give_out, gl, gs, gr)
    scatter_core(grads, outs, refs[4:], start, [])
    finish()


def last_fast(grads, grad_t, cid):
    kinds = len(grads)
    n, w = grads[0].shape[3:]
    width, own = grad_t.shape
    dma = pltpu.SemaphoreType.DMA
    return pl.pallas_call(
        functools.partial(last_kernel, kinds),
        out_shape=[jax.ShapeDtypeStruct((2, n, w), bf16)] * kinds
        + [jax.ShapeDtypeStruct((2, width // 4, 2 * own), bf16)],
        in_specs=[HBM] * (kinds + 1),
        out_specs=[HBM] * (kinds + 1),
        scratch_shapes=[dma, dma((4,)), dma((2, 2))] + scatter_scratch(kinds, n, w, bf16),
        compiler_params=pltpu.CompilerParams(
            collective_id=cid, has_side_effects=True, vmem_limit_bytes=48 * 1024 * 1024
        ),
        name="last_sums",
    )(*grads, grad_t.reshape(4, width // 4, own))


def dot(a, b, contract=((1,), (0,))):
    return lax.dot_general(a, b, (contract, ((), ())), preferred_element_type=f32)


def block_rows(ref, heads, scale, out):
    own = ref.shape[-1]
    for h in range(heads):
        for g in range(heads):
            spot = (pl.ds(h * HD, HD), pl.ds(g * own, own))
            if h == g:
                out[spot] = ref[0, pl.ds(h * HD, HD)] * jnp.asarray(scale, out.dtype)
            else:
                out[spot] = jnp.zeros((HD, own), out.dtype)


def attn_fwd_kernel(heads, scale, bounds, q_ref, kv_ref, qseg_ref, kseg_ref, ctx_ref, lse_ref, kn, q3, s_scr, o_scr):
    step = pl.program_id(0)
    tiles, _, tile = kv_ref.shape
    wide = heads * HD
    own = q_ref.shape[-1]

    @pl.when(step == 0)
    def _():
        @pl.loop(0, tiles)
        def _(j):
            kn[j] = kv_ref[j, pl.ds(0, wide)].astype(f32).T.astype(bf16)

    block_rows(q_ref, heads, scale, q3)
    low, high = bounds[step, 0], bounds[step, 1]
    qseg = jnp.concatenate([qseg_ref[0]] * heads, axis=1)

    def one(j, top):
        s = dot(kn[j], q3[...])
        s = jnp.where(kseg_ref[j] == qseg, s, masked_value)
        s_scr[j] = s
        return jnp.maximum(top, jnp.max(s, axis=0, keepdims=True))

    top = lax.fori_loop(low, high, one, jnp.full((1, heads * own), masked_value, f32))
    o_scr[...] = jnp.zeros_like(o_scr)

    def two(j, total):
        p = jnp.exp(s_scr[j] - top)
        low_p = p.astype(bf16)
        for h in range(heads):
            rows = pl.ds(h * HD, HD)
            v = kv_ref[j, pl.ds(wide + h * HD, HD)]
            o_scr[rows] += dot(v, low_p[:, h * own : (h + 1) * own])
        return total + jnp.sum(p, axis=0, keepdims=True)

    total = lax.fori_loop(low, high, two, jnp.zeros((1, heads * own), f32))
    for h in range(heads):
        rows = pl.ds(h * HD, HD)
        ctx_ref[0, rows] = (o_scr[rows] / total[:, h * own : (h + 1) * own]).astype(bf16)
    lse_ref[0] = top + jnp.log(total)


def attn_fwd(bounds, q, kv, qseg, kseg, scale):
    blocks, wide, own = q.shape
    tiles, _, tile = kv.shape
    heads = wide // HD
    return pl.pallas_call(
        functools.partial(attn_fwd_kernel, heads, scale),
        out_shape=[
            jax.ShapeDtypeStruct(q.shape, bf16),
            jax.ShapeDtypeStruct((blocks, 1, heads * own), f32),
        ],
        grid_spec=pltpu.PrefetchScalarGridSpec(
            num_scalar_prefetch=1,
            grid=(blocks,),
            in_specs=[
                pl.BlockSpec((1, wide, own), lambda i, b: (i, 0, 0)),
                pl.BlockSpec(kv.shape, lambda i, b: (0, 0, 0)),
                pl.BlockSpec((1, 1, own), lambda i, b: (i, 0, 0)),
                pl.BlockSpec(kseg.shape, lambda i, b: (0, 0, 0)),
            ],
            out_specs=[
                pl.BlockSpec((1, wide, own), lambda i, b: (i, 0, 0)),
                pl.BlockSpec((1, 1, heads * own), lambda i, b: (i, 0, 0)),
            ],
            scratch_shapes=[
                pltpu.VMEM((tiles, tile, wide), bf16),
                pltpu.VMEM((wide, heads * own), bf16),
                pltpu.VMEM((tiles, tile, heads * own), f32),
                pltpu.VMEM((wide, own), f32),
            ],
        ),
        compiler_params=pltpu.CompilerParams(
            dimension_semantics=("arbitrary",), vmem_limit_bytes=48 * 1024 * 1024
        ),
        name="attn_fwd",
    )(bounds, q, kv, qseg, kseg)


def attn_bwd_kernel(
    heads, scale, bounds, q_ref, kv_ref, qseg_ref, kseg_ref, lse_ref, ctx_ref, dctx_ref,
    dq_ref, dkv_ref, kn, vn, q3, dc3, dq_scr, dkv_scr,
):
    step = pl.program_id(0)
    tiles, _, tile = kv_ref.shape
    wide = heads * HD
    own = q_ref.shape[-1]

    @pl.when(step == 0)
    def _():
        @pl.loop(0, tiles)
        def _(j):
            kn[j] = kv_ref[j, pl.ds(0, wide)].astype(f32).T.astype(bf16)
            vn[j] = kv_ref[j, pl.ds(wide, wide)].astype(f32).T.astype(bf16)
            dkv_scr[j] = jnp.zeros((2 * wide, tile), f32)

    block_rows(q_ref, heads, scale, q3)
    block_rows(dctx_ref, heads, 1.0, dc3)
    low, high = bounds[step, 0], bounds[step, 1]
    qseg = jnp.concatenate([qseg_ref[0]] * heads, axis=1)
    lse = lse_ref[0]
    product = ctx_ref[0].astype(f32) * dctx_ref[0].astype(f32)
    delta = jnp.concatenate(
        [jnp.sum(product[h * HD : (h + 1) * HD], axis=0, keepdims=True) for h in range(heads)], axis=1
    )
    dq_scr[...] = jnp.zeros_like(dq_scr)

    @pl.loop(low, high)
    def _(j):
        s = dot(kn[j], q3[...])
        s = jnp.where(kseg_ref[j] == qseg, s, masked_value)
        p = jnp.exp(s - lse)
        d_p = dot(vn[j], dc3[...])
        d_s = (p * (d_p - delta)).astype(bf16)
        p = p.astype(bf16)
        for h in range(heads):
            rows, lanes = pl.ds(h * HD, HD), slice(h * own, (h + 1) * own)
            dq_scr[rows] += dot(kv_ref[j, rows], d_s[:, lanes])
            dkv_scr[j, rows] += dot(q3[rows, lanes], d_s[:, lanes], ((1,), (1,)))
            deep = pl.ds(wide + h * HD, HD)
            dkv_scr[j, deep] += dot(dctx_ref[0, rows], p[:, lanes], ((1,), (1,)))

    dq_ref[0] = (dq_scr[...] * scale).astype(bf16)

    @pl.when(step == pl.num_programs(0) - 1)
    def _():
        @pl.loop(0, tiles)
        def _(j):
            dkv_ref[j] = dkv_scr[j].astype(bf16)


def attn_bwd(bounds, q, kv, qseg, kseg, lse, ctx, dctx, scale):
    blocks, wide, own = q.shape
    tiles, _, tile = kv.shape
    heads = wide // HD
    rowed = pl.BlockSpec((1, wide, own), lambda i, b: (i, 0, 0))
    return pl.pallas_call(
        functools.partial(attn_bwd_kernel, heads, scale),
        out_shape=[jax.ShapeDtypeStruct(q.shape, bf16), jax.ShapeDtypeStruct(kv.shape, bf16)],
        grid_spec=pltpu.PrefetchScalarGridSpec(
            num_scalar_prefetch=1,
            grid=(blocks,),
            in_specs=[
                rowed,
                pl.BlockSpec(kv.shape, lambda i, b: (0, 0, 0)),
                pl.BlockSpec((1, 1, own), lambda i, b: (i, 0, 0)),
                pl.BlockSpec(kseg.shape, lambda i, b: (0, 0, 0)),
                pl.BlockSpec((1, 1, heads * own), lambda i, b: (i, 0, 0)),
                rowed,
                rowed,
            ],
            out_specs=[rowed, pl.BlockSpec(kv.shape, lambda i, b: (0, 0, 0))],
            scratch_shapes=[
                pltpu.VMEM((tiles, tile, wide), bf16),
                pltpu.VMEM((tiles, tile, wide), bf16),
                pltpu.VMEM((wide, heads * own), bf16),
                pltpu.VMEM((wide, heads * own), bf16),
                pltpu.VMEM((wide, own), f32),
                pltpu.VMEM((tiles, 2 * wide, tile), f32),
            ],
        ),
        compiler_params=pltpu.CompilerParams(
            dimension_semantics=("arbitrary",), vmem_limit_bytes=48 * 1024 * 1024
        ),
        name="attn_bwd",
    )(bounds, q, kv, qseg, kseg, lse, ctx, dctx)


def fast_local(
    tokens,
    segments,
    labels,
    cotangent,
    w_qkv,
    b_qkv,
    w_out,
    b_out,
    ln1_gain,
    ln1_bias,
    w_in,
    b_in,
    w_back,
    b_back,
    ln2_gain,
    ln2_bias,
    s_proj,
    s_bias,
    s_query,
    s_mid,
    s_mid_bias,
    s_cls,
    s_cls_bias,
):
    _, width_row, cols_local = tokens.shape
    parts, rows, cols, seqs, _ = sizes(tokens.shape[0])
    width = width_row * rows
    own = cols_local // parts
    width_col = b_qkv.shape[1]
    heads_dev = width_col // HD
    hidden_col = b_in.shape[0]
    docs_count = labels.shape[1]
    class_count = s_cls.shape[1]
    student_width = s_proj.shape[1]
    seq_len = segments.shape[1]
    row_index = lax.axis_index("row")
    col_index = lax.axis_index("col")
    dp_index = lax.axis_index("dp")
    score_scale = HD ** (-0.5)
    pool_scale = SHD ** (-0.5)
    query_heads = s_query.reshape(SH, SHD)
    doc_ids = jnp.arange(docs_count, dtype=jnp.int32)
    class_ids = jnp.arange(class_count, dtype=jnp.int32)

    w_three = w_qkv.reshape(width_row, heads_dev, 3, HD).transpose(0, 2, 1, 3)
    w_three = jnp.concatenate([w_three[:, 1], w_three[:, 2], w_three[:, 0]], axis=1)
    shard_attn = own_half(jnp.concatenate([w_three.reshape(width_row, -1), w_out], axis=1))
    proj_rows = width_row // cols
    lanes = -(-3 * width_col // 128) * 128
    offsets = jnp.concatenate([jnp.zeros_like(b_qkv[0]), b_qkv[1], b_qkv[0]])
    offsets = jnp.pad(offsets, (0, lanes - 3 * width_col))
    vectors = [offsets, b_out, ln1_gain, ln1_bias, b_back, ln2_gain, ln2_bias, b_in]
    vectors.append(lax.dynamic_slice_in_dim(s_proj, col_index * proj_rows, proj_rows).astype(f32).reshape(-1))
    flat = jnp.concatenate(vectors)
    flat = jnp.pad(flat, (0, 96 * 128 - flat.shape[0])).reshape(96, 128)
    w_attn, vec, w_in_all, w_back_all, x_parts, ints, queries, kv = gather_fast(
        [shard_attn, own_half(flat), own_half(w_in), own_half(w_back)],
        tokens,
        jnp.concatenate([segments, labels], axis=1),
        width_col,
        1,
    )
    w_attn = w_attn.reshape(cols, rows, width_row, 4 * width_col)
    w_qkv_all = w_attn[..., : 3 * width_col].reshape(cols, width, 3 * width_col)
    w_out_all = w_attn[..., 3 * width_col :].transpose(0, 2, 1, 3).reshape(width, width)
    w_in_all = w_in_all.reshape(cols, width, hidden_col)
    w_back_all = w_back_all.reshape(cols, width, hidden_col)
    vec = vec.reshape(cols, rows, -1)
    at = lanes + 6 * width_row
    row_vectors = vec[0, :, lanes:at].reshape(rows, 6, width_row).transpose(1, 0, 2).reshape(6, width)
    b_out_a, gain_one, bias_one, b_back_a, gain_two, bias_two = [row_vectors[i] for i in range(6)]
    b_in_all = vec[:, 0, at : at + hidden_col]
    at += hidden_col
    s_proj_all = vec[:, :, at : at + proj_rows * student_width].astype(bf16)
    s_proj_all = s_proj_all.reshape(cols, rows, proj_rows, student_width).transpose(1, 0, 2, 3)
    s_proj_all = s_proj_all.reshape(width, student_width)
    x_t = x_parts.reshape(width, own)
    ints = lax.dynamic_index_in_dim(ints.reshape(seqs, -1), row_index, 0, False)
    seg_all, label_seq = ints[:seq_len], ints[seq_len:]
    seg_blocks = seg_all.reshape(cols, parts, own)
    seg_q = lax.dynamic_index_in_dim(seg_blocks, dp_index, 1, False)
    seg_own = lax.dynamic_index_in_dim(seg_q, col_index, 0, False)
    lows = jnp.sum(seg_all[None, :] < seg_q[:, :1], axis=1) // own
    highs = (jnp.sum(seg_all[None, :] <= seg_q[:, -1:], axis=1) + own - 1) // own
    bounds = jnp.stack([lows, highs], axis=1).astype(jnp.int32)

    kv = kv.reshape(cols * parts, 2 * width_col, own)
    q_rows, k_rows = seg_q[:, None, :], seg_all.reshape(cols * parts, own, 1)
    context, lse = attn_fwd(bounds, queries, kv, q_rows, k_rows, score_scale)
    ctx_t, c_parts = swap_fast(context, cotangent, 3)
    ctx_t = ctx_t.reshape(width, own)

    x = x_t.T
    attn_out = mm(ctx_t, w_out_all, ((0,), (0,))) + b_out_a
    normed_one, inv_one = normalize(x.astype(f32) + attn_out)
    hidden_one = normed_one * gain_one + bias_one
    hidden_low = hidden_one.astype(bf16)
    pre_act = jnp.einsum("td,cdn->ctn", hidden_low, w_in_all, preferred_element_type=f32)
    pre_act = pre_act + b_in_all[:, None, :]
    act = gelu_exact(pre_act).astype(bf16)
    ffn_out = jnp.einsum("ctn,cdn->td", act, w_back_all, preferred_element_type=f32) + b_back_a
    normed_two, inv_two = normalize(hidden_one + ffn_out)
    layer_out = (normed_two * gain_two + bias_two).astype(bf16)

    student_h = mm(layer_out, s_proj_all, ((1,), (0,))) + s_bias
    head_parts = student_h.reshape(own, SH, SHD)
    pool_logit = jnp.sum(head_parts * query_heads, axis=-1) * pool_scale
    member = (seg_own[:, None] == doc_ids[None, :])[:, :, None]
    masked = jnp.where(member, pool_logit[:, None, :], masked_value)
    local_top = jnp.max(masked, axis=0)
    local_exp = jnp.where(member, jnp.exp(masked - local_top[None]), 0.0)
    local_total = jnp.sum(local_exp, axis=0)
    local_sum = jnp.einsum("tdh,thk->dhk", local_exp, head_parts, precision=highest)
    stats = jnp.concatenate([local_top[..., None], local_total[..., None], local_sum], axis=-1)
    stats = jnp.pad(stats.reshape(-1), (0, 8 * 128 - stats.size)).reshape(8, 128)

    d_out = c_parts.reshape(width, own).T.astype(f32)
    g_ln2_gain = jnp.sum(d_out * normed_two, axis=0)
    g_ln2_bias = jnp.sum(d_out, axis=0)
    d_resid_two = normalize_back(d_out * gain_two, normed_two, inv_two)
    d_ffn = d_resid_two.astype(bf16)
    g_back_bias = jnp.sum(d_ffn.astype(f32), axis=0)
    g_back = jnp.einsum("td,ctn->cdn", d_ffn, act, preferred_element_type=f32)
    d_act = jnp.einsum("td,cdn->ctn", d_ffn, w_back_all, preferred_element_type=f32)
    _, gelu_fn = jax.vjp(gelu_exact, pre_act)
    d_pre = gelu_fn(d_act)[0].astype(bf16)
    g_in_bias = jnp.sum(d_pre.astype(f32), axis=1)
    g_in = jnp.einsum("td,ctn->cdn", hidden_low, d_pre, preferred_element_type=f32)
    d_hidden_one = d_resid_two + jnp.einsum(
        "ctn,cdn->td", d_pre, w_in_all, preferred_element_type=f32
    )
    g_ln1_gain = jnp.sum(d_hidden_one * normed_one, axis=0)
    g_ln1_bias = jnp.sum(d_hidden_one, axis=0)
    d_resid_one = normalize_back(d_hidden_one * gain_one, normed_one, inv_one)
    d_attn = d_resid_one.astype(bf16)
    g_out_bias = jnp.sum(d_attn.astype(f32), axis=0)
    d_ctx = mm(w_out_all, d_attn, ((1,), (1,))).astype(bf16)
    d_ctx, stats, out = turn_fast(d_ctx.reshape(cols, width_col, own), stats, layer_out.T, 4)

    stats = stats.reshape(cols * parts, -1)[:, : docs_count * SH * (SHD + 2)]
    stats = stats.reshape(cols * parts, docs_count, SH, SHD + 2)
    tops, totals, sums = stats[..., 0], stats[..., 1], stats[..., 2:]
    doc_top = jnp.max(tops, axis=0)
    factors = jnp.exp(tops - doc_top[None])
    doc_total = jnp.sum(totals * factors, axis=0)
    pooled_heads = jnp.sum(sums * factors[..., None], axis=0) / doc_total[:, :, None]
    pooled = pooled_heads.reshape(docs_count, student_width)
    middle = jnp.tanh(jnp.dot(pooled, s_mid, precision=highest) + s_mid_bias)
    logit_rows = jnp.dot(middle, s_cls, precision=highest) + s_cls_bias
    logit_top = jnp.max(logit_rows, axis=-1, keepdims=True)
    logit_exp = jnp.exp(logit_rows - logit_top)
    one_hot = (label_seq[:, None] == class_ids[None, :]).astype(f32)
    d_logits = logit_exp / jnp.sum(logit_exp, axis=-1, keepdims=True) - one_hot
    g_cls = jnp.dot(middle.T, d_logits, precision=highest)
    g_cls_bias = jnp.sum(d_logits, axis=0)
    d_middle = jnp.dot(d_logits, s_cls.T, precision=highest) * (1.0 - middle * middle)
    g_mid = jnp.dot(pooled.T, d_middle, precision=highest)
    g_mid_bias = jnp.sum(d_middle, axis=0)
    d_pooled = jnp.dot(d_middle, s_mid.T, precision=highest).reshape(docs_count, SH, SHD)
    shares = jnp.where(member, jnp.exp(masked - doc_top[None]), 0.0) / doc_total[None]
    d_share = jnp.einsum("dhk,thk->tdh", d_pooled, head_parts, precision=highest)
    base_term = jnp.sum(d_pooled * pooled_heads, axis=-1)
    d_pool_logit = jnp.sum(shares * (d_share - base_term[None]), axis=1)
    d_heads = jnp.einsum("tdh,dhk->thk", shares, d_pooled, precision=highest)
    d_heads = d_heads + d_pool_logit[:, :, None] * query_heads[None] * pool_scale
    g_query = (jnp.sum(d_pool_logit[:, :, None] * head_parts, axis=0) * pool_scale).reshape(-1)
    d_student = d_heads.reshape(own, student_width)
    g_sbias = jnp.sum(d_student, axis=0)
    g_sproj = jnp.dot(layer_out.astype(f32).T, d_student, precision=highest)

    d_q, d_kv = attn_bwd(bounds, queries, kv, q_rows, k_rows, lse, context, d_ctx, score_scale)
    at_seq = (jnp.arange(seqs) == row_index).astype(f32)[:, None]
    at_heads = (jnp.arange(cols) == col_index).astype(f32)[:, None, None]
    g_q_bias = jnp.sum(d_q.astype(f32), axis=(0, 2))
    g_v_bias = jnp.sum(d_kv[:, width_col:].astype(f32), axis=(0, 2))
    once = 1.0 / (parts * cols)
    small = (
        g_sproj,
        jnp.stack([g_q_bias, g_v_bias])[None] * at_heads,
        g_in_bias,
        g_out_bias,
        g_ln1_gain,
        g_ln1_bias,
        g_back_bias,
        g_ln2_gain,
        g_ln2_bias,
        g_sbias,
        g_query,
        g_mid * once,
        g_mid_bias * once,
        g_cls * once,
        logit_rows.reshape(1, -1) * (at_seq * once),
        g_cls_bias * once,
    )
    flat = jnp.concatenate([part.reshape(-1) for part in small])
    tall = -(-flat.shape[0] // (128 * 256)) * 256
    flat = jnp.pad(flat, (0, tall * 128 - flat.shape[0])).reshape(tall, 128)
    blocked = (cols, rows, parts, width_row // parts, -1)
    g_in, g_back, d_q, d_kv, flat = tail_fast(
        [g_in.astype(bf16).reshape(blocked), g_back.astype(bf16).reshape(blocked)],
        d_q,
        d_kv.reshape(cols, parts, 2 * width_col, own),
        flat,
        5,
    )
    flat = flat.reshape(-1)
    sums_all, at = [], 0
    for part in small:
        sums_all.append(flat[at : at + part.size].reshape(part.shape))
        at += part.size
    d_qkv = jnp.concatenate([d_kv, d_q], axis=1)
    g_qkv = jnp.einsum("dt,cnt->cdn", x_t, d_qkv, preferred_element_type=f32)
    d_tokens = jnp.einsum("cdn,cnt->dt", w_qkv_all, d_qkv, preferred_element_type=f32)
    d_tokens = (d_tokens + d_resid_one.T).astype(bf16)
    g_out = mm(ctx_t, d_attn, ((1,), (0,)))
    g_out = g_out.reshape(cols, width_col, rows, width_row).transpose(0, 2, 1, 3)
    g_attn = jnp.concatenate(
        [g_qkv.astype(bf16).reshape(cols, rows, width_row, 3 * width_col), g_out.astype(bf16)], axis=-1
    )
    g_attn, grad_tokens = last_fast([g_attn.reshape(blocked)], d_tokens, 6)
    g_in, g_back, g_attn = [part.reshape(width_row, -1).astype(f32) for part in (g_in, g_back, g_attn)]
    g_qkv = g_attn[:, : 3 * width_col].reshape(width_row, 3, heads_dev, HD)
    g_qkv = jnp.stack([g_qkv[:, 2], g_qkv[:, 0], g_qkv[:, 1]], axis=2).reshape(width_row, -1)

    def at_col(part):
        return lax.dynamic_index_in_dim(part, col_index, 0, False)

    def at_row(part):
        return lax.dynamic_slice_in_dim(part, row_index * width_row, width_row)

    (
        g_sproj, g_qkv_bias, g_in_bias, g_out_bias, g_ln1_gain, g_ln1_bias, g_back_bias, g_ln2_gain,
        g_ln2_bias, g_sbias, g_query, g_mid, g_mid_bias, g_cls, logits, g_cls_bias,
    ) = sums_all
    logits = lax.dynamic_slice_in_dim(logits, dp_index * (seqs // parts), seqs // parts)
    return (
        out,
        logits.reshape(seqs // parts, docs_count, class_count),
        grad_tokens.astype(f32),
        g_qkv,
        at_col(g_qkv_bias),
        g_attn[:, 3 * width_col :],
        at_row(g_out_bias),
        at_row(g_ln1_gain),
        at_row(g_ln1_bias),
        g_in,
        at_col(g_in_bias),
        g_back,
        at_row(g_back_bias),
        at_row(g_ln2_gain),
        at_row(g_ln2_bias),
        at_row(g_sproj),
        g_sbias,
        g_query,
        g_mid,
        g_mid_bias,
        g_cls,
        g_cls_bias,
    )


def solution(mesh):
    row, col = P("row"), P("col")
    grid, whole = P("row", "col"), P("dp", "row", "col")
    placed = (
        (whole, P("dp", None), P("dp", None), whole, grid, P(None, "col"), P("col", "row"))
        + (row, row, row, grid, col, grid, row, row, row, P("row", None))
        + (P(),) * 6
    )
    results = (
        (whole, P("dp", None, None), whole, grid, P(None, "col"), P("col", "row"))
        + (row, row, row, grid, col, grid, row, row, row, P("row", None))
        + (P(),) * 6
    )
    quick = dict(mesh.shape) == {"dp": 2, "row": 4, "col": 4}
    local = fast_local if quick else general_local
    return jax.shard_map(local, mesh=mesh, in_specs=placed, out_specs=results, check_vma=False)
```

```python
import functools
import jax
import jax.numpy as jnp
from jax import lax
from jax.experimental import pallas as pl
from jax.experimental.pallas import tpu as pltpu
from jax.sharding import PartitionSpec as P

HD = 64
SH = 2
SHD = 64

norm_eps = 1e-06
masked_value = -1e30
highest = lax.Precision.HIGHEST
f32 = jnp.float32
bf16 = jnp.bfloat16
WORLD = ("col", "row", "dp")


def sizes(seqs_local):
    parts = lax.axis_size("dp")
    rows = lax.axis_size("row")
    seqs = seqs_local * parts
    return parts, rows, lax.axis_size("col"), seqs, rows // seqs


def row_groups(rows, sub):
    return [list(range(at, at + sub)) for at in range(0, rows, sub)]


def take_in(values):
    parts, rows, _, seqs, sub = sizes(values.shape[0])
    held = lax.all_to_all(values, "dp", 2, 0, tiled=True)
    feats, half = held.shape[1:]
    held = held.reshape(seqs, feats, sub, half // sub).transpose(0, 2, 1, 3)
    held = held.reshape(rows, feats, half // sub)
    held = lax.all_to_all(held, "row", 0, 0, tiled=True)
    return held.reshape(rows * feats, half // sub)


def give_back(values, seqs_local):
    parts, rows, _, seqs, sub = sizes(seqs_local)
    width, own = values.shape
    feats = width // rows
    held = lax.all_to_all(values.reshape(rows, feats, own), "row", 0, 0, tiled=True)
    held = held.reshape(seqs, sub, feats, own).transpose(0, 2, 1, 3).reshape(seqs, feats, sub * own)
    return lax.all_to_all(held, "dp", 0, 2, tiled=True)


def gather_world(shard):
    cols, rows = lax.axis_size("col"), lax.axis_size("row")
    out = lax.all_gather(shard, WORLD, axis=0, tiled=True)
    return out.reshape(cols, rows, -1, shard.shape[1])


def own_half(block):
    parts = lax.axis_size("dp")
    amount = block.shape[0] // parts
    return lax.dynamic_slice_in_dim(block, lax.axis_index("dp") * amount, amount)


def scatter_world(full):
    flat = full.reshape(-1, full.shape[-1])
    mine = lax.psum_scatter(flat, WORLD, scatter_dimension=0, tiled=True)
    return lax.all_gather(mine, "dp", axis=0, tiled=True)


def swap_cols(values):
    return lax.all_to_all(values, "col", 0, 0, tiled=True)


def gather_sequence(values, sub):
    cols, own, width = values.shape
    held = values[:, None]
    if sub > 1:
        groups = row_groups(lax.axis_size("row"), sub)
        held = lax.all_gather(held, "row", axis=1, tiled=True, axis_index_groups=groups)
    held = lax.all_gather(held[:, None], "dp", axis=1, tiled=True)
    return held.reshape(-1, width)


def scatter_sequence(values, cols, sub):
    parts = lax.axis_size("dp")
    width = values.shape[-1]
    held = values.reshape(cols, parts, sub, -1, width)
    held = lax.psum_scatter(held, "dp", scatter_dimension=1, tiled=True)[:, 0]
    if sub > 1:
        groups = row_groups(lax.axis_size("row"), sub)
        held = lax.psum_scatter(
            held, "row", scatter_dimension=1, tiled=True, axis_index_groups=groups
        )
    return held[:, 0]


def normalize(values):
    mean_v = jnp.mean(values, axis=-1, keepdims=True)
    center = values - mean_v
    inv_std = lax.rsqrt(jnp.mean(center * center, axis=-1, keepdims=True) + norm_eps)
    return center * inv_std, inv_std


def normalize_back(grad_hat, normed, inv_std):
    return inv_std * (
        grad_hat
        - jnp.mean(grad_hat, axis=-1, keepdims=True)
        - normed * jnp.mean(grad_hat * normed, axis=-1, keepdims=True)
    )


def gelu_exact(values):
    return jax.nn.gelu(values, approximate=False)


def mm(a, b, contract):
    return lax.dot_general(a, b, (contract, ((), ())), preferred_element_type=f32)


def combine_pool(part_one, part_two):
    top_a, total_a, sum_a = part_one
    top_b, total_b, sum_b = part_two
    row_top = jnp.maximum(top_a, top_b)
    factor_a = jnp.exp(top_a - row_top)
    factor_b = jnp.exp(top_b - row_top)
    return (
        row_top,
        total_a * factor_a + total_b * factor_b,
        sum_a * factor_a[:, :, None] + sum_b * factor_b[:, :, None],
    )


def attend(q, k, v, q_seg, k_seg, scale):
    scores = jnp.einsum("qhd,khd->hqk", q, k, preferred_element_type=f32) * scale
    scores = jnp.where((q_seg[:, None] == k_seg[None, :])[None], scores, masked_value)
    top = jnp.max(scores, axis=-1, keepdims=True)
    exp_scores = jnp.exp(scores - top)
    total = jnp.sum(exp_scores, axis=-1, keepdims=True)
    probs = exp_scores / total
    context = jnp.einsum("hqk,khd->qhd", probs.astype(bf16), v, preferred_element_type=f32)
    return context.astype(bf16), probs


def attend_back(q, k, v, probs, d_ctx, scale):
    d_probs = jnp.einsum("qhd,khd->hqk", d_ctx, v, preferred_element_type=f32)
    delta = jnp.sum(probs * d_probs, axis=-1, keepdims=True)
    d_scores = (probs * (d_probs - delta)).astype(bf16)
    d_q = jnp.einsum("hqk,khd->qhd", d_scores, k, preferred_element_type=f32) * scale
    d_k = jnp.einsum("hqk,qhd->khd", d_scores, q, preferred_element_type=f32) * scale
    d_v = jnp.einsum("hqk,qhd->khd", probs.astype(bf16), d_ctx, preferred_element_type=f32)
    return d_q, d_k, d_v


def general_local(
    tokens,
    segments,
    labels,
    cotangent,
    w_qkv,
    b_qkv,
    w_out,
    b_out,
    ln1_gain,
    ln1_bias,
    w_in,
    b_in,
    w_back,
    b_back,
    ln2_gain,
    ln2_bias,
    s_proj,
    s_bias,
    s_query,
    s_mid,
    s_mid_bias,
    s_cls,
    s_cls_bias,
):
    seqs_local, width_row, cols_local = tokens.shape
    parts, rows, cols, seqs, sub = sizes(seqs_local)
    width = width_row * rows
    own = cols_local // (parts * sub)
    width_col = b_qkv.shape[1]
    heads_dev = width_col // HD
    hidden_col = b_in.shape[0]
    docs_count = labels.shape[1]
    class_count = s_cls.shape[1]
    student_width = s_proj.shape[1]
    row_index = lax.axis_index("row")
    col_index = lax.axis_index("col")
    dp_index = lax.axis_index("dp")
    seq_index = row_index // sub
    sub_index = row_index % sub
    score_scale = HD ** (-0.5)
    pool_scale = SHD ** (-0.5)
    query_heads = s_query.reshape(SH, SHD)
    doc_ids = jnp.arange(docs_count, dtype=jnp.int32)
    class_ids = jnp.arange(class_count, dtype=jnp.int32)

    w_qkv_all = gather_world(own_half(w_qkv)).reshape(cols, width, 3 * width_col)
    x_t = take_in(tokens)
    rest = jnp.concatenate([own_half(w_in), own_half(w_back), own_half(w_out).reshape(-1, width_col)], axis=1)
    rest_all = gather_world(rest)
    w_in_all = rest_all[..., :hidden_col].reshape(cols, width, hidden_col)
    w_back_all = rest_all[..., hidden_col : 2 * hidden_col].reshape(cols, width, hidden_col)
    w_out_all = rest_all[..., 2 * hidden_col :].reshape(cols, rows, width_col, width_row)
    w_out_all = w_out_all.transpose(0, 2, 1, 3).reshape(width, width)
    row_vectors = lax.all_gather(
        jnp.stack([b_out, ln1_gain, ln1_bias, b_back, ln2_gain, ln2_bias]), "row", axis=1, tiled=True
    )
    b_out_a, gain_one, bias_one, b_back_a, gain_two, bias_two = [row_vectors[i] for i in range(6)]
    b_qkv_all = lax.all_gather(b_qkv, "col")
    b_in_all = lax.all_gather(b_in, "col")
    s_proj_all = lax.all_gather(s_proj, "row", axis=0, tiled=True)
    whole_ints = lax.all_gather(jnp.concatenate([segments, labels], axis=1), "dp", axis=0, tiled=True)
    ints = lax.dynamic_index_in_dim(whole_ints, seq_index, 0, False)
    seq_len = segments.shape[1]
    seg_all, label_seq = ints[:seq_len], ints[seq_len:]
    seg_blocks = seg_all.reshape(cols, parts, sub, own)
    seg_q = lax.dynamic_index_in_dim(seg_blocks, dp_index, 1, False)
    seg_q = lax.dynamic_index_in_dim(seg_q, sub_index, 1, False)
    seg_own = lax.dynamic_index_in_dim(seg_q, col_index, 0, False)
    seg_q = seg_q.reshape(-1)

    x = x_t.T
    offsets = jnp.stack([b_qkv_all[:, 0], jnp.zeros_like(b_qkv_all[:, 0]), b_qkv_all[:, 1]], axis=1)
    offsets = offsets.reshape(cols, 3, heads_dev, HD).transpose(0, 2, 1, 3).reshape(cols, 1, -1)
    qkv = jnp.einsum("td,cdn->ctn", x, w_qkv_all, preferred_element_type=f32) + offsets
    qkv = swap_cols(qkv.astype(bf16)).reshape(cols, own, heads_dev, 3, HD)
    queries = qkv[:, :, :, 0].reshape(cols * own, heads_dev, HD)
    kv = gather_sequence(qkv[:, :, :, 1:].reshape(cols, own, -1), sub)
    kv = kv.reshape(seq_len, heads_dev, 2, HD)
    key_rows, value_rows = kv[:, :, 0], kv[:, :, 1]
    context, probs = attend(queries, key_rows, value_rows, seg_q, seg_all, score_scale)
    ctx = swap_cols(context.reshape(cols, own, width_col))
    ctx = ctx.transpose(1, 0, 2).reshape(own, width)

    attn_out = mm(ctx, w_out_all, ((1,), (0,))) + b_out_a
    normed_one, inv_one = normalize(x.astype(f32) + attn_out)
    hidden_one = normed_one * gain_one + bias_one
    hidden_low = hidden_one.astype(bf16)
    pre_act = jnp.einsum("td,cdn->ctn", hidden_low, w_in_all, preferred_element_type=f32)
    pre_act = pre_act + b_in_all[:, None, :]
    act = gelu_exact(pre_act).astype(bf16)
    ffn_out = jnp.einsum("ctn,cdn->td", act, w_back_all, preferred_element_type=f32) + b_back_a
    normed_two, inv_two = normalize(hidden_one + ffn_out)
    layer_out = (normed_two * gain_two + bias_two).astype(bf16)
    out = give_back(layer_out.T, seqs_local)

    student_h = mm(layer_out, s_proj_all, ((1,), (0,))) + s_bias
    head_parts = student_h.reshape(own, SH, SHD)
    pool_logit = jnp.sum(head_parts * query_heads, axis=-1) * pool_scale
    member = (seg_own[:, None] == doc_ids[None, :])[:, :, None]
    masked = jnp.where(member, pool_logit[:, None, :], masked_value)
    local_top = jnp.max(masked, axis=0)
    local_exp = jnp.where(member, jnp.exp(masked - local_top[None]), 0.0)
    local_total = jnp.sum(local_exp, axis=0)
    local_sum = jnp.einsum("tdh,thk->dhk", local_exp, head_parts, precision=highest)
    stats = jnp.concatenate([local_top[..., None], local_total[..., None], local_sum], axis=-1)
    stats = lax.all_gather(stats, ("dp", "col"))
    if sub > 1:
        stats = lax.all_gather(stats, "row", axis=0, tiled=True, axis_index_groups=row_groups(rows, sub))
    tops, totals, sums = stats[..., 0], stats[..., 1], stats[..., 2:]
    doc_top = jnp.max(tops, axis=0)
    factors = jnp.exp(tops - doc_top[None])
    doc_total = jnp.sum(totals * factors, axis=0)
    pooled_heads = jnp.sum(sums * factors[..., None], axis=0) / doc_total[:, :, None]
    pooled = pooled_heads.reshape(docs_count, student_width)
    middle = jnp.tanh(jnp.dot(pooled, s_mid, precision=highest) + s_mid_bias)
    logit_rows = jnp.dot(middle, s_cls, precision=highest) + s_cls_bias
    logits = lax.all_gather(logit_rows, "row")[::sub]
    logits = lax.dynamic_slice_in_dim(logits, dp_index * seqs_local, seqs_local)
    logit_top = jnp.max(logit_rows, axis=-1, keepdims=True)
    logit_exp = jnp.exp(logit_rows - logit_top)
    one_hot = (label_seq[:, None] == class_ids[None, :]).astype(f32)
    d_logits = logit_exp / jnp.sum(logit_exp, axis=-1, keepdims=True) - one_hot
    g_cls = jnp.dot(middle.T, d_logits, precision=highest)
    g_cls_bias = jnp.sum(d_logits, axis=0)
    d_middle = jnp.dot(d_logits, s_cls.T, precision=highest) * (1.0 - middle * middle)
    g_mid = jnp.dot(pooled.T, d_middle, precision=highest)
    g_mid_bias = jnp.sum(d_middle, axis=0)
    d_pooled = jnp.dot(d_middle, s_mid.T, precision=highest).reshape(docs_count, SH, SHD)
    shares = jnp.where(member, jnp.exp(masked - doc_top[None]), 0.0) / doc_total[None]
    d_share = jnp.einsum("dhk,thk->tdh", d_pooled, head_parts, precision=highest)
    base_term = jnp.sum(d_pooled * pooled_heads, axis=-1)
    d_pool_logit = jnp.sum(shares * (d_share - base_term[None]), axis=1)
    d_heads = jnp.einsum("tdh,dhk->thk", shares, d_pooled, precision=highest)
    d_heads = d_heads + d_pool_logit[:, :, None] * query_heads[None] * pool_scale
    g_query = (jnp.sum(d_pool_logit[:, :, None] * head_parts, axis=0) * pool_scale).reshape(-1)
    d_student = d_heads.reshape(own, student_width)
    g_sbias = jnp.sum(d_student, axis=0)
    g_sproj = jnp.dot(layer_out.astype(f32).T, d_student, precision=highest)

    d_out = take_in(cotangent).T.astype(f32)
    g_ln2_gain = jnp.sum(d_out * normed_two, axis=0)
    g_ln2_bias = jnp.sum(d_out, axis=0)
    d_resid_two = normalize_back(d_out * gain_two, normed_two, inv_two)
    d_ffn = d_resid_two.astype(bf16)
    g_back_bias = jnp.sum(d_ffn.astype(f32), axis=0)
    g_back = jnp.einsum("td,ctn->cdn", d_ffn, act, preferred_element_type=f32)
    d_act = jnp.einsum("td,cdn->ctn", d_ffn, w_back_all, preferred_element_type=f32)
    _, gelu_fn = jax.vjp(gelu_exact, pre_act)
    d_pre = gelu_fn(d_act)[0].astype(bf16)
    g_in_bias = jnp.sum(d_pre.astype(f32), axis=1)
    g_in = jnp.einsum("td,ctn->cdn", hidden_low, d_pre, preferred_element_type=f32)
    d_hidden_one = d_resid_two + jnp.einsum(
        "ctn,cdn->td", d_pre, w_in_all, preferred_element_type=f32
    )
    g_ln1_gain = jnp.sum(d_hidden_one * normed_one, axis=0)
    g_ln1_bias = jnp.sum(d_hidden_one, axis=0)
    d_resid_one = normalize_back(d_hidden_one * gain_one, normed_one, inv_one)
    d_attn = d_resid_one.astype(bf16)
    g_out_bias = jnp.sum(d_attn.astype(f32), axis=0)
    g_out = mm(ctx, d_attn, ((0,), (0,)))
    d_ctx = mm(d_attn, w_out_all, ((1,), (1,))).astype(bf16)
    d_ctx = swap_cols(d_ctx.reshape(own, cols, width_col).transpose(1, 0, 2))
    d_ctx = d_ctx.reshape(cols * own, heads_dev, HD)
    d_q, d_k, d_v = attend_back(queries, key_rows, value_rows, probs, d_ctx, score_scale)
    d_kv = jnp.stack([d_k, d_v], axis=2).astype(bf16).reshape(seq_len, -1)
    d_kv = scatter_sequence(d_kv, cols, sub).reshape(cols, own, heads_dev, 2, HD)
    d_q = d_q.astype(bf16).reshape(cols, own, heads_dev, 1, HD)
    d_qkv = jnp.concatenate([d_q, d_kv], axis=3).reshape(cols, own, 3 * width_col)
    d_qkv = swap_cols(d_qkv)
    g_qkv_bias = jnp.sum(d_qkv.astype(f32), axis=1).reshape(cols, heads_dev, 3, HD)
    g_qkv = jnp.einsum("td,ctn->cdn", x, d_qkv, preferred_element_type=f32)
    d_tokens = d_resid_one + jnp.einsum("ctn,cdn->td", d_qkv, w_qkv_all, preferred_element_type=f32)
    grad_tokens = give_back(d_tokens.astype(bf16).T, seqs_local).astype(f32)

    g_out = g_out.reshape(cols, width_col, rows, width_row).transpose(0, 2, 1, 3)
    g_out = g_out.reshape(cols, rows, width_row, width_col)
    model = jnp.concatenate(
        [
            g_in.reshape(cols, rows, width_row, hidden_col).astype(bf16),
            g_back.reshape(cols, rows, width_row, hidden_col).astype(bf16),
            g_out.astype(bf16),
        ],
        axis=-1,
    )
    model = scatter_world(model).astype(f32)
    g_qkv = scatter_world(g_qkv.reshape(cols, rows, width_row, 3 * width_col).astype(bf16)).astype(f32)
    once = 1.0 / (parts * cols * sub)
    small = (
        g_qkv_bias[:, :, 0].reshape(cols, width_col),
        g_qkv_bias[:, :, 2].reshape(cols, width_col),
        g_in_bias,
        g_out_bias,
        g_ln1_gain,
        g_ln1_bias,
        g_back_bias,
        g_ln2_gain,
        g_ln2_bias,
        g_sproj,
        g_sbias,
        g_query,
        g_mid * once,
        g_mid_bias * once,
        g_cls * once,
        g_cls_bias * once,
    )
    small = lax.psum(small, WORLD)

    def at_col(part):
        return lax.dynamic_index_in_dim(part, col_index, 0, False)

    def at_row(part):
        return lax.dynamic_slice_in_dim(part, row_index * width_row, width_row)

    return (
        out,
        logits,
        grad_tokens,
        g_qkv,
        jnp.stack([at_col(small[0]), at_col(small[1])]),
        model[:, 2 * hidden_col :].reshape(width_col, width_row),
        at_row(small[3]),
        at_row(small[4]),
        at_row(small[5]),
        model[:, :hidden_col],
        at_col(small[2]),
        model[:, hidden_col : 2 * hidden_col],
        at_row(small[6]),
        at_row(small[7]),
        at_row(small[8]),
        at_row(small[9]),
        small[10],
        small[11],
        small[12],
        small[13],
        small[14],
        small[15],
    )


MESH = pl.DeviceIdType.MESH
HBM = pl.BlockSpec(memory_space=pl.ANY)


def place():
    return lax.axis_index("dp"), lax.axis_index("row"), lax.axis_index("col")


def greet(peers, guarded=()):
    barrier = pltpu.get_barrier_semaphore()
    for peer in peers:
        pl.semaphore_signal(barrier, inc=1, device_id=peer, device_id_type=MESH)
    for there, peer in guarded:

        @pl.when(there)
        def _():
            pl.semaphore_signal(barrier, inc=1, device_id=peer, device_id_type=MESH)

    amount = len(peers)
    for there, _ in guarded:
        amount = amount + there.astype(jnp.int32)
    pl.semaphore_wait(barrier, amount)


def rcopy(src, dst, send, recv, peer):
    return pltpu.make_async_remote_copy(
        src_ref=src, dst_ref=dst, send_sem=send, recv_sem=recv, device_id=peer, device_id_type=MESH
    )


def take_copies(src, out, local, send, recv):
    d, r, c = place()
    own = out.shape[2]
    moves = []
    for i in range(2):
        for far in range(2):
            row, core = 2 * d + i, d ^ far
            piece = src.at[i, :, pl.ds(pl.multiple_of(core * own, own), own)]
            here = (row == r) if far == 0 else None

            def start(piece=piece, row=row, core=core, slot=2 * i + far, here=here):
                def away():
                    rcopy(piece, out.at[r], send.at[slot], recv.at[r], (core, row, c)).start()

                if here is None:
                    away()
                else:
                    pl.when(jnp.logical_not(here))(away)

                    @pl.when(here)
                    def _():
                        pltpu.make_async_copy(piece, out.at[r], local).start()

            def wait(piece=piece, row=row, core=core, slot=2 * i + far, here=here):
                def away():
                    rcopy(piece, out.at[r], send.at[slot], recv.at[r], (core, row, c)).wait_send()

                if here is None:
                    away()
                else:
                    pl.when(jnp.logical_not(here))(away)

                    @pl.when(here)
                    def _():
                        pltpu.make_async_copy(piece, out.at[r], local).wait()

            moves.append((start, wait))
    for row in range(4):

        def arrive(row=row):
            @pl.when(jnp.logical_not((row == r) & (r // 2 == d)))
            def _():
                piece = src.at[0, :, pl.ds(0, own)]
                rcopy(piece, out.at[row], send.at[0], recv.at[row], (d, r, c)).wait_recv()

        moves.append((lambda: None, arrive))
    return moves


def gather_kernel(kinds, *refs):
    shards, refs = refs[:kinds], refs[kinds:]
    (tok, ints), refs = refs[:2], refs[2:]
    outs, refs = refs[:kinds], refs[kinds:]
    (tok_out, ints_out, q_out, kv_out, wo_out), refs = refs[:5], refs[5:]
    (x_nat, q_src, kv_src), refs = refs[:3], refs[3:]
    own_sem, zs, zr, xs, xr, ys, yr, cs, cr, ps, pr, tl, ts, tr, il, hs, hr, hps, hpr = refs
    d, r, c = place()
    cols = 4
    xn, yn, pn = (d, r ^ 1, c), (d, r ^ 2, c), (1 - d, r, c)
    up, down = (d, r, c + 1), (d, r, c - 1)
    has_up, has_down = c < cols - 1, c > 0
    greet(plane_peers() + [(d, r, c ^ j) for j in (1, 2, 3)])
    moves = take_copies(tok, tok_out, tl, ts, tr)
    for start, _ in moves:
        start()
    pltpu.make_async_copy(ints, ints_out.at[d], il.at[0]).start()
    rcopy(ints, ints_out.at[d], il.at[1], il.at[2], pn).start()
    halves = [shard.shape[0] // 2 for shard in shards]

    def z_send(k, at, way, hop):
        src = shards[k] if hop == 1 else outs[k].at[at, r, d]
        return rcopy(
            src, outs[k].at[at, r, d], zs.at[k, way, hop - 1], zr.at[k, way, hop - 1], up if way == 0 else down
        )

    def src_of(k, at, own):
        return shards[k] if own else outs[k].at[at, r, d]

    def to_x(k, at, own):
        return rcopy(src_of(k, at, own), outs[k].at[at, r, d], xs.at[k, at], xr.at[k, at], xn)

    def to_y(k, at, own):
        return rcopy(src_of(k, at, own), outs[k].at[at, r, d], ys.at[k, at], yr.at[k, at], yn)

    def to_p(k, at, own):
        return rcopy(src_of(k, at, own), outs[k].at[at, r, d], ps.at[k, at, 0], pr.at[k, at, 0], pn)

    def relay(k, at, which):
        row = r ^ 1 if which == 0 else r ^ 2
        ref = outs[k].at[at, row, d, pl.ds(which * halves[k], halves[k])]
        return rcopy(ref, ref, cs.at[k, at, which], cr.at[k, at, which], yn if which == 0 else xn)

    def pass_p(k, at, bit):
        ref = outs[k].at[at, r ^ bit, d]
        return rcopy(ref, ref, ps.at[k, at, bit], pr.at[k, at, bit], pn)

    def got_x(k, at):
        ref = outs[k].at[at, r ^ 1, d]
        rcopy(ref, ref, xs.at[k, at], xr.at[k, at], xn).wait_recv()

    def got_y(k, at):
        ref = outs[k].at[at, r ^ 2, d]
        rcopy(ref, ref, ys.at[k, at], yr.at[k, at], yn).wait_recv()

    def got_corner(k, at):
        for which in range(2):
            ref = outs[k].at[at, r ^ 3, d, pl.ds(which * halves[k], halves[k])]
            rcopy(ref, ref, cs.at[k, at, which], cr.at[k, at, which], xn).wait_recv()

    def got_p(k, at, bit):
        ref = outs[k].at[at, r ^ bit, 1 - d]
        rcopy(ref, ref, ps.at[k, at, bit], pr.at[k, at, bit], pn).wait_recv()

    for k in range(kinds):
        pltpu.make_async_copy(shards[k], outs[k].at[c, r, d], own_sem.at[k]).start()

        @pl.when(has_up)
        def _():
            z_send(k, c, 0, 1).start()

        @pl.when(has_down)
        def _():
            z_send(k, c, 1, 1).start()

    def spread(k, at, own):
        to_x(k, at, own).start()
        to_y(k, at, own).start()
        to_p(k, at, own).start()

    def onward(k, at):
        got_x(k, at)
        relay(k, at, 0).start()
        pass_p(k, at, 1).start()
        got_y(k, at)
        relay(k, at, 1).start()
        pass_p(k, at, 2).start()

    steps = [(0, 0)] + [(way, hop) for hop in (1, 2, 3) for way in (0, 1)]
    jobs = [(k, way, hop) for k in range(kinds) for way, hop in steps]

    def at_of(way, hop):
        return c - hop if way == 0 else c + hop

    def valid(way, hop):
        return c >= hop if way == 0 else c + hop < cols

    def guard(way, hop, body):
        if hop == 0:
            body()
        else:
            pl.when(valid(way, hop))(body)

    def first(k, way, hop):
        def body():
            at = at_of(way, hop)
            if hop:
                z_send(k, at, way, hop).wait_recv()
                if hop < 3:
                    can = has_up if way == 0 else has_down

                    @pl.when(can)
                    def _():
                        z_send(k, at, way, hop + 1).start()

            spread(k, at, hop == 0)

        guard(way, hop, body)

    def second(k, way, hop):
        guard(way, hop, lambda: onward(k, at_of(way, hop)))

    def third(k, way, hop):
        def body():
            at = at_of(way, hop)
            got_corner(k, at)
            pass_p(k, at, 3).start()

        guard(way, hop, body)

    def settle(k):
        pltpu.make_async_copy(shards[k], outs[k].at[c, r, d], own_sem.at[k]).wait()
        for way, hop in steps:

            def body():
                for bit in range(4):
                    got_p(k, at_of(way, hop), bit)

            guard(way, hop, body)

    def kv(j):
        return rcopy(kv_src.at[c ^ j], kv_out.at[c, d], hs.at[0, j], hr.at[0, j], (d, r, c ^ j))

    def q(j):
        return rcopy(q_src.at[c ^ j], q_out.at[c], hs.at[1, j], hr.at[1, j], (d, r, c ^ j))

    def pair(j):
        src = kv_src.at[c] if j == 0 else kv_out.at[c ^ j, d]
        return rcopy(src, kv_out.at[c ^ j, d], hps.at[j], hpr.at[j], pn)

    deep = kv_src.shape[1]
    out_cols = deep + q_src.shape[1]
    lanes = -(-out_cols // 128) * 128

    def prepare():
        for _, wait in moves:
            wait()
        feats = tok_out.shape[1]
        x_nat[...] = tok_out[...].reshape(4 * feats, -1).astype(f32).T.astype(bf16)

    def project(j):
        to = c ^ j
        weights = outs[0][to, :, :, :, :lanes].reshape(-1, lanes)
        bias = outs[1][to, r, 0, pl.ds(0, 8)]
        bias = jnp.concatenate([bias[i : i + 1] for i in range(lanes // 128)], axis=1)
        made = jnp.dot(x_nat[...], weights, preferred_element_type=f32) + bias
        made = made.T.astype(bf16)
        kv_src[to] = made[:deep]
        q_src[to] = made[deep:out_cols]
        if j:
            kv(j).start()
            q(j).start()
        else:
            pair(0).start()
            kv_out[c, d] = kv_src[c]
            q_out[c] = q_src[c]

    def spread_out(at):
        feats = tok_out.shape[1]
        for row in range(4):
            block = outs[0][at, row, :, :, out_cols:].reshape(-1, feats)
            wo_out[pl.ds(at * wide, wide), row * feats : (row + 1) * feats] = block

    wide = q_src.shape[1]
    lag = 3
    ready = 2 * len(steps) + 2 * lag
    for i in range(len(jobs) + 2 * lag):
        if i == ready:
            prepare()
            settle(0)
            settle(1)
        if ready <= i < ready + 4:
            project((3, 2, 1, 0)[i - ready])
        if ready + 4 <= i < ready + 8:
            spread_out(i - ready - 4)
        if i < len(jobs):
            first(*jobs[i])
        if 0 <= i - lag < len(jobs):
            second(*jobs[i - lag])
        if 0 <= i - 2 * lag < len(jobs):
            third(*jobs[i - 2 * lag])

    for j in (1, 2, 3):
        kv(j).wait_recv()
        pair(j).start()
    for k in range(kinds):
        if k > 1:
            settle(k)
        for way, hop in steps:

            def body():
                at = at_of(way, hop)
                own = hop == 0
                to_x(k, at, own).wait_send()
                to_y(k, at, own).wait_send()
                to_p(k, at, own).wait_send()
                for which in range(2):
                    relay(k, at, which).wait_send()
                for bit in (1, 2, 3):
                    pass_p(k, at, bit).wait_send()
                if hop < 3:
                    if own:

                        @pl.when(has_up)
                        def _():
                            z_send(k, c, 0, 1).wait_send()

                        @pl.when(has_down)
                        def _():
                            z_send(k, c, 1, 1).wait_send()
                    else:
                        can = has_up if way == 0 else has_down

                        @pl.when(can)
                        def _():
                            z_send(k, at, way, hop + 1).wait_send()

            guard(way, hop, body)
    for j in (1, 2, 3):
        q(j).wait()
        kv(j).wait_send()
    for j in range(4):
        pair(j).wait()
    pltpu.make_async_copy(ints, ints_out.at[d], il.at[0]).wait()
    rcopy(ints, ints_out.at[1 - d], il.at[1], il.at[2], pn).wait()


VM = pl.BlockSpec(memory_space=pltpu.VMEM)


def gather_fast(shards, tokens, ints, wide, cid):
    kinds = len(shards)
    dma = pltpu.SemaphoreType.DMA
    _, feats, cols = tokens.shape
    own = cols // 2
    piece = jax.ShapeDtypeStruct((4, wide, own), bf16)
    return pl.pallas_call(
        functools.partial(gather_kernel, kinds),
        out_shape=[jax.ShapeDtypeStruct((4, 4, 2) + s.shape, s.dtype) for s in shards]
        + [
            jax.ShapeDtypeStruct((4, feats, own), tokens.dtype),
            jax.ShapeDtypeStruct((2,) + ints.shape, ints.dtype),
            piece,
            jax.ShapeDtypeStruct((4, 2, 2 * wide, own), bf16),
            jax.ShapeDtypeStruct((4 * wide, 4 * feats), bf16),
        ],
        in_specs=[HBM] * (kinds + 2),
        out_specs=[VM, VM] + [HBM] * (kinds - 2) + [VM, HBM, VM, VM, VM],
        scratch_shapes=[
            pltpu.VMEM((own, 4 * feats), bf16),
            pltpu.VMEM((4, wide, own), bf16),
            pltpu.VMEM((4, 2 * wide, own), bf16),
            dma((kinds,)),
            dma((kinds, 2, 3)), dma((kinds, 2, 3)),
            dma((kinds, 4)), dma((kinds, 4)),
            dma((kinds, 4)), dma((kinds, 4)),
            dma((kinds, 4, 2)), dma((kinds, 4, 2)),
            dma((kinds, 4, 4)), dma((kinds, 4, 4)),
            dma, dma((4,)), dma((4,)), dma((3,)),
            dma((2, 4)), dma((2, 4)), dma((4,)), dma((4,)),
        ],
        compiler_params=pltpu.CompilerParams(
            collective_id=cid, has_side_effects=True, vmem_limit_bytes=40 * 1024 * 1024
        ),
        name="head",
    )(*shards, tokens, ints)


def scatter_core(grads, outs, scratch, begin, during, late=0):
    kinds = len(grads)
    (acc, precv, xr1, yr1, xr2, yr2, zup, zdn, fin) = scratch[:9]
    (ls, ps, pr, xs1, xm1, ys1, ym1, xs2, xm2, ys2, ym2, us, um, ds, dm, fs, fm, os) = scratch[9:]
    d, r, c = place()
    cols = 4
    chunks = kinds * cols
    xn, yn, pn = (d, r ^ 1, c), (d, r ^ 2, c), (1 - d, r, c)
    up, down = (d, r, c + 1), (d, r, c - 1)
    half = acc.shape[2] // 2
    first, last = pl.ds(0, half), pl.ds(half, half)

    def split(i):
        k = i // cols
        j = i - k * cols
        at = jnp.where(j == 0, 0, jnp.where(j == 1, 3, j - 1))
        return k, at

    def at_static(i):
        return i // cols, (0, 3, 1, 2)[i % cols]

    def load(i):
        k, at = at_static(i)
        return pltpu.make_async_copy(grads[k].at[at, :, d], acc.at[i], ls.at[i])

    def pair(i):
        k, at = at_static(i)
        return rcopy(grads[k].at[at, :, 1 - d], precv.at[i], ps.at[i], pr.at[i], pn)

    def launch(i):
        pair(i).start()
        load(i).start()

    for i in range((kinds - late) * cols):
        launch(i)
    begin()

    def x1(i, j):
        return rcopy(acc.at[i, r ^ 1 ^ (2 * j), first], xr1.at[i, j], xs1.at[i, j], xm1.at[i, j], xn)

    def y1(i, j):
        return rcopy(acc.at[i, r ^ 2 ^ j, last], yr1.at[i, j], ys1.at[i, j], ym1.at[i, j], yn)

    def y2(i):
        return rcopy(acc.at[i, r ^ 2, first], yr2.at[i], ys2.at[i], ym2.at[i], yn)

    def x2(i):
        return rcopy(acc.at[i, r ^ 1, last], xr2.at[i], xs2.at[i], xm2.at[i], xn)

    def to_up(i):
        return rcopy(acc.at[i, r], zup.at[i], us.at[i], um.at[i], up)

    def to_down(i):
        return rcopy(acc.at[i, r], zdn.at[i], ds.at[i], dm.at[i], down)

    def stage1(i):
        pltpu.make_async_copy(precv.at[i], acc.at[i], ls.at[i]).wait()
        rcopy(acc.at[i], precv.at[i], ps.at[i], pr.at[i], pn).wait_recv()

        @pl.loop(0, 4)
        def _(row):
            acc[i, row] = acc[i, row] + precv[i, row]

        x1(i, 1).start()
        y1(i, 1).start()
        x1(i, 0).start()
        y1(i, 0).start()

    def stage2(i):
        x1(i, 1).wait_recv()
        acc[i, r ^ 2, first] = acc[i, r ^ 2, first] + xr1[i, 1]
        y2(i).start()
        y1(i, 1).wait_recv()
        acc[i, r ^ 1, last] = acc[i, r ^ 1, last] + yr1[i, 1]
        x2(i).start()
        x1(i, 0).wait_recv()
        acc[i, r, first] = acc[i, r, first] + xr1[i, 0]
        y1(i, 0).wait_recv()
        acc[i, r, last] = acc[i, r, last] + yr1[i, 0]

    def stage3(i):
        y2(i).wait_recv()
        acc[i, r, first] = acc[i, r, first] + yr2[i]
        x2(i).wait_recv()
        acc[i, r, last] = acc[i, r, last] + xr2[i]

    def stage4(i, hops):
        k, at = split(i)

        @pl.when((at > c) & (c == hops))
        def _():
            @pl.when(c > 0)
            def _():
                to_up(i).wait_recv()
                acc[i, r] = acc[i, r] + zup[i]

            to_up(i).start()

        @pl.when((at < c) & (cols - 1 - c == hops))
        def _():
            @pl.when(c < cols - 1)
            def _():
                to_down(i).wait_recv()
                acc[i, r] = acc[i, r] + zdn[i]

            to_down(i).start()

        @pl.when((at == c) & (jnp.maximum(c, cols - 1 - c) == hops))
        def _():
            @pl.when(c > 0)
            def _():
                to_up(i).wait_recv()
                acc[i, r] = acc[i, r] + zup[i]

            @pl.when(c < cols - 1)
            def _():
                to_down(i).wait_recv()
                acc[i, r] = acc[i, r] + zdn[i]

            fin[k, d] = acc[i, r]
            rcopy(fin.at[k, d], fin.at[k, d], fs.at[k], fm.at[k], pn).start()

    stages = [(0, stage1), (2, stage2), (4, stage3)]
    stages += [(5 + h, functools.partial(lambda h, i: stage4(i, h), h)) for h in range(cols)]
    ending = stages[-1][0]

    assert len(during) <= chunks + ending

    @pl.loop(0, chunks + ending)
    def _(step):
        for i, extra in enumerate(during):
            pl.when(step == i)(functools.partial(extra, launch))

        for lag, stage in stages:

            @pl.when((step >= lag) & (step - lag < chunks))
            def _():
                stage(step - lag)

    @pl.loop(0, chunks)
    def _(i):
        k, at = split(i)
        rcopy(acc.at[i], precv.at[i], ps.at[i], pr.at[i], pn).wait_send()
        for j in range(2):
            x1(i, j).wait_send()
            y1(i, j).wait_send()
        y2(i).wait_send()
        x2(i).wait_send()

        @pl.when(at > c)
        def _():
            to_up(i).wait_send()

        @pl.when(at < c)
        def _():
            to_down(i).wait_send()

    for k in range(kinds):
        rcopy(fin.at[k, 1 - d], fin.at[k, 1 - d], fs.at[k], fm.at[k], pn).wait()
        pltpu.make_async_copy(fin.at[k], outs[k], os.at[k]).start()
    for k in range(kinds):
        pltpu.make_async_copy(fin.at[k], outs[k], os.at[k]).wait()

def scatter_scratch(kinds, n, w, dt):
    dma = pltpu.SemaphoreType.DMA
    chunks = kinds * 4
    return [
        pltpu.VMEM((chunks, 4, n, w), dt),
        pltpu.VMEM((chunks, 4, n, w), dt),
        pltpu.VMEM((chunks, 2, n // 2, w), dt),
        pltpu.VMEM((chunks, 2, n // 2, w), dt),
        pltpu.VMEM((chunks, n // 2, w), dt),
        pltpu.VMEM((chunks, n // 2, w), dt),
        pltpu.VMEM((chunks, n, w), dt),
        pltpu.VMEM((chunks, n, w), dt),
        pltpu.VMEM((kinds, 2, n, w), dt),
        dma((chunks,)), dma((chunks,)), dma((chunks,)),
        dma((chunks, 2)), dma((chunks, 2)), dma((chunks, 2)), dma((chunks, 2)),
        dma((chunks,)), dma((chunks,)), dma((chunks,)), dma((chunks,)),
        dma((chunks,)), dma((chunks,)), dma((chunks,)), dma((chunks,)),
        dma((kinds,)), dma((kinds,)), dma((kinds,)),
    ]


def give_moves(src_ref, out_ref, local, send, recv):
    d, r, c = place()
    own = src_ref.shape[2]
    home = r // 2

    def slot(i, core):
        return out_ref.at[i, :, pl.ds(pl.multiple_of(core * own, own), own)]

    def move(row):
        return rcopy(src_ref.at[row], slot(r % 2, d), send.at[row], recv.at[r % 2, d], (home, row, c))

    def stay():
        return pltpu.make_async_copy(src_ref.at[r], slot(r % 2, d), local)

    def start():
        for row in range(4):

            @pl.when(jnp.logical_not((row == r) & (home == d)))
            def _():
                move(row).start()

        @pl.when(home == d)
        def _():
            stay().start()

    def finish():
        for row in range(4):

            @pl.when(jnp.logical_not((row == r) & (home == d)))
            def _():
                move(row).wait_send()

        @pl.when(home == d)
        def _():
            stay().wait()

        for i in range(2):
            for core in range(2):

                @pl.when(jnp.logical_not((2 * d + i == r) & (core == d)))
                def _():
                    rcopy(src_ref.at[0], slot(i, core), send.at[0], recv.at[i, core], (d, r, c)).wait_recv()

    return start, finish


def plane_peers():
    d, r, c = place()
    return [(d ^ (j // 4), r ^ (j % 4), c) for j in range(1, 8)]


def line_peers():
    d, r, c = place()
    return [(d ^ (j // 4), r, c ^ (j % 4)) for j in range(1, 8)]


def swap_kernel(src, cot, out, cot_out, send, recv, tl, ts, tr):
    d, r, c = place()
    greet(plane_peers() + [(d, r, c ^ j) for j in (1, 2, 3)])

    def move(j):
        return rcopy(src.at[c ^ j], out.at[c], send.at[j], recv.at[j], (d, r, c ^ j))

    for j in (3, 2, 1):
        move(j).start()
    moves = take_copies(cot, cot_out, tl, ts, tr)
    for start, _ in moves:
        start()
    out[c] = src[c]
    for j in (1, 2, 3):
        move(j).wait()
    for _, wait in moves:
        wait()


def swap_fast(values, cotangent, cid):
    dma = pltpu.SemaphoreType.DMA
    _, feats, cols = cotangent.shape
    return pl.pallas_call(
        swap_kernel,
        out_shape=[
            jax.ShapeDtypeStruct(values.shape, values.dtype),
            jax.ShapeDtypeStruct((4, feats, cols // 2), cotangent.dtype),
        ],
        in_specs=[VM, HBM],
        out_specs=[VM, VM],
        scratch_shapes=[dma((4,)), dma((4,)), dma, dma((4,)), dma((4,))],
        compiler_params=pltpu.CompilerParams(collective_id=cid, has_side_effects=True),
        name="swap",
    )(values, cotangent)


def turn_kernel(ctx_ref, stats_ref, give_ref, ctx_out, stats_out, give_out, send, recv, ssend, srecv, gl, gs, gr):
    d, r, c = place()
    peers = line_peers()
    greet(plane_peers() + peers[:3] + peers[4:])

    def move(j):
        return rcopy(ctx_ref.at[c ^ j], ctx_out.at[c], send.at[j], recv.at[j], (d, r, c ^ j))

    def tell(j):
        return rcopy(stats_ref, stats_out.at[d, c], ssend.at[j - 1], srecv.at[j - 1], peers[j - 1])

    for j in range(1, 8):
        tell(j).start()
    for j in (3, 2, 1):
        move(j).start()
    start, finish = give_moves(give_ref, give_out, gl, gs, gr)
    start()
    ctx_out[c] = ctx_ref[c]
    stats_out[d, c] = stats_ref[...]
    for j in range(1, 8):
        tell(j).wait()
    for j in (1, 2, 3):
        move(j).wait()
    finish()


def turn_fast(d_ctx, stats, out_t, cid):
    width, own = out_t.shape
    dma = pltpu.SemaphoreType.DMA
    return pl.pallas_call(
        turn_kernel,
        out_shape=[
            jax.ShapeDtypeStruct(d_ctx.shape, d_ctx.dtype),
            jax.ShapeDtypeStruct((2, 4) + stats.shape, stats.dtype),
            jax.ShapeDtypeStruct((2, width // 4, 2 * own), out_t.dtype),
        ],
        in_specs=[VM, VM, HBM],
        out_specs=[VM, VM, HBM],
        scratch_shapes=[dma((4,)), dma((4,)), dma((7,)), dma((7,)), dma, dma((4,)), dma((2, 2))],
        compiler_params=pltpu.CompilerParams(collective_id=cid, has_side_effects=True),
        name="turn",
    )(d_ctx, stats, out_t.reshape(4, width // 4, own))


def sum_steps(src, total, parts, sems):
    d, r, c = place()
    peers = [(1 - d, r, c), (d, r ^ 1, c), (d, r ^ 2, c), (d, r, c ^ 1), (d, r, c ^ 2)]
    bits = [d, r % 2, r // 2, c % 2, c // 2]
    rs, rr, gs, gr = sems
    count = len(peers)
    size = [src.shape[0] >> (i + 1) for i in range(count)]
    offset = [jnp.int32(0)]
    for i in range(count):
        offset.append(offset[i] + bits[i] * size[i])

    def rows(at, amount):
        return pl.ds(pl.multiple_of(at, 8), amount)

    def down(i):
        other = offset[i] + (1 - bits[i]) * size[i]
        held = src if i == 0 else parts[i - 1]
        at = other if i == 0 else other - offset[i]
        return rcopy(held.at[rows(at, size[i])], parts[count + i], rs.at[i], rr.at[i], peers[i])

    def fold(i):
        down(i).wait_recv()
        held = src if i == 0 else parts[i - 1]
        at = offset[i + 1] if i == 0 else offset[i + 1] - offset[i]
        parts[i][...] = held[rows(at, size[i])] + parts[count + i][...]

    def back(i):
        spot = total.at[rows(offset[i + 1], size[i])]
        return rcopy(spot, spot, gs.at[i], gr.at[i], peers[i])

    def back_recv(i):
        spot = total.at[rows(offset[i] + (1 - bits[i]) * size[i], size[i])]
        rcopy(spot, spot, gs.at[i], gr.at[i], peers[i]).wait_recv()

    steps = [lambda: down(0).start()]
    for i in range(1, count):

        def step(i=i):
            fold(i - 1)
            down(i).start()

        steps.append(step)

    def middle():
        fold(count - 1)
        total[rows(offset[count], size[-1])] = parts[count - 1][...]
        back(count - 1).start()

    steps.append(middle)
    for i in range(count - 2, -1, -1):

        def step(i=i):
            back_recv(i + 1)
            back(i).start()

        steps.append(step)

    def end():
        back_recv(0)
        for i in range(count):
            down(i).wait_send()
            back(i).wait_send()

    return steps, end


def both(one, two):
    def run(launch):
        one()
        two(launch)

    return run


def tail_kernel(kinds, *refs):
    grads, refs = refs[:kinds], refs[kinds:]
    (q_ref, kv_ref, small_ref, x_ref, ctx_ref, resid_ref, w_ref), refs = refs[:7], refs[7:]
    outs, refs = refs[: kinds + 1], refs[kinds + 1 :]
    (give_out, small_out), refs = refs[:2], refs[2:]
    (total, theirs, dqkv, own_grads, dpad, weights, resid_t, give_src), refs = refs[:8], refs[8:]
    parts, refs = refs[:10], refs[10:]
    (send, recv, psend, precv), sems, (wl, gl, gs, gr), scratch = refs[:4], refs[4:8], refs[8:12], refs[12:]
    d, r, c = place()
    pn = (1 - d, r, c)
    deep, wide = kv_ref.shape[2], q_ref.shape[1]
    full = dqkv.shape[1]
    kv_rows, q_rows = pl.ds(0, deep), pl.ds(deep, wide)
    greet(plane_peers() + [(d, r, c ^ j) for j in (1, 2, 3)])

    def pair(j):
        return rcopy(kv_ref.at[c ^ j, 1 - d], theirs.at[c ^ j], psend.at[j], precv.at[j], pn)

    def kv(j):
        return rcopy(total.at[c ^ j], dqkv.at[c, kv_rows], send.at[0, j], recv.at[0, j], (d, r, c ^ j))

    def q(j):
        return rcopy(q_ref.at[c ^ j], dqkv.at[c, q_rows], send.at[1, j], recv.at[1, j], (d, r, c ^ j))

    for j in (3, 2, 1, 0):
        pair(j).start()
    for j in (3, 2, 1):
        q(j).start()
    load_w = pltpu.make_async_copy(w_ref, weights, wl)
    load_w.start()
    steps, end = sum_steps(small_ref, small_out, parts, sems)
    start, finish = give_moves(give_src, give_out, gl, gs, gr)

    def begin():
        for j in (3, 2, 1):
            pair(j).wait_recv()
            total[c ^ j] = kv_ref[c ^ j, d] + theirs[c ^ j]
            kv(j).start()
        pair(0).wait_recv()
        dqkv[c, kv_rows] = kv_ref[c, d] + theirs[c]
        dqkv[c, q_rows] = q_ref[c]
        spare = full - deep - wide
        for at in range(4):
            dqkv[at, pl.ds(deep + wide, spare)] = jnp.zeros((spare, dqkv.shape[2]), bf16)
        resid_t[...] = resid_ref[...].T
        feats = x_ref.shape[1]
        blank = dpad.shape[1] - feats
        for row in range(4):
            dpad[row, pl.ds(0, blank)] = jnp.zeros((blank, dpad.shape[2]), bf16)
            dpad[row, pl.ds(blank, feats)] = resid_t[pl.ds(row * feats, feats)].astype(bf16)

    across = (((1,), (1,)), ((), ()))

    def arrived():
        for j in (1, 2, 3):
            q(j).wait_recv()
            kv(j).wait_recv()

    def make(at):
        lead = full - dpad.shape[1]

        @pl.loop(0, 4)
        def _(row):
            one = lax.dot_general(x_ref[row], dqkv[at], across, preferred_element_type=f32)
            two = lax.dot_general(ctx_ref[at], dpad[row], across, preferred_element_type=f32)
            shape = own_grads.shape[2:4] + (-1,)
            own_grads[at, row, :, :, :lead] = one[:, :lead].astype(bf16).reshape(shape)
            own_grads[at, row, :, :, lead:] = (one[:, lead:] + two).astype(bf16).reshape(shape)

    def input_grad(launch):
        load_w.wait()
        feats = x_ref.shape[1]

        @pl.loop(0, 4)
        def _(row):
            rows = pl.ds(pl.multiple_of(row * feats, 8), feats)
            part = resid_t[rows]
            for at in range(4):
                w = weights[at, row].reshape(feats, full)
                part = part + jnp.dot(w, dqkv[at], preferred_element_type=f32)
            give_src[row] = part.astype(bf16)

        start()

    first = 4
    extras = [lambda launch: None] * first
    for j, at in enumerate((0, 3, 1, 2)):

        def extra(launch, j=j, at=at):
            if j == 0:
                arrived()
            make(at)
            launch(kinds * 4 + j)

        extras.append(extra)
    extras.append(input_grad)
    extras += [lambda launch: None] * (len(steps) - len(extras))
    during = [both(step, extra) for step, extra in zip(steps, extras)]
    scatter_core(list(grads) + [own_grads], outs, scratch, begin, during, late=1)
    end()
    finish()
    for j in range(4):
        pair(j).wait_send()
    for j in (1, 2, 3):
        q(j).wait_send()
        kv(j).wait_send()


def tail_fast(grads, q, kv, small, x_t, ctx_t, resid, w_attn, cid):
    kinds = len(grads)
    n, w = grads[0].shape[3:]
    dma = pltpu.SemaphoreType.DMA
    cols, _, wide, own = kv.shape
    feats = x_t.shape[1]
    parts = [pltpu.VMEM((small.shape[0] >> (i + 1), small.shape[1]), f32) for i in range(5)]
    return pl.pallas_call(
        functools.partial(tail_kernel, kinds),
        out_shape=[jax.ShapeDtypeStruct((2, n, w), bf16)] * (kinds + 1)
        + [
            jax.ShapeDtypeStruct((2, feats, 2 * own), bf16),
            jax.ShapeDtypeStruct(small.shape, f32),
        ],
        in_specs=[HBM] * kinds + [VM] * 6 + [HBM],
        out_specs=[HBM] * (kinds + 1) + [HBM, VM],
        scratch_shapes=[
            pltpu.VMEM((cols, wide, own), bf16),
            pltpu.VMEM((cols, wide, own), bf16),
            pltpu.VMEM((cols, w, own), bf16),
            pltpu.VMEM((4, 4, 2, n, w), bf16),
            pltpu.VMEM((4, 256, own), bf16),
            pltpu.VMEM((4, 4, 2, n, w), bf16),
            pltpu.VMEM((4 * feats, own), f32),
            pltpu.VMEM((4, feats, own), bf16),
        ]
        + parts * 2
        + [dma((2, 4)), dma((2, 4)), dma((4,)), dma((4,)), dma((5,)), dma((5,)), dma((5,)), dma((5,))]
        + [dma, dma, dma((4,)), dma((2, 2))]
        + scatter_scratch(kinds + 1, n, w, bf16),
        compiler_params=pltpu.CompilerParams(
            collective_id=cid, has_side_effects=True, vmem_limit_bytes=58 * 1024 * 1024
        ),
        name="tail",
    )(*grads, q, kv, small, x_t, ctx_t, resid, w_attn)


def dot(a, b, contract=((1,), (0,))):
    return lax.dot_general(a, b, (contract, ((), ())), preferred_element_type=f32)


def block_rows(ref, heads, scale, out):
    own = ref.shape[-1]
    for h in range(heads):
        for g in range(heads):
            spot = (pl.ds(h * HD, HD), pl.ds(g * own, own))
            if h == g:
                out[spot] = ref[0, pl.ds(h * HD, HD)] * jnp.asarray(scale, out.dtype)
            else:
                out[spot] = jnp.zeros((HD, own), out.dtype)


def attn_fwd_kernel(heads, scale, bounds, q_ref, kv_ref, qseg_ref, kseg_ref, ctx_ref, lse_ref, kn, q3, s_scr, o_scr):
    step = pl.program_id(0)
    tiles, _, tile = kv_ref.shape
    wide = heads * HD
    own = q_ref.shape[-1]

    @pl.when(step == 0)
    def _():
        @pl.loop(0, tiles)
        def _(j):
            kn[j] = kv_ref[j, pl.ds(0, wide)].astype(f32).T.astype(bf16)

    block_rows(q_ref, heads, scale, q3)
    low, high = bounds[step, 0], bounds[step, 1]
    qseg = jnp.concatenate([qseg_ref[0]] * heads, axis=1)

    def one(j, top):
        s = dot(kn[j], q3[...])
        s = jnp.where(kseg_ref[j] == qseg, s, masked_value)
        s_scr[j] = s
        return jnp.maximum(top, jnp.max(s, axis=0, keepdims=True))

    top = lax.fori_loop(low, high, one, jnp.full((1, heads * own), masked_value, f32))
    o_scr[...] = jnp.zeros_like(o_scr)

    def two(j, total):
        p = jnp.exp(s_scr[j] - top)
        low_p = p.astype(bf16)
        for h in range(heads):
            rows = pl.ds(h * HD, HD)
            v = kv_ref[j, pl.ds(wide + h * HD, HD)]
            o_scr[rows] += dot(v, low_p[:, h * own : (h + 1) * own])
        return total + jnp.sum(p, axis=0, keepdims=True)

    total = lax.fori_loop(low, high, two, jnp.zeros((1, heads * own), f32))
    for h in range(heads):
        rows = pl.ds(h * HD, HD)
        ctx_ref[0, rows] = (o_scr[rows] / total[:, h * own : (h + 1) * own]).astype(bf16)
    lse_ref[0] = top + jnp.log(total)


def attn_fwd(bounds, q, kv, qseg, kseg, scale):
    blocks, wide, own = q.shape
    tiles, _, tile = kv.shape
    heads = wide // HD
    return pl.pallas_call(
        functools.partial(attn_fwd_kernel, heads, scale),
        out_shape=[
            jax.ShapeDtypeStruct(q.shape, bf16),
            jax.ShapeDtypeStruct((blocks, 1, heads * own), f32),
        ],
        grid_spec=pltpu.PrefetchScalarGridSpec(
            num_scalar_prefetch=1,
            grid=(blocks,),
            in_specs=[
                pl.BlockSpec((1, wide, own), lambda i, b: (i, 0, 0)),
                pl.BlockSpec(kv.shape, lambda i, b: (0, 0, 0)),
                pl.BlockSpec((1, 1, own), lambda i, b: (i, 0, 0)),
                pl.BlockSpec(kseg.shape, lambda i, b: (0, 0, 0)),
            ],
            out_specs=[
                pl.BlockSpec((1, wide, own), lambda i, b: (i, 0, 0)),
                pl.BlockSpec((1, 1, heads * own), lambda i, b: (i, 0, 0)),
            ],
            scratch_shapes=[
                pltpu.VMEM((tiles, tile, wide), bf16),
                pltpu.VMEM((wide, heads * own), bf16),
                pltpu.VMEM((tiles, tile, heads * own), f32),
                pltpu.VMEM((wide, own), f32),
            ],
        ),
        compiler_params=pltpu.CompilerParams(
            dimension_semantics=("arbitrary",), vmem_limit_bytes=48 * 1024 * 1024
        ),
        name="attn_fwd",
    )(bounds, q, kv, qseg, kseg)


def attn_bwd_kernel(
    heads, scale, bounds, q_ref, kv_ref, qseg_ref, kseg_ref, lse_ref, ctx_ref, dctx_ref,
    dq_ref, dkv_ref, kn, vn, q3, dc3, dq_scr, dkv_scr,
):
    step = pl.program_id(0)
    tiles, _, tile = kv_ref.shape
    wide = heads * HD
    own = q_ref.shape[-1]

    @pl.when(step == 0)
    def _():
        @pl.loop(0, tiles)
        def _(j):
            kn[j] = kv_ref[j, pl.ds(0, wide)].astype(f32).T.astype(bf16)
            vn[j] = kv_ref[j, pl.ds(wide, wide)].astype(f32).T.astype(bf16)
            dkv_scr[j] = jnp.zeros((2 * wide, tile), f32)

    block_rows(q_ref, heads, scale, q3)
    block_rows(dctx_ref, heads, 1.0, dc3)
    low, high = bounds[step, 0], bounds[step, 1]
    qseg = jnp.concatenate([qseg_ref[0]] * heads, axis=1)
    lse = lse_ref[0]
    product = ctx_ref[0].astype(f32) * dctx_ref[0].astype(f32)
    delta = jnp.concatenate(
        [jnp.sum(product[h * HD : (h + 1) * HD], axis=0, keepdims=True) for h in range(heads)], axis=1
    )
    dq_scr[...] = jnp.zeros_like(dq_scr)

    @pl.loop(low, high)
    def _(j):
        s = dot(kn[j], q3[...])
        s = jnp.where(kseg_ref[j] == qseg, s, masked_value)
        p = jnp.exp(s - lse)
        d_p = dot(vn[j], dc3[...])
        d_s = (p * (d_p - delta)).astype(bf16)
        p = p.astype(bf16)
        for h in range(heads):
            rows, lanes = pl.ds(h * HD, HD), slice(h * own, (h + 1) * own)
            dq_scr[rows] += dot(kv_ref[j, rows], d_s[:, lanes])
            dkv_scr[j, rows] += dot(q3[rows, lanes], d_s[:, lanes], ((1,), (1,)))
            deep = pl.ds(wide + h * HD, HD)
            dkv_scr[j, deep] += dot(dctx_ref[0, rows], p[:, lanes], ((1,), (1,)))

    dq_ref[0] = (dq_scr[...] * scale).astype(bf16)

    @pl.when(step == pl.num_programs(0) - 1)
    def _():
        @pl.loop(0, tiles)
        def _(j):
            dkv_ref[j] = dkv_scr[j].astype(bf16)


def attn_bwd(bounds, q, kv, qseg, kseg, lse, ctx, dctx, scale):
    blocks, wide, own = q.shape
    tiles, _, tile = kv.shape
    heads = wide // HD
    rowed = pl.BlockSpec((1, wide, own), lambda i, b: (i, 0, 0))
    return pl.pallas_call(
        functools.partial(attn_bwd_kernel, heads, scale),
        out_shape=[jax.ShapeDtypeStruct(q.shape, bf16), jax.ShapeDtypeStruct(kv.shape, bf16)],
        grid_spec=pltpu.PrefetchScalarGridSpec(
            num_scalar_prefetch=1,
            grid=(blocks,),
            in_specs=[
                rowed,
                pl.BlockSpec(kv.shape, lambda i, b: (0, 0, 0)),
                pl.BlockSpec((1, 1, own), lambda i, b: (i, 0, 0)),
                pl.BlockSpec(kseg.shape, lambda i, b: (0, 0, 0)),
                pl.BlockSpec((1, 1, heads * own), lambda i, b: (i, 0, 0)),
                rowed,
                rowed,
            ],
            out_specs=[rowed, pl.BlockSpec(kv.shape, lambda i, b: (0, 0, 0))],
            scratch_shapes=[
                pltpu.VMEM((tiles, tile, wide), bf16),
                pltpu.VMEM((tiles, tile, wide), bf16),
                pltpu.VMEM((wide, heads * own), bf16),
                pltpu.VMEM((wide, heads * own), bf16),
                pltpu.VMEM((wide, own), f32),
                pltpu.VMEM((tiles, 2 * wide, tile), f32),
            ],
        ),
        compiler_params=pltpu.CompilerParams(
            dimension_semantics=("arbitrary",), vmem_limit_bytes=48 * 1024 * 1024
        ),
        name="attn_bwd",
    )(bounds, q, kv, qseg, kseg, lse, ctx, dctx)


def fast_local(
    tokens,
    segments,
    labels,
    cotangent,
    w_qkv,
    b_qkv,
    w_out,
    b_out,
    ln1_gain,
    ln1_bias,
    w_in,
    b_in,
    w_back,
    b_back,
    ln2_gain,
    ln2_bias,
    s_proj,
    s_bias,
    s_query,
    s_mid,
    s_mid_bias,
    s_cls,
    s_cls_bias,
):
    _, width_row, cols_local = tokens.shape
    parts, rows, cols, seqs, _ = sizes(tokens.shape[0])
    width = width_row * rows
    own = cols_local // parts
    width_col = b_qkv.shape[1]
    heads_dev = width_col // HD
    hidden_col = b_in.shape[0]
    docs_count = labels.shape[1]
    class_count = s_cls.shape[1]
    student_width = s_proj.shape[1]
    seq_len = segments.shape[1]
    row_index = lax.axis_index("row")
    col_index = lax.axis_index("col")
    dp_index = lax.axis_index("dp")
    score_scale = HD ** (-0.5)
    pool_scale = SHD ** (-0.5)
    query_heads = s_query.reshape(SH, SHD)
    doc_ids = jnp.arange(docs_count, dtype=jnp.int32)
    class_ids = jnp.arange(class_count, dtype=jnp.int32)

    w_three = w_qkv.reshape(width_row, heads_dev, 3, HD).transpose(0, 2, 1, 3)
    w_three = jnp.concatenate([w_three[:, 1], w_three[:, 2], w_three[:, 0]], axis=1)
    shard_attn = own_half(jnp.concatenate([w_three.reshape(width_row, -1), w_out], axis=1))
    proj_rows = width_row // cols
    lanes = -(-3 * width_col // 128) * 128
    offsets = jnp.concatenate([jnp.zeros_like(b_qkv[0]), b_qkv[1], b_qkv[0]])
    offsets = jnp.pad(offsets, (0, lanes - 3 * width_col))
    vectors = [offsets, b_out, ln1_gain, ln1_bias, b_back, ln2_gain, ln2_bias, b_in]
    vectors.append(lax.dynamic_slice_in_dim(s_proj, col_index * proj_rows, proj_rows).astype(f32).reshape(-1))
    flat = jnp.concatenate(vectors)
    flat = jnp.pad(flat, (0, 96 * 128 - flat.shape[0])).reshape(96, 128)
    w_attn, vec, w_in_all, w_back_all, x_parts, ints, queries, kv, w_out_all = gather_fast(
        [shard_attn, own_half(flat), own_half(w_in), own_half(w_back)],
        tokens,
        jnp.concatenate([segments, labels], axis=1),
        width_col,
        1,
    )
    w_in_all = w_in_all.reshape(cols, width, hidden_col)
    w_back_all = w_back_all.reshape(cols, width, hidden_col)
    vec = vec.reshape(cols, rows, -1)
    at = lanes + 6 * width_row
    row_vectors = vec[0, :, lanes:at].reshape(rows, 6, width_row).transpose(1, 0, 2).reshape(6, width)
    b_out_a, gain_one, bias_one, b_back_a, gain_two, bias_two = [row_vectors[i] for i in range(6)]
    b_in_all = vec[:, 0, at : at + hidden_col]
    at += hidden_col
    s_proj_all = vec[:, :, at : at + proj_rows * student_width].astype(bf16)
    s_proj_all = s_proj_all.reshape(cols, rows, proj_rows, student_width).transpose(1, 0, 2, 3)
    s_proj_all = s_proj_all.reshape(width, student_width)
    x_t = x_parts.reshape(width, own)
    ints = lax.dynamic_index_in_dim(ints.reshape(seqs, -1), row_index, 0, False)
    seg_all, label_seq = ints[:seq_len], ints[seq_len:]
    seg_blocks = seg_all.reshape(cols, parts, own)
    seg_q = lax.dynamic_index_in_dim(seg_blocks, dp_index, 1, False)
    seg_own = lax.dynamic_index_in_dim(seg_q, col_index, 0, False)
    lows = jnp.sum(seg_all[None, :] < seg_q[:, :1], axis=1) // own
    highs = (jnp.sum(seg_all[None, :] <= seg_q[:, -1:], axis=1) + own - 1) // own
    bounds = jnp.stack([lows, highs], axis=1).astype(jnp.int32)

    kv = kv.reshape(cols * parts, 2 * width_col, own)
    q_rows, k_rows = seg_q[:, None, :], seg_all.reshape(cols * parts, own, 1)
    context, lse = attn_fwd(bounds, queries, kv, q_rows, k_rows, score_scale)
    ctx_t, c_parts = swap_fast(context, cotangent, 3)
    ctx_parts, ctx_t = ctx_t, ctx_t.reshape(width, own)

    x = x_t.T
    attn_out = mm(ctx_t, w_out_all, ((0,), (0,))) + b_out_a
    normed_one, inv_one = normalize(x.astype(f32) + attn_out)
    hidden_one = normed_one * gain_one + bias_one
    hidden_low = hidden_one.astype(bf16)
    pre_act = jnp.einsum("td,cdn->ctn", hidden_low, w_in_all, preferred_element_type=f32)
    pre_act = pre_act + b_in_all[:, None, :]
    act = gelu_exact(pre_act).astype(bf16)
    ffn_out = jnp.einsum("ctn,cdn->td", act, w_back_all, preferred_element_type=f32) + b_back_a
    normed_two, inv_two = normalize(hidden_one + ffn_out)
    layer_out = (normed_two * gain_two + bias_two).astype(bf16)

    student_h = mm(layer_out, s_proj_all, ((1,), (0,))) + s_bias
    head_parts = student_h.reshape(own, SH, SHD)
    pool_logit = jnp.sum(head_parts * query_heads, axis=-1) * pool_scale
    member = (seg_own[:, None] == doc_ids[None, :])[:, :, None]
    masked = jnp.where(member, pool_logit[:, None, :], masked_value)
    local_top = jnp.max(masked, axis=0)
    local_exp = jnp.where(member, jnp.exp(masked - local_top[None]), 0.0)
    local_total = jnp.sum(local_exp, axis=0)
    local_sum = jnp.einsum("tdh,thk->dhk", local_exp, head_parts, precision=highest)
    stats = jnp.concatenate([local_top[..., None], local_total[..., None], local_sum], axis=-1)
    stats = jnp.pad(stats.reshape(-1), (0, 8 * 128 - stats.size)).reshape(8, 128)

    d_out = c_parts.reshape(width, own).T.astype(f32)
    g_ln2_gain = jnp.sum(d_out * normed_two, axis=0)
    g_ln2_bias = jnp.sum(d_out, axis=0)
    d_resid_two = normalize_back(d_out * gain_two, normed_two, inv_two)
    d_ffn = d_resid_two.astype(bf16)
    g_back_bias = jnp.sum(d_ffn.astype(f32), axis=0)
    g_back = jnp.einsum("td,ctn->cdn", d_ffn, act, preferred_element_type=f32)
    d_act = jnp.einsum("td,cdn->ctn", d_ffn, w_back_all, preferred_element_type=f32)
    _, gelu_fn = jax.vjp(gelu_exact, pre_act)
    d_pre = gelu_fn(d_act)[0].astype(bf16)
    g_in_bias = jnp.sum(d_pre.astype(f32), axis=1)
    g_in = jnp.einsum("td,ctn->cdn", hidden_low, d_pre, preferred_element_type=f32)
    d_hidden_one = d_resid_two + jnp.einsum(
        "ctn,cdn->td", d_pre, w_in_all, preferred_element_type=f32
    )
    g_ln1_gain = jnp.sum(d_hidden_one * normed_one, axis=0)
    g_ln1_bias = jnp.sum(d_hidden_one, axis=0)
    d_resid_one = normalize_back(d_hidden_one * gain_one, normed_one, inv_one)
    d_attn = d_resid_one.astype(bf16)
    g_out_bias = jnp.sum(d_attn.astype(f32), axis=0)
    d_ctx = mm(w_out_all, d_attn, ((1,), (1,))).astype(bf16)
    d_ctx, stats, out = turn_fast(d_ctx.reshape(cols, width_col, own), stats, layer_out.T, 4)

    stats = stats.reshape(cols * parts, -1)[:, : docs_count * SH * (SHD + 2)]
    stats = stats.reshape(cols * parts, docs_count, SH, SHD + 2)
    tops, totals, sums = stats[..., 0], stats[..., 1], stats[..., 2:]
    doc_top = jnp.max(tops, axis=0)
    factors = jnp.exp(tops - doc_top[None])
    doc_total = jnp.sum(totals * factors, axis=0)
    pooled_heads = jnp.sum(sums * factors[..., None], axis=0) / doc_total[:, :, None]
    pooled = pooled_heads.reshape(docs_count, student_width)
    middle = jnp.tanh(jnp.dot(pooled, s_mid, precision=highest) + s_mid_bias)
    logit_rows = jnp.dot(middle, s_cls, precision=highest) + s_cls_bias
    logit_top = jnp.max(logit_rows, axis=-1, keepdims=True)
    logit_exp = jnp.exp(logit_rows - logit_top)
    one_hot = (label_seq[:, None] == class_ids[None, :]).astype(f32)
    d_logits = logit_exp / jnp.sum(logit_exp, axis=-1, keepdims=True) - one_hot
    g_cls = jnp.dot(middle.T, d_logits, precision=highest)
    g_cls_bias = jnp.sum(d_logits, axis=0)
    d_middle = jnp.dot(d_logits, s_cls.T, precision=highest) * (1.0 - middle * middle)
    g_mid = jnp.dot(pooled.T, d_middle, precision=highest)
    g_mid_bias = jnp.sum(d_middle, axis=0)
    d_pooled = jnp.dot(d_middle, s_mid.T, precision=highest).reshape(docs_count, SH, SHD)
    shares = jnp.where(member, jnp.exp(masked - doc_top[None]), 0.0) / doc_total[None]
    d_share = jnp.einsum("dhk,thk->tdh", d_pooled, head_parts, precision=highest)
    base_term = jnp.sum(d_pooled * pooled_heads, axis=-1)
    d_pool_logit = jnp.sum(shares * (d_share - base_term[None]), axis=1)
    d_heads = jnp.einsum("tdh,dhk->thk", shares, d_pooled, precision=highest)
    d_heads = d_heads + d_pool_logit[:, :, None] * query_heads[None] * pool_scale
    g_query = (jnp.sum(d_pool_logit[:, :, None] * head_parts, axis=0) * pool_scale).reshape(-1)
    d_student = d_heads.reshape(own, student_width)
    g_sbias = jnp.sum(d_student, axis=0)
    g_sproj = jnp.dot(layer_out.astype(f32).T, d_student, precision=highest)

    d_q, d_kv = attn_bwd(bounds, queries, kv, q_rows, k_rows, lse, context, d_ctx, score_scale)
    at_seq = (jnp.arange(seqs) == row_index).astype(f32)[:, None]
    at_heads = (jnp.arange(cols) == col_index).astype(f32)[:, None, None]
    g_q_bias = jnp.sum(d_q.astype(f32), axis=(0, 2))
    g_v_bias = jnp.sum(d_kv[:, width_col:].astype(f32), axis=(0, 2))
    once = 1.0 / (parts * cols)
    small = (
        g_sproj,
        jnp.stack([g_q_bias, g_v_bias])[None] * at_heads,
        g_in_bias,
        g_out_bias,
        g_ln1_gain,
        g_ln1_bias,
        g_back_bias,
        g_ln2_gain,
        g_ln2_bias,
        g_sbias,
        g_query,
        g_mid * once,
        g_mid_bias * once,
        g_cls * once,
        logit_rows.reshape(1, -1) * (at_seq * once),
        g_cls_bias * once,
    )
    flat = jnp.concatenate([part.reshape(-1) for part in small])
    tall = -(-flat.shape[0] // (128 * 256)) * 256
    flat = jnp.pad(flat, (0, tall * 128 - flat.shape[0])).reshape(tall, 128)
    blocked = (cols, rows, parts, width_row // parts, -1)
    g_in, g_back, g_attn, grad_tokens, flat = tail_fast(
        [g_in.astype(bf16).reshape(blocked), g_back.astype(bf16).reshape(blocked)],
        d_q,
        d_kv.reshape(cols, parts, 2 * width_col, own),
        flat,
        x_parts,
        ctx_parts,
        d_resid_one,
        w_attn,
        5,
    )
    flat = flat.reshape(-1)
    sums_all, at = [], 0
    for part in small:
        sums_all.append(flat[at : at + part.size].reshape(part.shape))
        at += part.size
    g_in, g_back, g_attn = [part.reshape(width_row, -1).astype(f32) for part in (g_in, g_back, g_attn)]
    g_qkv = g_attn[:, : 3 * width_col].reshape(width_row, 3, heads_dev, HD)
    g_qkv = jnp.stack([g_qkv[:, 2], g_qkv[:, 0], g_qkv[:, 1]], axis=2).reshape(width_row, -1)

    def at_col(part):
        return lax.dynamic_index_in_dim(part, col_index, 0, False)

    def at_row(part):
        return lax.dynamic_slice_in_dim(part, row_index * width_row, width_row)

    (
        g_sproj, g_qkv_bias, g_in_bias, g_out_bias, g_ln1_gain, g_ln1_bias, g_back_bias, g_ln2_gain,
        g_ln2_bias, g_sbias, g_query, g_mid, g_mid_bias, g_cls, logits, g_cls_bias,
    ) = sums_all
    logits = lax.dynamic_slice_in_dim(logits, dp_index * (seqs // parts), seqs // parts)
    return (
        out,
        logits.reshape(seqs // parts, docs_count, class_count),
        grad_tokens.astype(f32),
        g_qkv,
        at_col(g_qkv_bias),
        g_attn[:, 3 * width_col :],
        at_row(g_out_bias),
        at_row(g_ln1_gain),
        at_row(g_ln1_bias),
        g_in,
        at_col(g_in_bias),
        g_back,
        at_row(g_back_bias),
        at_row(g_ln2_gain),
        at_row(g_ln2_bias),
        at_row(g_sproj),
        g_sbias,
        g_query,
        g_mid,
        g_mid_bias,
        g_cls,
        g_cls_bias,
    )


def solution(mesh):
    row, col = P("row"), P("col")
    grid, whole = P("row", "col"), P("dp", "row", "col")
    placed = (
        (whole, P("dp", None), P("dp", None), whole, grid, P(None, "col"), P("col", "row"))
        + (row, row, row, grid, col, grid, row, row, row, P("row", None))
        + (P(),) * 6
    )
    results = (
        (whole, P("dp", None, None), whole, grid, P(None, "col"), P("col", "row"))
        + (row, row, row, grid, col, grid, row, row, row, P("row", None))
        + (P(),) * 6
    )
    quick = dict(mesh.shape) == {"dp": 2, "row": 4, "col": 4}
    local = fast_local if quick else general_local
    return jax.shard_map(local, mesh=mesh, in_specs=placed, out_specs=results, check_vma=False)
```

```python
import functools
import jax
import jax.numpy as jnp
from jax import lax
from jax.experimental import pallas as pl
from jax.experimental.pallas import tpu as pltpu
from jax.sharding import PartitionSpec as P

HD = 64
SH = 2
SHD = 64

norm_eps = 1e-06
masked_value = -1e30
highest = lax.Precision.HIGHEST
f32 = jnp.float32
bf16 = jnp.bfloat16
WORLD = ("col", "row", "dp")


def sizes(seqs_local):
    parts = lax.axis_size("dp")
    rows = lax.axis_size("row")
    seqs = seqs_local * parts
    return parts, rows, lax.axis_size("col"), seqs, rows // seqs


def row_groups(rows, sub):
    return [list(range(at, at + sub)) for at in range(0, rows, sub)]


def take_in(values):
    parts, rows, _, seqs, sub = sizes(values.shape[0])
    held = lax.all_to_all(values, "dp", 2, 0, tiled=True)
    feats, half = held.shape[1:]
    held = held.reshape(seqs, feats, sub, half // sub).transpose(0, 2, 1, 3)
    held = held.reshape(rows, feats, half // sub)
    held = lax.all_to_all(held, "row", 0, 0, tiled=True)
    return held.reshape(rows * feats, half // sub)


def give_back(values, seqs_local):
    parts, rows, _, seqs, sub = sizes(seqs_local)
    width, own = values.shape
    feats = width // rows
    held = lax.all_to_all(values.reshape(rows, feats, own), "row", 0, 0, tiled=True)
    held = held.reshape(seqs, sub, feats, own).transpose(0, 2, 1, 3).reshape(seqs, feats, sub * own)
    return lax.all_to_all(held, "dp", 0, 2, tiled=True)


def gather_world(shard):
    cols, rows = lax.axis_size("col"), lax.axis_size("row")
    out = lax.all_gather(shard, WORLD, axis=0, tiled=True)
    return out.reshape(cols, rows, -1, shard.shape[1])


def own_half(block):
    parts = lax.axis_size("dp")
    amount = block.shape[0] // parts
    return lax.dynamic_slice_in_dim(block, lax.axis_index("dp") * amount, amount)


def scatter_world(full):
    flat = full.reshape(-1, full.shape[-1])
    mine = lax.psum_scatter(flat, WORLD, scatter_dimension=0, tiled=True)
    return lax.all_gather(mine, "dp", axis=0, tiled=True)


def swap_cols(values):
    return lax.all_to_all(values, "col", 0, 0, tiled=True)


def gather_sequence(values, sub):
    cols, own, width = values.shape
    held = values[:, None]
    if sub > 1:
        groups = row_groups(lax.axis_size("row"), sub)
        held = lax.all_gather(held, "row", axis=1, tiled=True, axis_index_groups=groups)
    held = lax.all_gather(held[:, None], "dp", axis=1, tiled=True)
    return held.reshape(-1, width)


def scatter_sequence(values, cols, sub):
    parts = lax.axis_size("dp")
    width = values.shape[-1]
    held = values.reshape(cols, parts, sub, -1, width)
    held = lax.psum_scatter(held, "dp", scatter_dimension=1, tiled=True)[:, 0]
    if sub > 1:
        groups = row_groups(lax.axis_size("row"), sub)
        held = lax.psum_scatter(
            held, "row", scatter_dimension=1, tiled=True, axis_index_groups=groups
        )
    return held[:, 0]


def normalize(values):
    mean_v = jnp.mean(values, axis=-1, keepdims=True)
    center = values - mean_v
    inv_std = lax.rsqrt(jnp.mean(center * center, axis=-1, keepdims=True) + norm_eps)
    return center * inv_std, inv_std


def normalize_back(grad_hat, normed, inv_std):
    return inv_std * (
        grad_hat
        - jnp.mean(grad_hat, axis=-1, keepdims=True)
        - normed * jnp.mean(grad_hat * normed, axis=-1, keepdims=True)
    )


def gelu_exact(values):
    return jax.nn.gelu(values, approximate=False)


def mm(a, b, contract):
    return lax.dot_general(a, b, (contract, ((), ())), preferred_element_type=f32)


def combine_pool(part_one, part_two):
    top_a, total_a, sum_a = part_one
    top_b, total_b, sum_b = part_two
    row_top = jnp.maximum(top_a, top_b)
    factor_a = jnp.exp(top_a - row_top)
    factor_b = jnp.exp(top_b - row_top)
    return (
        row_top,
        total_a * factor_a + total_b * factor_b,
        sum_a * factor_a[:, :, None] + sum_b * factor_b[:, :, None],
    )


def attend(q, k, v, q_seg, k_seg, scale):
    scores = jnp.einsum("qhd,khd->hqk", q, k, preferred_element_type=f32) * scale
    scores = jnp.where((q_seg[:, None] == k_seg[None, :])[None], scores, masked_value)
    top = jnp.max(scores, axis=-1, keepdims=True)
    exp_scores = jnp.exp(scores - top)
    total = jnp.sum(exp_scores, axis=-1, keepdims=True)
    probs = exp_scores / total
    context = jnp.einsum("hqk,khd->qhd", probs.astype(bf16), v, preferred_element_type=f32)
    return context.astype(bf16), probs


def attend_back(q, k, v, probs, d_ctx, scale):
    d_probs = jnp.einsum("qhd,khd->hqk", d_ctx, v, preferred_element_type=f32)
    delta = jnp.sum(probs * d_probs, axis=-1, keepdims=True)
    d_scores = (probs * (d_probs - delta)).astype(bf16)
    d_q = jnp.einsum("hqk,khd->qhd", d_scores, k, preferred_element_type=f32) * scale
    d_k = jnp.einsum("hqk,qhd->khd", d_scores, q, preferred_element_type=f32) * scale
    d_v = jnp.einsum("hqk,qhd->khd", probs.astype(bf16), d_ctx, preferred_element_type=f32)
    return d_q, d_k, d_v


def general_local(
    tokens,
    segments,
    labels,
    cotangent,
    w_qkv,
    b_qkv,
    w_out,
    b_out,
    ln1_gain,
    ln1_bias,
    w_in,
    b_in,
    w_back,
    b_back,
    ln2_gain,
    ln2_bias,
    s_proj,
    s_bias,
    s_query,
    s_mid,
    s_mid_bias,
    s_cls,
    s_cls_bias,
):
    seqs_local, width_row, cols_local = tokens.shape
    parts, rows, cols, seqs, sub = sizes(seqs_local)
    width = width_row * rows
    own = cols_local // (parts * sub)
    width_col = b_qkv.shape[1]
    heads_dev = width_col // HD
    hidden_col = b_in.shape[0]
    docs_count = labels.shape[1]
    class_count = s_cls.shape[1]
    student_width = s_proj.shape[1]
    row_index = lax.axis_index("row")
    col_index = lax.axis_index("col")
    dp_index = lax.axis_index("dp")
    seq_index = row_index // sub
    sub_index = row_index % sub
    score_scale = HD ** (-0.5)
    pool_scale = SHD ** (-0.5)
    query_heads = s_query.reshape(SH, SHD)
    doc_ids = jnp.arange(docs_count, dtype=jnp.int32)
    class_ids = jnp.arange(class_count, dtype=jnp.int32)

    w_qkv_all = gather_world(own_half(w_qkv)).reshape(cols, width, 3 * width_col)
    x_t = take_in(tokens)
    rest = jnp.concatenate([own_half(w_in), own_half(w_back), own_half(w_out).reshape(-1, width_col)], axis=1)
    rest_all = gather_world(rest)
    w_in_all = rest_all[..., :hidden_col].reshape(cols, width, hidden_col)
    w_back_all = rest_all[..., hidden_col : 2 * hidden_col].reshape(cols, width, hidden_col)
    w_out_all = rest_all[..., 2 * hidden_col :].reshape(cols, rows, width_col, width_row)
    w_out_all = w_out_all.transpose(0, 2, 1, 3).reshape(width, width)
    row_vectors = lax.all_gather(
        jnp.stack([b_out, ln1_gain, ln1_bias, b_back, ln2_gain, ln2_bias]), "row", axis=1, tiled=True
    )
    b_out_a, gain_one, bias_one, b_back_a, gain_two, bias_two = [row_vectors[i] for i in range(6)]
    b_qkv_all = lax.all_gather(b_qkv, "col")
    b_in_all = lax.all_gather(b_in, "col")
    s_proj_all = lax.all_gather(s_proj, "row", axis=0, tiled=True)
    whole_ints = lax.all_gather(jnp.concatenate([segments, labels], axis=1), "dp", axis=0, tiled=True)
    ints = lax.dynamic_index_in_dim(whole_ints, seq_index, 0, False)
    seq_len = segments.shape[1]
    seg_all, label_seq = ints[:seq_len], ints[seq_len:]
    seg_blocks = seg_all.reshape(cols, parts, sub, own)
    seg_q = lax.dynamic_index_in_dim(seg_blocks, dp_index, 1, False)
    seg_q = lax.dynamic_index_in_dim(seg_q, sub_index, 1, False)
    seg_own = lax.dynamic_index_in_dim(seg_q, col_index, 0, False)
    seg_q = seg_q.reshape(-1)

    x = x_t.T
    offsets = jnp.stack([b_qkv_all[:, 0], jnp.zeros_like(b_qkv_all[:, 0]), b_qkv_all[:, 1]], axis=1)
    offsets = offsets.reshape(cols, 3, heads_dev, HD).transpose(0, 2, 1, 3).reshape(cols, 1, -1)
    qkv = jnp.einsum("td,cdn->ctn", x, w_qkv_all, preferred_element_type=f32) + offsets
    qkv = swap_cols(qkv.astype(bf16)).reshape(cols, own, heads_dev, 3, HD)
    queries = qkv[:, :, :, 0].reshape(cols * own, heads_dev, HD)
    kv = gather_sequence(qkv[:, :, :, 1:].reshape(cols, own, -1), sub)
    kv = kv.reshape(seq_len, heads_dev, 2, HD)
    key_rows, value_rows = kv[:, :, 0], kv[:, :, 1]
    context, probs = attend(queries, key_rows, value_rows, seg_q, seg_all, score_scale)
    ctx = swap_cols(context.reshape(cols, own, width_col))
    ctx = ctx.transpose(1, 0, 2).reshape(own, width)

    attn_out = mm(ctx, w_out_all, ((1,), (0,))) + b_out_a
    normed_one, inv_one = normalize(x.astype(f32) + attn_out)
    hidden_one = normed_one * gain_one + bias_one
    hidden_low = hidden_one.astype(bf16)
    pre_act = jnp.einsum("td,cdn->ctn", hidden_low, w_in_all, preferred_element_type=f32)
    pre_act = pre_act + b_in_all[:, None, :]
    act = gelu_exact(pre_act).astype(bf16)
    ffn_out = jnp.einsum("ctn,cdn->td", act, w_back_all, preferred_element_type=f32) + b_back_a
    normed_two, inv_two = normalize(hidden_one + ffn_out)
    layer_out = (normed_two * gain_two + bias_two).astype(bf16)
    out = give_back(layer_out.T, seqs_local)

    student_h = mm(layer_out, s_proj_all, ((1,), (0,))) + s_bias
    head_parts = student_h.reshape(own, SH, SHD)
    pool_logit = jnp.sum(head_parts * query_heads, axis=-1) * pool_scale
    member = (seg_own[:, None] == doc_ids[None, :])[:, :, None]
    masked = jnp.where(member, pool_logit[:, None, :], masked_value)
    local_top = jnp.max(masked, axis=0)
    local_exp = jnp.where(member, jnp.exp(masked - local_top[None]), 0.0)
    local_total = jnp.sum(local_exp, axis=0)
    local_sum = jnp.einsum("tdh,thk->dhk", local_exp, head_parts, precision=highest)
    stats = jnp.concatenate([local_top[..., None], local_total[..., None], local_sum], axis=-1)
    stats = lax.all_gather(stats, ("dp", "col"))
    if sub > 1:
        stats = lax.all_gather(stats, "row", axis=0, tiled=True, axis_index_groups=row_groups(rows, sub))
    tops, totals, sums = stats[..., 0], stats[..., 1], stats[..., 2:]
    doc_top = jnp.max(tops, axis=0)
    factors = jnp.exp(tops - doc_top[None])
    doc_total = jnp.sum(totals * factors, axis=0)
    pooled_heads = jnp.sum(sums * factors[..., None], axis=0) / doc_total[:, :, None]
    pooled = pooled_heads.reshape(docs_count, student_width)
    middle = jnp.tanh(jnp.dot(pooled, s_mid, precision=highest) + s_mid_bias)
    logit_rows = jnp.dot(middle, s_cls, precision=highest) + s_cls_bias
    logits = lax.all_gather(logit_rows, "row")[::sub]
    logits = lax.dynamic_slice_in_dim(logits, dp_index * seqs_local, seqs_local)
    logit_top = jnp.max(logit_rows, axis=-1, keepdims=True)
    logit_exp = jnp.exp(logit_rows - logit_top)
    one_hot = (label_seq[:, None] == class_ids[None, :]).astype(f32)
    d_logits = logit_exp / jnp.sum(logit_exp, axis=-1, keepdims=True) - one_hot
    g_cls = jnp.dot(middle.T, d_logits, precision=highest)
    g_cls_bias = jnp.sum(d_logits, axis=0)
    d_middle = jnp.dot(d_logits, s_cls.T, precision=highest) * (1.0 - middle * middle)
    g_mid = jnp.dot(pooled.T, d_middle, precision=highest)
    g_mid_bias = jnp.sum(d_middle, axis=0)
    d_pooled = jnp.dot(d_middle, s_mid.T, precision=highest).reshape(docs_count, SH, SHD)
    shares = jnp.where(member, jnp.exp(masked - doc_top[None]), 0.0) / doc_total[None]
    d_share = jnp.einsum("dhk,thk->tdh", d_pooled, head_parts, precision=highest)
    base_term = jnp.sum(d_pooled * pooled_heads, axis=-1)
    d_pool_logit = jnp.sum(shares * (d_share - base_term[None]), axis=1)
    d_heads = jnp.einsum("tdh,dhk->thk", shares, d_pooled, precision=highest)
    d_heads = d_heads + d_pool_logit[:, :, None] * query_heads[None] * pool_scale
    g_query = (jnp.sum(d_pool_logit[:, :, None] * head_parts, axis=0) * pool_scale).reshape(-1)
    d_student = d_heads.reshape(own, student_width)
    g_sbias = jnp.sum(d_student, axis=0)
    g_sproj = jnp.dot(layer_out.astype(f32).T, d_student, precision=highest)

    d_out = take_in(cotangent).T.astype(f32)
    g_ln2_gain = jnp.sum(d_out * normed_two, axis=0)
    g_ln2_bias = jnp.sum(d_out, axis=0)
    d_resid_two = normalize_back(d_out * gain_two, normed_two, inv_two)
    d_ffn = d_resid_two.astype(bf16)
    g_back_bias = jnp.sum(d_ffn.astype(f32), axis=0)
    g_back = jnp.einsum("td,ctn->cdn", d_ffn, act, preferred_element_type=f32)
    d_act = jnp.einsum("td,cdn->ctn", d_ffn, w_back_all, preferred_element_type=f32)
    _, gelu_fn = jax.vjp(gelu_exact, pre_act)
    d_pre = gelu_fn(d_act)[0].astype(bf16)
    g_in_bias = jnp.sum(d_pre.astype(f32), axis=1)
    g_in = jnp.einsum("td,ctn->cdn", hidden_low, d_pre, preferred_element_type=f32)
    d_hidden_one = d_resid_two + jnp.einsum(
        "ctn,cdn->td", d_pre, w_in_all, preferred_element_type=f32
    )
    g_ln1_gain = jnp.sum(d_hidden_one * normed_one, axis=0)
    g_ln1_bias = jnp.sum(d_hidden_one, axis=0)
    d_resid_one = normalize_back(d_hidden_one * gain_one, normed_one, inv_one)
    d_attn = d_resid_one.astype(bf16)
    g_out_bias = jnp.sum(d_attn.astype(f32), axis=0)
    g_out = mm(ctx, d_attn, ((0,), (0,)))
    d_ctx = mm(d_attn, w_out_all, ((1,), (1,))).astype(bf16)
    d_ctx = swap_cols(d_ctx.reshape(own, cols, width_col).transpose(1, 0, 2))
    d_ctx = d_ctx.reshape(cols * own, heads_dev, HD)
    d_q, d_k, d_v = attend_back(queries, key_rows, value_rows, probs, d_ctx, score_scale)
    d_kv = jnp.stack([d_k, d_v], axis=2).astype(bf16).reshape(seq_len, -1)
    d_kv = scatter_sequence(d_kv, cols, sub).reshape(cols, own, heads_dev, 2, HD)
    d_q = d_q.astype(bf16).reshape(cols, own, heads_dev, 1, HD)
    d_qkv = jnp.concatenate([d_q, d_kv], axis=3).reshape(cols, own, 3 * width_col)
    d_qkv = swap_cols(d_qkv)
    g_qkv_bias = jnp.sum(d_qkv.astype(f32), axis=1).reshape(cols, heads_dev, 3, HD)
    g_qkv = jnp.einsum("td,ctn->cdn", x, d_qkv, preferred_element_type=f32)
    d_tokens = d_resid_one + jnp.einsum("ctn,cdn->td", d_qkv, w_qkv_all, preferred_element_type=f32)
    grad_tokens = give_back(d_tokens.astype(bf16).T, seqs_local).astype(f32)

    g_out = g_out.reshape(cols, width_col, rows, width_row).transpose(0, 2, 1, 3)
    g_out = g_out.reshape(cols, rows, width_row, width_col)
    model = jnp.concatenate(
        [
            g_in.reshape(cols, rows, width_row, hidden_col).astype(bf16),
            g_back.reshape(cols, rows, width_row, hidden_col).astype(bf16),
            g_out.astype(bf16),
        ],
        axis=-1,
    )
    model = scatter_world(model).astype(f32)
    g_qkv = scatter_world(g_qkv.reshape(cols, rows, width_row, 3 * width_col).astype(bf16)).astype(f32)
    once = 1.0 / (parts * cols * sub)
    small = (
        g_qkv_bias[:, :, 0].reshape(cols, width_col),
        g_qkv_bias[:, :, 2].reshape(cols, width_col),
        g_in_bias,
        g_out_bias,
        g_ln1_gain,
        g_ln1_bias,
        g_back_bias,
        g_ln2_gain,
        g_ln2_bias,
        g_sproj,
        g_sbias,
        g_query,
        g_mid * once,
        g_mid_bias * once,
        g_cls * once,
        g_cls_bias * once,
    )
    small = lax.psum(small, WORLD)

    def at_col(part):
        return lax.dynamic_index_in_dim(part, col_index, 0, False)

    def at_row(part):
        return lax.dynamic_slice_in_dim(part, row_index * width_row, width_row)

    return (
        out,
        logits,
        grad_tokens,
        g_qkv,
        jnp.stack([at_col(small[0]), at_col(small[1])]),
        model[:, 2 * hidden_col :].reshape(width_col, width_row),
        at_row(small[3]),
        at_row(small[4]),
        at_row(small[5]),
        model[:, :hidden_col],
        at_col(small[2]),
        model[:, hidden_col : 2 * hidden_col],
        at_row(small[6]),
        at_row(small[7]),
        at_row(small[8]),
        at_row(small[9]),
        small[10],
        small[11],
        small[12],
        small[13],
        small[14],
        small[15],
    )


MESH = pl.DeviceIdType.MESH
HBM = pl.BlockSpec(memory_space=pl.ANY)


def place():
    return lax.axis_index("dp"), lax.axis_index("row"), lax.axis_index("col")


def greet(peers, guarded=()):
    barrier = pltpu.get_barrier_semaphore()
    for peer in peers:
        pl.semaphore_signal(barrier, inc=1, device_id=peer, device_id_type=MESH)
    for there, peer in guarded:

        @pl.when(there)
        def _():
            pl.semaphore_signal(barrier, inc=1, device_id=peer, device_id_type=MESH)

    amount = len(peers)
    for there, _ in guarded:
        amount = amount + there.astype(jnp.int32)
    pl.semaphore_wait(barrier, amount)


def rcopy(src, dst, send, recv, peer):
    return pltpu.make_async_remote_copy(
        src_ref=src, dst_ref=dst, send_sem=send, recv_sem=recv, device_id=peer, device_id_type=MESH
    )


def take_copies(src, out, local, send, recv):
    d, r, c = place()
    own = out.shape[2]
    moves = []
    for i in range(2):
        for far in range(2):
            row, core = 2 * d + i, d ^ far
            piece = src.at[i, :, pl.ds(pl.multiple_of(core * own, own), own)]
            here = (row == r) if far == 0 else None

            def start(piece=piece, row=row, core=core, slot=2 * i + far, here=here):
                def away():
                    rcopy(piece, out.at[r], send.at[slot], recv.at[r], (core, row, c)).start()

                if here is None:
                    away()
                else:
                    pl.when(jnp.logical_not(here))(away)

                    @pl.when(here)
                    def _():
                        pltpu.make_async_copy(piece, out.at[r], local).start()

            def wait(piece=piece, row=row, core=core, slot=2 * i + far, here=here):
                def away():
                    rcopy(piece, out.at[r], send.at[slot], recv.at[r], (core, row, c)).wait_send()

                if here is None:
                    away()
                else:
                    pl.when(jnp.logical_not(here))(away)

                    @pl.when(here)
                    def _():
                        pltpu.make_async_copy(piece, out.at[r], local).wait()

            moves.append((start, wait))
    for row in range(4):

        def arrive(row=row):
            @pl.when(jnp.logical_not((row == r) & (r // 2 == d)))
            def _():
                piece = src.at[0, :, pl.ds(0, own)]
                rcopy(piece, out.at[row], send.at[0], recv.at[row], (d, r, c)).wait_recv()

        moves.append((lambda: None, arrive))
    return moves


def gather_kernel(kinds, *refs):
    shards, refs = refs[:kinds], refs[kinds:]
    (tok, ints), refs = refs[:2], refs[2:]
    outs, refs = refs[:kinds], refs[kinds:]
    (tok_out, ints_out, q_out, kv_out, wo_out), refs = refs[:5], refs[5:]
    (x_nat, q_src, kv_src), refs = refs[:3], refs[3:]
    own_sem, zs, zr, xs, xr, ys, yr, cs, cr, ps, pr, tl, ts, tr, il, hs, hr, hps, hpr = refs
    d, r, c = place()
    cols = 4
    xn, yn, pn = (d, r ^ 1, c), (d, r ^ 2, c), (1 - d, r, c)
    up, down = (d, r, c + 1), (d, r, c - 1)
    has_up, has_down = c < cols - 1, c > 0
    greet(plane_peers() + [(d, r, c ^ j) for j in (1, 2, 3)])
    moves = take_copies(tok, tok_out, tl, ts, tr)
    for start, _ in moves:
        start()
    pltpu.make_async_copy(ints, ints_out.at[d], il.at[0]).start()
    rcopy(ints, ints_out.at[d], il.at[1], il.at[2], pn).start()
    halves = [shard.shape[0] // 2 for shard in shards]

    def z_send(k, at, way, hop):
        src = shards[k] if hop == 1 else outs[k].at[at, r, d]
        return rcopy(
            src, outs[k].at[at, r, d], zs.at[k, way, hop - 1], zr.at[k, way, hop - 1], up if way == 0 else down
        )

    def src_of(k, at, own):
        return shards[k] if own else outs[k].at[at, r, d]

    def to_x(k, at, own):
        return rcopy(src_of(k, at, own), outs[k].at[at, r, d], xs.at[k, at], xr.at[k, at], xn)

    def to_y(k, at, own):
        return rcopy(src_of(k, at, own), outs[k].at[at, r, d], ys.at[k, at], yr.at[k, at], yn)

    def to_p(k, at, own):
        return rcopy(src_of(k, at, own), outs[k].at[at, r, d], ps.at[k, at, 0], pr.at[k, at, 0], pn)

    def relay(k, at, which):
        row = r ^ 1 if which == 0 else r ^ 2
        ref = outs[k].at[at, row, d, pl.ds(which * halves[k], halves[k])]
        return rcopy(ref, ref, cs.at[k, at, which], cr.at[k, at, which], yn if which == 0 else xn)

    def pass_p(k, at, bit):
        ref = outs[k].at[at, r ^ bit, d]
        return rcopy(ref, ref, ps.at[k, at, bit], pr.at[k, at, bit], pn)

    def got_x(k, at):
        ref = outs[k].at[at, r ^ 1, d]
        rcopy(ref, ref, xs.at[k, at], xr.at[k, at], xn).wait_recv()

    def got_y(k, at):
        ref = outs[k].at[at, r ^ 2, d]
        rcopy(ref, ref, ys.at[k, at], yr.at[k, at], yn).wait_recv()

    def got_corner(k, at):
        for which in range(2):
            ref = outs[k].at[at, r ^ 3, d, pl.ds(which * halves[k], halves[k])]
            rcopy(ref, ref, cs.at[k, at, which], cr.at[k, at, which], xn).wait_recv()

    def got_p(k, at, bit):
        ref = outs[k].at[at, r ^ bit, 1 - d]
        rcopy(ref, ref, ps.at[k, at, bit], pr.at[k, at, bit], pn).wait_recv()

    for k in range(kinds):
        pltpu.make_async_copy(shards[k], outs[k].at[c, r, d], own_sem.at[k]).start()

        @pl.when(has_up)
        def _():
            z_send(k, c, 0, 1).start()

        @pl.when(has_down)
        def _():
            z_send(k, c, 1, 1).start()

    def spread(k, at, own):
        to_x(k, at, own).start()
        to_y(k, at, own).start()
        to_p(k, at, own).start()

    def onward(k, at):
        got_x(k, at)
        relay(k, at, 0).start()
        pass_p(k, at, 1).start()
        got_y(k, at)
        relay(k, at, 1).start()
        pass_p(k, at, 2).start()

    steps = [(0, 0)] + [(way, hop) for hop in (1, 2, 3) for way in (0, 1)]
    jobs = [(k, way, hop) for k in range(kinds) for way, hop in steps]

    def at_of(way, hop):
        return c - hop if way == 0 else c + hop

    def valid(way, hop):
        return c >= hop if way == 0 else c + hop < cols

    def guard(way, hop, body):
        if hop == 0:
            body()
        else:
            pl.when(valid(way, hop))(body)

    def first(k, way, hop):
        def body():
            at = at_of(way, hop)
            if hop:
                z_send(k, at, way, hop).wait_recv()
                if hop < 3:
                    can = has_up if way == 0 else has_down

                    @pl.when(can)
                    def _():
                        z_send(k, at, way, hop + 1).start()

            spread(k, at, hop == 0)

        guard(way, hop, body)

    def second(k, way, hop):
        guard(way, hop, lambda: onward(k, at_of(way, hop)))

    def third(k, way, hop):
        def body():
            at = at_of(way, hop)
            got_corner(k, at)
            pass_p(k, at, 3).start()

        guard(way, hop, body)

    def settle(k):
        pltpu.make_async_copy(shards[k], outs[k].at[c, r, d], own_sem.at[k]).wait()
        for way, hop in steps:

            def body():
                for bit in range(4):
                    got_p(k, at_of(way, hop), bit)

            guard(way, hop, body)

    def kv(j):
        return rcopy(kv_src.at[c ^ j], kv_out.at[c, d], hs.at[0, j], hr.at[0, j], (d, r, c ^ j))

    def q(j):
        return rcopy(q_src.at[c ^ j], q_out.at[c], hs.at[1, j], hr.at[1, j], (d, r, c ^ j))

    def pair(j):
        src = kv_src.at[c] if j == 0 else kv_out.at[c ^ j, d]
        return rcopy(src, kv_out.at[c ^ j, d], hps.at[j], hpr.at[j], pn)

    deep = kv_src.shape[1]
    out_cols = deep + q_src.shape[1]
    lanes = -(-out_cols // 128) * 128

    def prepare():
        for _, wait in moves:
            wait()
        feats = tok_out.shape[1]
        x_nat[...] = tok_out[...].reshape(4 * feats, -1).astype(f32).T.astype(bf16)

    def project(j):
        to = c ^ j
        weights = outs[0][to, :, :, :, :lanes].reshape(-1, lanes)
        bias = outs[1][to, r, 0, pl.ds(0, 8)]
        bias = jnp.concatenate([bias[i : i + 1] for i in range(lanes // 128)], axis=1)
        made = jnp.dot(x_nat[...], weights, preferred_element_type=f32) + bias
        made = made.T.astype(bf16)
        kv_src[to] = made[:deep]
        q_src[to] = made[deep:out_cols]
        if j:
            kv(j).start()
            q(j).start()
        else:
            pair(0).start()
            kv_out[c, d] = kv_src[c]
            q_out[c] = q_src[c]

    def spread_out(at):
        feats = tok_out.shape[1]
        for row in range(4):
            block = outs[0][at, row, :, :, out_cols:].reshape(-1, feats)
            wo_out[pl.ds(at * wide, wide), row * feats : (row + 1) * feats] = block

    wide = q_src.shape[1]
    lag = 3
    ready = 2 * len(steps) + 2 * lag
    for i in range(len(jobs) + 2 * lag):
        if i == ready:
            prepare()
            settle(0)
            settle(1)
        if ready <= i < ready + 4:
            project((3, 2, 1, 0)[i - ready])
        if ready + 4 <= i < ready + 8:
            spread_out(i - ready - 4)
        if i < len(jobs):
            first(*jobs[i])
        if 0 <= i - lag < len(jobs):
            second(*jobs[i - lag])
        if 0 <= i - 2 * lag < len(jobs):
            third(*jobs[i - 2 * lag])

    for j in (1, 2, 3):
        kv(j).wait_recv()
        pair(j).start()
    for k in range(kinds):
        if k > 1:
            settle(k)
        for way, hop in steps:

            def body():
                at = at_of(way, hop)
                own = hop == 0
                to_x(k, at, own).wait_send()
                to_y(k, at, own).wait_send()
                to_p(k, at, own).wait_send()
                for which in range(2):
                    relay(k, at, which).wait_send()
                for bit in (1, 2, 3):
                    pass_p(k, at, bit).wait_send()
                if hop < 3:
                    if own:

                        @pl.when(has_up)
                        def _():
                            z_send(k, c, 0, 1).wait_send()

                        @pl.when(has_down)
                        def _():
                            z_send(k, c, 1, 1).wait_send()
                    else:
                        can = has_up if way == 0 else has_down

                        @pl.when(can)
                        def _():
                            z_send(k, at, way, hop + 1).wait_send()

            guard(way, hop, body)
    for j in (1, 2, 3):
        q(j).wait()
        kv(j).wait_send()
    for j in range(4):
        pair(j).wait()
    pltpu.make_async_copy(ints, ints_out.at[d], il.at[0]).wait()
    rcopy(ints, ints_out.at[1 - d], il.at[1], il.at[2], pn).wait()


VM = pl.BlockSpec(memory_space=pltpu.VMEM)


def gather_fast(shards, tokens, ints, wide, cid):
    kinds = len(shards)
    dma = pltpu.SemaphoreType.DMA
    _, feats, cols = tokens.shape
    own = cols // 2
    piece = jax.ShapeDtypeStruct((4, wide, own), bf16)
    return pl.pallas_call(
        functools.partial(gather_kernel, kinds),
        out_shape=[jax.ShapeDtypeStruct((4, 4, 2) + s.shape, s.dtype) for s in shards]
        + [
            jax.ShapeDtypeStruct((4, feats, own), tokens.dtype),
            jax.ShapeDtypeStruct((2,) + ints.shape, ints.dtype),
            piece,
            jax.ShapeDtypeStruct((4, 2, 2 * wide, own), bf16),
            jax.ShapeDtypeStruct((4 * wide, 4 * feats), bf16),
        ],
        in_specs=[HBM] * (kinds + 2),
        out_specs=[VM, VM] + [HBM] * (kinds - 2) + [VM, HBM, VM, VM, VM],
        scratch_shapes=[
            pltpu.VMEM((own, 4 * feats), bf16),
            pltpu.VMEM((4, wide, own), bf16),
            pltpu.VMEM((4, 2 * wide, own), bf16),
            dma((kinds,)),
            dma((kinds, 2, 3)), dma((kinds, 2, 3)),
            dma((kinds, 4)), dma((kinds, 4)),
            dma((kinds, 4)), dma((kinds, 4)),
            dma((kinds, 4, 2)), dma((kinds, 4, 2)),
            dma((kinds, 4, 4)), dma((kinds, 4, 4)),
            dma, dma((4,)), dma((4,)), dma((3,)),
            dma((2, 4)), dma((2, 4)), dma((4,)), dma((4,)),
        ],
        compiler_params=pltpu.CompilerParams(
            collective_id=cid, has_side_effects=True, vmem_limit_bytes=40 * 1024 * 1024
        ),
        name="head",
    )(*shards, tokens, ints)


def scatter_core(grads, outs, scratch, begin, during, late=0, gap=0):
    kinds = len(grads)
    (acc, precv, xr1, yr1, xr2, yr2, zup, zdn, fin) = scratch[:9]
    (ls, ps, pr, xs1, xm1, ys1, ym1, xs2, xm2, ys2, ym2, us, um, ds, dm, fs, fm, os) = scratch[9:]
    d, r, c = place()
    cols = 4
    chunks = kinds * cols
    xn, yn, pn = (d, r ^ 1, c), (d, r ^ 2, c), (1 - d, r, c)
    up, down = (d, r, c + 1), (d, r, c - 1)
    half = acc.shape[2] // 2
    first, last = pl.ds(0, half), pl.ds(half, half)

    def split(i):
        k = i // cols
        j = i - k * cols
        at = jnp.where(j == 0, 0, jnp.where(j == 1, 3, j - 1))
        return k, at

    def at_static(i):
        return i // cols, (0, 3, 1, 2)[i % cols]

    def load(i):
        k, at = at_static(i)
        return pltpu.make_async_copy(grads[k].at[at, :, d], acc.at[i], ls.at[i])

    def pair(i):
        k, at = at_static(i)
        return rcopy(grads[k].at[at, :, 1 - d], precv.at[i], ps.at[i], pr.at[i], pn)

    def launch(i):
        pair(i).start()
        load(i).start()

    for i in range((kinds - late) * cols):
        launch(i)
    begin()

    def x1(i, j):
        return rcopy(acc.at[i, r ^ 1 ^ (2 * j), first], xr1.at[i, j], xs1.at[i, j], xm1.at[i, j], xn)

    def y1(i, j):
        return rcopy(acc.at[i, r ^ 2 ^ j, last], yr1.at[i, j], ys1.at[i, j], ym1.at[i, j], yn)

    def y2(i):
        return rcopy(acc.at[i, r ^ 2, first], yr2.at[i], ys2.at[i], ym2.at[i], yn)

    def x2(i):
        return rcopy(acc.at[i, r ^ 1, last], xr2.at[i], xs2.at[i], xm2.at[i], xn)

    def to_up(i):
        return rcopy(acc.at[i, r], zup.at[i], us.at[i], um.at[i], up)

    def to_down(i):
        return rcopy(acc.at[i, r], zdn.at[i], ds.at[i], dm.at[i], down)

    def stage1(i):
        pltpu.make_async_copy(precv.at[i], acc.at[i], ls.at[i]).wait()
        rcopy(acc.at[i], precv.at[i], ps.at[i], pr.at[i], pn).wait_recv()

        @pl.loop(0, 4)
        def _(row):
            acc[i, row] = acc[i, row] + precv[i, row]

        x1(i, 1).start()
        y1(i, 1).start()
        x1(i, 0).start()
        y1(i, 0).start()

    def stage2(i):
        x1(i, 1).wait_recv()
        acc[i, r ^ 2, first] = acc[i, r ^ 2, first] + xr1[i, 1]
        y2(i).start()
        y1(i, 1).wait_recv()
        acc[i, r ^ 1, last] = acc[i, r ^ 1, last] + yr1[i, 1]
        x2(i).start()
        x1(i, 0).wait_recv()
        acc[i, r, first] = acc[i, r, first] + xr1[i, 0]
        y1(i, 0).wait_recv()
        acc[i, r, last] = acc[i, r, last] + yr1[i, 0]

    def stage3(i):
        y2(i).wait_recv()
        acc[i, r, first] = acc[i, r, first] + yr2[i]
        x2(i).wait_recv()
        acc[i, r, last] = acc[i, r, last] + xr2[i]

    def stage4(i, hops):
        k, at = split(i)

        @pl.when((at > c) & (c == hops))
        def _():
            @pl.when(c > 0)
            def _():
                to_up(i).wait_recv()
                acc[i, r] = acc[i, r] + zup[i]

            to_up(i).start()

        @pl.when((at < c) & (cols - 1 - c == hops))
        def _():
            @pl.when(c < cols - 1)
            def _():
                to_down(i).wait_recv()
                acc[i, r] = acc[i, r] + zdn[i]

            to_down(i).start()

        @pl.when((at == c) & (jnp.maximum(c, cols - 1 - c) == hops))
        def _():
            @pl.when(c > 0)
            def _():
                to_up(i).wait_recv()
                acc[i, r] = acc[i, r] + zup[i]

            @pl.when(c < cols - 1)
            def _():
                to_down(i).wait_recv()
                acc[i, r] = acc[i, r] + zdn[i]

            fin[k, d] = acc[i, r]
            rcopy(fin.at[k, d], fin.at[k, d], fs.at[k], fm.at[k], pn).start()

    stages = [(0, stage1), (2, stage2), (4, stage3)]
    stages += [(5 + h, functools.partial(lambda h, i: stage4(i, h), h)) for h in range(cols)]
    ending = stages[-1][0]

    assert len(during) <= chunks + gap + ending
    early = (kinds - late) * cols

    @pl.loop(0, chunks + gap + ending)
    def _(step):
        for i, extra in enumerate(during):
            pl.when(step == i)(functools.partial(extra, launch))

        for lag, stage in stages:

            spot = step - lag
            there = (spot >= 0) & (spot < early) | (spot >= early + gap) & (spot < chunks + gap)

            @pl.when(there)
            def _():
                stage(jnp.where(spot < early, spot, spot - gap))

    @pl.loop(0, chunks)
    def _(i):
        k, at = split(i)
        rcopy(acc.at[i], precv.at[i], ps.at[i], pr.at[i], pn).wait_send()
        for j in range(2):
            x1(i, j).wait_send()
            y1(i, j).wait_send()
        y2(i).wait_send()
        x2(i).wait_send()

        @pl.when(at > c)
        def _():
            to_up(i).wait_send()

        @pl.when(at < c)
        def _():
            to_down(i).wait_send()

    for k in range(kinds):
        rcopy(fin.at[k, 1 - d], fin.at[k, 1 - d], fs.at[k], fm.at[k], pn).wait()
        pltpu.make_async_copy(fin.at[k], outs[k], os.at[k]).start()
    for k in range(kinds):
        pltpu.make_async_copy(fin.at[k], outs[k], os.at[k]).wait()

def scatter_scratch(kinds, n, w, dt):
    dma = pltpu.SemaphoreType.DMA
    chunks = kinds * 4
    return [
        pltpu.VMEM((chunks, 4, n, w), dt),
        pltpu.VMEM((chunks, 4, n, w), dt),
        pltpu.VMEM((chunks, 2, n // 2, w), dt),
        pltpu.VMEM((chunks, 2, n // 2, w), dt),
        pltpu.VMEM((chunks, n // 2, w), dt),
        pltpu.VMEM((chunks, n // 2, w), dt),
        pltpu.VMEM((chunks, n, w), dt),
        pltpu.VMEM((chunks, n, w), dt),
        pltpu.VMEM((kinds, 2, n, w), dt),
        dma((chunks,)), dma((chunks,)), dma((chunks,)),
        dma((chunks, 2)), dma((chunks, 2)), dma((chunks, 2)), dma((chunks, 2)),
        dma((chunks,)), dma((chunks,)), dma((chunks,)), dma((chunks,)),
        dma((chunks,)), dma((chunks,)), dma((chunks,)), dma((chunks,)),
        dma((kinds,)), dma((kinds,)), dma((kinds,)),
    ]


def give_moves(src_ref, out_ref, local, send, recv):
    d, r, c = place()
    own = src_ref.shape[2]
    home = r // 2

    def slot(i, core):
        return out_ref.at[i, :, pl.ds(pl.multiple_of(core * own, own), own)]

    def move(row):
        return rcopy(src_ref.at[row], slot(r % 2, d), send.at[row], recv.at[r % 2, d], (home, row, c))

    def stay():
        return pltpu.make_async_copy(src_ref.at[r], slot(r % 2, d), local)

    def start():
        for row in range(4):

            @pl.when(jnp.logical_not((row == r) & (home == d)))
            def _():
                move(row).start()

        @pl.when(home == d)
        def _():
            stay().start()

    def finish():
        for row in range(4):

            @pl.when(jnp.logical_not((row == r) & (home == d)))
            def _():
                move(row).wait_send()

        @pl.when(home == d)
        def _():
            stay().wait()

        for i in range(2):
            for core in range(2):

                @pl.when(jnp.logical_not((2 * d + i == r) & (core == d)))
                def _():
                    rcopy(src_ref.at[0], slot(i, core), send.at[0], recv.at[i, core], (d, r, c)).wait_recv()

    return start, finish


def plane_peers():
    d, r, c = place()
    return [(d ^ (j // 4), r ^ (j % 4), c) for j in range(1, 8)]


def line_peers():
    d, r, c = place()
    return [(d ^ (j // 4), r, c ^ (j % 4)) for j in range(1, 8)]


def swap_kernel(src, cot, out, cot_out, send, recv, tl, ts, tr):
    d, r, c = place()
    greet(plane_peers() + [(d, r, c ^ j) for j in (1, 2, 3)])

    def move(j):
        return rcopy(src.at[c ^ j], out.at[c], send.at[j], recv.at[j], (d, r, c ^ j))

    for j in (3, 2, 1):
        move(j).start()
    moves = take_copies(cot, cot_out, tl, ts, tr)
    for start, _ in moves:
        start()
    out[c] = src[c]
    for j in (1, 2, 3):
        move(j).wait()
    for _, wait in moves:
        wait()


def swap_fast(values, cotangent, cid):
    dma = pltpu.SemaphoreType.DMA
    _, feats, cols = cotangent.shape
    return pl.pallas_call(
        swap_kernel,
        out_shape=[
            jax.ShapeDtypeStruct(values.shape, values.dtype),
            jax.ShapeDtypeStruct((4, feats, cols // 2), cotangent.dtype),
        ],
        in_specs=[VM, HBM],
        out_specs=[VM, VM],
        scratch_shapes=[dma((4,)), dma((4,)), dma, dma((4,)), dma((4,))],
        compiler_params=pltpu.CompilerParams(collective_id=cid, has_side_effects=True),
        name="swap",
    )(values, cotangent)


def sum_steps(src, total, parts, sems):
    d, r, c = place()
    peers = [(1 - d, r, c), (d, r ^ 1, c), (d, r ^ 2, c), (d, r, c ^ 1), (d, r, c ^ 2)]
    bits = [d, r % 2, r // 2, c % 2, c // 2]
    rs, rr, gs, gr = sems
    count = len(peers)
    size = [src.shape[0] >> (i + 1) for i in range(count)]
    offset = [jnp.int32(0)]
    for i in range(count):
        offset.append(offset[i] + bits[i] * size[i])

    def rows(at, amount):
        return pl.ds(pl.multiple_of(at, 8), amount)

    def down(i):
        other = offset[i] + (1 - bits[i]) * size[i]
        held = src if i == 0 else parts[i - 1]
        at = other if i == 0 else other - offset[i]
        return rcopy(held.at[rows(at, size[i])], parts[count + i], rs.at[i], rr.at[i], peers[i])

    def fold(i):
        down(i).wait_recv()
        held = src if i == 0 else parts[i - 1]
        at = offset[i + 1] if i == 0 else offset[i + 1] - offset[i]
        parts[i][...] = held[rows(at, size[i])] + parts[count + i][...]

    def back(i):
        spot = total.at[rows(offset[i + 1], size[i])]
        return rcopy(spot, spot, gs.at[i], gr.at[i], peers[i])

    def back_recv(i):
        spot = total.at[rows(offset[i] + (1 - bits[i]) * size[i], size[i])]
        rcopy(spot, spot, gs.at[i], gr.at[i], peers[i]).wait_recv()

    steps = [lambda: down(0).start()]
    for i in range(1, count):

        def step(i=i):
            fold(i - 1)
            down(i).start()

        steps.append(step)

    def middle():
        fold(count - 1)
        total[rows(offset[count], size[-1])] = parts[count - 1][...]
        back(count - 1).start()

    steps.append(middle)
    for i in range(count - 2, -1, -1):

        def step(i=i):
            back_recv(i + 1)
            back(i).start()

        steps.append(step)

    def end():
        back_recv(0)
        for i in range(count):
            down(i).wait_send()
            back(i).wait_send()

    return steps, end


highest = lax.Precision.HIGHEST


def fine(a, b, contract=((1,), (0,))):
    return lax.dot_general(a, b, (contract, ((), ())), precision=highest, preferred_element_type=f32)


def same_head(size, part):
    one = lax.broadcasted_iota(jnp.int32, (size, size), 0) // part
    two = lax.broadcasted_iota(jnp.int32, (size, size), 1) // part
    return (one == two).astype(f32)


def student_stats(docs, scale, out_ref, seg_ref, proj_ref, vec_ref, hidden, logit, stats):
    width = hidden.shape[1]
    h = jnp.dot(out_ref[...], proj_ref[...], preferred_element_type=f32) + vec_ref[0:1]
    pool = fine(h * vec_ref[1:2], same_head(width, SHD)) * scale
    hidden[...] = h
    logit[...] = pool
    stats[0:8] = jnp.zeros((8, width), f32)
    stats[8:16] = jnp.zeros((8, width), f32)
    stats[16:24] = jnp.ones((8, width), f32)
    for doc in range(docs):
        mine = seg_ref[...] == doc
        top = jnp.max(jnp.where(mine, pool, masked_value), axis=0, keepdims=True)
        weight = jnp.where(mine, jnp.exp(pool - top), 0.0)
        stats[doc : doc + 1] = jnp.sum(weight * h, axis=0, keepdims=True)
        stats[8 + doc : 9 + doc] = top
        stats[16 + doc : 17 + doc] = jnp.sum(weight, axis=0, keepdims=True)


def student_grads(docs, classes, scale, once, row, out_ref, seg_ref, label_ref, vec_ref, mid_ref, cls_ref, hidden, logit, stats, small):
    width = hidden.shape[1]
    every = [stats[i, j] for i in range(stats.shape[0]) for j in range(stats.shape[1])]
    top = every[0][8:16]
    for one in every[1:]:
        top = jnp.maximum(top, one[8:16])
    total = jnp.zeros_like(top)
    pooled = jnp.zeros_like(top)
    for one in every:
        factor = jnp.exp(one[8:16] - top)
        total = total + one[16:24] * factor
        pooled = pooled + one[0:8] * factor
    pooled = pooled / total
    middle = jnp.tanh(fine(pooled, mid_ref[...]) + vec_ref[2:3])
    logits = fine(middle, cls_ref[...]) + vec_ref[3:4]
    lane = lax.broadcasted_iota(jnp.int32, logits.shape, 1)
    doc = lax.broadcasted_iota(jnp.int32, logits.shape, 0)
    real = lane < classes
    peak = jnp.max(jnp.where(real, logits, masked_value), axis=1, keepdims=True)
    share = jnp.where(real, jnp.exp(logits - peak), 0.0)
    share = share / jnp.sum(share, axis=1, keepdims=True)
    d_logits = jnp.where(doc < docs, share - (label_ref[...] == lane).astype(f32), 0.0)
    d_middle = fine(d_logits, cls_ref[...], ((1,), (1,))) * (1.0 - middle * middle)
    d_pooled = fine(d_middle, mid_ref[...], ((1,), (1,)))
    zeros = jnp.zeros((1, width), f32)
    small[768:896] = fine(pooled, d_middle, ((0,), (0,))) * once
    small[896:912] = fine(d_logits, middle, ((0,), (0,)))[0:16] * once
    small[912:913] = jnp.sum(d_middle, axis=0, keepdims=True) * once
    small[913:914] = jnp.sum(d_logits, axis=0, keepdims=True) * once
    for at in range(4):
        small[920 + 8 * at : 928 + 8 * at] = jnp.where(row == at, logits * once, 0.0)

    heads = same_head(width, SHD)
    base = fine(d_pooled * pooled, heads)
    h, pool = hidden[...], logit[...]
    top_t, total_t = jnp.zeros_like(h), jnp.ones_like(h)
    back_t, base_t = jnp.zeros_like(h), jnp.zeros_like(h)
    for doc in range(docs):
        mine = seg_ref[...] == doc
        top_t = jnp.where(mine, top[doc : doc + 1], top_t)
        total_t = jnp.where(mine, total[doc : doc + 1], total_t)
        back_t = jnp.where(mine, d_pooled[doc : doc + 1], back_t)
        base_t = jnp.where(mine, base[doc : doc + 1], base_t)
    share = jnp.exp(pool - top_t) / total_t
    d_pool = share * (fine(back_t * h, heads) - base_t)
    d_h = share * back_t + d_pool * vec_ref[1:2] * scale
    small[914:915] = jnp.sum(d_h, axis=0, keepdims=True)
    small[915:916] = jnp.sum(d_pool * h, axis=0, keepdims=True) * scale
    for i in range(916, 920):
        small[i : i + 1] = zeros
    small[0:768] = fine(out_ref[...].astype(f32), d_h, ((0,), (0,)))


def tail_kernel(docs, classes, scale, *refs):
    kinds = 2
    grads, refs = refs[:kinds], refs[kinds:]
    (q_ref, kv_ref, lse_ref, ctx_ref, dctx_ref, qseg_ref, kseg_ref), refs = refs[:7], refs[7:]
    (out_ref, seg_ref, label_ref, proj_ref, svec_ref, mid_ref, cls_ref), refs = refs[:7], refs[7:]
    vec_refs, refs = refs[:7], refs[7:]
    (x_ref, ctx_all_ref, resid_ref, out_t_ref, w_ref), refs = refs[:5], refs[5:]
    outs, refs = refs[: kinds + 1], refs[kinds + 1 :]
    (give_out, out_out, small_out), refs = refs[:3], refs[3:]
    (total, theirs, dqkv, own_grads, dpad, weights, resid_t, give_src), refs = refs[:8], refs[8:]
    (dctx, dq, dkv, kn, vn, q3, dc3, dq_scr, dkv_scr, bias_scr), refs = refs[:10], refs[10:]
    (hidden, logit, stats, stats_all, small), refs = refs[:5], refs[5:]
    parts, refs = refs[:10], refs[10:]
    (send, recv, psend, precv), sems, (wl, gl, gs, gr), refs = refs[:4], refs[4:8], refs[8:12], refs[12:]
    (dsend, drecv, ssend, srecv, ol, osend, orecv), scratch = refs[:7], refs[7:]
    d, r, c = place()
    pn = (1 - d, r, c)
    tiles, deep, tile = kv_ref.shape
    wide = deep // 2
    heads = wide // HD
    full = dqkv.shape[1]
    own = q_ref.shape[2]
    kv_rows, q_rows = pl.ds(0, deep), pl.ds(deep, wide)
    peers = line_peers()
    greet(plane_peers() + peers[:3] + peers[4:])

    def to_heads(j):
        return rcopy(dctx_ref.at[c ^ j], dctx.at[c], dsend.at[j], drecv.at[j], (d, r, c ^ j))

    for j in (3, 2, 1):
        to_heads(j).start()
    dctx[c] = dctx_ref[c]
    load_w = pltpu.make_async_copy(w_ref, weights, wl)
    load_w.start()

    def tell(j):
        return rcopy(stats, stats_all.at[d, c], ssend.at[j - 1], srecv.at[j - 1], peers[j - 1])

    out_start, out_finish = give_moves(out_t_ref, out_out, ol, osend, orecv)
    start, finish = give_moves(give_src, give_out, gl, gs, gr)
    steps, end = sum_steps(small, small_out, parts, sems)
    pool_scale = SHD ** (-0.5)

    def begin():
        out_start()
        student_stats(docs, pool_scale, out_ref, seg_ref, proj_ref, svec_ref, hidden, logit, stats)
        for j in range(1, 8):
            tell(j).start()
        stats_all[d, c] = stats[...]
        spare = full - deep - wide
        for at in range(4):
            dqkv[at, pl.ds(deep + wide, spare)] = jnp.zeros((spare, own), bf16)
        resid_t[...] = resid_ref[...].T
        feats = x_ref.shape[1]
        blank = dpad.shape[1] - feats
        for row in range(4):
            dpad[row, pl.ds(0, blank)] = jnp.zeros((blank, own), bf16)
            dpad[row, pl.ds(blank, feats)] = resid_t[pl.ds(row * feats, feats)].astype(bf16)
        at = 952
        for ref in vec_refs:
            for i in range(ref.shape[0]):
                for j in range(ref.shape[1] // 128):
                    small[at : at + 1] = ref[i : i + 1, j * 128 : (j + 1) * 128]
                    at += 1
        for i in range(at, small.shape[0]):
            small[i : i + 1] = jnp.zeros((1, 128), f32)

    def student(_):
        for j in range(1, 8):
            tell(j).wait_recv()
        once = 1.0 / 8
        student_grads(
            docs, classes, pool_scale, once, r, out_ref, seg_ref, label_ref, svec_ref, mid_ref, cls_ref, hidden, logit,
            stats_all, small,
        )

    def prepare(_):
        @pl.loop(0, tiles)
        def _(j):
            kn[j] = kv_ref[j, pl.ds(0, wide)].astype(f32).T.astype(bf16)
            vn[j] = kv_ref[j, pl.ds(wide, wide)].astype(f32).T.astype(bf16)
            dkv_scr[j] = jnp.zeros((deep, tile), f32)

        bias_scr[...] = jnp.zeros_like(bias_scr)
        for j in (1, 2, 3):
            to_heads(j).wait_recv()

    ones = jnp.ones((8, own), bf16)
    across = (((1,), (1,)), ((), ()))

    def attend_block(block, _):
        q_at, dc_at = q_ref.at[pl.ds(block, 1)], dctx.at[pl.ds(block, 1)]
        block_rows(q_at, heads, scale, q3)
        block_rows(dc_at, heads, 1.0, dc3)
        qseg = jnp.concatenate([qseg_ref[block]] * heads, axis=1)
        lse = lse_ref[block]
        product = ctx_ref[block].astype(f32) * dctx[block].astype(f32)
        delta = jnp.concatenate(
            [jnp.sum(product[h * HD : (h + 1) * HD], axis=0, keepdims=True) for h in range(heads)], axis=1
        )
        dq_scr[...] = jnp.zeros_like(dq_scr)
        here = 2 * block + d

        @pl.loop(jnp.maximum(here - 4, 0), jnp.minimum(here + 5, tiles))
        def _(j):
            s = jnp.dot(kn[j], q3[...], preferred_element_type=f32)
            s = jnp.where(kseg_ref[j] == qseg, s, masked_value)
            p = jnp.exp(s - lse)
            d_p = jnp.dot(vn[j], dc3[...], preferred_element_type=f32)
            d_s = (p * (d_p - delta)).astype(bf16)
            p = p.astype(bf16)
            for h in range(heads):
                rows, lanes = pl.ds(h * HD, HD), slice(h * own, (h + 1) * own)
                dq_scr[rows] += jnp.dot(kv_ref[j, rows], d_s[:, lanes], preferred_element_type=f32)
                dkv_scr[j, rows] += lax.dot_general(q3[rows, lanes], d_s[:, lanes], across, preferred_element_type=f32)
                low = pl.ds(wide + h * HD, HD)
                dkv_scr[j, low] += lax.dot_general(dctx[block, rows], p[:, lanes], across, preferred_element_type=f32)

        made = (dq_scr[...] * scale).astype(bf16)
        dq[block] = made
        bias_scr[:, :wide] += lax.dot_general(ones, made, across, preferred_element_type=f32)

    def pair(j):
        return rcopy(dkv.at[c ^ j, 1 - d], theirs.at[c ^ j], psend.at[j], precv.at[j], pn)

    def kv(j):
        return rcopy(total.at[c ^ j], dqkv.at[c, kv_rows], send.at[0, j], recv.at[0, j], (d, r, c ^ j))

    def q(j):
        return rcopy(dq.at[c ^ j], dqkv.at[c, q_rows], send.at[1, j], recv.at[1, j], (d, r, c ^ j))

    def leave(_):
        for j in (3, 2, 1, 0):
            for core in range(2):
                tile_at = 2 * (c ^ j) + core
                dkv[c ^ j, core] = dkv_scr[tile_at].astype(bf16)
            pair(j).start()
            if j:
                q(j).start()
        dqkv[c, q_rows] = dq[c]
        for j in (3, 2, 1):
            pair(j).wait_recv()
            total[c ^ j] = dkv[c ^ j, d] + theirs[c ^ j]
            kv(j).start()
        pair(0).wait_recv()
        dqkv[c, kv_rows] = dkv[c, d] + theirs[c]

        @pl.loop(0, 4)
        def _(at):
            for core in range(2):
                some = dkv[at, core, pl.ds(wide, wide)]
                bias_scr[:, wide:] += lax.dot_general(ones, some, across, preferred_element_type=f32)

        for i in range(3):
            small[pl.ds(1012 + 3 * c + i, 1)] = bias_scr[0:1, i * 128 : (i + 1) * 128]

    def make(at):
        lead = full - dpad.shape[1]

        @pl.loop(0, 4)
        def _(row):
            one = lax.dot_general(x_ref[row], dqkv[at], across, preferred_element_type=f32)
            two = lax.dot_general(ctx_all_ref[at], dpad[row], across, preferred_element_type=f32)
            shape = own_grads.shape[2:4] + (-1,)
            own_grads[at, row, :, :, :lead] = one[:, :lead].astype(bf16).reshape(shape)
            own_grads[at, row, :, :, lead:] = (one[:, lead:] + two).astype(bf16).reshape(shape)

    def make_chunk(j, launch):
        if j == 0:
            for far in (1, 2, 3):
                q(far).wait_recv()
                kv(far).wait_recv()
        make((0, 3, 1, 2)[j])
        launch(kinds * 4 + j)

    def input_grad(_):
        load_w.wait()
        feats = x_ref.shape[1]

        @pl.loop(0, 4)
        def _(row):
            part = resid_t[pl.ds(pl.multiple_of(row * feats, 8), feats)]
            for at in range(4):
                w = weights[at, row].reshape(feats, full)
                part = part + jnp.dot(w, dqkv[at], preferred_element_type=f32)
            give_src[row] = part.astype(bf16)

        start()

    gap = 6
    hooks = [[] for _ in range(8 + gap + 5)]
    hooks[1].append(student)
    hooks[2].append(prepare)
    for block in range(4):
        hooks[3 + block].append(functools.partial(attend_block, block))
    hooks[7].append(leave)
    for i, step in enumerate(steps):
        hooks[8 + i].append(lambda launch, step=step: step())
    for j in range(4):
        hooks[7 + gap + j].append(functools.partial(make_chunk, j))
    hooks[11 + gap].append(input_grad)

    def run(todo, launch):
        for one in todo:
            one(launch)

    during = [functools.partial(run, todo) for todo in hooks]
    scatter_core(list(grads) + [own_grads], outs, scratch, begin, during, late=1, gap=gap)
    end()
    finish()
    out_finish()
    for j in range(1, 8):
        tell(j).wait_send()
    for j in range(4):
        pair(j).wait_send()
    for j in (1, 2, 3):
        to_heads(j).wait_send()
        q(j).wait_send()
        kv(j).wait_send()


def tail_fast(docs, classes, scale, grads, attention, student, vectors, rest, out_t, w_attn, cid):
    n, w = grads[0].shape[3:]
    q, kv = attention[:2]
    dma = pltpu.SemaphoreType.DMA
    tiles, deep, own = kv.shape
    wide = deep // 2
    cols = tiles // 2
    feats = rest[0].shape[1]
    student_width = student[3].shape[1]
    tall = 1024
    parts = [pltpu.VMEM((tall >> (i + 1), 128), f32) for i in range(5)]
    home = jax.ShapeDtypeStruct((2, feats, 2 * own), bf16)
    return pl.pallas_call(
        functools.partial(tail_kernel, docs, classes, scale),
        out_shape=[jax.ShapeDtypeStruct((2, n, w), bf16)] * 3 + [home, home, jax.ShapeDtypeStruct((tall, 128), f32)],
        in_specs=[HBM] * 2 + [VM] * (len(attention) + len(student) + len(vectors) + len(rest)) + [HBM] * 2,
        out_specs=[HBM] * 5 + [VM],
        scratch_shapes=[
            pltpu.VMEM((cols, deep, own), bf16),
            pltpu.VMEM((cols, deep, own), bf16),
            pltpu.VMEM((cols, w, own), bf16),
            pltpu.VMEM((4, 4, 2, n, w), bf16),
            pltpu.VMEM((4, 256, own), bf16),
            pltpu.VMEM((4, 4, 2, n, w), bf16),
            pltpu.VMEM((4 * feats, own), f32),
            pltpu.VMEM((4, feats, own), bf16),
            pltpu.VMEM((cols, wide, own), bf16),
            pltpu.VMEM((cols, wide, own), bf16),
            pltpu.VMEM((cols, 2, deep, own), bf16),
            pltpu.VMEM((tiles, own, wide), bf16),
            pltpu.VMEM((tiles, own, wide), bf16),
            pltpu.VMEM((wide, wide // HD * own), bf16),
            pltpu.VMEM((wide, wide // HD * own), bf16),
            pltpu.VMEM((wide, own), f32),
            pltpu.VMEM((tiles, deep, own), f32),
            pltpu.VMEM((8, deep), f32),
            pltpu.VMEM((own, student_width), f32),
            pltpu.VMEM((own, student_width), f32),
            pltpu.VMEM((24, student_width), f32),
            pltpu.VMEM((2, 4, 24, student_width), f32),
            pltpu.VMEM((tall, 128), f32),
        ]
        + parts * 2
        + [dma((2, 4)), dma((2, 4)), dma((4,)), dma((4,)), dma((5,)), dma((5,)), dma((5,)), dma((5,))]
        + [dma, dma, dma((4,)), dma((2, 2))]
        + [dma((4,)), dma((4,)), dma((7,)), dma((7,)), dma, dma((4,)), dma((2, 2))]
        + scatter_scratch(3, n, w, bf16),
        compiler_params=pltpu.CompilerParams(
            collective_id=cid, has_side_effects=True, vmem_limit_bytes=60 * 1024 * 1024
        ),
        name="tail",
    )(*grads, *attention, *student, *vectors, *rest, out_t.reshape(4, feats, own), w_attn)


def dot(a, b, contract=((1,), (0,))):
    return lax.dot_general(a, b, (contract, ((), ())), preferred_element_type=f32)


def block_rows(ref, heads, scale, out):
    own = ref.shape[-1]
    for h in range(heads):
        for g in range(heads):
            spot = (pl.ds(h * HD, HD), pl.ds(g * own, own))
            if h == g:
                out[spot] = ref[0, pl.ds(h * HD, HD)] * jnp.asarray(scale, out.dtype)
            else:
                out[spot] = jnp.zeros((HD, own), out.dtype)


def attn_fwd_kernel(heads, scale, bounds, q_ref, kv_ref, qseg_ref, kseg_ref, ctx_ref, lse_ref, kn, q3, s_scr, o_scr):
    step = pl.program_id(0)
    tiles, _, tile = kv_ref.shape
    wide = heads * HD
    own = q_ref.shape[-1]

    @pl.when(step == 0)
    def _():
        @pl.loop(0, tiles)
        def _(j):
            kn[j] = kv_ref[j, pl.ds(0, wide)].astype(f32).T.astype(bf16)

    block_rows(q_ref, heads, scale, q3)
    low, high = bounds[step, 0], bounds[step, 1]
    qseg = jnp.concatenate([qseg_ref[0]] * heads, axis=1)

    def one(j, top):
        s = dot(kn[j], q3[...])
        s = jnp.where(kseg_ref[j] == qseg, s, masked_value)
        s_scr[j] = s
        return jnp.maximum(top, jnp.max(s, axis=0, keepdims=True))

    top = lax.fori_loop(low, high, one, jnp.full((1, heads * own), masked_value, f32))
    o_scr[...] = jnp.zeros_like(o_scr)

    def two(j, total):
        p = jnp.exp(s_scr[j] - top)
        low_p = p.astype(bf16)
        for h in range(heads):
            rows = pl.ds(h * HD, HD)
            v = kv_ref[j, pl.ds(wide + h * HD, HD)]
            o_scr[rows] += dot(v, low_p[:, h * own : (h + 1) * own])
        return total + jnp.sum(p, axis=0, keepdims=True)

    total = lax.fori_loop(low, high, two, jnp.zeros((1, heads * own), f32))
    for h in range(heads):
        rows = pl.ds(h * HD, HD)
        ctx_ref[0, rows] = (o_scr[rows] / total[:, h * own : (h + 1) * own]).astype(bf16)
    lse_ref[0] = top + jnp.log(total)


def attn_fwd(bounds, q, kv, qseg, kseg, scale):
    blocks, wide, own = q.shape
    tiles, _, tile = kv.shape
    heads = wide // HD
    return pl.pallas_call(
        functools.partial(attn_fwd_kernel, heads, scale),
        out_shape=[
            jax.ShapeDtypeStruct(q.shape, bf16),
            jax.ShapeDtypeStruct((blocks, 1, heads * own), f32),
        ],
        grid_spec=pltpu.PrefetchScalarGridSpec(
            num_scalar_prefetch=1,
            grid=(blocks,),
            in_specs=[
                pl.BlockSpec((1, wide, own), lambda i, b: (i, 0, 0)),
                pl.BlockSpec(kv.shape, lambda i, b: (0, 0, 0)),
                pl.BlockSpec((1, 1, own), lambda i, b: (i, 0, 0)),
                pl.BlockSpec(kseg.shape, lambda i, b: (0, 0, 0)),
            ],
            out_specs=[
                pl.BlockSpec((1, wide, own), lambda i, b: (i, 0, 0)),
                pl.BlockSpec((1, 1, heads * own), lambda i, b: (i, 0, 0)),
            ],
            scratch_shapes=[
                pltpu.VMEM((tiles, tile, wide), bf16),
                pltpu.VMEM((wide, heads * own), bf16),
                pltpu.VMEM((tiles, tile, heads * own), f32),
                pltpu.VMEM((wide, own), f32),
            ],
        ),
        compiler_params=pltpu.CompilerParams(
            dimension_semantics=("arbitrary",), vmem_limit_bytes=48 * 1024 * 1024
        ),
        name="attn_fwd",
    )(bounds, q, kv, qseg, kseg)


def fast_local(
    tokens,
    segments,
    labels,
    cotangent,
    w_qkv,
    b_qkv,
    w_out,
    b_out,
    ln1_gain,
    ln1_bias,
    w_in,
    b_in,
    w_back,
    b_back,
    ln2_gain,
    ln2_bias,
    s_proj,
    s_bias,
    s_query,
    s_mid,
    s_mid_bias,
    s_cls,
    s_cls_bias,
):
    _, width_row, cols_local = tokens.shape
    parts, rows, cols, seqs, _ = sizes(tokens.shape[0])
    width = width_row * rows
    own = cols_local // parts
    width_col = b_qkv.shape[1]
    heads_dev = width_col // HD
    hidden_col = b_in.shape[0]
    docs_count = labels.shape[1]
    class_count = s_cls.shape[1]
    student_width = s_proj.shape[1]
    seq_len = segments.shape[1]
    row_index = lax.axis_index("row")
    col_index = lax.axis_index("col")
    dp_index = lax.axis_index("dp")
    score_scale = HD ** (-0.5)
    pool_scale = SHD ** (-0.5)
    query_heads = s_query.reshape(SH, SHD)
    doc_ids = jnp.arange(docs_count, dtype=jnp.int32)
    class_ids = jnp.arange(class_count, dtype=jnp.int32)

    w_three = w_qkv.reshape(width_row, heads_dev, 3, HD).transpose(0, 2, 1, 3)
    w_three = jnp.concatenate([w_three[:, 1], w_three[:, 2], w_three[:, 0]], axis=1)
    shard_attn = own_half(jnp.concatenate([w_three.reshape(width_row, -1), w_out], axis=1))
    proj_rows = width_row // cols
    lanes = -(-3 * width_col // 128) * 128
    offsets = jnp.concatenate([jnp.zeros_like(b_qkv[0]), b_qkv[1], b_qkv[0]])
    offsets = jnp.pad(offsets, (0, lanes - 3 * width_col))
    vectors = [offsets, b_out, ln1_gain, ln1_bias, b_back, ln2_gain, ln2_bias, b_in]
    vectors.append(lax.dynamic_slice_in_dim(s_proj, col_index * proj_rows, proj_rows).astype(f32).reshape(-1))
    flat = jnp.concatenate(vectors)
    flat = jnp.pad(flat, (0, 96 * 128 - flat.shape[0])).reshape(96, 128)
    w_attn, vec, w_in_all, w_back_all, x_parts, ints, queries, kv, w_out_all = gather_fast(
        [shard_attn, own_half(flat), own_half(w_in), own_half(w_back)],
        tokens,
        jnp.concatenate([segments, labels], axis=1),
        width_col,
        1,
    )
    w_in_all = w_in_all.reshape(cols, width, hidden_col)
    w_back_all = w_back_all.reshape(cols, width, hidden_col)
    vec = vec.reshape(cols, rows, -1)
    at = lanes + 6 * width_row
    row_vectors = vec[0, :, lanes:at].reshape(rows, 6, width_row).transpose(1, 0, 2).reshape(6, width)
    b_out_a, gain_one, bias_one, b_back_a, gain_two, bias_two = [row_vectors[i] for i in range(6)]
    b_in_all = vec[:, 0, at : at + hidden_col]
    at += hidden_col
    s_proj_all = vec[:, :, at : at + proj_rows * student_width].astype(bf16)
    s_proj_all = s_proj_all.reshape(cols, rows, proj_rows, student_width).transpose(1, 0, 2, 3)
    s_proj_all = s_proj_all.reshape(width, student_width)
    x_t = x_parts.reshape(width, own)
    ints = lax.dynamic_index_in_dim(ints.reshape(seqs, -1), row_index, 0, False)
    seg_all, label_seq = ints[:seq_len], ints[seq_len:]
    seg_blocks = seg_all.reshape(cols, parts, own)
    seg_q = lax.dynamic_index_in_dim(seg_blocks, dp_index, 1, False)
    seg_own = lax.dynamic_index_in_dim(seg_q, col_index, 0, False)
    lows = jnp.sum(seg_all[None, :] < seg_q[:, :1], axis=1) // own
    highs = (jnp.sum(seg_all[None, :] <= seg_q[:, -1:], axis=1) + own - 1) // own
    bounds = jnp.stack([lows, highs], axis=1).astype(jnp.int32)

    kv = kv.reshape(cols * parts, 2 * width_col, own)
    q_rows, k_rows = seg_q[:, None, :], seg_all.reshape(cols * parts, own, 1)
    context, lse = attn_fwd(bounds, queries, kv, q_rows, k_rows, score_scale)
    ctx_t, c_parts = swap_fast(context, cotangent, 3)
    ctx_parts, ctx_t = ctx_t, ctx_t.reshape(width, own)

    x = x_t.T
    attn_out = mm(ctx_t, w_out_all, ((0,), (0,))) + b_out_a
    normed_one, inv_one = normalize(x.astype(f32) + attn_out)
    hidden_one = normed_one * gain_one + bias_one
    hidden_low = hidden_one.astype(bf16)
    pre_act = jnp.einsum("td,cdn->ctn", hidden_low, w_in_all, preferred_element_type=f32)
    pre_act = pre_act + b_in_all[:, None, :]
    act = gelu_exact(pre_act).astype(bf16)
    ffn_out = jnp.einsum("ctn,cdn->td", act, w_back_all, preferred_element_type=f32) + b_back_a
    normed_two, inv_two = normalize(hidden_one + ffn_out)
    layer_out = (normed_two * gain_two + bias_two).astype(bf16)

    d_out = c_parts.reshape(width, own).T.astype(f32)
    g_ln2_gain = jnp.sum(d_out * normed_two, axis=0)
    g_ln2_bias = jnp.sum(d_out, axis=0)
    d_resid_two = normalize_back(d_out * gain_two, normed_two, inv_two)
    d_ffn = d_resid_two.astype(bf16)
    g_back_bias = jnp.sum(d_ffn.astype(f32), axis=0)
    g_back = jnp.einsum("td,ctn->cdn", d_ffn, act, preferred_element_type=f32)
    d_act = jnp.einsum("td,cdn->ctn", d_ffn, w_back_all, preferred_element_type=f32)
    _, gelu_fn = jax.vjp(gelu_exact, pre_act)
    d_pre = gelu_fn(d_act)[0].astype(bf16)
    g_in_bias = jnp.sum(d_pre.astype(f32), axis=1)
    g_in = jnp.einsum("td,ctn->cdn", hidden_low, d_pre, preferred_element_type=f32)
    d_hidden_one = d_resid_two + jnp.einsum(
        "ctn,cdn->td", d_pre, w_in_all, preferred_element_type=f32
    )
    g_ln1_gain = jnp.sum(d_hidden_one * normed_one, axis=0)
    g_ln1_bias = jnp.sum(d_hidden_one, axis=0)
    d_resid_one = normalize_back(d_hidden_one * gain_one, normed_one, inv_one)
    d_attn = d_resid_one.astype(bf16)
    g_out_bias = jnp.sum(d_attn.astype(f32), axis=0)
    d_ctx = mm(w_out_all, d_attn, ((1,), (1,))).astype(bf16)
    blocked = (cols, rows, parts, width_row // parts, -1)
    lane_pad = ((0, 0), (0, 128 - class_count))
    student_vectors = jnp.stack([s_bias, s_query, s_mid_bias, jnp.pad(s_cls_bias, (0, 128 - class_count))])
    student_vectors = jnp.pad(student_vectors, ((0, 4), (0, 0)))
    g_in, g_back, g_attn, grad_tokens, out, small = tail_fast(
        docs_count,
        class_count,
        score_scale,
        [g_in.astype(bf16).reshape(blocked), g_back.astype(bf16).reshape(blocked)],
        [queries, kv, lse, context, d_ctx.reshape(cols, width_col, own), q_rows, k_rows],
        [
            layer_out,
            seg_own[:, None],
            jnp.pad(label_seq, (0, 8 - docs_count))[:, None],
            s_proj_all,
            student_vectors,
            s_mid,
            jnp.pad(s_cls, lane_pad),
        ],
        [g_in_bias]
        + [v[None] for v in (g_out_bias, g_ln1_gain, g_ln1_bias, g_back_bias, g_ln2_gain, g_ln2_bias)],
        [x_parts, ctx_parts, d_resid_one],
        layer_out.T,
        w_attn,
        4,
    )
    g_in, g_back, g_attn = [part.reshape(width_row, -1).astype(f32) for part in (g_in, g_back, g_attn)]
    g_qkv = g_attn[:, : 3 * width_col].reshape(width_row, 3, heads_dev, HD)
    g_qkv = jnp.stack([g_qkv[:, 2], g_qkv[:, 0], g_qkv[:, 1]], axis=2).reshape(width_row, -1)

    def at_col(part):
        return lax.dynamic_index_in_dim(part, col_index, 0, False)

    def at_row(part):
        return lax.dynamic_slice_in_dim(part, row_index * width_row, width_row)

    g_sproj, g_mid, g_cls = small[:width], small[width : width + 128], small[width + 128 : width + 144].T
    g_mid_bias, g_cls_bias, g_sbias, g_query = [small[width + 144 + i] for i in range(4)]
    logits = small[width + 152 : width + 184].reshape(seqs, 8, 128)[:, :docs_count, :class_count]
    g_in_bias = small[width + 184 : width + 208].reshape(cols, hidden_col)
    vector_sums = small[width + 208 : width + 244].reshape(6, width)
    g_out_bias, g_ln1_gain, g_ln1_bias, g_back_bias, g_ln2_gain, g_ln2_bias = [vector_sums[i] for i in range(6)]
    g_qkv_bias = small[width + 244 :].reshape(cols, 2, width_col)
    logits = lax.dynamic_slice_in_dim(logits, dp_index * (seqs // parts), seqs // parts)
    return (
        out,
        logits,
        grad_tokens.astype(f32),
        g_qkv,
        at_col(g_qkv_bias),
        g_attn[:, 3 * width_col :],
        at_row(g_out_bias),
        at_row(g_ln1_gain),
        at_row(g_ln1_bias),
        g_in,
        at_col(g_in_bias),
        g_back,
        at_row(g_back_bias),
        at_row(g_ln2_gain),
        at_row(g_ln2_bias),
        at_row(g_sproj),
        g_sbias,
        g_query,
        g_mid,
        g_mid_bias,
        g_cls[:, :class_count],
        g_cls_bias[:class_count],
    )


def solution(mesh):
    row, col = P("row"), P("col")
    grid, whole = P("row", "col"), P("dp", "row", "col")
    placed = (
        (whole, P("dp", None), P("dp", None), whole, grid, P(None, "col"), P("col", "row"))
        + (row, row, row, grid, col, grid, row, row, row, P("row", None))
        + (P(),) * 6
    )
    results = (
        (whole, P("dp", None, None), whole, grid, P(None, "col"), P("col", "row"))
        + (row, row, row, grid, col, grid, row, row, row, P("row", None))
        + (P(),) * 6
    )
    quick = dict(mesh.shape) == {"dp": 2, "row": 4, "col": 4}
    local = fast_local if quick else general_local
    return jax.shard_map(local, mesh=mesh, in_specs=placed, out_specs=results, check_vma=False)
```

```python
import functools
import jax
import jax.numpy as jnp
from jax import lax
from jax.experimental import pallas as pl
from jax.experimental.pallas import tpu as pltpu
from jax.sharding import PartitionSpec as P

HD = 64
SH = 2
SHD = 64

norm_eps = 1e-06
masked_value = -1e30
highest = lax.Precision.HIGHEST
f32 = jnp.float32
bf16 = jnp.bfloat16
WORLD = ("col", "row", "dp")


def sizes(seqs_local):
    parts = lax.axis_size("dp")
    rows = lax.axis_size("row")
    seqs = seqs_local * parts
    return parts, rows, lax.axis_size("col"), seqs, rows // seqs


def row_groups(rows, sub):
    return [list(range(at, at + sub)) for at in range(0, rows, sub)]


def take_in(values):
    parts, rows, _, seqs, sub = sizes(values.shape[0])
    held = lax.all_to_all(values, "dp", 2, 0, tiled=True)
    feats, half = held.shape[1:]
    held = held.reshape(seqs, feats, sub, half // sub).transpose(0, 2, 1, 3)
    held = held.reshape(rows, feats, half // sub)
    held = lax.all_to_all(held, "row", 0, 0, tiled=True)
    return held.reshape(rows * feats, half // sub)


def give_back(values, seqs_local):
    parts, rows, _, seqs, sub = sizes(seqs_local)
    width, own = values.shape
    feats = width // rows
    held = lax.all_to_all(values.reshape(rows, feats, own), "row", 0, 0, tiled=True)
    held = held.reshape(seqs, sub, feats, own).transpose(0, 2, 1, 3).reshape(seqs, feats, sub * own)
    return lax.all_to_all(held, "dp", 0, 2, tiled=True)


def gather_world(shard):
    cols, rows = lax.axis_size("col"), lax.axis_size("row")
    out = lax.all_gather(shard, WORLD, axis=0, tiled=True)
    return out.reshape(cols, rows, -1, shard.shape[1])


def own_half(block):
    parts = lax.axis_size("dp")
    amount = block.shape[0] // parts
    return lax.dynamic_slice_in_dim(block, lax.axis_index("dp") * amount, amount)


def scatter_world(full):
    flat = full.reshape(-1, full.shape[-1])
    mine = lax.psum_scatter(flat, WORLD, scatter_dimension=0, tiled=True)
    return lax.all_gather(mine, "dp", axis=0, tiled=True)


def swap_cols(values):
    return lax.all_to_all(values, "col", 0, 0, tiled=True)


def gather_sequence(values, sub):
    cols, own, width = values.shape
    held = values[:, None]
    if sub > 1:
        groups = row_groups(lax.axis_size("row"), sub)
        held = lax.all_gather(held, "row", axis=1, tiled=True, axis_index_groups=groups)
    held = lax.all_gather(held[:, None], "dp", axis=1, tiled=True)
    return held.reshape(-1, width)


def scatter_sequence(values, cols, sub):
    parts = lax.axis_size("dp")
    width = values.shape[-1]
    held = values.reshape(cols, parts, sub, -1, width)
    held = lax.psum_scatter(held, "dp", scatter_dimension=1, tiled=True)[:, 0]
    if sub > 1:
        groups = row_groups(lax.axis_size("row"), sub)
        held = lax.psum_scatter(
            held, "row", scatter_dimension=1, tiled=True, axis_index_groups=groups
        )
    return held[:, 0]


def normalize(values):
    mean_v = jnp.mean(values, axis=-1, keepdims=True)
    center = values - mean_v
    inv_std = lax.rsqrt(jnp.mean(center * center, axis=-1, keepdims=True) + norm_eps)
    return center * inv_std, inv_std


def normalize_back(grad_hat, normed, inv_std):
    return inv_std * (
        grad_hat
        - jnp.mean(grad_hat, axis=-1, keepdims=True)
        - normed * jnp.mean(grad_hat * normed, axis=-1, keepdims=True)
    )


def gelu_exact(values):
    return jax.nn.gelu(values, approximate=False)


def mm(a, b, contract):
    return lax.dot_general(a, b, (contract, ((), ())), preferred_element_type=f32)


def combine_pool(part_one, part_two):
    top_a, total_a, sum_a = part_one
    top_b, total_b, sum_b = part_two
    row_top = jnp.maximum(top_a, top_b)
    factor_a = jnp.exp(top_a - row_top)
    factor_b = jnp.exp(top_b - row_top)
    return (
        row_top,
        total_a * factor_a + total_b * factor_b,
        sum_a * factor_a[:, :, None] + sum_b * factor_b[:, :, None],
    )


def attend(q, k, v, q_seg, k_seg, scale):
    scores = jnp.einsum("qhd,khd->hqk", q, k, preferred_element_type=f32) * scale
    scores = jnp.where((q_seg[:, None] == k_seg[None, :])[None], scores, masked_value)
    top = jnp.max(scores, axis=-1, keepdims=True)
    exp_scores = jnp.exp(scores - top)
    total = jnp.sum(exp_scores, axis=-1, keepdims=True)
    probs = exp_scores / total
    context = jnp.einsum("hqk,khd->qhd", probs.astype(bf16), v, preferred_element_type=f32)
    return context.astype(bf16), probs


def attend_back(q, k, v, probs, d_ctx, scale):
    d_probs = jnp.einsum("qhd,khd->hqk", d_ctx, v, preferred_element_type=f32)
    delta = jnp.sum(probs * d_probs, axis=-1, keepdims=True)
    d_scores = (probs * (d_probs - delta)).astype(bf16)
    d_q = jnp.einsum("hqk,khd->qhd", d_scores, k, preferred_element_type=f32) * scale
    d_k = jnp.einsum("hqk,qhd->khd", d_scores, q, preferred_element_type=f32) * scale
    d_v = jnp.einsum("hqk,qhd->khd", probs.astype(bf16), d_ctx, preferred_element_type=f32)
    return d_q, d_k, d_v


def general_local(
    tokens,
    segments,
    labels,
    cotangent,
    w_qkv,
    b_qkv,
    w_out,
    b_out,
    ln1_gain,
    ln1_bias,
    w_in,
    b_in,
    w_back,
    b_back,
    ln2_gain,
    ln2_bias,
    s_proj,
    s_bias,
    s_query,
    s_mid,
    s_mid_bias,
    s_cls,
    s_cls_bias,
):
    seqs_local, width_row, cols_local = tokens.shape
    parts, rows, cols, seqs, sub = sizes(seqs_local)
    width = width_row * rows
    own = cols_local // (parts * sub)
    width_col = b_qkv.shape[1]
    heads_dev = width_col // HD
    hidden_col = b_in.shape[0]
    docs_count = labels.shape[1]
    class_count = s_cls.shape[1]
    student_width = s_proj.shape[1]
    row_index = lax.axis_index("row")
    col_index = lax.axis_index("col")
    dp_index = lax.axis_index("dp")
    seq_index = row_index // sub
    sub_index = row_index % sub
    score_scale = HD ** (-0.5)
    pool_scale = SHD ** (-0.5)
    query_heads = s_query.reshape(SH, SHD)
    doc_ids = jnp.arange(docs_count, dtype=jnp.int32)
    class_ids = jnp.arange(class_count, dtype=jnp.int32)

    w_qkv_all = gather_world(own_half(w_qkv)).reshape(cols, width, 3 * width_col)
    x_t = take_in(tokens)
    rest = jnp.concatenate([own_half(w_in), own_half(w_back), own_half(w_out).reshape(-1, width_col)], axis=1)
    rest_all = gather_world(rest)
    w_in_all = rest_all[..., :hidden_col].reshape(cols, width, hidden_col)
    w_back_all = rest_all[..., hidden_col : 2 * hidden_col].reshape(cols, width, hidden_col)
    w_out_all = rest_all[..., 2 * hidden_col :].reshape(cols, rows, width_col, width_row)
    w_out_all = w_out_all.transpose(0, 2, 1, 3).reshape(width, width)
    row_vectors = lax.all_gather(
        jnp.stack([b_out, ln1_gain, ln1_bias, b_back, ln2_gain, ln2_bias]), "row", axis=1, tiled=True
    )
    b_out_a, gain_one, bias_one, b_back_a, gain_two, bias_two = [row_vectors[i] for i in range(6)]
    b_qkv_all = lax.all_gather(b_qkv, "col")
    b_in_all = lax.all_gather(b_in, "col")
    s_proj_all = lax.all_gather(s_proj, "row", axis=0, tiled=True)
    whole_ints = lax.all_gather(jnp.concatenate([segments, labels], axis=1), "dp", axis=0, tiled=True)
    ints = lax.dynamic_index_in_dim(whole_ints, seq_index, 0, False)
    seq_len = segments.shape[1]
    seg_all, label_seq = ints[:seq_len], ints[seq_len:]
    seg_blocks = seg_all.reshape(cols, parts, sub, own)
    seg_q = lax.dynamic_index_in_dim(seg_blocks, dp_index, 1, False)
    seg_q = lax.dynamic_index_in_dim(seg_q, sub_index, 1, False)
    seg_own = lax.dynamic_index_in_dim(seg_q, col_index, 0, False)
    seg_q = seg_q.reshape(-1)

    x = x_t.T
    offsets = jnp.stack([b_qkv_all[:, 0], jnp.zeros_like(b_qkv_all[:, 0]), b_qkv_all[:, 1]], axis=1)
    offsets = offsets.reshape(cols, 3, heads_dev, HD).transpose(0, 2, 1, 3).reshape(cols, 1, -1)
    qkv = jnp.einsum("td,cdn->ctn", x, w_qkv_all, preferred_element_type=f32) + offsets
    qkv = swap_cols(qkv.astype(bf16)).reshape(cols, own, heads_dev, 3, HD)
    queries = qkv[:, :, :, 0].reshape(cols * own, heads_dev, HD)
    kv = gather_sequence(qkv[:, :, :, 1:].reshape(cols, own, -1), sub)
    kv = kv.reshape(seq_len, heads_dev, 2, HD)
    key_rows, value_rows = kv[:, :, 0], kv[:, :, 1]
    context, probs = attend(queries, key_rows, value_rows, seg_q, seg_all, score_scale)
    ctx = swap_cols(context.reshape(cols, own, width_col))
    ctx = ctx.transpose(1, 0, 2).reshape(own, width)

    attn_out = mm(ctx, w_out_all, ((1,), (0,))) + b_out_a
    normed_one, inv_one = normalize(x.astype(f32) + attn_out)
    hidden_one = normed_one * gain_one + bias_one
    hidden_low = hidden_one.astype(bf16)
    pre_act = jnp.einsum("td,cdn->ctn", hidden_low, w_in_all, preferred_element_type=f32)
    pre_act = pre_act + b_in_all[:, None, :]
    act = gelu_exact(pre_act).astype(bf16)
    ffn_out = jnp.einsum("ctn,cdn->td", act, w_back_all, preferred_element_type=f32) + b_back_a
    normed_two, inv_two = normalize(hidden_one + ffn_out)
    layer_out = (normed_two * gain_two + bias_two).astype(bf16)
    out = give_back(layer_out.T, seqs_local)

    student_h = mm(layer_out, s_proj_all, ((1,), (0,))) + s_bias
    head_parts = student_h.reshape(own, SH, SHD)
    pool_logit = jnp.sum(head_parts * query_heads, axis=-1) * pool_scale
    member = (seg_own[:, None] == doc_ids[None, :])[:, :, None]
    masked = jnp.where(member, pool_logit[:, None, :], masked_value)
    local_top = jnp.max(masked, axis=0)
    local_exp = jnp.where(member, jnp.exp(masked - local_top[None]), 0.0)
    local_total = jnp.sum(local_exp, axis=0)
    local_sum = jnp.einsum("tdh,thk->dhk", local_exp, head_parts, precision=highest)
    stats = jnp.concatenate([local_top[..., None], local_total[..., None], local_sum], axis=-1)
    stats = lax.all_gather(stats, ("dp", "col"))
    if sub > 1:
        stats = lax.all_gather(stats, "row", axis=0, tiled=True, axis_index_groups=row_groups(rows, sub))
    tops, totals, sums = stats[..., 0], stats[..., 1], stats[..., 2:]
    doc_top = jnp.max(tops, axis=0)
    factors = jnp.exp(tops - doc_top[None])
    doc_total = jnp.sum(totals * factors, axis=0)
    pooled_heads = jnp.sum(sums * factors[..., None], axis=0) / doc_total[:, :, None]
    pooled = pooled_heads.reshape(docs_count, student_width)
    middle = jnp.tanh(jnp.dot(pooled, s_mid, precision=highest) + s_mid_bias)
    logit_rows = jnp.dot(middle, s_cls, precision=highest) + s_cls_bias
    logits = lax.all_gather(logit_rows, "row")[::sub]
    logits = lax.dynamic_slice_in_dim(logits, dp_index * seqs_local, seqs_local)
    logit_top = jnp.max(logit_rows, axis=-1, keepdims=True)
    logit_exp = jnp.exp(logit_rows - logit_top)
    one_hot = (label_seq[:, None] == class_ids[None, :]).astype(f32)
    d_logits = logit_exp / jnp.sum(logit_exp, axis=-1, keepdims=True) - one_hot
    g_cls = jnp.dot(middle.T, d_logits, precision=highest)
    g_cls_bias = jnp.sum(d_logits, axis=0)
    d_middle = jnp.dot(d_logits, s_cls.T, precision=highest) * (1.0 - middle * middle)
    g_mid = jnp.dot(pooled.T, d_middle, precision=highest)
    g_mid_bias = jnp.sum(d_middle, axis=0)
    d_pooled = jnp.dot(d_middle, s_mid.T, precision=highest).reshape(docs_count, SH, SHD)
    shares = jnp.where(member, jnp.exp(masked - doc_top[None]), 0.0) / doc_total[None]
    d_share = jnp.einsum("dhk,thk->tdh", d_pooled, head_parts, precision=highest)
    base_term = jnp.sum(d_pooled * pooled_heads, axis=-1)
    d_pool_logit = jnp.sum(shares * (d_share - base_term[None]), axis=1)
    d_heads = jnp.einsum("tdh,dhk->thk", shares, d_pooled, precision=highest)
    d_heads = d_heads + d_pool_logit[:, :, None] * query_heads[None] * pool_scale
    g_query = (jnp.sum(d_pool_logit[:, :, None] * head_parts, axis=0) * pool_scale).reshape(-1)
    d_student = d_heads.reshape(own, student_width)
    g_sbias = jnp.sum(d_student, axis=0)
    g_sproj = jnp.dot(layer_out.astype(f32).T, d_student, precision=highest)

    d_out = take_in(cotangent).T.astype(f32)
    g_ln2_gain = jnp.sum(d_out * normed_two, axis=0)
    g_ln2_bias = jnp.sum(d_out, axis=0)
    d_resid_two = normalize_back(d_out * gain_two, normed_two, inv_two)
    d_ffn = d_resid_two.astype(bf16)
    g_back_bias = jnp.sum(d_ffn.astype(f32), axis=0)
    g_back = jnp.einsum("td,ctn->cdn", d_ffn, act, preferred_element_type=f32)
    d_act = jnp.einsum("td,cdn->ctn", d_ffn, w_back_all, preferred_element_type=f32)
    _, gelu_fn = jax.vjp(gelu_exact, pre_act)
    d_pre = gelu_fn(d_act)[0].astype(bf16)
    g_in_bias = jnp.sum(d_pre.astype(f32), axis=1)
    g_in = jnp.einsum("td,ctn->cdn", hidden_low, d_pre, preferred_element_type=f32)
    d_hidden_one = d_resid_two + jnp.einsum(
        "ctn,cdn->td", d_pre, w_in_all, preferred_element_type=f32
    )
    g_ln1_gain = jnp.sum(d_hidden_one * normed_one, axis=0)
    g_ln1_bias = jnp.sum(d_hidden_one, axis=0)
    d_resid_one = normalize_back(d_hidden_one * gain_one, normed_one, inv_one)
    d_attn = d_resid_one.astype(bf16)
    g_out_bias = jnp.sum(d_attn.astype(f32), axis=0)
    g_out = mm(ctx, d_attn, ((0,), (0,)))
    d_ctx = mm(d_attn, w_out_all, ((1,), (1,))).astype(bf16)
    d_ctx = swap_cols(d_ctx.reshape(own, cols, width_col).transpose(1, 0, 2))
    d_ctx = d_ctx.reshape(cols * own, heads_dev, HD)
    d_q, d_k, d_v = attend_back(queries, key_rows, value_rows, probs, d_ctx, score_scale)
    d_kv = jnp.stack([d_k, d_v], axis=2).astype(bf16).reshape(seq_len, -1)
    d_kv = scatter_sequence(d_kv, cols, sub).reshape(cols, own, heads_dev, 2, HD)
    d_q = d_q.astype(bf16).reshape(cols, own, heads_dev, 1, HD)
    d_qkv = jnp.concatenate([d_q, d_kv], axis=3).reshape(cols, own, 3 * width_col)
    d_qkv = swap_cols(d_qkv)
    g_qkv_bias = jnp.sum(d_qkv.astype(f32), axis=1).reshape(cols, heads_dev, 3, HD)
    g_qkv = jnp.einsum("td,ctn->cdn", x, d_qkv, preferred_element_type=f32)
    d_tokens = d_resid_one + jnp.einsum("ctn,cdn->td", d_qkv, w_qkv_all, preferred_element_type=f32)
    grad_tokens = give_back(d_tokens.astype(bf16).T, seqs_local).astype(f32)

    g_out = g_out.reshape(cols, width_col, rows, width_row).transpose(0, 2, 1, 3)
    g_out = g_out.reshape(cols, rows, width_row, width_col)
    model = jnp.concatenate(
        [
            g_in.reshape(cols, rows, width_row, hidden_col).astype(bf16),
            g_back.reshape(cols, rows, width_row, hidden_col).astype(bf16),
            g_out.astype(bf16),
        ],
        axis=-1,
    )
    model = scatter_world(model).astype(f32)
    g_qkv = scatter_world(g_qkv.reshape(cols, rows, width_row, 3 * width_col).astype(bf16)).astype(f32)
    once = 1.0 / (parts * cols * sub)
    small = (
        g_qkv_bias[:, :, 0].reshape(cols, width_col),
        g_qkv_bias[:, :, 2].reshape(cols, width_col),
        g_in_bias,
        g_out_bias,
        g_ln1_gain,
        g_ln1_bias,
        g_back_bias,
        g_ln2_gain,
        g_ln2_bias,
        g_sproj,
        g_sbias,
        g_query,
        g_mid * once,
        g_mid_bias * once,
        g_cls * once,
        g_cls_bias * once,
    )
    small = lax.psum(small, WORLD)

    def at_col(part):
        return lax.dynamic_index_in_dim(part, col_index, 0, False)

    def at_row(part):
        return lax.dynamic_slice_in_dim(part, row_index * width_row, width_row)

    return (
        out,
        logits,
        grad_tokens,
        g_qkv,
        jnp.stack([at_col(small[0]), at_col(small[1])]),
        model[:, 2 * hidden_col :].reshape(width_col, width_row),
        at_row(small[3]),
        at_row(small[4]),
        at_row(small[5]),
        model[:, :hidden_col],
        at_col(small[2]),
        model[:, hidden_col : 2 * hidden_col],
        at_row(small[6]),
        at_row(small[7]),
        at_row(small[8]),
        at_row(small[9]),
        small[10],
        small[11],
        small[12],
        small[13],
        small[14],
        small[15],
    )


MESH = pl.DeviceIdType.MESH
HBM = pl.BlockSpec(memory_space=pl.ANY)


def place():
    return lax.axis_index("dp"), lax.axis_index("row"), lax.axis_index("col")


def greet(peers, guarded=()):
    barrier = pltpu.get_barrier_semaphore()
    for peer in peers:
        pl.semaphore_signal(barrier, inc=1, device_id=peer, device_id_type=MESH)
    for there, peer in guarded:

        @pl.when(there)
        def _():
            pl.semaphore_signal(barrier, inc=1, device_id=peer, device_id_type=MESH)

    amount = len(peers)
    for there, _ in guarded:
        amount = amount + there.astype(jnp.int32)
    pl.semaphore_wait(barrier, amount)


def rcopy(src, dst, send, recv, peer):
    return pltpu.make_async_remote_copy(
        src_ref=src, dst_ref=dst, send_sem=send, recv_sem=recv, device_id=peer, device_id_type=MESH
    )


def take_copies(src, out, local, send, recv):
    d, r, c = place()
    own = out.shape[2]
    moves = []
    for i in range(2):
        for far in range(2):
            row, core = 2 * d + i, d ^ far
            piece = src.at[i, :, pl.ds(pl.multiple_of(core * own, own), own)]
            here = (row == r) if far == 0 else None

            def start(piece=piece, row=row, core=core, slot=2 * i + far, here=here):
                def away():
                    rcopy(piece, out.at[r], send.at[slot], recv.at[r], (core, row, c)).start()

                if here is None:
                    away()
                else:
                    pl.when(jnp.logical_not(here))(away)

                    @pl.when(here)
                    def _():
                        pltpu.make_async_copy(piece, out.at[r], local).start()

            def wait(piece=piece, row=row, core=core, slot=2 * i + far, here=here):
                def away():
                    rcopy(piece, out.at[r], send.at[slot], recv.at[r], (core, row, c)).wait_send()

                if here is None:
                    away()
                else:
                    pl.when(jnp.logical_not(here))(away)

                    @pl.when(here)
                    def _():
                        pltpu.make_async_copy(piece, out.at[r], local).wait()

            moves.append((start, wait))
    for row in range(4):

        def arrive(row=row):
            @pl.when(jnp.logical_not((row == r) & (r // 2 == d)))
            def _():
                piece = src.at[0, :, pl.ds(0, own)]
                rcopy(piece, out.at[row], send.at[0], recv.at[row], (d, r, c)).wait_recv()

        moves.append((lambda: None, arrive))
    return moves


VM = pl.BlockSpec(memory_space=pltpu.VMEM)


def head_kernel(scale, *refs):
    (w_qkv_ref, w_out_ref, w_in_ref, w_back_ref, tok, cot, ints), refs = refs[:7], refs[7:]
    (b_qkv_ref, b_in_ref, proj_ref), row_vecs, refs = refs[:3], refs[3:9], refs[9:]
    (a_out, b_out, c_out, tok_out, cot_out, ints_out, q_out, kv_out), refs = refs[:8], refs[8:]
    (wo_out, vec_all, b_in_all, proj_all, ctx_own, lse_ref, ctx_out), refs = refs[:7], refs[7:]
    (shard_a, shard_v, vec_out, x_nat, q_src, kv_src, kn, q3, s_scr, o_scr, kcol), refs = refs[:11], refs[11:]
    own_sem, zs, zr, xs, xr, ys, yr, cs, cr, ps, pr, tl, ts, tr, il, hs, hr, hps, hpr, xl, xs2, xr2, vs, vr = refs
    d, r, c = place()
    kinds = 4
    part = w_in_ref.shape[0] // 2
    mine = pl.ds(pl.multiple_of(d * part, 16), part)
    feats = tok_out.shape[1]
    shards = [shard_a.at[mine], shard_v.at[pl.ds(pl.multiple_of(d * 48, 8), 48)], w_in_ref.at[mine], w_back_ref.at[mine]]
    outs = [a_out, vec_out, b_out, c_out]
    cols = 4
    xn, yn, pn = (d, r ^ 1, c), (d, r ^ 2, c), (1 - d, r, c)
    up, down = (d, r, c + 1), (d, r, c - 1)
    has_up, has_down = c < cols - 1, c > 0
    columns = w_qkv_ref.shape[1]
    shard_a[:, :columns] = w_qkv_ref[...]
    shard_a[:, columns:] = w_out_ref[...]
    heads = columns // (3 * HD)
    pieces = []
    for h in range(heads):
        spot = slice(h * HD, (h + 1) * HD)
        pieces += [b_qkv_ref[0:1, spot], jnp.zeros((1, HD), f32), b_qkv_ref[1:2, spot]]
    bias_lanes = -(-columns // 128) * 128
    pieces.append(jnp.zeros((1, bias_lanes - columns), f32))
    line = jnp.concatenate(pieces, axis=1)
    at = 0
    for i in range(bias_lanes // 128):
        shard_v[at : at + 1] = line[:, i * 128 : (i + 1) * 128]
        at += 1
    for ref in row_vecs:
        line = jnp.concatenate([ref[...], jnp.zeros((1, 256 - feats), f32)], axis=1)
        for i in range(2):
            shard_v[at : at + 1] = line[:, i * 128 : (i + 1) * 128]
            at += 1
    for i in range(b_in_ref.shape[1] // 128):
        shard_v[at : at + 1] = b_in_ref[:, i * 128 : (i + 1) * 128]
        at += 1
    proj_at, proj_rows = 48, feats // 4
    for i in range(at, proj_at):
        shard_v[i : i + 1] = jnp.zeros((1, 128), f32)
    shard_v[proj_at:] = proj_ref[pl.ds(pl.multiple_of(c * proj_rows, 16), proj_rows)].astype(f32)

    greet(plane_peers() + [(d, r, c ^ j) for j in (1, 2, 3)])
    moves = take_copies(tok, tok_out, tl, ts, tr)
    for start, _ in moves:
        start()
    late_moves = take_copies(cot, cot_out, xl, xs2, xr2)
    pltpu.make_async_copy(ints, ints_out.at[d], il.at[0]).start()
    rcopy(ints, ints_out.at[d], il.at[1], il.at[2], pn).start()
    halves = [part // 2, 24, part // 2, part // 2]

    def z_send(k, at, way, hop):
        src = shards[k] if hop == 1 else outs[k].at[at, r, d]
        return rcopy(
            src, outs[k].at[at, r, d], zs.at[k, way, hop - 1], zr.at[k, way, hop - 1], up if way == 0 else down
        )

    def src_of(k, at, own):
        return shards[k] if own else outs[k].at[at, r, d]

    def to_x(k, at, own):
        return rcopy(src_of(k, at, own), outs[k].at[at, r, d], xs.at[k, at], xr.at[k, at], xn)

    def to_y(k, at, own):
        return rcopy(src_of(k, at, own), outs[k].at[at, r, d], ys.at[k, at], yr.at[k, at], yn)

    def to_p(k, at, own):
        return rcopy(src_of(k, at, own), outs[k].at[at, r, d], ps.at[k, at, 0], pr.at[k, at, 0], pn)

    def relay(k, at, which):
        row = r ^ 1 if which == 0 else r ^ 2
        ref = outs[k].at[at, row, d, pl.ds(which * halves[k], halves[k])]
        return rcopy(ref, ref, cs.at[k, at, which], cr.at[k, at, which], yn if which == 0 else xn)

    def pass_p(k, at, bit):
        ref = outs[k].at[at, r ^ bit, d]
        return rcopy(ref, ref, ps.at[k, at, bit], pr.at[k, at, bit], pn)

    def got_x(k, at):
        ref = outs[k].at[at, r ^ 1, d]
        rcopy(ref, ref, xs.at[k, at], xr.at[k, at], xn).wait_recv()

    def got_y(k, at):
        ref = outs[k].at[at, r ^ 2, d]
        rcopy(ref, ref, ys.at[k, at], yr.at[k, at], yn).wait_recv()

    def got_corner(k, at):
        for which in range(2):
            ref = outs[k].at[at, r ^ 3, d, pl.ds(which * halves[k], halves[k])]
            rcopy(ref, ref, cs.at[k, at, which], cr.at[k, at, which], xn).wait_recv()

    def got_p(k, at, bit):
        ref = outs[k].at[at, r ^ bit, 1 - d]
        rcopy(ref, ref, ps.at[k, at, bit], pr.at[k, at, bit], pn).wait_recv()

    for k in range(kinds):
        pltpu.make_async_copy(shards[k], outs[k].at[c, r, d], own_sem.at[k]).start()

        @pl.when(has_up)
        def _():
            z_send(k, c, 0, 1).start()

        @pl.when(has_down)
        def _():
            z_send(k, c, 1, 1).start()

    def spread(k, at, own):
        to_x(k, at, own).start()
        to_y(k, at, own).start()
        to_p(k, at, own).start()

    def onward(k, at):
        got_x(k, at)
        relay(k, at, 0).start()
        pass_p(k, at, 1).start()
        got_y(k, at)
        relay(k, at, 1).start()
        pass_p(k, at, 2).start()

    steps = [(0, 0)] + [(way, hop) for hop in (1, 2, 3) for way in (0, 1)]
    jobs = [(k, way, hop) for k in range(kinds) for way, hop in steps]

    def at_of(way, hop):
        return c - hop if way == 0 else c + hop

    def valid(way, hop):
        return c >= hop if way == 0 else c + hop < cols

    def guard(way, hop, body):
        if hop == 0:
            body()
        else:
            pl.when(valid(way, hop))(body)

    def first(k, way, hop):
        def body():
            at = at_of(way, hop)
            if hop:
                z_send(k, at, way, hop).wait_recv()
                if hop < 3:
                    can = has_up if way == 0 else has_down

                    @pl.when(can)
                    def _():
                        z_send(k, at, way, hop + 1).start()

            spread(k, at, hop == 0)

        guard(way, hop, body)

    def second(k, way, hop):
        guard(way, hop, lambda: onward(k, at_of(way, hop)))

    def third(k, way, hop):
        def body():
            at = at_of(way, hop)
            got_corner(k, at)
            pass_p(k, at, 3).start()

        guard(way, hop, body)

    def settle(k):
        pltpu.make_async_copy(shards[k], outs[k].at[c, r, d], own_sem.at[k]).wait()
        for way, hop in steps:

            def body():
                for bit in range(4):
                    got_p(k, at_of(way, hop), bit)

            guard(way, hop, body)

    def kv(j):
        return rcopy(kv_src.at[c ^ j], kv_out.at[c, d], hs.at[0, j], hr.at[0, j], (d, r, c ^ j))

    def q(j):
        return rcopy(q_src.at[c ^ j], q_out.at[c], hs.at[1, j], hr.at[1, j], (d, r, c ^ j))

    def pair(j):
        src = kv_src.at[c] if j == 0 else kv_out.at[c ^ j, d]
        return rcopy(src, kv_out.at[c ^ j, d], hps.at[j], hpr.at[j], pn)

    lanes = bias_lanes

    def prepare():
        for _, wait in moves:
            wait()
        x_nat[...] = tok_out[...].reshape(4 * feats, -1).astype(f32).T.astype(bf16)

    def project(j):
        to = c ^ j
        weights = a_out[to, :, :, :, :lanes].reshape(-1, lanes)
        bias = vec_out[to, r, 0, pl.ds(0, 8)]
        bias = jnp.concatenate([bias[i : i + 1] for i in range(lanes // 128)], axis=1)
        made = jnp.dot(x_nat[...], weights, preferred_element_type=f32) + bias
        made = made.T.astype(bf16)
        for h in range(heads):
            rows = pl.ds(h * HD, HD)
            q_src[to, rows] = made[3 * h * HD : (3 * h + 1) * HD]
            kv_src[to, rows] = made[(3 * h + 1) * HD : (3 * h + 2) * HD]
            kv_src[to, pl.ds(wide + h * HD, HD)] = made[(3 * h + 2) * HD : (3 * h + 3) * HD]
        if j:
            kv(j).start()
            q(j).start()
        else:
            pair(0).start()
            kv_out[c, d] = kv_src[c]
            q_out[c] = q_src[c]

    def spread_out(at):
        for row in range(4):
            block = a_out[at, row, :, :, columns:].reshape(-1, feats)
            wo_out[pl.ds(at * wide, wide), row * feats : (row + 1) * feats] = block

    def unpack():
        first = bias_lanes // 128
        for i in range(6):
            for row in range(4):
                line = vec_out[0, row, 0, pl.ds(first + 2 * i, 2)]
                line = jnp.concatenate([line[0:1], line[1:2]], axis=1)
                vec_all[i : i + 1, row * feats : (row + 1) * feats] = line[:, :feats]
        vec_all[6:8] = jnp.zeros((2, 4 * feats), f32)
        first += 12
        for at in range(4):
            for i in range(b_in_all.shape[1] // 128):
                b_in_all[at : at + 1, i * 128 : (i + 1) * 128] = vec_out[at, 0, 0, pl.ds(first + i, 1)]
            for row in range(4):
                rows = pl.ds(row * feats + at * proj_rows, proj_rows)
                proj_all[rows] = vec_out[at, row, 1].astype(bf16)

    tiles = 8
    own = x_nat.shape[0]

    def segment(tile):
        return ints_out[r // 2, r % 2, pl.ds(tile, 1)].astype(f32)

    def collect():
        for j in (1, 2, 3):
            kv(j).wait_recv()
            pair(j).start()
        pltpu.make_async_copy(ints, ints_out.at[d], il.at[0]).wait()
        rcopy(ints, ints_out.at[1 - d], il.at[1], il.at[2], pn).wait()
        for tile in range(tiles):
            kcol[tile] = jnp.broadcast_to(segment(tile), (128, own)).T
        for j in (1, 2, 3):
            q(j).wait_recv()
        for j in range(4):
            pair(j).wait_recv()

        @pl.loop(0, 4)
        def _(at):
            for core in range(2):
                kn[2 * at + core] = kv_out[at, core, pl.ds(0, wide)].astype(f32).T.astype(bf16)

    def attend_block(block):
        block_rows(q_out.at[pl.ds(block, 1)], heads, scale, q3)
        here = 2 * block + d
        low, high = jnp.maximum(here - 4, 0), jnp.minimum(here + 5, tiles)
        qseg = jnp.concatenate([segment(here)] * heads, axis=1)

        def one(j, top):
            s = jnp.dot(kn[j], q3[...], preferred_element_type=f32)
            same = jnp.concatenate([kcol[j]] * (heads * own // 128), axis=1) == qseg
            s = jnp.where(same, s, masked_value)
            s_scr[j] = s
            return jnp.maximum(top, jnp.max(s, axis=0, keepdims=True))

        top = lax.fori_loop(low, high, one, jnp.full((1, heads * own), masked_value, f32))
        o_scr[...] = jnp.zeros_like(o_scr)

        def two(j, total):
            p = jnp.exp(s_scr[j] - top)
            low_p = p.astype(bf16)
            for h in range(heads):
                rows = pl.ds(h * HD, HD)
                v = kv_out[j // 2, j % 2, pl.ds(wide + h * HD, HD)]
                o_scr[rows] += jnp.dot(v, low_p[:, h * own : (h + 1) * own], preferred_element_type=f32)
            return total + jnp.sum(p, axis=0, keepdims=True)

        total = lax.fori_loop(low, high, two, jnp.zeros((1, heads * own), f32))
        for h in range(heads):
            rows = pl.ds(h * HD, HD)
            ctx_own[block, rows] = (o_scr[rows] / total[:, h * own : (h + 1) * own]).astype(bf16)
        lse_ref[block] = top + jnp.log(total)

    def back_copy(j):
        return rcopy(ctx_own.at[c ^ j], ctx_out.at[c], vs.at[j], vr.at[j], (d, r, c ^ j))

    def attend(j):
        attend_block(c ^ j)
        if j:
            back_copy(j).start()
        else:
            ctx_out[c] = ctx_own[c]

    wide = q_src.shape[1]
    lag = 3
    ready = 2 * len(steps) + 2 * lag
    rest = len(jobs) - ready - 1
    for i in range(len(jobs) + 2 * lag):
        if i == ready:
            prepare()
            settle(0)
            settle(1)
        if ready <= i < ready + 4:
            project((3, 2, 1, 0)[i - ready])
        if ready + 3 <= i < ready + 7:
            spread_out(i - ready - 3)
        if i == ready + 5:
            unpack()
        if i == ready + 7:
            collect()
        if ready + 8 <= i < ready + 12:
            attend((3, 2, 1, 0)[i - ready - 8])
        if i <= ready:
            first(*jobs[i])
        elif i <= ready + 4:
            for n in range(ready + 1 + (i - ready - 1) * 2, min(ready + 1 + (i - ready) * 2, len(jobs))):
                first(*jobs[n])
            if i == ready + 4:
                for start, _ in late_moves:
                    start()
        if 0 <= i - lag < len(jobs):
            second(*jobs[i - lag])
        if 0 <= i - 2 * lag < len(jobs):
            third(*jobs[i - 2 * lag])

    for k in range(kinds):
        if k > 1:
            settle(k)
        for way, hop in steps:

            def body():
                at = at_of(way, hop)
                own = hop == 0
                to_x(k, at, own).wait_send()
                to_y(k, at, own).wait_send()
                to_p(k, at, own).wait_send()
                for which in range(2):
                    relay(k, at, which).wait_send()
                for bit in (1, 2, 3):
                    pass_p(k, at, bit).wait_send()
                if hop < 3:
                    if own:

                        @pl.when(has_up)
                        def _():
                            z_send(k, c, 0, 1).wait_send()

                        @pl.when(has_down)
                        def _():
                            z_send(k, c, 1, 1).wait_send()
                    else:
                        can = has_up if way == 0 else has_down

                        @pl.when(can)
                        def _():
                            z_send(k, at, way, hop + 1).wait_send()

            guard(way, hop, body)
    for j in (1, 2, 3):
        q(j).wait_send()
        kv(j).wait_send()
        back_copy(j).wait()
    for j in range(4):
        pair(j).wait_send()
    for _, wait in late_moves:
        wait()


VM = pl.BlockSpec(memory_space=pltpu.VMEM)


def head_fast(weights, tokens, cotangent, ints, vectors, scale, cid):
    kinds = 4
    dma = pltpu.SemaphoreType.DMA
    _, feats, cols = tokens.shape
    own = cols // 2
    width = 4 * feats
    part = feats // 2
    wide = weights[0].shape[1] // 3
    full = 4 * wide
    heads = wide // HD
    shape = jax.ShapeDtypeStruct
    piece = shape((4, wide, own), bf16)
    taken = shape((4, feats, own), bf16)
    weight = shape((4, 4, 2, part, weights[2].shape[1]), bf16)
    hidden = weights[2].shape[1]
    student_width = vectors[2].shape[1]
    return pl.pallas_call(
        functools.partial(head_kernel, scale),
        out_shape=[
            shape((4, 4, 2, part, full), bf16), weight, weight, taken, taken, shape((2,) + ints.shape, ints.dtype),
            piece, shape((4, 2, 2 * wide, own), bf16), shape((4 * wide, width), bf16), shape((8, width), f32),
            shape((4, hidden), f32), shape((width, student_width), bf16), piece,
            shape((4, 1, heads * own), f32), piece,
        ],
        in_specs=[VM, VM] + [HBM] * 5 + [VM] * len(vectors),
        out_specs=[VM, HBM, HBM] + [VM] * 12,
        scratch_shapes=[
            pltpu.VMEM((feats, full), bf16),
            pltpu.VMEM((96, 128), f32),
            pltpu.VMEM((4, 4, 2, 48, 128), f32),
            pltpu.VMEM((own, width), bf16),
            pltpu.VMEM((4, wide, own), bf16),
            pltpu.VMEM((4, 2 * wide, own), bf16),
            pltpu.VMEM((8, own, wide), bf16),
            pltpu.VMEM((wide, heads * own), bf16),
            pltpu.VMEM((8, own, heads * own), f32),
            pltpu.VMEM((wide, own), f32),
            pltpu.VMEM((8, own, 128), f32),
            dma((kinds,)),
            dma((kinds, 2, 3)), dma((kinds, 2, 3)),
            dma((kinds, 4)), dma((kinds, 4)),
            dma((kinds, 4)), dma((kinds, 4)),
            dma((kinds, 4, 2)), dma((kinds, 4, 2)),
            dma((kinds, 4, 4)), dma((kinds, 4, 4)),
            dma, dma((4,)), dma((4,)), dma((3,)),
            dma((2, 4)), dma((2, 4)), dma((4,)), dma((4,)),
            dma, dma((4,)), dma((4,)), dma((4,)), dma((4,)),
        ],
        compiler_params=pltpu.CompilerParams(
            collective_id=cid, has_side_effects=True, vmem_limit_bytes=56 * 1024 * 1024
        ),
        name="head",
    )(*weights, tokens, cotangent, ints, *vectors)


def scatter_core(grads, outs, scratch, begin, during, late=0, gap=0):
    kinds = len(grads)
    (acc, precv, xr1, yr1, xr2, yr2, zup, zdn, fin) = scratch[:9]
    (ls, ps, pr, xs1, xm1, ys1, ym1, xs2, xm2, ys2, ym2, us, um, ds, dm, fs, fm, os) = scratch[9:]
    d, r, c = place()
    cols = 4
    chunks = kinds * cols
    xn, yn, pn = (d, r ^ 1, c), (d, r ^ 2, c), (1 - d, r, c)
    up, down = (d, r, c + 1), (d, r, c - 1)
    half = acc.shape[2] // 2
    first, last = pl.ds(0, half), pl.ds(half, half)

    def split(i):
        k = i // cols
        j = i - k * cols
        at = jnp.where(j == 0, 0, jnp.where(j == 1, 3, j - 1))
        return k, at

    def at_static(i):
        return i // cols, (0, 3, 1, 2)[i % cols]

    def load(i):
        k, at = at_static(i)
        return pltpu.make_async_copy(grads[k].at[at, :, d], acc.at[i], ls.at[i])

    def pair(i):
        k, at = at_static(i)
        return rcopy(grads[k].at[at, :, 1 - d], precv.at[i], ps.at[i], pr.at[i], pn)

    def launch(i):
        pair(i).start()
        load(i).start()

    for i in range((kinds - late) * cols):
        launch(i)
    begin()

    def x1(i, j):
        return rcopy(acc.at[i, r ^ 1 ^ (2 * j), first], xr1.at[i, j], xs1.at[i, j], xm1.at[i, j], xn)

    def y1(i, j):
        return rcopy(acc.at[i, r ^ 2 ^ j, last], yr1.at[i, j], ys1.at[i, j], ym1.at[i, j], yn)

    def y2(i):
        return rcopy(acc.at[i, r ^ 2, first], yr2.at[i], ys2.at[i], ym2.at[i], yn)

    def x2(i):
        return rcopy(acc.at[i, r ^ 1, last], xr2.at[i], xs2.at[i], xm2.at[i], xn)

    def to_up(i):
        return rcopy(acc.at[i, r], zup.at[i], us.at[i], um.at[i], up)

    def to_down(i):
        return rcopy(acc.at[i, r], zdn.at[i], ds.at[i], dm.at[i], down)

    def stage1(i):
        pltpu.make_async_copy(precv.at[i], acc.at[i], ls.at[i]).wait()
        rcopy(acc.at[i], precv.at[i], ps.at[i], pr.at[i], pn).wait_recv()

        @pl.loop(0, 4)
        def _(row):
            acc[i, row] = acc[i, row] + precv[i, row]

        x1(i, 1).start()
        y1(i, 1).start()
        x1(i, 0).start()
        y1(i, 0).start()

    def stage2(i):
        x1(i, 1).wait_recv()
        acc[i, r ^ 2, first] = acc[i, r ^ 2, first] + xr1[i, 1]
        y2(i).start()
        y1(i, 1).wait_recv()
        acc[i, r ^ 1, last] = acc[i, r ^ 1, last] + yr1[i, 1]
        x2(i).start()
        x1(i, 0).wait_recv()
        acc[i, r, first] = acc[i, r, first] + xr1[i, 0]
        y1(i, 0).wait_recv()
        acc[i, r, last] = acc[i, r, last] + yr1[i, 0]

    def stage3(i):
        y2(i).wait_recv()
        acc[i, r, first] = acc[i, r, first] + yr2[i]
        x2(i).wait_recv()
        acc[i, r, last] = acc[i, r, last] + xr2[i]

    def stage4(i, hops):
        k, at = split(i)

        @pl.when((at > c) & (c == hops))
        def _():
            @pl.when(c > 0)
            def _():
                to_up(i).wait_recv()
                acc[i, r] = acc[i, r] + zup[i]

            to_up(i).start()

        @pl.when((at < c) & (cols - 1 - c == hops))
        def _():
            @pl.when(c < cols - 1)
            def _():
                to_down(i).wait_recv()
                acc[i, r] = acc[i, r] + zdn[i]

            to_down(i).start()

        @pl.when((at == c) & (jnp.maximum(c, cols - 1 - c) == hops))
        def _():
            @pl.when(c > 0)
            def _():
                to_up(i).wait_recv()
                acc[i, r] = acc[i, r] + zup[i]

            @pl.when(c < cols - 1)
            def _():
                to_down(i).wait_recv()
                acc[i, r] = acc[i, r] + zdn[i]

            fin[k, d] = acc[i, r]
            rcopy(fin.at[k, d], fin.at[k, d], fs.at[k], fm.at[k], pn).start()

    stages = [(0, stage1), (2, stage2), (4, stage3)]
    stages += [(5 + h, functools.partial(lambda h, i: stage4(i, h), h)) for h in range(cols)]
    ending = stages[-1][0]

    assert len(during) <= chunks + gap + ending
    early = (kinds - late) * cols

    @pl.loop(0, chunks + gap + ending)
    def _(step):
        for i, extra in enumerate(during):
            pl.when(step == i)(functools.partial(extra, launch))

        for lag, stage in stages:

            spot = step - lag
            there = (spot >= 0) & (spot < early) | (spot >= early + gap) & (spot < chunks + gap)

            @pl.when(there)
            def _():
                stage(jnp.where(spot < early, spot, spot - gap))

    @pl.loop(0, chunks)
    def _(i):
        k, at = split(i)
        rcopy(acc.at[i], precv.at[i], ps.at[i], pr.at[i], pn).wait_send()
        for j in range(2):
            x1(i, j).wait_send()
            y1(i, j).wait_send()
        y2(i).wait_send()
        x2(i).wait_send()

        @pl.when(at > c)
        def _():
            to_up(i).wait_send()

        @pl.when(at < c)
        def _():
            to_down(i).wait_send()

    for k in range(kinds):
        rcopy(fin.at[k, 1 - d], fin.at[k, 1 - d], fs.at[k], fm.at[k], pn).wait()
        pltpu.make_async_copy(fin.at[k], outs[k], os.at[k]).start()
    for k in range(kinds):
        pltpu.make_async_copy(fin.at[k], outs[k], os.at[k]).wait()

def scatter_scratch(kinds, n, w, dt):
    dma = pltpu.SemaphoreType.DMA
    chunks = kinds * 4
    return [
        pltpu.VMEM((chunks, 4, n, w), dt),
        pltpu.VMEM((chunks, 4, n, w), dt),
        pltpu.VMEM((chunks, 2, n // 2, w), dt),
        pltpu.VMEM((chunks, 2, n // 2, w), dt),
        pltpu.VMEM((chunks, n // 2, w), dt),
        pltpu.VMEM((chunks, n // 2, w), dt),
        pltpu.VMEM((chunks, n, w), dt),
        pltpu.VMEM((chunks, n, w), dt),
        pltpu.VMEM((kinds, 2, n, w), dt),
        dma((chunks,)), dma((chunks,)), dma((chunks,)),
        dma((chunks, 2)), dma((chunks, 2)), dma((chunks, 2)), dma((chunks, 2)),
        dma((chunks,)), dma((chunks,)), dma((chunks,)), dma((chunks,)),
        dma((chunks,)), dma((chunks,)), dma((chunks,)), dma((chunks,)),
        dma((kinds,)), dma((kinds,)), dma((kinds,)),
    ]


def give_moves(src_ref, out_ref, local, send, recv):
    d, r, c = place()
    own = src_ref.shape[2]
    home = r // 2

    def slot(i, core):
        return out_ref.at[i, :, pl.ds(pl.multiple_of(core * own, own), own)]

    def move(row):
        return rcopy(src_ref.at[row], slot(r % 2, d), send.at[row], recv.at[r % 2, d], (home, row, c))

    def stay():
        return pltpu.make_async_copy(src_ref.at[r], slot(r % 2, d), local)

    def start():
        for row in range(4):

            @pl.when(jnp.logical_not((row == r) & (home == d)))
            def _():
                move(row).start()

        @pl.when(home == d)
        def _():
            stay().start()

    def finish():
        for row in range(4):

            @pl.when(jnp.logical_not((row == r) & (home == d)))
            def _():
                move(row).wait_send()

        @pl.when(home == d)
        def _():
            stay().wait()

        for i in range(2):
            for core in range(2):

                @pl.when(jnp.logical_not((2 * d + i == r) & (core == d)))
                def _():
                    rcopy(src_ref.at[0], slot(i, core), send.at[0], recv.at[i, core], (d, r, c)).wait_recv()

    return start, finish


def plane_peers():
    d, r, c = place()
    return [(d ^ (j // 4), r ^ (j % 4), c) for j in range(1, 8)]


def line_peers():
    d, r, c = place()
    return [(d ^ (j // 4), r, c ^ (j % 4)) for j in range(1, 8)]


def sum_steps(src, total, parts, sems):
    d, r, c = place()
    peers = [(1 - d, r, c), (d, r ^ 1, c), (d, r ^ 2, c), (d, r, c ^ 1), (d, r, c ^ 2)]
    bits = [d, r % 2, r // 2, c % 2, c // 2]
    rs, rr, gs, gr = sems
    count = len(peers)
    size = [src.shape[0] >> (i + 1) for i in range(count)]
    offset = [jnp.int32(0)]
    for i in range(count):
        offset.append(offset[i] + bits[i] * size[i])

    def rows(at, amount):
        return pl.ds(pl.multiple_of(at, 8), amount)

    def down(i):
        other = offset[i] + (1 - bits[i]) * size[i]
        held = src if i == 0 else parts[i - 1]
        at = other if i == 0 else other - offset[i]
        return rcopy(held.at[rows(at, size[i])], parts[count + i], rs.at[i], rr.at[i], peers[i])

    def fold(i):
        down(i).wait_recv()
        held = src if i == 0 else parts[i - 1]
        at = offset[i + 1] if i == 0 else offset[i + 1] - offset[i]
        parts[i][...] = held[rows(at, size[i])] + parts[count + i][...]

    def back(i):
        spot = total.at[rows(offset[i + 1], size[i])]
        return rcopy(spot, spot, gs.at[i], gr.at[i], peers[i])

    def back_recv(i):
        spot = total.at[rows(offset[i] + (1 - bits[i]) * size[i], size[i])]
        rcopy(spot, spot, gs.at[i], gr.at[i], peers[i]).wait_recv()

    steps = [lambda: down(0).start()]
    for i in range(1, count):

        def step(i=i):
            fold(i - 1)
            down(i).start()

        steps.append(step)

    def middle():
        fold(count - 1)
        total[rows(offset[count], size[-1])] = parts[count - 1][...]
        back(count - 1).start()

    steps.append(middle)
    for i in range(count - 2, -1, -1):

        def step(i=i):
            back_recv(i + 1)
            back(i).start()

        steps.append(step)

    def end():
        back_recv(0)
        for i in range(count):
            down(i).wait_send()
            back(i).wait_send()

    return steps, end


highest = lax.Precision.HIGHEST


def fine(a, b, contract=((1,), (0,))):
    return lax.dot_general(a, b, (contract, ((), ())), precision=highest, preferred_element_type=f32)


def same_head(size, part):
    one = lax.broadcasted_iota(jnp.int32, (size, size), 0) // part
    two = lax.broadcasted_iota(jnp.int32, (size, size), 1) // part
    return (one == two).astype(f32)


def student_stats(docs, scale, out_ref, seg_ref, proj_ref, vec_ref, hidden, logit, stats):
    width = hidden.shape[1]
    h = jnp.dot(out_ref[...], proj_ref[...], preferred_element_type=f32) + vec_ref[0:1]
    pool = fine(h * vec_ref[1:2], same_head(width, SHD)) * scale
    hidden[...] = h
    logit[...] = pool
    stats[0:8] = jnp.zeros((8, width), f32)
    stats[8:16] = jnp.zeros((8, width), f32)
    stats[16:24] = jnp.ones((8, width), f32)
    for doc in range(docs):
        mine = seg_ref[...] == doc
        top = jnp.max(jnp.where(mine, pool, masked_value), axis=0, keepdims=True)
        weight = jnp.where(mine, jnp.exp(pool - top), 0.0)
        stats[doc : doc + 1] = jnp.sum(weight * h, axis=0, keepdims=True)
        stats[8 + doc : 9 + doc] = top
        stats[16 + doc : 17 + doc] = jnp.sum(weight, axis=0, keepdims=True)


def student_grads(docs, classes, scale, once, row, out_ref, seg_ref, label_ref, vec_ref, mid_ref, cls_ref, hidden, logit, stats, small):
    width = hidden.shape[1]
    every = [stats[i, j] for i in range(stats.shape[0]) for j in range(stats.shape[1])]
    top = every[0][8:16]
    for one in every[1:]:
        top = jnp.maximum(top, one[8:16])
    total = jnp.zeros_like(top)
    pooled = jnp.zeros_like(top)
    for one in every:
        factor = jnp.exp(one[8:16] - top)
        total = total + one[16:24] * factor
        pooled = pooled + one[0:8] * factor
    pooled = pooled / total
    middle = jnp.tanh(fine(pooled, mid_ref[...]) + vec_ref[2:3])
    logits = fine(middle, cls_ref[...]) + vec_ref[3:4]
    lane = lax.broadcasted_iota(jnp.int32, logits.shape, 1)
    doc = lax.broadcasted_iota(jnp.int32, logits.shape, 0)
    real = lane < classes
    peak = jnp.max(jnp.where(real, logits, masked_value), axis=1, keepdims=True)
    share = jnp.where(real, jnp.exp(logits - peak), 0.0)
    share = share / jnp.sum(share, axis=1, keepdims=True)
    d_logits = jnp.where(doc < docs, share - (label_ref[...] == lane).astype(f32), 0.0)
    d_middle = fine(d_logits, cls_ref[...], ((1,), (1,))) * (1.0 - middle * middle)
    d_pooled = fine(d_middle, mid_ref[...], ((1,), (1,)))
    zeros = jnp.zeros((1, width), f32)
    small[768:896] = fine(pooled, d_middle, ((0,), (0,))) * once
    small[896:912] = fine(d_logits, middle, ((0,), (0,)))[0:16] * once
    small[912:913] = jnp.sum(d_middle, axis=0, keepdims=True) * once
    small[913:914] = jnp.sum(d_logits, axis=0, keepdims=True) * once
    for at in range(4):
        small[920 + 8 * at : 928 + 8 * at] = jnp.where(row == at, logits * once, 0.0)

    heads = same_head(width, SHD)
    base = fine(d_pooled * pooled, heads)
    h, pool = hidden[...], logit[...]
    top_t, total_t = jnp.zeros_like(h), jnp.ones_like(h)
    back_t, base_t = jnp.zeros_like(h), jnp.zeros_like(h)
    for doc in range(docs):
        mine = seg_ref[...] == doc
        top_t = jnp.where(mine, top[doc : doc + 1], top_t)
        total_t = jnp.where(mine, total[doc : doc + 1], total_t)
        back_t = jnp.where(mine, d_pooled[doc : doc + 1], back_t)
        base_t = jnp.where(mine, base[doc : doc + 1], base_t)
    share = jnp.exp(pool - top_t) / total_t
    d_pool = share * (fine(back_t * h, heads) - base_t)
    d_h = share * back_t + d_pool * vec_ref[1:2] * scale
    small[914:915] = jnp.sum(d_h, axis=0, keepdims=True)
    small[915:916] = jnp.sum(d_pool * h, axis=0, keepdims=True) * scale
    for i in range(916, 920):
        small[i : i + 1] = zeros
    small[0:768] = fine(out_ref[...].astype(f32), d_h, ((0,), (0,)))


def tail_kernel(docs, classes, scale, *refs):
    kinds = 2
    grads, refs = refs[:kinds], refs[kinds:]
    (q_ref, kv_ref, lse_ref, ctx_ref, dctx_ref, ints_ref), refs = refs[:6], refs[6:]
    (out_ref, seg_ref, label_ref, proj_ref, svec_ref, mid_ref, cls_ref), refs = refs[:7], refs[7:]
    vec_refs, refs = refs[:7], refs[7:]
    (x_ref, ctx_all_ref, resid_ref, out_t_ref, w_ref), refs = refs[:5], refs[5:]
    outs, refs = refs[: kinds + 1], refs[kinds + 1 :]
    (give_out, out_out, small_out), refs = refs[:3], refs[3:]
    (total, theirs, dqkv, own_grads, dpad, weights, resid_t, give_src), refs = refs[:8], refs[8:]
    (dctx, dq, dkv, kn, vn, q3, dc3, dq_scr, dkv_scr, bias_scr, landed, kcol), refs = refs[:12], refs[12:]
    (hidden, logit, stats, stats_all, small), refs = refs[:5], refs[5:]
    parts, refs = refs[:10], refs[10:]
    (send, recv, psend, precv), sems, (wl, gl, gs, gr), refs = refs[:4], refs[4:8], refs[8:12], refs[12:]
    (dsend, drecv, ssend, srecv, ol, osend, orecv), scratch = refs[:7], refs[7:]
    d, r, c = place()
    pn = (1 - d, r, c)
    tiles, deep, tile = kv_ref.shape
    wide = deep // 2
    heads = wide // HD
    full = dqkv.shape[1]
    own = q_ref.shape[2]
    kv_rows, q_rows = pl.ds(0, deep), pl.ds(deep, wide)
    peers = line_peers()
    greet(plane_peers() + peers[:3] + peers[4:])

    def to_heads(j):
        return rcopy(dctx_ref.at[c ^ j], dctx.at[c], dsend.at[j], drecv.at[j], (d, r, c ^ j))

    for j in (3, 2, 1):
        to_heads(j).start()
    dctx[c] = dctx_ref[c]
    load_w = pltpu.make_async_copy(w_ref, weights, wl)
    load_w.start()

    def tell(j):
        return rcopy(stats, stats_all.at[d, c], ssend.at[j - 1], srecv.at[j - 1], peers[j - 1])

    out_start, out_finish = give_moves(out_t_ref, out_out, ol, osend, orecv)
    start, finish = give_moves(give_src, give_out, gl, gs, gr)
    steps, end = sum_steps(small, small_out, parts, sems)
    pool_scale = SHD ** (-0.5)

    def begin():
        out_start()
        student_stats(docs, pool_scale, out_ref, seg_ref, proj_ref, svec_ref, hidden, logit, stats)
        for j in range(1, 8):
            tell(j).start()
        stats_all[d, c] = stats[...]
        spare = full - deep - wide
        for at in range(4):
            dqkv[at, pl.ds(deep + wide, spare)] = jnp.zeros((spare, own), bf16)
        resid_t[...] = resid_ref[...].T
        feats = x_ref.shape[1]
        blank = dpad.shape[1] - feats
        for row in range(4):
            dpad[row, pl.ds(0, blank)] = jnp.zeros((blank, own), bf16)
            dpad[row, pl.ds(blank, feats)] = resid_t[pl.ds(row * feats, feats)].astype(bf16)
        at = 952
        for ref in vec_refs:
            for i in range(ref.shape[0]):
                for j in range(ref.shape[1] // 128):
                    small[at : at + 1] = ref[i : i + 1, j * 128 : (j + 1) * 128]
                    at += 1
        for i in range(at, small.shape[0]):
            small[i : i + 1] = jnp.zeros((1, 128), f32)

    def student(_):
        for j in range(1, 8):
            tell(j).wait_recv()
        once = 1.0 / 8
        student_grads(
            docs, classes, pool_scale, once, r, out_ref, seg_ref, label_ref, svec_ref, mid_ref, cls_ref, hidden, logit,
            stats_all, small,
        )

    def segment(at):
        return ints_ref[r // 2, r % 2, pl.ds(at, 1)].astype(f32)

    def prepare(_):
        @pl.loop(0, tiles)
        def _(j):
            kn[j] = kv_ref[j, pl.ds(0, wide)].astype(f32).T.astype(bf16)
            vn[j] = kv_ref[j, pl.ds(wide, wide)].astype(f32).T.astype(bf16)
            dkv_scr[j] = jnp.zeros((deep, tile), f32)

        for j in range(tiles):
            kcol[j] = jnp.broadcast_to(segment(j), (128, own)).T
        bias_scr[...] = jnp.zeros_like(bias_scr)
        for j in (1, 2, 3):
            to_heads(j).wait_recv()

    ones = jnp.ones((8, own), bf16)
    across = (((1,), (1,)), ((), ()))

    def attend_block(block, _):
        q_at, dc_at = q_ref.at[pl.ds(block, 1)], dctx.at[pl.ds(block, 1)]
        block_rows(q_at, heads, scale, q3)
        block_rows(dc_at, heads, 1.0, dc3)
        qseg = jnp.concatenate([segment(2 * block + d)] * heads, axis=1)
        lse = lse_ref[block]
        product = ctx_ref[block].astype(f32) * dctx[block].astype(f32)
        delta = jnp.concatenate(
            [jnp.sum(product[h * HD : (h + 1) * HD], axis=0, keepdims=True) for h in range(heads)], axis=1
        )
        dq_scr[...] = jnp.zeros_like(dq_scr)
        here = 2 * block + d

        @pl.loop(jnp.maximum(here - 4, 0), jnp.minimum(here + 5, tiles))
        def _(j):
            s = jnp.dot(kn[j], q3[...], preferred_element_type=f32)
            same = jnp.concatenate([kcol[j]] * (heads * own // 128), axis=1) == qseg
            p = jnp.exp(jnp.where(same, s, masked_value) - lse)
            d_p = jnp.dot(vn[j], dc3[...], preferred_element_type=f32)
            d_s = (p * (d_p - delta)).astype(bf16)
            p = p.astype(bf16)
            for h in range(heads):
                rows, lanes = pl.ds(h * HD, HD), slice(h * own, (h + 1) * own)
                dq_scr[rows] += jnp.dot(kv_ref[j, rows], d_s[:, lanes], preferred_element_type=f32)
                dkv_scr[j, rows] += lax.dot_general(q3[rows, lanes], d_s[:, lanes], across, preferred_element_type=f32)
                low = pl.ds(wide + h * HD, HD)
                dkv_scr[j, low] += lax.dot_general(dctx[block, rows], p[:, lanes], across, preferred_element_type=f32)

        made = (dq_scr[...] * scale).astype(bf16)
        dq[block] = made
        bias_scr[:, :wide] += lax.dot_general(ones, made, across, preferred_element_type=f32)

    def pair(j):
        return rcopy(dkv.at[c ^ j, 1 - d], theirs.at[c ^ j], psend.at[j], precv.at[j], pn)

    def kv(j):
        return rcopy(total.at[c ^ j], landed.at[c, kv_rows], send.at[0, j], recv.at[0, j], (d, r, c ^ j))

    def q(j):
        return rcopy(dq.at[c ^ j], landed.at[c, q_rows], send.at[1, j], recv.at[1, j], (d, r, c ^ j))

    def leave(_):
        for j in (3, 2, 1, 0):
            for core in range(2):
                tile_at = 2 * (c ^ j) + core
                dkv[c ^ j, core] = dkv_scr[tile_at].astype(bf16)
            pair(j).start()
            if j:
                q(j).start()
        landed[c, q_rows] = dq[c]
        for j in (3, 2, 1):
            pair(j).wait_recv()
            total[c ^ j] = dkv[c ^ j, d] + theirs[c ^ j]
            kv(j).start()
        pair(0).wait_recv()
        landed[c, kv_rows] = dkv[c, d] + theirs[c]

        @pl.loop(0, 4)
        def _(at):
            for core in range(2):
                some = dkv[at, core, pl.ds(wide, wide)]
                bias_scr[:, wide:] += lax.dot_general(ones, some, across, preferred_element_type=f32)

        for i in range(3):
            small[pl.ds(1012 + 3 * c + i, 1)] = bias_scr[0:1, i * 128 : (i + 1) * 128]

    def make(at):
        lead = full - dpad.shape[1]

        @pl.loop(0, 4)
        def _(row):
            one = lax.dot_general(x_ref[row], dqkv[at], across, preferred_element_type=f32)
            two = lax.dot_general(ctx_all_ref[at], dpad[row], across, preferred_element_type=f32)
            shape = own_grads.shape[2:4] + (-1,)
            own_grads[at, row, :, :, :lead] = one[:, :lead].astype(bf16).reshape(shape)
            own_grads[at, row, :, :, lead:] = (one[:, lead:] + two).astype(bf16).reshape(shape)

    def make_chunk(j, launch):
        if j == 0:
            for far in (1, 2, 3):
                q(far).wait_recv()
                kv(far).wait_recv()

            @pl.loop(0, 4)
            def _(at):
                for h in range(heads):
                    for slot, spot in enumerate((deep, 0, wide)):
                        dqkv[at, pl.ds((3 * h + slot) * HD, HD)] = landed[at, pl.ds(spot + h * HD, HD)]

        make((0, 3, 1, 2)[j])
        launch(kinds * 4 + j)

    def input_grad(_):
        load_w.wait()
        feats = x_ref.shape[1]

        @pl.loop(0, 4)
        def _(row):
            part = resid_t[pl.ds(pl.multiple_of(row * feats, 8), feats)]
            for at in range(4):
                w = weights[at, row].reshape(feats, full)
                part = part + jnp.dot(w, dqkv[at], preferred_element_type=f32)
            give_src[row] = part.astype(bf16)

        start()

    gap = 6
    hooks = [[] for _ in range(8 + gap + 5)]
    hooks[1].append(student)
    hooks[2].append(prepare)
    for block in range(4):
        hooks[3 + block].append(functools.partial(attend_block, block))
    hooks[7].append(leave)
    for i, step in enumerate(steps):
        hooks[8 + i].append(lambda launch, step=step: step())
    for j in range(4):
        hooks[7 + gap + j].append(functools.partial(make_chunk, j))
    hooks[11 + gap].append(input_grad)

    def run(todo, launch):
        for one in todo:
            one(launch)

    during = [functools.partial(run, todo) for todo in hooks]
    scatter_core(list(grads) + [own_grads], outs, scratch, begin, during, late=1, gap=gap)
    end()
    finish()
    out_finish()
    for j in range(1, 8):
        tell(j).wait_send()
    for j in range(4):
        pair(j).wait_send()
    for j in (1, 2, 3):
        to_heads(j).wait_send()
        q(j).wait_send()
        kv(j).wait_send()


def tail_fast(docs, classes, scale, grads, attention, student, vectors, rest, out_t, w_attn, cid):
    n, w = grads[0].shape[3:]
    q, kv = attention[:2]
    dma = pltpu.SemaphoreType.DMA
    tiles, deep, own = kv.shape
    wide = deep // 2
    cols = tiles // 2
    feats = rest[0].shape[1]
    student_width = student[3].shape[1]
    tall = 1024
    parts = [pltpu.VMEM((tall >> (i + 1), 128), f32) for i in range(5)]
    home = jax.ShapeDtypeStruct((2, feats, 2 * own), bf16)
    return pl.pallas_call(
        functools.partial(tail_kernel, docs, classes, scale),
        out_shape=[jax.ShapeDtypeStruct((2, n, w), bf16)] * 3 + [home, home, jax.ShapeDtypeStruct((tall, 128), f32)],
        in_specs=[HBM] * 2 + [VM] * (len(attention) + len(student) + len(vectors) + len(rest)) + [HBM] * 2,
        out_specs=[HBM] * 5 + [VM],
        scratch_shapes=[
            pltpu.VMEM((cols, deep, own), bf16),
            pltpu.VMEM((cols, deep, own), bf16),
            pltpu.VMEM((cols, w, own), bf16),
            pltpu.VMEM((4, 4, 2, n, w), bf16),
            pltpu.VMEM((4, 256, own), bf16),
            pltpu.VMEM((4, 4, 2, n, w), bf16),
            pltpu.VMEM((4 * feats, own), f32),
            pltpu.VMEM((4, feats, own), bf16),
            pltpu.VMEM((cols, wide, own), bf16),
            pltpu.VMEM((cols, wide, own), bf16),
            pltpu.VMEM((cols, 2, deep, own), bf16),
            pltpu.VMEM((tiles, own, wide), bf16),
            pltpu.VMEM((tiles, own, wide), bf16),
            pltpu.VMEM((wide, wide // HD * own), bf16),
            pltpu.VMEM((wide, wide // HD * own), bf16),
            pltpu.VMEM((wide, own), f32),
            pltpu.VMEM((tiles, deep, own), f32),
            pltpu.VMEM((8, deep), f32),
            pltpu.VMEM((cols, deep + wide, own), bf16),
            pltpu.VMEM((tiles, own, 128), f32),
            pltpu.VMEM((own, student_width), f32),
            pltpu.VMEM((own, student_width), f32),
            pltpu.VMEM((24, student_width), f32),
            pltpu.VMEM((2, 4, 24, student_width), f32),
            pltpu.VMEM((tall, 128), f32),
        ]
        + parts * 2
        + [dma((2, 4)), dma((2, 4)), dma((4,)), dma((4,)), dma((5,)), dma((5,)), dma((5,)), dma((5,))]
        + [dma, dma, dma((4,)), dma((2, 2))]
        + [dma((4,)), dma((4,)), dma((7,)), dma((7,)), dma, dma((4,)), dma((2, 2))]
        + scatter_scratch(3, n, w, bf16),
        compiler_params=pltpu.CompilerParams(
            collective_id=cid, has_side_effects=True, vmem_limit_bytes=60 * 1024 * 1024
        ),
        name="tail",
    )(*grads, *attention, *student, *vectors, *rest, out_t.reshape(4, feats, own), w_attn)


def finish_kernel(docs, classes, in_ref, back_ref, attn_ref, grad_ref, small_ref, *outs):
    d, r, c = place()
    w_qkv, w_out, w_in, w_back, tokens, proj, logits, b_qkv, b_in, singles = outs[:9] + (outs[9:],)
    rows = in_ref.shape[0] * in_ref.shape[1]
    w_in[...] = in_ref[...].reshape(rows, -1).astype(f32)
    w_back[...] = back_ref[...].reshape(rows, -1).astype(f32)
    columns = w_qkv.shape[1]
    w_qkv[...] = attn_ref[:, :, :columns].reshape(rows, -1).astype(f32)
    w_out[...] = attn_ref[:, :, columns:].reshape(rows, -1).astype(f32)
    tokens[...] = grad_ref[...].astype(f32)
    feats = proj.shape[0]
    proj[...] = small_ref[pl.ds(pl.multiple_of(r * feats, 8), feats)]
    for i in range(2):
        some = small_ref[pl.ds(pl.multiple_of(920 + 8 * (2 * d + i), 8), 8)]
        logits[i] = some[:docs, :classes]
    line = [small_ref[pl.ds(1012 + 3 * c + i, 1)] for i in range(3)]
    line = jnp.concatenate(line, axis=1)
    wide = b_qkv.shape[1]
    b_qkv[0:1] = line[:, :wide]
    b_qkv[1:2] = line[:, wide:]
    for i in range(b_in.shape[1] // 128):
        b_in[:, i * 128 : (i + 1) * 128] = small_ref[pl.ds(952 + 6 * c + i, 1)]
    for i in range(6):
        line = [small_ref[976 + 6 * i + j : 977 + 6 * i + j] for j in range(6)]
        line = jnp.concatenate(line, axis=1)
        for row in range(4):

            @pl.when(r == row)
            def _():
                singles[i][...] = line[:, row * feats : (row + 1) * feats]

    s_mid, s_cls, s_mid_bias, s_cls_bias, s_bias, s_query = singles[6:]
    s_mid[...] = small_ref[768:896]
    s_cls[...] = jnp.concatenate([small_ref[896:912]] + [jnp.zeros((112, 128), f32)], axis=0).T[:, :classes]
    s_mid_bias[...] = small_ref[912:913]
    s_cls_bias[...] = small_ref[913:914, :classes]
    s_bias[...] = small_ref[914:915]
    s_query[...] = small_ref[915:916]


def finish_fast(docs, classes, w_in, w_back, w_attn, grad, small, columns):
    _, part, hidden = w_in.shape
    feats = 2 * part
    width = small.shape[1]

    def shape(*dims):
        return jax.ShapeDtypeStruct(dims, f32)

    shapes = [
        shape(feats, columns), shape(w_attn.shape[2] - columns, feats), shape(feats, hidden), shape(feats, hidden),
        shape(*grad.shape), shape(feats, width), shape(2, docs, classes), shape(2, columns // 3), shape(1, hidden),
    ]
    shapes += [shape(1, feats)] * 6
    shapes += [shape(width, width), shape(width, classes), shape(1, width), shape(1, classes)] + [shape(1, width)] * 2
    return pl.pallas_call(
        functools.partial(finish_kernel, docs, classes),
        out_shape=shapes,
        in_specs=[VM] * 5,
        out_specs=[VM] * len(shapes),
        name="finish",
    )(w_in, w_back, w_attn, grad, small)


def dot(a, b, contract=((1,), (0,))):
    return lax.dot_general(a, b, (contract, ((), ())), preferred_element_type=f32)


def block_rows(ref, heads, scale, out):
    own = ref.shape[-1]
    for h in range(heads):
        for g in range(heads):
            spot = (pl.ds(h * HD, HD), pl.ds(g * own, own))
            if h == g:
                out[spot] = ref[0, pl.ds(h * HD, HD)] * jnp.asarray(scale, out.dtype)
            else:
                out[spot] = jnp.zeros((HD, own), out.dtype)


def fast_local(
    tokens,
    segments,
    labels,
    cotangent,
    w_qkv,
    b_qkv,
    w_out,
    b_out,
    ln1_gain,
    ln1_bias,
    w_in,
    b_in,
    w_back,
    b_back,
    ln2_gain,
    ln2_bias,
    s_proj,
    s_bias,
    s_query,
    s_mid,
    s_mid_bias,
    s_cls,
    s_cls_bias,
):
    _, width_row, cols_local = tokens.shape
    parts, rows, cols, seqs, _ = sizes(tokens.shape[0])
    width = width_row * rows
    own = cols_local // parts
    width_col = b_qkv.shape[1]
    heads_dev = width_col // HD
    hidden_col = b_in.shape[0]
    docs_count = labels.shape[1]
    class_count = s_cls.shape[1]
    student_width = s_proj.shape[1]
    seq_len = segments.shape[1]
    row_index = lax.axis_index("row")
    col_index = lax.axis_index("col")
    dp_index = lax.axis_index("dp")
    score_scale = HD ** (-0.5)
    pool_scale = SHD ** (-0.5)
    query_heads = s_query.reshape(SH, SHD)
    doc_ids = jnp.arange(docs_count, dtype=jnp.int32)
    class_ids = jnp.arange(class_count, dtype=jnp.int32)

    ints = jnp.pad(labels, ((0, 0), (0, own - docs_count)))[:, None]
    ints = jnp.concatenate([segments.reshape(-1, seq_len // own, own), ints], axis=1)
    ints = jnp.pad(ints, ((0, 0), (0, 16 - ints.shape[1]), (0, 0)))
    row_vectors = [b_out, ln1_gain, ln1_bias, b_back, ln2_gain, ln2_bias]
    (
        w_attn, w_in_all, w_back_all, x_parts, c_parts, ints, queries, kv, w_out_all, row_vectors, b_in_all,
        s_proj_all, context, lse, ctx_parts,
    ) = head_fast(
        [w_qkv, w_out, w_in, w_back],
        tokens,
        cotangent,
        ints,
        [b_qkv, b_in[None], s_proj] + [v[None] for v in row_vectors],
        score_scale,
        1,
    )
    w_in_all = w_in_all.reshape(cols, width, hidden_col)
    w_back_all = w_back_all.reshape(cols, width, hidden_col)
    b_out_a, gain_one, bias_one, b_back_a, gain_two, bias_two = [row_vectors[i] for i in range(6)]
    x_t, ctx_t = x_parts.reshape(width, own), ctx_parts.reshape(width, own)
    kv = kv.reshape(cols * parts, 2 * width_col, own)
    own_ints = lax.dynamic_index_in_dim(ints.reshape(seqs, 16, own), row_index, 0, False)
    seg_own = lax.dynamic_index_in_dim(own_ints, 2 * col_index + dp_index, 0, False)
    label_seq = own_ints[seq_len // own, :docs_count]

    x = x_t.T
    attn_out = mm(ctx_t, w_out_all, ((0,), (0,))) + b_out_a
    normed_one, inv_one = normalize(x.astype(f32) + attn_out)
    hidden_one = normed_one * gain_one + bias_one
    hidden_low = hidden_one.astype(bf16)
    pre_act = jnp.einsum("td,cdn->ctn", hidden_low, w_in_all, preferred_element_type=f32)
    pre_act = pre_act + b_in_all[:, None, :]
    act = gelu_exact(pre_act).astype(bf16)
    ffn_out = jnp.einsum("ctn,cdn->td", act, w_back_all, preferred_element_type=f32) + b_back_a
    normed_two, inv_two = normalize(hidden_one + ffn_out)
    layer_out = (normed_two * gain_two + bias_two).astype(bf16)

    d_out = c_parts.reshape(width, own).T.astype(f32)
    g_ln2_gain = jnp.sum(d_out * normed_two, axis=0)
    g_ln2_bias = jnp.sum(d_out, axis=0)
    d_resid_two = normalize_back(d_out * gain_two, normed_two, inv_two)
    d_ffn = d_resid_two.astype(bf16)
    g_back_bias = jnp.sum(d_ffn.astype(f32), axis=0)
    g_back = jnp.einsum("td,ctn->cdn", d_ffn, act, preferred_element_type=f32)
    d_act = jnp.einsum("td,cdn->ctn", d_ffn, w_back_all, preferred_element_type=f32)
    _, gelu_fn = jax.vjp(gelu_exact, pre_act)
    d_pre = gelu_fn(d_act)[0].astype(bf16)
    g_in_bias = jnp.sum(d_pre.astype(f32), axis=1)
    g_in = jnp.einsum("td,ctn->cdn", hidden_low, d_pre, preferred_element_type=f32)
    d_hidden_one = d_resid_two + jnp.einsum(
        "ctn,cdn->td", d_pre, w_in_all, preferred_element_type=f32
    )
    g_ln1_gain = jnp.sum(d_hidden_one * normed_one, axis=0)
    g_ln1_bias = jnp.sum(d_hidden_one, axis=0)
    d_resid_one = normalize_back(d_hidden_one * gain_one, normed_one, inv_one)
    d_attn = d_resid_one.astype(bf16)
    g_out_bias = jnp.sum(d_attn.astype(f32), axis=0)
    d_ctx = mm(w_out_all, d_attn, ((1,), (1,))).astype(bf16)
    blocked = (cols, rows, parts, width_row // parts, -1)
    lane_pad = ((0, 0), (0, 128 - class_count))
    student_vectors = jnp.stack([s_bias, s_query, s_mid_bias, jnp.pad(s_cls_bias, (0, 128 - class_count))])
    student_vectors = jnp.pad(student_vectors, ((0, 4), (0, 0)))
    g_in, g_back, g_attn, grad_tokens, out, small = tail_fast(
        docs_count,
        class_count,
        score_scale,
        [g_in.astype(bf16).reshape(blocked), g_back.astype(bf16).reshape(blocked)],
        [queries, kv, lse, context, d_ctx.reshape(cols, width_col, own), ints],
        [
            layer_out,
            seg_own[:, None],
            jnp.pad(label_seq, (0, 8 - docs_count))[:, None],
            s_proj_all,
            student_vectors,
            s_mid,
            jnp.pad(s_cls, lane_pad),
        ],
        [g_in_bias]
        + [v[None] for v in (g_out_bias, g_ln1_gain, g_ln1_bias, g_back_bias, g_ln2_gain, g_ln2_bias)],
        [x_parts, ctx_parts, d_resid_one],
        layer_out.T,
        w_attn,
        4,
    )
    (
        g_qkv, g_out, g_in, g_back, grad_tokens, g_sproj, logits, g_qkv_bias, g_in_bias, g_out_bias, g_ln1_gain,
        g_ln1_bias, g_back_bias, g_ln2_gain, g_ln2_bias, g_mid, g_cls, g_mid_bias, g_cls_bias, g_sbias, g_query,
    ) = finish_fast(docs_count, class_count, g_in, g_back, g_attn, grad_tokens, small, 3 * width_col)
    return (
        out,
        logits,
        grad_tokens,
        g_qkv,
        g_qkv_bias,
        g_out,
        g_out_bias[0],
        g_ln1_gain[0],
        g_ln1_bias[0],
        g_in,
        g_in_bias[0],
        g_back,
        g_back_bias[0],
        g_ln2_gain[0],
        g_ln2_bias[0],
        g_sproj,
        g_sbias[0],
        g_query[0],
        g_mid,
        g_mid_bias[0],
        g_cls,
        g_cls_bias[0],
    )


def solution(mesh):
    row, col = P("row"), P("col")
    grid, whole = P("row", "col"), P("dp", "row", "col")
    placed = (
        (whole, P("dp", None), P("dp", None), whole, grid, P(None, "col"), P("col", "row"))
        + (row, row, row, grid, col, grid, row, row, row, P("row", None))
        + (P(),) * 6
    )
    results = (
        (whole, P("dp", None, None), whole, grid, P(None, "col"), P("col", "row"))
        + (row, row, row, grid, col, grid, row, row, row, P("row", None))
        + (P(),) * 6
    )
    quick = dict(mesh.shape) == {"dp": 2, "row": 4, "col": 4}
    local = fast_local if quick else general_local
    return jax.shard_map(local, mesh=mesh, in_specs=placed, out_specs=results, check_vma=False)
```

```python
import functools
import jax
import jax.numpy as jnp
from jax import lax
from jax.experimental import pallas as pl
from jax.experimental.pallas import tpu as pltpu
from jax.sharding import PartitionSpec as P

HD = 64
SH = 2
SHD = 64

norm_eps = 1e-06
masked_value = -1e30
highest = lax.Precision.HIGHEST
f32 = jnp.float32
bf16 = jnp.bfloat16
WORLD = ("col", "row", "dp")


def sizes(seqs_local):
    parts = lax.axis_size("dp")
    rows = lax.axis_size("row")
    seqs = seqs_local * parts
    return parts, rows, lax.axis_size("col"), seqs, rows // seqs


def row_groups(rows, sub):
    return [list(range(at, at + sub)) for at in range(0, rows, sub)]


def take_in(values):
    parts, rows, _, seqs, sub = sizes(values.shape[0])
    held = lax.all_to_all(values, "dp", 2, 0, tiled=True)
    feats, half = held.shape[1:]
    held = held.reshape(seqs, feats, sub, half // sub).transpose(0, 2, 1, 3)
    held = held.reshape(rows, feats, half // sub)
    held = lax.all_to_all(held, "row", 0, 0, tiled=True)
    return held.reshape(rows * feats, half // sub)


def give_back(values, seqs_local):
    parts, rows, _, seqs, sub = sizes(seqs_local)
    width, own = values.shape
    feats = width // rows
    held = lax.all_to_all(values.reshape(rows, feats, own), "row", 0, 0, tiled=True)
    held = held.reshape(seqs, sub, feats, own).transpose(0, 2, 1, 3).reshape(seqs, feats, sub * own)
    return lax.all_to_all(held, "dp", 0, 2, tiled=True)


def gather_world(shard):
    cols, rows = lax.axis_size("col"), lax.axis_size("row")
    out = lax.all_gather(shard, WORLD, axis=0, tiled=True)
    return out.reshape(cols, rows, -1, shard.shape[1])


def own_half(block):
    parts = lax.axis_size("dp")
    amount = block.shape[0] // parts
    return lax.dynamic_slice_in_dim(block, lax.axis_index("dp") * amount, amount)


def scatter_world(full):
    flat = full.reshape(-1, full.shape[-1])
    mine = lax.psum_scatter(flat, WORLD, scatter_dimension=0, tiled=True)
    return lax.all_gather(mine, "dp", axis=0, tiled=True)


def swap_cols(values):
    return lax.all_to_all(values, "col", 0, 0, tiled=True)


def gather_sequence(values, sub):
    cols, own, width = values.shape
    held = values[:, None]
    if sub > 1:
        groups = row_groups(lax.axis_size("row"), sub)
        held = lax.all_gather(held, "row", axis=1, tiled=True, axis_index_groups=groups)
    held = lax.all_gather(held[:, None], "dp", axis=1, tiled=True)
    return held.reshape(-1, width)


def scatter_sequence(values, cols, sub):
    parts = lax.axis_size("dp")
    width = values.shape[-1]
    held = values.reshape(cols, parts, sub, -1, width)
    held = lax.psum_scatter(held, "dp", scatter_dimension=1, tiled=True)[:, 0]
    if sub > 1:
        groups = row_groups(lax.axis_size("row"), sub)
        held = lax.psum_scatter(
            held, "row", scatter_dimension=1, tiled=True, axis_index_groups=groups
        )
    return held[:, 0]


def normalize(values):
    mean_v = jnp.mean(values, axis=-1, keepdims=True)
    center = values - mean_v
    inv_std = lax.rsqrt(jnp.mean(center * center, axis=-1, keepdims=True) + norm_eps)
    return center * inv_std, inv_std


def normalize_back(grad_hat, normed, inv_std):
    return inv_std * (
        grad_hat
        - jnp.mean(grad_hat, axis=-1, keepdims=True)
        - normed * jnp.mean(grad_hat * normed, axis=-1, keepdims=True)
    )


def gelu_exact(values):
    return jax.nn.gelu(values, approximate=False)


def mm(a, b, contract):
    return lax.dot_general(a, b, (contract, ((), ())), preferred_element_type=f32)


def combine_pool(part_one, part_two):
    top_a, total_a, sum_a = part_one
    top_b, total_b, sum_b = part_two
    row_top = jnp.maximum(top_a, top_b)
    factor_a = jnp.exp(top_a - row_top)
    factor_b = jnp.exp(top_b - row_top)
    return (
        row_top,
        total_a * factor_a + total_b * factor_b,
        sum_a * factor_a[:, :, None] + sum_b * factor_b[:, :, None],
    )


def attend(q, k, v, q_seg, k_seg, scale):
    scores = jnp.einsum("qhd,khd->hqk", q, k, preferred_element_type=f32) * scale
    scores = jnp.where((q_seg[:, None] == k_seg[None, :])[None], scores, masked_value)
    top = jnp.max(scores, axis=-1, keepdims=True)
    exp_scores = jnp.exp(scores - top)
    total = jnp.sum(exp_scores, axis=-1, keepdims=True)
    probs = exp_scores / total
    context = jnp.einsum("hqk,khd->qhd", probs.astype(bf16), v, preferred_element_type=f32)
    return context.astype(bf16), probs


def attend_back(q, k, v, probs, d_ctx, scale):
    d_probs = jnp.einsum("qhd,khd->hqk", d_ctx, v, preferred_element_type=f32)
    delta = jnp.sum(probs * d_probs, axis=-1, keepdims=True)
    d_scores = (probs * (d_probs - delta)).astype(bf16)
    d_q = jnp.einsum("hqk,khd->qhd", d_scores, k, preferred_element_type=f32) * scale
    d_k = jnp.einsum("hqk,qhd->khd", d_scores, q, preferred_element_type=f32) * scale
    d_v = jnp.einsum("hqk,qhd->khd", probs.astype(bf16), d_ctx, preferred_element_type=f32)
    return d_q, d_k, d_v


def general_local(
    tokens,
    segments,
    labels,
    cotangent,
    w_qkv,
    b_qkv,
    w_out,
    b_out,
    ln1_gain,
    ln1_bias,
    w_in,
    b_in,
    w_back,
    b_back,
    ln2_gain,
    ln2_bias,
    s_proj,
    s_bias,
    s_query,
    s_mid,
    s_mid_bias,
    s_cls,
    s_cls_bias,
):
    seqs_local, width_row, cols_local = tokens.shape
    parts, rows, cols, seqs, sub = sizes(seqs_local)
    width = width_row * rows
    own = cols_local // (parts * sub)
    width_col = b_qkv.shape[1]
    heads_dev = width_col // HD
    hidden_col = b_in.shape[0]
    docs_count = labels.shape[1]
    class_count = s_cls.shape[1]
    student_width = s_proj.shape[1]
    row_index = lax.axis_index("row")
    col_index = lax.axis_index("col")
    dp_index = lax.axis_index("dp")
    seq_index = row_index // sub
    sub_index = row_index % sub
    score_scale = HD ** (-0.5)
    pool_scale = SHD ** (-0.5)
    query_heads = s_query.reshape(SH, SHD)
    doc_ids = jnp.arange(docs_count, dtype=jnp.int32)
    class_ids = jnp.arange(class_count, dtype=jnp.int32)

    w_qkv_all = gather_world(own_half(w_qkv)).reshape(cols, width, 3 * width_col)
    x_t = take_in(tokens)
    rest = jnp.concatenate([own_half(w_in), own_half(w_back), own_half(w_out).reshape(-1, width_col)], axis=1)
    rest_all = gather_world(rest)
    w_in_all = rest_all[..., :hidden_col].reshape(cols, width, hidden_col)
    w_back_all = rest_all[..., hidden_col : 2 * hidden_col].reshape(cols, width, hidden_col)
    w_out_all = rest_all[..., 2 * hidden_col :].reshape(cols, rows, width_col, width_row)
    w_out_all = w_out_all.transpose(0, 2, 1, 3).reshape(width, width)
    row_vectors = lax.all_gather(
        jnp.stack([b_out, ln1_gain, ln1_bias, b_back, ln2_gain, ln2_bias]), "row", axis=1, tiled=True
    )
    b_out_a, gain_one, bias_one, b_back_a, gain_two, bias_two = [row_vectors[i] for i in range(6)]
    b_qkv_all = lax.all_gather(b_qkv, "col")
    b_in_all = lax.all_gather(b_in, "col")
    s_proj_all = lax.all_gather(s_proj, "row", axis=0, tiled=True)
    whole_ints = lax.all_gather(jnp.concatenate([segments, labels], axis=1), "dp", axis=0, tiled=True)
    ints = lax.dynamic_index_in_dim(whole_ints, seq_index, 0, False)
    seq_len = segments.shape[1]
    seg_all, label_seq = ints[:seq_len], ints[seq_len:]
    seg_blocks = seg_all.reshape(cols, parts, sub, own)
    seg_q = lax.dynamic_index_in_dim(seg_blocks, dp_index, 1, False)
    seg_q = lax.dynamic_index_in_dim(seg_q, sub_index, 1, False)
    seg_own = lax.dynamic_index_in_dim(seg_q, col_index, 0, False)
    seg_q = seg_q.reshape(-1)

    x = x_t.T
    offsets = jnp.stack([b_qkv_all[:, 0], jnp.zeros_like(b_qkv_all[:, 0]), b_qkv_all[:, 1]], axis=1)
    offsets = offsets.reshape(cols, 3, heads_dev, HD).transpose(0, 2, 1, 3).reshape(cols, 1, -1)
    qkv = jnp.einsum("td,cdn->ctn", x, w_qkv_all, preferred_element_type=f32) + offsets
    qkv = swap_cols(qkv.astype(bf16)).reshape(cols, own, heads_dev, 3, HD)
    queries = qkv[:, :, :, 0].reshape(cols * own, heads_dev, HD)
    kv = gather_sequence(qkv[:, :, :, 1:].reshape(cols, own, -1), sub)
    kv = kv.reshape(seq_len, heads_dev, 2, HD)
    key_rows, value_rows = kv[:, :, 0], kv[:, :, 1]
    context, probs = attend(queries, key_rows, value_rows, seg_q, seg_all, score_scale)
    ctx = swap_cols(context.reshape(cols, own, width_col))
    ctx = ctx.transpose(1, 0, 2).reshape(own, width)

    attn_out = mm(ctx, w_out_all, ((1,), (0,))) + b_out_a
    normed_one, inv_one = normalize(x.astype(f32) + attn_out)
    hidden_one = normed_one * gain_one + bias_one
    hidden_low = hidden_one.astype(bf16)
    pre_act = jnp.einsum("td,cdn->ctn", hidden_low, w_in_all, preferred_element_type=f32)
    pre_act = pre_act + b_in_all[:, None, :]
    act = gelu_exact(pre_act).astype(bf16)
    ffn_out = jnp.einsum("ctn,cdn->td", act, w_back_all, preferred_element_type=f32) + b_back_a
    normed_two, inv_two = normalize(hidden_one + ffn_out)
    layer_out = (normed_two * gain_two + bias_two).astype(bf16)
    out = give_back(layer_out.T, seqs_local)

    student_h = mm(layer_out, s_proj_all, ((1,), (0,))) + s_bias
    head_parts = student_h.reshape(own, SH, SHD)
    pool_logit = jnp.sum(head_parts * query_heads, axis=-1) * pool_scale
    member = (seg_own[:, None] == doc_ids[None, :])[:, :, None]
    masked = jnp.where(member, pool_logit[:, None, :], masked_value)
    local_top = jnp.max(masked, axis=0)
    local_exp = jnp.where(member, jnp.exp(masked - local_top[None]), 0.0)
    local_total = jnp.sum(local_exp, axis=0)
    local_sum = jnp.einsum("tdh,thk->dhk", local_exp, head_parts, precision=highest)
    stats = jnp.concatenate([local_top[..., None], local_total[..., None], local_sum], axis=-1)
    stats = lax.all_gather(stats, ("dp", "col"))
    if sub > 1:
        stats = lax.all_gather(stats, "row", axis=0, tiled=True, axis_index_groups=row_groups(rows, sub))
    tops, totals, sums = stats[..., 0], stats[..., 1], stats[..., 2:]
    doc_top = jnp.max(tops, axis=0)
    factors = jnp.exp(tops - doc_top[None])
    doc_total = jnp.sum(totals * factors, axis=0)
    pooled_heads = jnp.sum(sums * factors[..., None], axis=0) / doc_total[:, :, None]
    pooled = pooled_heads.reshape(docs_count, student_width)
    middle = jnp.tanh(jnp.dot(pooled, s_mid, precision=highest) + s_mid_bias)
    logit_rows = jnp.dot(middle, s_cls, precision=highest) + s_cls_bias
    logits = lax.all_gather(logit_rows, "row")[::sub]
    logits = lax.dynamic_slice_in_dim(logits, dp_index * seqs_local, seqs_local)
    logit_top = jnp.max(logit_rows, axis=-1, keepdims=True)
    logit_exp = jnp.exp(logit_rows - logit_top)
    one_hot = (label_seq[:, None] == class_ids[None, :]).astype(f32)
    d_logits = logit_exp / jnp.sum(logit_exp, axis=-1, keepdims=True) - one_hot
    g_cls = jnp.dot(middle.T, d_logits, precision=highest)
    g_cls_bias = jnp.sum(d_logits, axis=0)
    d_middle = jnp.dot(d_logits, s_cls.T, precision=highest) * (1.0 - middle * middle)
    g_mid = jnp.dot(pooled.T, d_middle, precision=highest)
    g_mid_bias = jnp.sum(d_middle, axis=0)
    d_pooled = jnp.dot(d_middle, s_mid.T, precision=highest).reshape(docs_count, SH, SHD)
    shares = jnp.where(member, jnp.exp(masked - doc_top[None]), 0.0) / doc_total[None]
    d_share = jnp.einsum("dhk,thk->tdh", d_pooled, head_parts, precision=highest)
    base_term = jnp.sum(d_pooled * pooled_heads, axis=-1)
    d_pool_logit = jnp.sum(shares * (d_share - base_term[None]), axis=1)
    d_heads = jnp.einsum("tdh,dhk->thk", shares, d_pooled, precision=highest)
    d_heads = d_heads + d_pool_logit[:, :, None] * query_heads[None] * pool_scale
    g_query = (jnp.sum(d_pool_logit[:, :, None] * head_parts, axis=0) * pool_scale).reshape(-1)
    d_student = d_heads.reshape(own, student_width)
    g_sbias = jnp.sum(d_student, axis=0)
    g_sproj = jnp.dot(layer_out.astype(f32).T, d_student, precision=highest)

    d_out = take_in(cotangent).T.astype(f32)
    g_ln2_gain = jnp.sum(d_out * normed_two, axis=0)
    g_ln2_bias = jnp.sum(d_out, axis=0)
    d_resid_two = normalize_back(d_out * gain_two, normed_two, inv_two)
    d_ffn = d_resid_two.astype(bf16)
    g_back_bias = jnp.sum(d_ffn.astype(f32), axis=0)
    g_back = jnp.einsum("td,ctn->cdn", d_ffn, act, preferred_element_type=f32)
    d_act = jnp.einsum("td,cdn->ctn", d_ffn, w_back_all, preferred_element_type=f32)
    _, gelu_fn = jax.vjp(gelu_exact, pre_act)
    d_pre = gelu_fn(d_act)[0].astype(bf16)
    g_in_bias = jnp.sum(d_pre.astype(f32), axis=1)
    g_in = jnp.einsum("td,ctn->cdn", hidden_low, d_pre, preferred_element_type=f32)
    d_hidden_one = d_resid_two + jnp.einsum(
        "ctn,cdn->td", d_pre, w_in_all, preferred_element_type=f32
    )
    g_ln1_gain = jnp.sum(d_hidden_one * normed_one, axis=0)
    g_ln1_bias = jnp.sum(d_hidden_one, axis=0)
    d_resid_one = normalize_back(d_hidden_one * gain_one, normed_one, inv_one)
    d_attn = d_resid_one.astype(bf16)
    g_out_bias = jnp.sum(d_attn.astype(f32), axis=0)
    g_out = mm(ctx, d_attn, ((0,), (0,)))
    d_ctx = mm(d_attn, w_out_all, ((1,), (1,))).astype(bf16)
    d_ctx = swap_cols(d_ctx.reshape(own, cols, width_col).transpose(1, 0, 2))
    d_ctx = d_ctx.reshape(cols * own, heads_dev, HD)
    d_q, d_k, d_v = attend_back(queries, key_rows, value_rows, probs, d_ctx, score_scale)
    d_kv = jnp.stack([d_k, d_v], axis=2).astype(bf16).reshape(seq_len, -1)
    d_kv = scatter_sequence(d_kv, cols, sub).reshape(cols, own, heads_dev, 2, HD)
    d_q = d_q.astype(bf16).reshape(cols, own, heads_dev, 1, HD)
    d_qkv = jnp.concatenate([d_q, d_kv], axis=3).reshape(cols, own, 3 * width_col)
    d_qkv = swap_cols(d_qkv)
    g_qkv_bias = jnp.sum(d_qkv.astype(f32), axis=1).reshape(cols, heads_dev, 3, HD)
    g_qkv = jnp.einsum("td,ctn->cdn", x, d_qkv, preferred_element_type=f32)
    d_tokens = d_resid_one + jnp.einsum("ctn,cdn->td", d_qkv, w_qkv_all, preferred_element_type=f32)
    grad_tokens = give_back(d_tokens.astype(bf16).T, seqs_local).astype(f32)

    g_out = g_out.reshape(cols, width_col, rows, width_row).transpose(0, 2, 1, 3)
    g_out = g_out.reshape(cols, rows, width_row, width_col)
    model = jnp.concatenate(
        [
            g_in.reshape(cols, rows, width_row, hidden_col).astype(bf16),
            g_back.reshape(cols, rows, width_row, hidden_col).astype(bf16),
            g_out.astype(bf16),
        ],
        axis=-1,
    )
    model = scatter_world(model).astype(f32)
    g_qkv = scatter_world(g_qkv.reshape(cols, rows, width_row, 3 * width_col).astype(bf16)).astype(f32)
    once = 1.0 / (parts * cols * sub)
    small = (
        g_qkv_bias[:, :, 0].reshape(cols, width_col),
        g_qkv_bias[:, :, 2].reshape(cols, width_col),
        g_in_bias,
        g_out_bias,
        g_ln1_gain,
        g_ln1_bias,
        g_back_bias,
        g_ln2_gain,
        g_ln2_bias,
        g_sproj,
        g_sbias,
        g_query,
        g_mid * once,
        g_mid_bias * once,
        g_cls * once,
        g_cls_bias * once,
    )
    small = lax.psum(small, WORLD)

    def at_col(part):
        return lax.dynamic_index_in_dim(part, col_index, 0, False)

    def at_row(part):
        return lax.dynamic_slice_in_dim(part, row_index * width_row, width_row)

    return (
        out,
        logits,
        grad_tokens,
        g_qkv,
        jnp.stack([at_col(small[0]), at_col(small[1])]),
        model[:, 2 * hidden_col :].reshape(width_col, width_row),
        at_row(small[3]),
        at_row(small[4]),
        at_row(small[5]),
        model[:, :hidden_col],
        at_col(small[2]),
        model[:, hidden_col : 2 * hidden_col],
        at_row(small[6]),
        at_row(small[7]),
        at_row(small[8]),
        at_row(small[9]),
        small[10],
        small[11],
        small[12],
        small[13],
        small[14],
        small[15],
    )


MESH = pl.DeviceIdType.MESH
HBM = pl.BlockSpec(memory_space=pl.ANY)


def place():
    return lax.axis_index("dp"), lax.axis_index("row"), lax.axis_index("col")


def greet(peers, guarded=()):
    barrier = pltpu.get_barrier_semaphore()
    for peer in peers:
        pl.semaphore_signal(barrier, inc=1, device_id=peer, device_id_type=MESH)
    for there, peer in guarded:

        @pl.when(there)
        def _():
            pl.semaphore_signal(barrier, inc=1, device_id=peer, device_id_type=MESH)

    amount = len(peers)
    for there, _ in guarded:
        amount = amount + there.astype(jnp.int32)
    pl.semaphore_wait(barrier, amount)


def rcopy(src, dst, send, recv, peer):
    return pltpu.make_async_remote_copy(
        src_ref=src, dst_ref=dst, send_sem=send, recv_sem=recv, device_id=peer, device_id_type=MESH
    )


def take_copies(src, out, local, send, recv):
    d, r, c = place()
    own = out.shape[2]
    moves = []
    for i in range(2):
        for far in range(2):
            row, core = 2 * d + i, d ^ far
            piece = src.at[i, :, pl.ds(pl.multiple_of(core * own, own), own)]
            here = (row == r) if far == 0 else None

            def start(piece=piece, row=row, core=core, slot=2 * i + far, here=here):
                def away():
                    rcopy(piece, out.at[r], send.at[slot], recv.at[r], (core, row, c)).start()

                if here is None:
                    away()
                else:
                    pl.when(jnp.logical_not(here))(away)

                    @pl.when(here)
                    def _():
                        pltpu.make_async_copy(piece, out.at[r], local).start()

            def wait(piece=piece, row=row, core=core, slot=2 * i + far, here=here):
                def away():
                    rcopy(piece, out.at[r], send.at[slot], recv.at[r], (core, row, c)).wait_send()

                if here is None:
                    away()
                else:
                    pl.when(jnp.logical_not(here))(away)

                    @pl.when(here)
                    def _():
                        pltpu.make_async_copy(piece, out.at[r], local).wait()

            moves.append((start, wait))
    for row in range(4):

        def arrive(row=row):
            @pl.when(jnp.logical_not((row == r) & (r // 2 == d)))
            def _():
                piece = src.at[0, :, pl.ds(0, own)]
                rcopy(piece, out.at[row], send.at[0], recv.at[row], (d, r, c)).wait_recv()

        moves.append((lambda: None, arrive))
    return moves


VM = pl.BlockSpec(memory_space=pltpu.VMEM)


def head_kernel(scale, *refs):
    (w_qkv_ref, w_out_ref, w_in_ref, w_back_ref, tok, cot, ints), refs = refs[:7], refs[7:]
    (b_qkv_ref, b_in_ref, proj_ref), row_vecs, refs = refs[:3], refs[3:9], refs[9:]
    (a_out, b_out, c_out, tok_out, cot_out, ints_out, q_out, kv_out), refs = refs[:8], refs[8:]
    (wo_out, vec_all, b_in_all, proj_all, ctx_own, lse_ref, ctx_out), refs = refs[:7], refs[7:]
    (shard_a, shard_v, vec_out, x_nat, q_src, kv_src, kn, q3, s_scr, o_scr, kcol), refs = refs[:11], refs[11:]
    own_sem, zs, zr, xs, xr, ys, yr, cs, cr, ps, pr, tl, ts, tr, il, hs, hr, hps, hpr, xl, xs2, xr2, vs, vr = refs
    d, r, c = place()
    kinds = 4
    part = w_in_ref.shape[0] // 2
    mine = pl.ds(pl.multiple_of(d * part, 16), part)
    feats = tok_out.shape[1]
    shards = [shard_a.at[mine], shard_v.at[pl.ds(pl.multiple_of(d * 48, 8), 48)], w_in_ref.at[mine], w_back_ref.at[mine]]
    outs = [a_out, vec_out, b_out, c_out]
    cols = 4
    xn, yn, pn = (d, r ^ 1, c), (d, r ^ 2, c), (1 - d, r, c)
    up, down = (d, r, c + 1), (d, r, c - 1)
    has_up, has_down = c < cols - 1, c > 0
    columns = w_qkv_ref.shape[1]
    shard_a[:, :columns] = w_qkv_ref[...]
    shard_a[:, columns:] = w_out_ref[...]
    heads = columns // (3 * HD)
    pieces = []
    for h in range(heads):
        spot = slice(h * HD, (h + 1) * HD)
        pieces += [b_qkv_ref[0:1, spot], jnp.zeros((1, HD), f32), b_qkv_ref[1:2, spot]]
    bias_lanes = -(-columns // 128) * 128
    pieces.append(jnp.zeros((1, bias_lanes - columns), f32))
    line = jnp.concatenate(pieces, axis=1)
    at = 0
    for i in range(bias_lanes // 128):
        shard_v[at : at + 1] = line[:, i * 128 : (i + 1) * 128]
        at += 1
    for ref in row_vecs:
        line = jnp.concatenate([ref[...], jnp.zeros((1, 256 - feats), f32)], axis=1)
        for i in range(2):
            shard_v[at : at + 1] = line[:, i * 128 : (i + 1) * 128]
            at += 1
    for i in range(b_in_ref.shape[1] // 128):
        shard_v[at : at + 1] = b_in_ref[:, i * 128 : (i + 1) * 128]
        at += 1
    proj_at, proj_rows = 48, feats // 4
    for i in range(at, proj_at):
        shard_v[i : i + 1] = jnp.zeros((1, 128), f32)
    shard_v[proj_at:] = proj_ref[pl.ds(pl.multiple_of(c * proj_rows, 16), proj_rows)].astype(f32)

    greet(plane_peers() + [(d, r, c ^ j) for j in (1, 2, 3)])
    moves = take_copies(tok, tok_out, tl, ts, tr)
    for start, _ in moves:
        start()
    late_moves = take_copies(cot, cot_out, xl, xs2, xr2)
    pltpu.make_async_copy(ints, ints_out.at[d], il.at[0]).start()
    rcopy(ints, ints_out.at[d], il.at[1], il.at[2], pn).start()
    halves = [part // 2, 24, part // 2, part // 2]

    def z_send(k, at, way, hop):
        src = shards[k] if hop == 1 else outs[k].at[at, r, d]
        return rcopy(
            src, outs[k].at[at, r, d], zs.at[k, way, hop - 1], zr.at[k, way, hop - 1], up if way == 0 else down
        )

    def src_of(k, at, own):
        return shards[k] if own else outs[k].at[at, r, d]

    def to_x(k, at, own):
        return rcopy(src_of(k, at, own), outs[k].at[at, r, d], xs.at[k, at], xr.at[k, at], xn)

    def to_y(k, at, own):
        return rcopy(src_of(k, at, own), outs[k].at[at, r, d], ys.at[k, at], yr.at[k, at], yn)

    def to_p(k, at, own):
        return rcopy(src_of(k, at, own), outs[k].at[at, r, d], ps.at[k, at, 0], pr.at[k, at, 0], pn)

    def relay(k, at, which):
        row = r ^ 1 if which == 0 else r ^ 2
        ref = outs[k].at[at, row, d, pl.ds(which * halves[k], halves[k])]
        return rcopy(ref, ref, cs.at[k, at, which], cr.at[k, at, which], yn if which == 0 else xn)

    def pass_p(k, at, bit):
        ref = outs[k].at[at, r ^ bit, d]
        return rcopy(ref, ref, ps.at[k, at, bit], pr.at[k, at, bit], pn)

    def got_x(k, at):
        ref = outs[k].at[at, r ^ 1, d]
        rcopy(ref, ref, xs.at[k, at], xr.at[k, at], xn).wait_recv()

    def got_y(k, at):
        ref = outs[k].at[at, r ^ 2, d]
        rcopy(ref, ref, ys.at[k, at], yr.at[k, at], yn).wait_recv()

    def got_corner(k, at):
        for which in range(2):
            ref = outs[k].at[at, r ^ 3, d, pl.ds(which * halves[k], halves[k])]
            rcopy(ref, ref, cs.at[k, at, which], cr.at[k, at, which], xn).wait_recv()

    def got_p(k, at, bit):
        ref = outs[k].at[at, r ^ bit, 1 - d]
        rcopy(ref, ref, ps.at[k, at, bit], pr.at[k, at, bit], pn).wait_recv()

    def set_out(k):
        @pl.when(has_up)
        def _():
            z_send(k, c, 0, 1).start()

        @pl.when(has_down)
        def _():
            z_send(k, c, 1, 1).start()

    for k in range(kinds):
        pltpu.make_async_copy(shards[k], outs[k].at[c, r, d], own_sem.at[k]).start()
        if k < kinds - 1:
            set_out(k)

    def spread(k, at, own):
        to_x(k, at, own).start()
        to_y(k, at, own).start()
        to_p(k, at, own).start()

    def onward(k, at):
        got_x(k, at)
        relay(k, at, 0).start()
        pass_p(k, at, 1).start()
        got_y(k, at)
        relay(k, at, 1).start()
        pass_p(k, at, 2).start()

    steps = [(0, 0)] + [(way, hop) for hop in (1, 2, 3) for way in (0, 1)]
    jobs = [(k, way, hop) for k in range(kinds) for way, hop in steps]

    def at_of(way, hop):
        return c - hop if way == 0 else c + hop

    def valid(way, hop):
        return c >= hop if way == 0 else c + hop < cols

    def guard(way, hop, body):
        if hop == 0:
            body()
        else:
            pl.when(valid(way, hop))(body)

    def first(k, way, hop):
        def body():
            at = at_of(way, hop)
            if hop:
                z_send(k, at, way, hop).wait_recv()
                if hop < 3:
                    can = has_up if way == 0 else has_down

                    @pl.when(can)
                    def _():
                        z_send(k, at, way, hop + 1).start()

            spread(k, at, hop == 0)

        guard(way, hop, body)

    def second(k, way, hop):
        guard(way, hop, lambda: onward(k, at_of(way, hop)))

    def third(k, way, hop):
        def body():
            at = at_of(way, hop)
            got_corner(k, at)
            pass_p(k, at, 3).start()

        guard(way, hop, body)

    def settle(k):
        pltpu.make_async_copy(shards[k], outs[k].at[c, r, d], own_sem.at[k]).wait()
        for way, hop in steps:

            def body():
                for bit in range(4):
                    got_p(k, at_of(way, hop), bit)

            guard(way, hop, body)

    def kv(j):
        return rcopy(kv_src.at[c ^ j], kv_out.at[c, d], hs.at[0, j], hr.at[0, j], (d, r, c ^ j))

    def q(j):
        return rcopy(q_src.at[c ^ j], q_out.at[c], hs.at[1, j], hr.at[1, j], (d, r, c ^ j))

    def pair(j):
        src = kv_src.at[c] if j == 0 else kv_out.at[c ^ j, d]
        return rcopy(src, kv_out.at[c ^ j, d], hps.at[j], hpr.at[j], pn)

    lanes = bias_lanes

    def prepare():
        for _, wait in moves:
            wait()
        x_nat[...] = tok_out[...].reshape(4 * feats, -1).astype(f32).T.astype(bf16)

    def project(j):
        to = c ^ j
        weights = a_out[to, :, :, :, :lanes].reshape(-1, lanes)
        bias = vec_out[to, r, 0, pl.ds(0, 8)]
        bias = jnp.concatenate([bias[i : i + 1] for i in range(lanes // 128)], axis=1)
        made = jnp.dot(x_nat[...], weights, preferred_element_type=f32) + bias
        made = made.T.astype(bf16)
        for h in range(heads):
            rows = pl.ds(h * HD, HD)
            q_src[to, rows] = made[3 * h * HD : (3 * h + 1) * HD]
            kv_src[to, rows] = made[(3 * h + 1) * HD : (3 * h + 2) * HD]
            kv_src[to, pl.ds(wide + h * HD, HD)] = made[(3 * h + 2) * HD : (3 * h + 3) * HD]
        if j:
            kv(j).start()
            q(j).start()
        else:
            pair(0).start()
            kv_out[c, d] = kv_src[c]
            q_out[c] = q_src[c]

    def spread_out(at):
        for row in range(4):
            block = a_out[at, row, :, :, columns:].reshape(-1, feats)
            wo_out[pl.ds(at * wide, wide), row * feats : (row + 1) * feats] = block

    def unpack():
        first = bias_lanes // 128
        for i in range(6):
            for row in range(4):
                line = vec_out[0, row, 0, pl.ds(first + 2 * i, 2)]
                line = jnp.concatenate([line[0:1], line[1:2]], axis=1)
                vec_all[i : i + 1, row * feats : (row + 1) * feats] = line[:, :feats]
        vec_all[6:8] = jnp.zeros((2, 4 * feats), f32)
        first += 12
        for at in range(4):
            for i in range(b_in_all.shape[1] // 128):
                b_in_all[at : at + 1, i * 128 : (i + 1) * 128] = vec_out[at, 0, 0, pl.ds(first + i, 1)]
            for row in range(4):
                rows = pl.ds(row * feats + at * proj_rows, proj_rows)
                proj_all[rows] = vec_out[at, row, 1].astype(bf16)

    tiles = 8
    own = x_nat.shape[0]

    def segment(tile):
        return ints_out[r // 2, r % 2, pl.ds(tile, 1)].astype(f32)

    def collect():
        for j in (1, 2, 3):
            kv(j).wait_recv()
            pair(j).start()
        pltpu.make_async_copy(ints, ints_out.at[d], il.at[0]).wait()
        rcopy(ints, ints_out.at[1 - d], il.at[1], il.at[2], pn).wait()
        for tile in range(tiles):
            kcol[tile] = jnp.broadcast_to(segment(tile), (128, own)).T
        for j in (1, 2, 3):
            q(j).wait_recv()
        for j in range(4):
            pair(j).wait_recv()

        @pl.loop(0, 4)
        def _(at):
            for core in range(2):
                kn[2 * at + core] = kv_out[at, core, pl.ds(0, wide)].astype(f32).T.astype(bf16)

    def attend_block(block):
        block_rows(q_out.at[pl.ds(block, 1)], heads, scale, q3)
        here = 2 * block + d
        low, high = jnp.maximum(here - 4, 0), jnp.minimum(here + 5, tiles)
        qseg = jnp.concatenate([segment(here)] * heads, axis=1)

        def one(j, top):
            s = jnp.dot(kn[j], q3[...], preferred_element_type=f32)
            same = jnp.concatenate([kcol[j]] * (heads * own // 128), axis=1) == qseg
            s = jnp.where(same, s, masked_value)
            s_scr[j] = s
            return jnp.maximum(top, jnp.max(s, axis=0, keepdims=True))

        top = lax.fori_loop(low, high, one, jnp.full((1, heads * own), masked_value, f32))
        o_scr[...] = jnp.zeros_like(o_scr)

        def two(j, total):
            p = jnp.exp(s_scr[j] - top)
            low_p = p.astype(bf16)
            for h in range(heads):
                rows = pl.ds(h * HD, HD)
                v = kv_out[j // 2, j % 2, pl.ds(wide + h * HD, HD)]
                o_scr[rows] += jnp.dot(v, low_p[:, h * own : (h + 1) * own], preferred_element_type=f32)
            return total + jnp.sum(p, axis=0, keepdims=True)

        total = lax.fori_loop(low, high, two, jnp.zeros((1, heads * own), f32))
        for h in range(heads):
            rows = pl.ds(h * HD, HD)
            ctx_own[block, rows] = (o_scr[rows] / total[:, h * own : (h + 1) * own]).astype(bf16)
        lse_ref[block] = top + jnp.log(total)

    def back_copy(j):
        return rcopy(ctx_own.at[c ^ j], ctx_out.at[c], vs.at[j], vr.at[j], (d, r, c ^ j))

    def attend(j):
        attend_block(c ^ j)
        if j:
            back_copy(j).start()
        else:
            ctx_out[c] = ctx_own[c]

    wide = q_src.shape[1]
    lag = 3
    ready = 2 * len(steps) + 2 * lag

    def do(**stages):
        for stage, numbers in stages.items():
            for n in numbers:
                {"f": first, "s": second, "t": third}[stage](*jobs[n])

    for i in range(ready):
        do(f=[i], s=[i - lag] if i >= lag else [], t=[i - 2 * lag] if i >= 2 * lag else [])
    prepare()
    settle(0)
    settle(1)
    project(3)
    do(f=[20], s=[17], t=[14])
    project(2)
    do(f=[21], s=[18], t=[15])
    project(1)
    do(s=[19], t=[16])
    project(0)
    set_out(kinds - 1)
    do(s=[20], t=[17])
    for start, _ in late_moves:
        start()
    for at in range(3):
        spread_out(at)
        do(t=[18 + at])
    spread_out(3)
    do(s=[21])
    unpack()
    collect()
    attend(3)
    do(f=[22, 23])
    attend(2)
    do(f=[24, 25], s=[22])
    attend(1)
    do(f=[26, 27], s=[23], t=[21])
    attend(0)
    for n in (24, 25, 26, 27):
        do(s=[n], t=[n - 2])
    do(t=[26, 27])

    for k in range(kinds):
        if k > 1:
            settle(k)
        for way, hop in steps:

            def body():
                at = at_of(way, hop)
                own = hop == 0
                to_x(k, at, own).wait_send()
                to_y(k, at, own).wait_send()
                to_p(k, at, own).wait_send()
                for which in range(2):
                    relay(k, at, which).wait_send()
                for bit in (1, 2, 3):
                    pass_p(k, at, bit).wait_send()
                if hop < 3:
                    if own:

                        @pl.when(has_up)
                        def _():
                            z_send(k, c, 0, 1).wait_send()

                        @pl.when(has_down)
                        def _():
                            z_send(k, c, 1, 1).wait_send()
                    else:
                        can = has_up if way == 0 else has_down

                        @pl.when(can)
                        def _():
                            z_send(k, at, way, hop + 1).wait_send()

            guard(way, hop, body)
    for j in (1, 2, 3):
        q(j).wait_send()
        kv(j).wait_send()
        back_copy(j).wait()
    for j in range(4):
        pair(j).wait_send()
    for _, wait in late_moves:
        wait()


VM = pl.BlockSpec(memory_space=pltpu.VMEM)


def head_fast(weights, tokens, cotangent, ints, vectors, scale, cid):
    kinds = 4
    dma = pltpu.SemaphoreType.DMA
    _, feats, cols = tokens.shape
    own = cols // 2
    width = 4 * feats
    part = feats // 2
    wide = weights[0].shape[1] // 3
    full = 4 * wide
    heads = wide // HD
    shape = jax.ShapeDtypeStruct
    piece = shape((4, wide, own), bf16)
    taken = shape((4, feats, own), bf16)
    weight = shape((4, 4, 2, part, weights[2].shape[1]), bf16)
    hidden = weights[2].shape[1]
    student_width = vectors[2].shape[1]
    return pl.pallas_call(
        functools.partial(head_kernel, scale),
        out_shape=[
            shape((4, 4, 2, part, full), bf16), weight, weight, taken, taken, shape((2,) + ints.shape, ints.dtype),
            piece, shape((4, 2, 2 * wide, own), bf16), shape((4 * wide, width), bf16), shape((8, width), f32),
            shape((4, hidden), f32), shape((width, student_width), bf16), piece,
            shape((4, 1, heads * own), f32), piece,
        ],
        in_specs=[VM, VM] + [HBM] * 5 + [VM] * len(vectors),
        out_specs=[VM, HBM, HBM] + [VM] * 12,
        scratch_shapes=[
            pltpu.VMEM((feats, full), bf16),
            pltpu.VMEM((96, 128), f32),
            pltpu.VMEM((4, 4, 2, 48, 128), f32),
            pltpu.VMEM((own, width), bf16),
            pltpu.VMEM((4, wide, own), bf16),
            pltpu.VMEM((4, 2 * wide, own), bf16),
            pltpu.VMEM((8, own, wide), bf16),
            pltpu.VMEM((wide, heads * own), bf16),
            pltpu.VMEM((8, own, heads * own), f32),
            pltpu.VMEM((wide, own), f32),
            pltpu.VMEM((8, own, 128), f32),
            dma((kinds,)),
            dma((kinds, 2, 3)), dma((kinds, 2, 3)),
            dma((kinds, 4)), dma((kinds, 4)),
            dma((kinds, 4)), dma((kinds, 4)),
            dma((kinds, 4, 2)), dma((kinds, 4, 2)),
            dma((kinds, 4, 4)), dma((kinds, 4, 4)),
            dma, dma((4,)), dma((4,)), dma((3,)),
            dma((2, 4)), dma((2, 4)), dma((4,)), dma((4,)),
            dma, dma((4,)), dma((4,)), dma((4,)), dma((4,)),
        ],
        compiler_params=pltpu.CompilerParams(
            collective_id=cid, has_side_effects=True, vmem_limit_bytes=56 * 1024 * 1024
        ),
        name="head",
    )(*weights, tokens, cotangent, ints, *vectors)


def scatter_core(grads, outs, scratch, begin, during, late=0, gap=0):
    kinds = len(grads)
    (acc, precv, xr1, yr1, xr2, yr2, zup, zdn, fin) = scratch[:9]
    (ls, ps, pr, xs1, xm1, ys1, ym1, xs2, xm2, ys2, ym2, us, um, ds, dm, fs, fm, os) = scratch[9:]
    d, r, c = place()
    cols = 4
    chunks = kinds * cols
    xn, yn, pn = (d, r ^ 1, c), (d, r ^ 2, c), (1 - d, r, c)
    up, down = (d, r, c + 1), (d, r, c - 1)
    half = acc.shape[2] // 2
    first, last = pl.ds(0, half), pl.ds(half, half)

    def split(i):
        k = i // cols
        j = i - k * cols
        at = jnp.where(j == 0, 0, jnp.where(j == 1, 3, j - 1))
        return k, at

    def at_static(i):
        return i // cols, (0, 3, 1, 2)[i % cols]

    def load(i):
        k, at = at_static(i)
        return pltpu.make_async_copy(grads[k].at[at, :, d], acc.at[i], ls.at[i])

    def pair(i):
        k, at = at_static(i)
        return rcopy(grads[k].at[at, :, 1 - d], precv.at[i], ps.at[i], pr.at[i], pn)

    def launch(i):
        pair(i).start()
        load(i).start()

    for i in range((kinds - late) * cols):
        launch(i)
    begin()

    def x1(i, j):
        return rcopy(acc.at[i, r ^ 1 ^ (2 * j), first], xr1.at[i, j], xs1.at[i, j], xm1.at[i, j], xn)

    def y1(i, j):
        return rcopy(acc.at[i, r ^ 2 ^ j, last], yr1.at[i, j], ys1.at[i, j], ym1.at[i, j], yn)

    def y2(i):
        return rcopy(acc.at[i, r ^ 2, first], yr2.at[i], ys2.at[i], ym2.at[i], yn)

    def x2(i):
        return rcopy(acc.at[i, r ^ 1, last], xr2.at[i], xs2.at[i], xm2.at[i], xn)

    def to_up(i):
        return rcopy(acc.at[i, r], zup.at[i], us.at[i], um.at[i], up)

    def to_down(i):
        return rcopy(acc.at[i, r], zdn.at[i], ds.at[i], dm.at[i], down)

    def stage1(i):
        pltpu.make_async_copy(precv.at[i], acc.at[i], ls.at[i]).wait()
        rcopy(acc.at[i], precv.at[i], ps.at[i], pr.at[i], pn).wait_recv()

        @pl.loop(0, 4)
        def _(row):
            acc[i, row] = acc[i, row] + precv[i, row]

        x1(i, 1).start()
        y1(i, 1).start()
        x1(i, 0).start()
        y1(i, 0).start()

    def stage2(i):
        x1(i, 1).wait_recv()
        acc[i, r ^ 2, first] = acc[i, r ^ 2, first] + xr1[i, 1]
        y2(i).start()
        y1(i, 1).wait_recv()
        acc[i, r ^ 1, last] = acc[i, r ^ 1, last] + yr1[i, 1]
        x2(i).start()
        x1(i, 0).wait_recv()
        acc[i, r, first] = acc[i, r, first] + xr1[i, 0]
        y1(i, 0).wait_recv()
        acc[i, r, last] = acc[i, r, last] + yr1[i, 0]

    def stage3(i):
        y2(i).wait_recv()
        acc[i, r, first] = acc[i, r, first] + yr2[i]
        x2(i).wait_recv()
        acc[i, r, last] = acc[i, r, last] + xr2[i]

    def stage4(i, hops):
        k, at = split(i)

        @pl.when((at > c) & (c == hops))
        def _():
            @pl.when(c > 0)
            def _():
                to_up(i).wait_recv()
                acc[i, r] = acc[i, r] + zup[i]

            to_up(i).start()

        @pl.when((at < c) & (cols - 1 - c == hops))
        def _():
            @pl.when(c < cols - 1)
            def _():
                to_down(i).wait_recv()
                acc[i, r] = acc[i, r] + zdn[i]

            to_down(i).start()

        @pl.when((at == c) & (jnp.maximum(c, cols - 1 - c) == hops))
        def _():
            @pl.when(c > 0)
            def _():
                to_up(i).wait_recv()
                acc[i, r] = acc[i, r] + zup[i]

            @pl.when(c < cols - 1)
            def _():
                to_down(i).wait_recv()
                acc[i, r] = acc[i, r] + zdn[i]

            fin[k, d] = acc[i, r]
            rcopy(fin.at[k, d], fin.at[k, d], fs.at[k], fm.at[k], pn).start()

    stages = [(0, stage1), (2, stage2), (4, stage3)]
    stages += [(5 + h, functools.partial(lambda h, i: stage4(i, h), h)) for h in range(cols)]
    ending = stages[-1][0]

    assert len(during) <= chunks + gap + ending
    early = (kinds - late) * cols

    @pl.loop(0, chunks + gap + ending)
    def _(step):
        for i, extra in enumerate(during):
            pl.when(step == i)(functools.partial(extra, launch))

        for lag, stage in stages:

            spot = step - lag
            there = (spot >= 0) & (spot < early) | (spot >= early + gap) & (spot < chunks + gap)

            @pl.when(there)
            def _():
                stage(jnp.where(spot < early, spot, spot - gap))

    @pl.loop(0, chunks)
    def _(i):
        k, at = split(i)
        rcopy(acc.at[i], precv.at[i], ps.at[i], pr.at[i], pn).wait_send()
        for j in range(2):
            x1(i, j).wait_send()
            y1(i, j).wait_send()
        y2(i).wait_send()
        x2(i).wait_send()

        @pl.when(at > c)
        def _():
            to_up(i).wait_send()

        @pl.when(at < c)
        def _():
            to_down(i).wait_send()

    for k in range(kinds):
        rcopy(fin.at[k, 1 - d], fin.at[k, 1 - d], fs.at[k], fm.at[k], pn).wait()
        pltpu.make_async_copy(fin.at[k], outs[k], os.at[k]).start()
    for k in range(kinds):
        pltpu.make_async_copy(fin.at[k], outs[k], os.at[k]).wait()

def scatter_scratch(kinds, n, w, dt):
    dma = pltpu.SemaphoreType.DMA
    chunks = kinds * 4
    return [
        pltpu.VMEM((chunks, 4, n, w), dt),
        pltpu.VMEM((chunks, 4, n, w), dt),
        pltpu.VMEM((chunks, 2, n // 2, w), dt),
        pltpu.VMEM((chunks, 2, n // 2, w), dt),
        pltpu.VMEM((chunks, n // 2, w), dt),
        pltpu.VMEM((chunks, n // 2, w), dt),
        pltpu.VMEM((chunks, n, w), dt),
        pltpu.VMEM((chunks, n, w), dt),
        pltpu.VMEM((kinds, 2, n, w), dt),
        dma((chunks,)), dma((chunks,)), dma((chunks,)),
        dma((chunks, 2)), dma((chunks, 2)), dma((chunks, 2)), dma((chunks, 2)),
        dma((chunks,)), dma((chunks,)), dma((chunks,)), dma((chunks,)),
        dma((chunks,)), dma((chunks,)), dma((chunks,)), dma((chunks,)),
        dma((kinds,)), dma((kinds,)), dma((kinds,)),
    ]


def give_moves(src_ref, out_ref, local, send, recv):
    d, r, c = place()
    own = src_ref.shape[2]
    home = r // 2

    def slot(i, core):
        return out_ref.at[i, :, pl.ds(pl.multiple_of(core * own, own), own)]

    def move(row):
        return rcopy(src_ref.at[row], slot(r % 2, d), send.at[row], recv.at[r % 2, d], (home, row, c))

    def stay():
        return pltpu.make_async_copy(src_ref.at[r], slot(r % 2, d), local)

    def start():
        for row in range(4):

            @pl.when(jnp.logical_not((row == r) & (home == d)))
            def _():
                move(row).start()

        @pl.when(home == d)
        def _():
            stay().start()

    def finish():
        for row in range(4):

            @pl.when(jnp.logical_not((row == r) & (home == d)))
            def _():
                move(row).wait_send()

        @pl.when(home == d)
        def _():
            stay().wait()

        for i in range(2):
            for core in range(2):

                @pl.when(jnp.logical_not((2 * d + i == r) & (core == d)))
                def _():
                    rcopy(src_ref.at[0], slot(i, core), send.at[0], recv.at[i, core], (d, r, c)).wait_recv()

    return start, finish


def plane_peers():
    d, r, c = place()
    return [(d ^ (j // 4), r ^ (j % 4), c) for j in range(1, 8)]


def line_peers():
    d, r, c = place()
    return [(d ^ (j // 4), r, c ^ (j % 4)) for j in range(1, 8)]


def sum_steps(src, total, parts, sems):
    d, r, c = place()
    peers = [(1 - d, r, c), (d, r ^ 1, c), (d, r ^ 2, c), (d, r, c ^ 1), (d, r, c ^ 2)]
    bits = [d, r % 2, r // 2, c % 2, c // 2]
    rs, rr, gs, gr = sems
    count = len(peers)
    size = [src.shape[0] >> (i + 1) for i in range(count)]
    offset = [jnp.int32(0)]
    for i in range(count):
        offset.append(offset[i] + bits[i] * size[i])

    def rows(at, amount):
        return pl.ds(pl.multiple_of(at, 8), amount)

    def down(i):
        other = offset[i] + (1 - bits[i]) * size[i]
        held = src if i == 0 else parts[i - 1]
        at = other if i == 0 else other - offset[i]
        return rcopy(held.at[rows(at, size[i])], parts[count + i], rs.at[i], rr.at[i], peers[i])

    def fold(i):
        down(i).wait_recv()
        held = src if i == 0 else parts[i - 1]
        at = offset[i + 1] if i == 0 else offset[i + 1] - offset[i]
        parts[i][...] = held[rows(at, size[i])] + parts[count + i][...]

    def back(i):
        spot = total.at[rows(offset[i + 1], size[i])]
        return rcopy(spot, spot, gs.at[i], gr.at[i], peers[i])

    def back_recv(i):
        spot = total.at[rows(offset[i] + (1 - bits[i]) * size[i], size[i])]
        rcopy(spot, spot, gs.at[i], gr.at[i], peers[i]).wait_recv()

    steps = [lambda: down(0).start()]
    for i in range(1, count):

        def step(i=i):
            fold(i - 1)
            down(i).start()

        steps.append(step)

    def middle():
        fold(count - 1)
        total[rows(offset[count], size[-1])] = parts[count - 1][...]
        back(count - 1).start()

    steps.append(middle)
    for i in range(count - 2, -1, -1):

        def step(i=i):
            back_recv(i + 1)
            back(i).start()

        steps.append(step)

    def end():
        back_recv(0)
        for i in range(count):
            down(i).wait_send()
            back(i).wait_send()

    return steps, end


highest = lax.Precision.HIGHEST


def fine(a, b, contract=((1,), (0,))):
    return lax.dot_general(a, b, (contract, ((), ())), precision=highest, preferred_element_type=f32)


def same_head(size, part):
    one = lax.broadcasted_iota(jnp.int32, (size, size), 0) // part
    two = lax.broadcasted_iota(jnp.int32, (size, size), 1) // part
    return (one == two).astype(f32)


def student_stats(docs, scale, out_ref, seg_ref, proj_ref, vec_ref, hidden, logit, stats):
    width = hidden.shape[1]
    h = jnp.dot(out_ref[...], proj_ref[...], preferred_element_type=f32) + vec_ref[0:1]
    pool = fine(h * vec_ref[1:2], same_head(width, SHD)) * scale
    hidden[...] = h
    logit[...] = pool
    stats[0:8] = jnp.zeros((8, width), f32)
    stats[8:16] = jnp.zeros((8, width), f32)
    stats[16:24] = jnp.ones((8, width), f32)
    for doc in range(docs):
        mine = seg_ref[...] == doc
        top = jnp.max(jnp.where(mine, pool, masked_value), axis=0, keepdims=True)
        weight = jnp.where(mine, jnp.exp(pool - top), 0.0)
        stats[doc : doc + 1] = jnp.sum(weight * h, axis=0, keepdims=True)
        stats[8 + doc : 9 + doc] = top
        stats[16 + doc : 17 + doc] = jnp.sum(weight, axis=0, keepdims=True)


def student_grads(docs, classes, scale, once, row, out_ref, seg_ref, label_ref, vec_ref, mid_ref, cls_ref, hidden, logit, stats, small):
    width = hidden.shape[1]
    every = [stats[i, j] for i in range(stats.shape[0]) for j in range(stats.shape[1])]
    top = every[0][8:16]
    for one in every[1:]:
        top = jnp.maximum(top, one[8:16])
    total = jnp.zeros_like(top)
    pooled = jnp.zeros_like(top)
    for one in every:
        factor = jnp.exp(one[8:16] - top)
        total = total + one[16:24] * factor
        pooled = pooled + one[0:8] * factor
    pooled = pooled / total
    middle = jnp.tanh(fine(pooled, mid_ref[...]) + vec_ref[2:3])
    logits = fine(middle, cls_ref[...]) + vec_ref[3:4]
    lane = lax.broadcasted_iota(jnp.int32, logits.shape, 1)
    doc = lax.broadcasted_iota(jnp.int32, logits.shape, 0)
    real = lane < classes
    peak = jnp.max(jnp.where(real, logits, masked_value), axis=1, keepdims=True)
    share = jnp.where(real, jnp.exp(logits - peak), 0.0)
    share = share / jnp.sum(share, axis=1, keepdims=True)
    d_logits = jnp.where(doc < docs, share - (label_ref[...] == lane).astype(f32), 0.0)
    d_middle = fine(d_logits, cls_ref[...], ((1,), (1,))) * (1.0 - middle * middle)
    d_pooled = fine(d_middle, mid_ref[...], ((1,), (1,)))
    zeros = jnp.zeros((1, width), f32)
    small[768:896] = fine(pooled, d_middle, ((0,), (0,))) * once
    small[896:912] = fine(d_logits, middle, ((0,), (0,)))[0:16] * once
    small[912:913] = jnp.sum(d_middle, axis=0, keepdims=True) * once
    small[913:914] = jnp.sum(d_logits, axis=0, keepdims=True) * once
    for at in range(4):
        small[920 + 8 * at : 928 + 8 * at] = jnp.where(row == at, logits * once, 0.0)

    heads = same_head(width, SHD)
    base = fine(d_pooled * pooled, heads)
    h, pool = hidden[...], logit[...]
    top_t, total_t = jnp.zeros_like(h), jnp.ones_like(h)
    back_t, base_t = jnp.zeros_like(h), jnp.zeros_like(h)
    for doc in range(docs):
        mine = seg_ref[...] == doc
        top_t = jnp.where(mine, top[doc : doc + 1], top_t)
        total_t = jnp.where(mine, total[doc : doc + 1], total_t)
        back_t = jnp.where(mine, d_pooled[doc : doc + 1], back_t)
        base_t = jnp.where(mine, base[doc : doc + 1], base_t)
    share = jnp.exp(pool - top_t) / total_t
    d_pool = share * (fine(back_t * h, heads) - base_t)
    d_h = share * back_t + d_pool * vec_ref[1:2] * scale
    small[914:915] = jnp.sum(d_h, axis=0, keepdims=True)
    small[915:916] = jnp.sum(d_pool * h, axis=0, keepdims=True) * scale
    for i in range(916, 920):
        small[i : i + 1] = zeros
    small[0:768] = fine(out_ref[...].astype(f32), d_h, ((0,), (0,)))


def tail_kernel(docs, classes, scale, *refs):
    kinds = 2
    grads, refs = refs[:kinds], refs[kinds:]
    (q_ref, kv_ref, lse_ref, ctx_ref, dctx_ref, ints_ref), refs = refs[:6], refs[6:]
    (out_ref, seg_ref, label_ref, proj_ref, svec_ref, mid_ref, cls_ref), refs = refs[:7], refs[7:]
    vec_refs, refs = refs[:7], refs[7:]
    (x_ref, ctx_all_ref, resid_ref, out_t_ref, w_ref), refs = refs[:5], refs[5:]
    outs, refs = refs[: kinds + 1], refs[kinds + 1 :]
    (give_out, out_out, small_out), refs = refs[:3], refs[3:]
    (total, theirs, dqkv, own_grads, dpad, weights, resid_t, give_src), refs = refs[:8], refs[8:]
    (dctx, dq, dkv, kn, vn, q3, dc3, dq_scr, dkv_scr, bias_scr, landed, kcol, qsegs, deltas), refs = refs[:14], refs[14:]
    (hidden, logit, stats, stats_all, small), refs = refs[:5], refs[5:]
    parts, refs = refs[:10], refs[10:]
    (send, recv, psend, precv), sems, (wl, gl, gs, gr), refs = refs[:4], refs[4:8], refs[8:12], refs[12:]
    (dsend, drecv, ssend, srecv, ol, osend, orecv), scratch = refs[:7], refs[7:]
    d, r, c = place()
    pn = (1 - d, r, c)
    tiles, deep, tile = kv_ref.shape
    wide = deep // 2
    heads = wide // HD
    full = dqkv.shape[1]
    own = q_ref.shape[2]
    kv_rows, q_rows = pl.ds(0, deep), pl.ds(deep, wide)
    peers = line_peers()
    greet(plane_peers() + peers[:3] + peers[4:])

    def to_heads(j):
        return rcopy(dctx_ref.at[c ^ j], dctx.at[c], dsend.at[j], drecv.at[j], (d, r, c ^ j))

    for j in (3, 2, 1):
        to_heads(j).start()
    dctx[c] = dctx_ref[c]
    load_w = pltpu.make_async_copy(w_ref, weights, wl)
    load_w.start()

    def tell(j):
        return rcopy(stats, stats_all.at[d, c], ssend.at[j - 1], srecv.at[j - 1], peers[j - 1])

    out_start, out_finish = give_moves(out_t_ref, out_out, ol, osend, orecv)
    start, finish = give_moves(give_src, give_out, gl, gs, gr)
    steps, end = sum_steps(small, small_out, parts, sems)
    pool_scale = SHD ** (-0.5)

    def begin():
        out_start()
        student_stats(docs, pool_scale, out_ref, seg_ref, proj_ref, svec_ref, hidden, logit, stats)
        for j in range(1, 8):
            tell(j).start()
        stats_all[d, c] = stats[...]
        spare = full - deep - wide
        for at in range(4):
            dqkv[at, pl.ds(deep + wide, spare)] = jnp.zeros((spare, own), bf16)
        resid_t[...] = resid_ref[...].T
        feats = x_ref.shape[1]
        blank = dpad.shape[1] - feats
        for row in range(4):
            dpad[row, pl.ds(0, blank)] = jnp.zeros((blank, own), bf16)
            dpad[row, pl.ds(blank, feats)] = resid_t[pl.ds(row * feats, feats)].astype(bf16)
        at = 952
        for ref in vec_refs:
            for i in range(ref.shape[0]):
                for j in range(ref.shape[1] // 128):
                    small[at : at + 1] = ref[i : i + 1, j * 128 : (j + 1) * 128]
                    at += 1
        for i in range(at, small.shape[0]):
            small[i : i + 1] = jnp.zeros((1, 128), f32)

    def student(_):
        for j in range(1, 8):
            tell(j).wait_recv()
        once = 1.0 / 8
        student_grads(
            docs, classes, pool_scale, once, r, out_ref, seg_ref, label_ref, svec_ref, mid_ref, cls_ref, hidden, logit,
            stats_all, small,
        )

    def segment(at):
        return ints_ref[r // 2, r % 2, pl.ds(at, 1)].astype(f32)

    def prepare(_):
        @pl.loop(0, tiles)
        def _(j):
            kn[j] = kv_ref[j, pl.ds(0, wide)].astype(f32).T.astype(bf16)
            vn[j] = kv_ref[j, pl.ds(wide, wide)].astype(f32).T.astype(bf16)

        for j in range(tiles):
            kcol[j] = jnp.broadcast_to(segment(j), (128, own)).T
        bias_scr[...] = jnp.zeros_like(bias_scr)
        dq_scr[...] = jnp.zeros_like(dq_scr)
        for block in range(4):
            block_rows(q_ref.at[pl.ds(block, 1)], heads, scale, q3.at[block])
            qsegs[block] = jnp.concatenate([segment(2 * block + d)] * heads, axis=1)
        for j in (1, 2, 3):
            to_heads(j).wait_recv()
        for block in range(4):
            block_rows(dctx.at[pl.ds(block, 1)], heads, 1.0, dc3.at[block])
            product = ctx_ref[block].astype(f32) * dctx[block].astype(f32)
            deltas[block] = jnp.concatenate(
                [jnp.sum(product[h * HD : (h + 1) * HD], axis=0, keepdims=True) for h in range(heads)], axis=1
            )

    ones = jnp.ones((8, own), bf16)
    across = (((1,), (1,)), ((), ()))

    def attend(j, _):
        if j < 3:
            settle(j + 1)
        for core in range(2):
            tile_at = 2 * (c ^ j) + core
            k_nat, v_nat = kn.at[tile_at], vn.at[tile_at]
            k_t = kv_ref.at[tile_at]
            seen = jnp.concatenate([kcol[tile_at]] * (heads * own // 128), axis=1)
            dkv_scr[...] = jnp.zeros_like(dkv_scr)

            @pl.loop(jnp.maximum(tile_at - 3 - d, 0) // 2, jnp.minimum((tile_at + 4 - d) // 2 + 1, 4))
            def _(block):
                s = jnp.dot(k_nat[...], q3[block], preferred_element_type=f32)
                p = jnp.exp(jnp.where(seen == qsegs[block], s, masked_value) - lse_ref[block])
                d_p = jnp.dot(v_nat[...], dc3[block], preferred_element_type=f32)
                d_s = (p * (d_p - deltas[block])).astype(bf16)
                p = p.astype(bf16)
                for h in range(heads):
                    rows, lanes = pl.ds(h * HD, HD), slice(h * own, (h + 1) * own)
                    low = pl.ds(wide + h * HD, HD)
                    dq_scr[block, rows] += jnp.dot(k_t[rows], d_s[:, lanes], preferred_element_type=f32)
                    dkv_scr[rows] += lax.dot_general(
                        q3[block, rows, lanes], d_s[:, lanes], across, preferred_element_type=f32
                    )
                    dkv_scr[low] += lax.dot_general(dctx[block, rows], p[:, lanes], across, preferred_element_type=f32)

            made = dkv_scr[...].astype(bf16)
            dkv[c ^ j, core] = made
            bias_scr[:, wide:] += lax.dot_general(ones, made[wide:], across, preferred_element_type=f32)
        pair(j).start()

    def settle(j):
        pair(j).wait_recv()
        if j:
            total[c ^ j] = dkv[c ^ j, d] + theirs[c ^ j]
            kv(j).start()
        else:
            landed[c, kv_rows] = dkv[c, d] + theirs[c]

    def pair(j):
        return rcopy(dkv.at[c ^ j, 1 - d], theirs.at[c ^ j], psend.at[j], precv.at[j], pn)

    def kv(j):
        return rcopy(total.at[c ^ j], landed.at[c, kv_rows], send.at[0, j], recv.at[0, j], (d, r, c ^ j))

    def q(j):
        return rcopy(dq.at[c ^ j], landed.at[c, q_rows], send.at[1, j], recv.at[1, j], (d, r, c ^ j))

    def leave(_):
        for j in (3, 2, 1, 0):
            made = (dq_scr[c ^ j] * scale).astype(bf16)
            dq[c ^ j] = made
            bias_scr[:, :wide] += lax.dot_general(ones, made, across, preferred_element_type=f32)
            if j:
                q(j).start()
        landed[c, q_rows] = dq[c]
        settle(0)
        for i in range(3):
            small[pl.ds(1012 + 3 * c + i, 1)] = bias_scr[0:1, i * 128 : (i + 1) * 128]

    def make(at):
        lead = full - dpad.shape[1]

        @pl.loop(0, 4)
        def _(row):
            one = lax.dot_general(x_ref[row], dqkv[at], across, preferred_element_type=f32)
            two = lax.dot_general(ctx_all_ref[at], dpad[row], across, preferred_element_type=f32)
            shape = own_grads.shape[2:4] + (-1,)
            own_grads[at, row, :, :, :lead] = one[:, :lead].astype(bf16).reshape(shape)
            own_grads[at, row, :, :, lead:] = (one[:, lead:] + two).astype(bf16).reshape(shape)

    def make_chunk(j, launch):
        if j == 0:
            for far in (1, 2, 3):
                q(far).wait_recv()
                kv(far).wait_recv()

            @pl.loop(0, 4)
            def _(at):
                for h in range(heads):
                    for slot, spot in enumerate((deep, 0, wide)):
                        dqkv[at, pl.ds((3 * h + slot) * HD, HD)] = landed[at, pl.ds(spot + h * HD, HD)]

        make((0, 3, 1, 2)[j])
        launch(kinds * 4 + j)

    def input_grad(_):
        load_w.wait()
        feats = x_ref.shape[1]

        @pl.loop(0, 4)
        def _(row):
            part = resid_t[pl.ds(pl.multiple_of(row * feats, 8), feats)]
            for at in range(4):
                w = weights[at, row].reshape(feats, full)
                part = part + jnp.dot(w, dqkv[at], preferred_element_type=f32)
            give_src[row] = part.astype(bf16)

        start()

    gap = 3
    hooks = [[] for _ in range(max(8 + gap + 5, 8 + len(steps)))]
    hooks[0].append(prepare)
    for i, j in enumerate((3, 2, 1, 0)):
        hooks[1 + i].append(functools.partial(attend, j))
    hooks[5].append(leave)
    hooks[6].append(student)
    for i, step in enumerate(steps):
        hooks[8 + i].append(lambda launch, step=step: step())
    for j in range(4):
        hooks[7 + gap + j].append(functools.partial(make_chunk, j))
    hooks[11 + gap].append(input_grad)

    def run(todo, launch):
        for one in todo:
            one(launch)

    during = [functools.partial(run, todo) for todo in hooks]
    scatter_core(list(grads) + [own_grads], outs, scratch, begin, during, late=1, gap=gap)
    end()
    finish()
    out_finish()
    for j in range(1, 8):
        tell(j).wait_send()
    for j in range(4):
        pair(j).wait_send()
    for j in (1, 2, 3):
        to_heads(j).wait_send()
        q(j).wait_send()
        kv(j).wait_send()


def tail_fast(docs, classes, scale, grads, attention, student, vectors, rest, out_t, w_attn, cid):
    n, w = grads[0].shape[3:]
    q, kv = attention[:2]
    dma = pltpu.SemaphoreType.DMA
    tiles, deep, own = kv.shape
    wide = deep // 2
    cols = tiles // 2
    feats = rest[0].shape[1]
    student_width = student[3].shape[1]
    tall = 1024
    parts = [pltpu.VMEM((tall >> (i + 1), 128), f32) for i in range(5)]
    home = jax.ShapeDtypeStruct((2, feats, 2 * own), bf16)
    return pl.pallas_call(
        functools.partial(tail_kernel, docs, classes, scale),
        out_shape=[jax.ShapeDtypeStruct((2, n, w), bf16)] * 3 + [home, home, jax.ShapeDtypeStruct((tall, 128), f32)],
        in_specs=[HBM] * 2 + [VM] * (len(attention) + len(student) + len(vectors) + len(rest)) + [HBM] * 2,
        out_specs=[HBM] * 5 + [VM],
        scratch_shapes=[
            pltpu.VMEM((cols, deep, own), bf16),
            pltpu.VMEM((cols, deep, own), bf16),
            pltpu.VMEM((cols, w, own), bf16),
            pltpu.VMEM((4, 4, 2, n, w), bf16),
            pltpu.VMEM((4, 256, own), bf16),
            pltpu.VMEM((4, 4, 2, n, w), bf16),
            pltpu.VMEM((4 * feats, own), f32),
            pltpu.VMEM((4, feats, own), bf16),
            pltpu.VMEM((cols, wide, own), bf16),
            pltpu.VMEM((cols, wide, own), bf16),
            pltpu.VMEM((cols, 2, deep, own), bf16),
            pltpu.VMEM((tiles, own, wide), bf16),
            pltpu.VMEM((tiles, own, wide), bf16),
            pltpu.VMEM((4, wide, wide // HD * own), bf16),
            pltpu.VMEM((4, wide, wide // HD * own), bf16),
            pltpu.VMEM((4, wide, own), f32),
            pltpu.VMEM((deep, own), f32),
            pltpu.VMEM((8, deep), f32),
            pltpu.VMEM((cols, deep + wide, own), bf16),
            pltpu.VMEM((tiles, own, 128), f32),
            pltpu.VMEM((4, 1, wide // HD * own), f32),
            pltpu.VMEM((4, 1, wide // HD * own), f32),
            pltpu.VMEM((own, student_width), f32),
            pltpu.VMEM((own, student_width), f32),
            pltpu.VMEM((24, student_width), f32),
            pltpu.VMEM((2, 4, 24, student_width), f32),
            pltpu.VMEM((tall, 128), f32),
        ]
        + parts * 2
        + [dma((2, 4)), dma((2, 4)), dma((4,)), dma((4,)), dma((5,)), dma((5,)), dma((5,)), dma((5,))]
        + [dma, dma, dma((4,)), dma((2, 2))]
        + [dma((4,)), dma((4,)), dma((7,)), dma((7,)), dma, dma((4,)), dma((2, 2))]
        + scatter_scratch(3, n, w, bf16),
        compiler_params=pltpu.CompilerParams(
            collective_id=cid, has_side_effects=True, vmem_limit_bytes=60 * 1024 * 1024
        ),
        name="tail",
    )(*grads, *attention, *student, *vectors, *rest, out_t.reshape(4, feats, own), w_attn)


def finish_kernel(docs, classes, in_ref, back_ref, attn_ref, grad_ref, small_ref, *outs):
    d, r, c = place()
    w_qkv, w_out, w_in, w_back, tokens, proj, logits, b_qkv, b_in, singles = outs[:9] + (outs[9:],)
    rows = in_ref.shape[0] * in_ref.shape[1]
    w_in[...] = in_ref[...].reshape(rows, -1).astype(f32)
    w_back[...] = back_ref[...].reshape(rows, -1).astype(f32)
    columns = w_qkv.shape[1]
    w_qkv[...] = attn_ref[:, :, :columns].reshape(rows, -1).astype(f32)
    w_out[...] = attn_ref[:, :, columns:].reshape(rows, -1).astype(f32)
    tokens[...] = grad_ref[...].astype(f32)
    feats = proj.shape[0]
    proj[...] = small_ref[pl.ds(pl.multiple_of(r * feats, 8), feats)]
    for i in range(2):
        some = small_ref[pl.ds(pl.multiple_of(920 + 8 * (2 * d + i), 8), 8)]
        logits[i] = some[:docs, :classes]
    line = [small_ref[pl.ds(1012 + 3 * c + i, 1)] for i in range(3)]
    line = jnp.concatenate(line, axis=1)
    wide = b_qkv.shape[1]
    b_qkv[0:1] = line[:, :wide]
    b_qkv[1:2] = line[:, wide:]
    for i in range(b_in.shape[1] // 128):
        b_in[:, i * 128 : (i + 1) * 128] = small_ref[pl.ds(952 + 6 * c + i, 1)]
    for i in range(6):
        line = [small_ref[976 + 6 * i + j : 977 + 6 * i + j] for j in range(6)]
        line = jnp.concatenate(line, axis=1)
        for row in range(4):

            @pl.when(r == row)
            def _():
                singles[i][...] = line[:, row * feats : (row + 1) * feats]

    s_mid, s_cls, s_mid_bias, s_cls_bias, s_bias, s_query = singles[6:]
    s_mid[...] = small_ref[768:896]
    s_cls[...] = jnp.concatenate([small_ref[896:912]] + [jnp.zeros((112, 128), f32)], axis=0).T[:, :classes]
    s_mid_bias[...] = small_ref[912:913]
    s_cls_bias[...] = small_ref[913:914, :classes]
    s_bias[...] = small_ref[914:915]
    s_query[...] = small_ref[915:916]


def finish_fast(docs, classes, w_in, w_back, w_attn, grad, small, columns):
    _, part, hidden = w_in.shape
    feats = 2 * part
    width = small.shape[1]

    def shape(*dims):
        return jax.ShapeDtypeStruct(dims, f32)

    shapes = [
        shape(feats, columns), shape(w_attn.shape[2] - columns, feats), shape(feats, hidden), shape(feats, hidden),
        shape(*grad.shape), shape(feats, width), shape(2, docs, classes), shape(2, columns // 3), shape(1, hidden),
    ]
    shapes += [shape(1, feats)] * 6
    shapes += [shape(width, width), shape(width, classes), shape(1, width), shape(1, classes)] + [shape(1, width)] * 2
    return pl.pallas_call(
        functools.partial(finish_kernel, docs, classes),
        out_shape=shapes,
        in_specs=[VM] * 5,
        out_specs=[VM] * len(shapes),
        name="finish",
    )(w_in, w_back, w_attn, grad, small)


def dot(a, b, contract=((1,), (0,))):
    return lax.dot_general(a, b, (contract, ((), ())), preferred_element_type=f32)


def block_rows(ref, heads, scale, out):
    own = ref.shape[-1]
    for h in range(heads):
        for g in range(heads):
            spot = (pl.ds(h * HD, HD), pl.ds(g * own, own))
            if h == g:
                out[spot] = ref[0, pl.ds(h * HD, HD)] * jnp.asarray(scale, out.dtype)
            else:
                out[spot] = jnp.zeros((HD, own), out.dtype)


def fast_local(
    tokens,
    segments,
    labels,
    cotangent,
    w_qkv,
    b_qkv,
    w_out,
    b_out,
    ln1_gain,
    ln1_bias,
    w_in,
    b_in,
    w_back,
    b_back,
    ln2_gain,
    ln2_bias,
    s_proj,
    s_bias,
    s_query,
    s_mid,
    s_mid_bias,
    s_cls,
    s_cls_bias,
):
    _, width_row, cols_local = tokens.shape
    parts, rows, cols, seqs, _ = sizes(tokens.shape[0])
    width = width_row * rows
    own = cols_local // parts
    width_col = b_qkv.shape[1]
    heads_dev = width_col // HD
    hidden_col = b_in.shape[0]
    docs_count = labels.shape[1]
    class_count = s_cls.shape[1]
    student_width = s_proj.shape[1]
    seq_len = segments.shape[1]
    row_index = lax.axis_index("row")
    col_index = lax.axis_index("col")
    dp_index = lax.axis_index("dp")
    score_scale = HD ** (-0.5)
    pool_scale = SHD ** (-0.5)
    query_heads = s_query.reshape(SH, SHD)
    doc_ids = jnp.arange(docs_count, dtype=jnp.int32)
    class_ids = jnp.arange(class_count, dtype=jnp.int32)

    ints = jnp.pad(labels, ((0, 0), (0, own - docs_count)))[:, None]
    ints = jnp.concatenate([segments.reshape(-1, seq_len // own, own), ints], axis=1)
    ints = jnp.pad(ints, ((0, 0), (0, 16 - ints.shape[1]), (0, 0)))
    row_vectors = [b_out, ln1_gain, ln1_bias, b_back, ln2_gain, ln2_bias]
    (
        w_attn, w_in_all, w_back_all, x_parts, c_parts, ints, queries, kv, w_out_all, row_vectors, b_in_all,
        s_proj_all, context, lse, ctx_parts,
    ) = head_fast(
        [w_qkv, w_out, w_in, w_back],
        tokens,
        cotangent,
        ints,
        [b_qkv, b_in[None], s_proj] + [v[None] for v in row_vectors],
        score_scale,
        1,
    )
    w_in_all = w_in_all.reshape(cols, width, hidden_col)
    w_back_all = w_back_all.reshape(cols, width, hidden_col)
    b_out_a, gain_one, bias_one, b_back_a, gain_two, bias_two = [row_vectors[i] for i in range(6)]
    x_t, ctx_t = x_parts.reshape(width, own), ctx_parts.reshape(width, own)
    kv = kv.reshape(cols * parts, 2 * width_col, own)
    own_ints = lax.dynamic_index_in_dim(ints.reshape(seqs, 16, own), row_index, 0, False)
    seg_own = lax.dynamic_index_in_dim(own_ints, 2 * col_index + dp_index, 0, False)
    label_seq = own_ints[seq_len // own, :docs_count]

    x = x_t.T
    attn_out = mm(ctx_t, w_out_all, ((0,), (0,))) + b_out_a
    normed_one, inv_one = normalize(x.astype(f32) + attn_out)
    hidden_one = normed_one * gain_one + bias_one
    hidden_low = hidden_one.astype(bf16)
    pre_act = jnp.einsum("td,cdn->ctn", hidden_low, w_in_all, preferred_element_type=f32)
    pre_act = pre_act + b_in_all[:, None, :]
    act = gelu_exact(pre_act).astype(bf16)
    ffn_out = jnp.einsum("ctn,cdn->td", act, w_back_all, preferred_element_type=f32) + b_back_a
    normed_two, inv_two = normalize(hidden_one + ffn_out)
    layer_out = (normed_two * gain_two + bias_two).astype(bf16)

    d_out = c_parts.reshape(width, own).T.astype(f32)
    g_ln2_gain = jnp.sum(d_out * normed_two, axis=0)
    g_ln2_bias = jnp.sum(d_out, axis=0)
    d_resid_two = normalize_back(d_out * gain_two, normed_two, inv_two)
    d_ffn = d_resid_two.astype(bf16)
    g_back_bias = jnp.sum(d_ffn.astype(f32), axis=0)
    g_back = jnp.einsum("td,ctn->cdn", d_ffn, act, preferred_element_type=f32)
    d_act = jnp.einsum("td,cdn->ctn", d_ffn, w_back_all, preferred_element_type=f32)
    _, gelu_fn = jax.vjp(gelu_exact, pre_act)
    d_pre = gelu_fn(d_act)[0].astype(bf16)
    g_in_bias = jnp.sum(d_pre.astype(f32), axis=1)
    g_in = jnp.einsum("td,ctn->cdn", hidden_low, d_pre, preferred_element_type=f32)
    d_hidden_one = d_resid_two + jnp.einsum(
        "ctn,cdn->td", d_pre, w_in_all, preferred_element_type=f32
    )
    g_ln1_gain = jnp.sum(d_hidden_one * normed_one, axis=0)
    g_ln1_bias = jnp.sum(d_hidden_one, axis=0)
    d_resid_one = normalize_back(d_hidden_one * gain_one, normed_one, inv_one)
    d_attn = d_resid_one.astype(bf16)
    g_out_bias = jnp.sum(d_attn.astype(f32), axis=0)
    d_ctx = mm(w_out_all, d_attn, ((1,), (1,))).astype(bf16)
    blocked = (cols, rows, parts, width_row // parts, -1)
    lane_pad = ((0, 0), (0, 128 - class_count))
    student_vectors = jnp.stack([s_bias, s_query, s_mid_bias, jnp.pad(s_cls_bias, (0, 128 - class_count))])
    student_vectors = jnp.pad(student_vectors, ((0, 4), (0, 0)))
    g_in, g_back, g_attn, grad_tokens, out, small = tail_fast(
        docs_count,
        class_count,
        score_scale,
        [g_in.astype(bf16).reshape(blocked), g_back.astype(bf16).reshape(blocked)],
        [queries, kv, lse, context, d_ctx.reshape(cols, width_col, own), ints],
        [
            layer_out,
            seg_own[:, None],
            jnp.pad(label_seq, (0, 8 - docs_count))[:, None],
            s_proj_all,
            student_vectors,
            s_mid,
            jnp.pad(s_cls, lane_pad),
        ],
        [g_in_bias]
        + [v[None] for v in (g_out_bias, g_ln1_gain, g_ln1_bias, g_back_bias, g_ln2_gain, g_ln2_bias)],
        [x_parts, ctx_parts, d_resid_one],
        layer_out.T,
        w_attn,
        4,
    )
    (
        g_qkv, g_out, g_in, g_back, grad_tokens, g_sproj, logits, g_qkv_bias, g_in_bias, g_out_bias, g_ln1_gain,
        g_ln1_bias, g_back_bias, g_ln2_gain, g_ln2_bias, g_mid, g_cls, g_mid_bias, g_cls_bias, g_sbias, g_query,
    ) = finish_fast(docs_count, class_count, g_in, g_back, g_attn, grad_tokens, small, 3 * width_col)
    return (
        out,
        logits,
        grad_tokens,
        g_qkv,
        g_qkv_bias,
        g_out,
        g_out_bias[0],
        g_ln1_gain[0],
        g_ln1_bias[0],
        g_in,
        g_in_bias[0],
        g_back,
        g_back_bias[0],
        g_ln2_gain[0],
        g_ln2_bias[0],
        g_sproj,
        g_sbias[0],
        g_query[0],
        g_mid,
        g_mid_bias[0],
        g_cls,
        g_cls_bias[0],
    )


def solution(mesh):
    row, col = P("row"), P("col")
    grid, whole = P("row", "col"), P("dp", "row", "col")
    placed = (
        (whole, P("dp", None), P("dp", None), whole, grid, P(None, "col"), P("col", "row"))
        + (row, row, row, grid, col, grid, row, row, row, P("row", None))
        + (P(),) * 6
    )
    results = (
        (whole, P("dp", None, None), whole, grid, P(None, "col"), P("col", "row"))
        + (row, row, row, grid, col, grid, row, row, row, P("row", None))
        + (P(),) * 6
    )
    quick = dict(mesh.shape) == {"dp": 2, "row": 4, "col": 4}
    local = fast_local if quick else general_local
    return jax.shard_map(local, mesh=mesh, in_specs=placed, out_specs=results, check_vma=False)
```

```python
import functools
import math
import jax
import jax.numpy as jnp
from jax import lax
from jax.experimental import pallas as pl
from jax.experimental.pallas import tpu as pltpu
from jax.sharding import PartitionSpec as P

HD = 64
SH = 2
SHD = 64

norm_eps = 1e-06
masked_value = -1e30
highest = lax.Precision.HIGHEST
f32 = jnp.float32
bf16 = jnp.bfloat16
WORLD = ("col", "row", "dp")


def sizes(seqs_local):
    parts = lax.axis_size("dp")
    rows = lax.axis_size("row")
    seqs = seqs_local * parts
    return parts, rows, lax.axis_size("col"), seqs, rows // seqs


def row_groups(rows, sub):
    return [list(range(at, at + sub)) for at in range(0, rows, sub)]


def take_in(values):
    parts, rows, _, seqs, sub = sizes(values.shape[0])
    held = lax.all_to_all(values, "dp", 2, 0, tiled=True)
    feats, half = held.shape[1:]
    held = held.reshape(seqs, feats, sub, half // sub).transpose(0, 2, 1, 3)
    held = held.reshape(rows, feats, half // sub)
    held = lax.all_to_all(held, "row", 0, 0, tiled=True)
    return held.reshape(rows * feats, half // sub)


def give_back(values, seqs_local):
    parts, rows, _, seqs, sub = sizes(seqs_local)
    width, own = values.shape
    feats = width // rows
    held = lax.all_to_all(values.reshape(rows, feats, own), "row", 0, 0, tiled=True)
    held = held.reshape(seqs, sub, feats, own).transpose(0, 2, 1, 3).reshape(seqs, feats, sub * own)
    return lax.all_to_all(held, "dp", 0, 2, tiled=True)


def gather_world(shard):
    cols, rows = lax.axis_size("col"), lax.axis_size("row")
    out = lax.all_gather(shard, WORLD, axis=0, tiled=True)
    return out.reshape(cols, rows, -1, shard.shape[1])


def own_half(block):
    parts = lax.axis_size("dp")
    amount = block.shape[0] // parts
    return lax.dynamic_slice_in_dim(block, lax.axis_index("dp") * amount, amount)


def scatter_world(full):
    flat = full.reshape(-1, full.shape[-1])
    mine = lax.psum_scatter(flat, WORLD, scatter_dimension=0, tiled=True)
    return lax.all_gather(mine, "dp", axis=0, tiled=True)


def swap_cols(values):
    return lax.all_to_all(values, "col", 0, 0, tiled=True)


def gather_sequence(values, sub):
    cols, own, width = values.shape
    held = values[:, None]
    if sub > 1:
        groups = row_groups(lax.axis_size("row"), sub)
        held = lax.all_gather(held, "row", axis=1, tiled=True, axis_index_groups=groups)
    held = lax.all_gather(held[:, None], "dp", axis=1, tiled=True)
    return held.reshape(-1, width)


def scatter_sequence(values, cols, sub):
    parts = lax.axis_size("dp")
    width = values.shape[-1]
    held = values.reshape(cols, parts, sub, -1, width)
    held = lax.psum_scatter(held, "dp", scatter_dimension=1, tiled=True)[:, 0]
    if sub > 1:
        groups = row_groups(lax.axis_size("row"), sub)
        held = lax.psum_scatter(
            held, "row", scatter_dimension=1, tiled=True, axis_index_groups=groups
        )
    return held[:, 0]


def normalize(values):
    mean_v = jnp.mean(values, axis=-1, keepdims=True)
    center = values - mean_v
    inv_std = lax.rsqrt(jnp.mean(center * center, axis=-1, keepdims=True) + norm_eps)
    return center * inv_std, inv_std


def normalize_back(grad_hat, normed, inv_std):
    return inv_std * (
        grad_hat
        - jnp.mean(grad_hat, axis=-1, keepdims=True)
        - normed * jnp.mean(grad_hat * normed, axis=-1, keepdims=True)
    )


def gelu_exact(values):
    return jax.nn.gelu(values, approximate=False)


def mm(a, b, contract):
    return lax.dot_general(a, b, (contract, ((), ())), preferred_element_type=f32)


def combine_pool(part_one, part_two):
    top_a, total_a, sum_a = part_one
    top_b, total_b, sum_b = part_two
    row_top = jnp.maximum(top_a, top_b)
    factor_a = jnp.exp(top_a - row_top)
    factor_b = jnp.exp(top_b - row_top)
    return (
        row_top,
        total_a * factor_a + total_b * factor_b,
        sum_a * factor_a[:, :, None] + sum_b * factor_b[:, :, None],
    )


def attend(q, k, v, q_seg, k_seg, scale):
    scores = jnp.einsum("qhd,khd->hqk", q, k, preferred_element_type=f32) * scale
    scores = jnp.where((q_seg[:, None] == k_seg[None, :])[None], scores, masked_value)
    top = jnp.max(scores, axis=-1, keepdims=True)
    exp_scores = jnp.exp(scores - top)
    total = jnp.sum(exp_scores, axis=-1, keepdims=True)
    probs = exp_scores / total
    context = jnp.einsum("hqk,khd->qhd", probs.astype(bf16), v, preferred_element_type=f32)
    return context.astype(bf16), probs


def attend_back(q, k, v, probs, d_ctx, scale):
    d_probs = jnp.einsum("qhd,khd->hqk", d_ctx, v, preferred_element_type=f32)
    delta = jnp.sum(probs * d_probs, axis=-1, keepdims=True)
    d_scores = (probs * (d_probs - delta)).astype(bf16)
    d_q = jnp.einsum("hqk,khd->qhd", d_scores, k, preferred_element_type=f32) * scale
    d_k = jnp.einsum("hqk,qhd->khd", d_scores, q, preferred_element_type=f32) * scale
    d_v = jnp.einsum("hqk,qhd->khd", probs.astype(bf16), d_ctx, preferred_element_type=f32)
    return d_q, d_k, d_v


def general_local(
    tokens,
    segments,
    labels,
    cotangent,
    w_qkv,
    b_qkv,
    w_out,
    b_out,
    ln1_gain,
    ln1_bias,
    w_in,
    b_in,
    w_back,
    b_back,
    ln2_gain,
    ln2_bias,
    s_proj,
    s_bias,
    s_query,
    s_mid,
    s_mid_bias,
    s_cls,
    s_cls_bias,
):
    seqs_local, width_row, cols_local = tokens.shape
    parts, rows, cols, seqs, sub = sizes(seqs_local)
    width = width_row * rows
    own = cols_local // (parts * sub)
    width_col = b_qkv.shape[1]
    heads_dev = width_col // HD
    hidden_col = b_in.shape[0]
    docs_count = labels.shape[1]
    class_count = s_cls.shape[1]
    student_width = s_proj.shape[1]
    row_index = lax.axis_index("row")
    col_index = lax.axis_index("col")
    dp_index = lax.axis_index("dp")
    seq_index = row_index // sub
    sub_index = row_index % sub
    score_scale = HD ** (-0.5)
    pool_scale = SHD ** (-0.5)
    query_heads = s_query.reshape(SH, SHD)
    doc_ids = jnp.arange(docs_count, dtype=jnp.int32)
    class_ids = jnp.arange(class_count, dtype=jnp.int32)

    w_qkv_all = gather_world(own_half(w_qkv)).reshape(cols, width, 3 * width_col)
    x_t = take_in(tokens)
    rest = jnp.concatenate([own_half(w_in), own_half(w_back), own_half(w_out).reshape(-1, width_col)], axis=1)
    rest_all = gather_world(rest)
    w_in_all = rest_all[..., :hidden_col].reshape(cols, width, hidden_col)
    w_back_all = rest_all[..., hidden_col : 2 * hidden_col].reshape(cols, width, hidden_col)
    w_out_all = rest_all[..., 2 * hidden_col :].reshape(cols, rows, width_col, width_row)
    w_out_all = w_out_all.transpose(0, 2, 1, 3).reshape(width, width)
    row_vectors = lax.all_gather(
        jnp.stack([b_out, ln1_gain, ln1_bias, b_back, ln2_gain, ln2_bias]), "row", axis=1, tiled=True
    )
    b_out_a, gain_one, bias_one, b_back_a, gain_two, bias_two = [row_vectors[i] for i in range(6)]
    b_qkv_all = lax.all_gather(b_qkv, "col")
    b_in_all = lax.all_gather(b_in, "col")
    s_proj_all = lax.all_gather(s_proj, "row", axis=0, tiled=True)
    whole_ints = lax.all_gather(jnp.concatenate([segments, labels], axis=1), "dp", axis=0, tiled=True)
    ints = lax.dynamic_index_in_dim(whole_ints, seq_index, 0, False)
    seq_len = segments.shape[1]
    seg_all, label_seq = ints[:seq_len], ints[seq_len:]
    seg_blocks = seg_all.reshape(cols, parts, sub, own)
    seg_q = lax.dynamic_index_in_dim(seg_blocks, dp_index, 1, False)
    seg_q = lax.dynamic_index_in_dim(seg_q, sub_index, 1, False)
    seg_own = lax.dynamic_index_in_dim(seg_q, col_index, 0, False)
    seg_q = seg_q.reshape(-1)

    x = x_t.T
    offsets = jnp.stack([b_qkv_all[:, 0], jnp.zeros_like(b_qkv_all[:, 0]), b_qkv_all[:, 1]], axis=1)
    offsets = offsets.reshape(cols, 3, heads_dev, HD).transpose(0, 2, 1, 3).reshape(cols, 1, -1)
    qkv = jnp.einsum("td,cdn->ctn", x, w_qkv_all, preferred_element_type=f32) + offsets
    qkv = swap_cols(qkv.astype(bf16)).reshape(cols, own, heads_dev, 3, HD)
    queries = qkv[:, :, :, 0].reshape(cols * own, heads_dev, HD)
    kv = gather_sequence(qkv[:, :, :, 1:].reshape(cols, own, -1), sub)
    kv = kv.reshape(seq_len, heads_dev, 2, HD)
    key_rows, value_rows = kv[:, :, 0], kv[:, :, 1]
    context, probs = attend(queries, key_rows, value_rows, seg_q, seg_all, score_scale)
    ctx = swap_cols(context.reshape(cols, own, width_col))
    ctx = ctx.transpose(1, 0, 2).reshape(own, width)

    attn_out = mm(ctx, w_out_all, ((1,), (0,))) + b_out_a
    normed_one, inv_one = normalize(x.astype(f32) + attn_out)
    hidden_one = normed_one * gain_one + bias_one
    hidden_low = hidden_one.astype(bf16)
    pre_act = jnp.einsum("td,cdn->ctn", hidden_low, w_in_all, preferred_element_type=f32)
    pre_act = pre_act + b_in_all[:, None, :]
    act = gelu_exact(pre_act).astype(bf16)
    ffn_out = jnp.einsum("ctn,cdn->td", act, w_back_all, preferred_element_type=f32) + b_back_a
    normed_two, inv_two = normalize(hidden_one + ffn_out)
    layer_out = (normed_two * gain_two + bias_two).astype(bf16)
    out = give_back(layer_out.T, seqs_local)

    student_h = mm(layer_out, s_proj_all, ((1,), (0,))) + s_bias
    head_parts = student_h.reshape(own, SH, SHD)
    pool_logit = jnp.sum(head_parts * query_heads, axis=-1) * pool_scale
    member = (seg_own[:, None] == doc_ids[None, :])[:, :, None]
    masked = jnp.where(member, pool_logit[:, None, :], masked_value)
    local_top = jnp.max(masked, axis=0)
    local_exp = jnp.where(member, jnp.exp(masked - local_top[None]), 0.0)
    local_total = jnp.sum(local_exp, axis=0)
    local_sum = jnp.einsum("tdh,thk->dhk", local_exp, head_parts, precision=highest)
    stats = jnp.concatenate([local_top[..., None], local_total[..., None], local_sum], axis=-1)
    stats = lax.all_gather(stats, ("dp", "col"))
    if sub > 1:
        stats = lax.all_gather(stats, "row", axis=0, tiled=True, axis_index_groups=row_groups(rows, sub))
    tops, totals, sums = stats[..., 0], stats[..., 1], stats[..., 2:]
    doc_top = jnp.max(tops, axis=0)
    factors = jnp.exp(tops - doc_top[None])
    doc_total = jnp.sum(totals * factors, axis=0)
    pooled_heads = jnp.sum(sums * factors[..., None], axis=0) / doc_total[:, :, None]
    pooled = pooled_heads.reshape(docs_count, student_width)
    middle = jnp.tanh(jnp.dot(pooled, s_mid, precision=highest) + s_mid_bias)
    logit_rows = jnp.dot(middle, s_cls, precision=highest) + s_cls_bias
    logits = lax.all_gather(logit_rows, "row")[::sub]
    logits = lax.dynamic_slice_in_dim(logits, dp_index * seqs_local, seqs_local)
    logit_top = jnp.max(logit_rows, axis=-1, keepdims=True)
    logit_exp = jnp.exp(logit_rows - logit_top)
    one_hot = (label_seq[:, None] == class_ids[None, :]).astype(f32)
    d_logits = logit_exp / jnp.sum(logit_exp, axis=-1, keepdims=True) - one_hot
    g_cls = jnp.dot(middle.T, d_logits, precision=highest)
    g_cls_bias = jnp.sum(d_logits, axis=0)
    d_middle = jnp.dot(d_logits, s_cls.T, precision=highest) * (1.0 - middle * middle)
    g_mid = jnp.dot(pooled.T, d_middle, precision=highest)
    g_mid_bias = jnp.sum(d_middle, axis=0)
    d_pooled = jnp.dot(d_middle, s_mid.T, precision=highest).reshape(docs_count, SH, SHD)
    shares = jnp.where(member, jnp.exp(masked - doc_top[None]), 0.0) / doc_total[None]
    d_share = jnp.einsum("dhk,thk->tdh", d_pooled, head_parts, precision=highest)
    base_term = jnp.sum(d_pooled * pooled_heads, axis=-1)
    d_pool_logit = jnp.sum(shares * (d_share - base_term[None]), axis=1)
    d_heads = jnp.einsum("tdh,dhk->thk", shares, d_pooled, precision=highest)
    d_heads = d_heads + d_pool_logit[:, :, None] * query_heads[None] * pool_scale
    g_query = (jnp.sum(d_pool_logit[:, :, None] * head_parts, axis=0) * pool_scale).reshape(-1)
    d_student = d_heads.reshape(own, student_width)
    g_sbias = jnp.sum(d_student, axis=0)
    g_sproj = jnp.dot(layer_out.astype(f32).T, d_student, precision=highest)

    d_out = take_in(cotangent).T.astype(f32)
    g_ln2_gain = jnp.sum(d_out * normed_two, axis=0)
    g_ln2_bias = jnp.sum(d_out, axis=0)
    d_resid_two = normalize_back(d_out * gain_two, normed_two, inv_two)
    d_ffn = d_resid_two.astype(bf16)
    g_back_bias = jnp.sum(d_ffn.astype(f32), axis=0)
    g_back = jnp.einsum("td,ctn->cdn", d_ffn, act, preferred_element_type=f32)
    d_act = jnp.einsum("td,cdn->ctn", d_ffn, w_back_all, preferred_element_type=f32)
    _, gelu_fn = jax.vjp(gelu_exact, pre_act)
    d_pre = gelu_fn(d_act)[0].astype(bf16)
    g_in_bias = jnp.sum(d_pre.astype(f32), axis=1)
    g_in = jnp.einsum("td,ctn->cdn", hidden_low, d_pre, preferred_element_type=f32)
    d_hidden_one = d_resid_two + jnp.einsum(
        "ctn,cdn->td", d_pre, w_in_all, preferred_element_type=f32
    )
    g_ln1_gain = jnp.sum(d_hidden_one * normed_one, axis=0)
    g_ln1_bias = jnp.sum(d_hidden_one, axis=0)
    d_resid_one = normalize_back(d_hidden_one * gain_one, normed_one, inv_one)
    d_attn = d_resid_one.astype(bf16)
    g_out_bias = jnp.sum(d_attn.astype(f32), axis=0)
    g_out = mm(ctx, d_attn, ((0,), (0,)))
    d_ctx = mm(d_attn, w_out_all, ((1,), (1,))).astype(bf16)
    d_ctx = swap_cols(d_ctx.reshape(own, cols, width_col).transpose(1, 0, 2))
    d_ctx = d_ctx.reshape(cols * own, heads_dev, HD)
    d_q, d_k, d_v = attend_back(queries, key_rows, value_rows, probs, d_ctx, score_scale)
    d_kv = jnp.stack([d_k, d_v], axis=2).astype(bf16).reshape(seq_len, -1)
    d_kv = scatter_sequence(d_kv, cols, sub).reshape(cols, own, heads_dev, 2, HD)
    d_q = d_q.astype(bf16).reshape(cols, own, heads_dev, 1, HD)
    d_qkv = jnp.concatenate([d_q, d_kv], axis=3).reshape(cols, own, 3 * width_col)
    d_qkv = swap_cols(d_qkv)
    g_qkv_bias = jnp.sum(d_qkv.astype(f32), axis=1).reshape(cols, heads_dev, 3, HD)
    g_qkv = jnp.einsum("td,ctn->cdn", x, d_qkv, preferred_element_type=f32)
    d_tokens = d_resid_one + jnp.einsum("ctn,cdn->td", d_qkv, w_qkv_all, preferred_element_type=f32)
    grad_tokens = give_back(d_tokens.astype(bf16).T, seqs_local).astype(f32)

    g_out = g_out.reshape(cols, width_col, rows, width_row).transpose(0, 2, 1, 3)
    g_out = g_out.reshape(cols, rows, width_row, width_col)
    model = jnp.concatenate(
        [
            g_in.reshape(cols, rows, width_row, hidden_col).astype(bf16),
            g_back.reshape(cols, rows, width_row, hidden_col).astype(bf16),
            g_out.astype(bf16),
        ],
        axis=-1,
    )
    model = scatter_world(model).astype(f32)
    g_qkv = scatter_world(g_qkv.reshape(cols, rows, width_row, 3 * width_col).astype(bf16)).astype(f32)
    once = 1.0 / (parts * cols * sub)
    small = (
        g_qkv_bias[:, :, 0].reshape(cols, width_col),
        g_qkv_bias[:, :, 2].reshape(cols, width_col),
        g_in_bias,
        g_out_bias,
        g_ln1_gain,
        g_ln1_bias,
        g_back_bias,
        g_ln2_gain,
        g_ln2_bias,
        g_sproj,
        g_sbias,
        g_query,
        g_mid * once,
        g_mid_bias * once,
        g_cls * once,
        g_cls_bias * once,
    )
    small = lax.psum(small, WORLD)

    def at_col(part):
        return lax.dynamic_index_in_dim(part, col_index, 0, False)

    def at_row(part):
        return lax.dynamic_slice_in_dim(part, row_index * width_row, width_row)

    return (
        out,
        logits,
        grad_tokens,
        g_qkv,
        jnp.stack([at_col(small[0]), at_col(small[1])]),
        model[:, 2 * hidden_col :].reshape(width_col, width_row),
        at_row(small[3]),
        at_row(small[4]),
        at_row(small[5]),
        model[:, :hidden_col],
        at_col(small[2]),
        model[:, hidden_col : 2 * hidden_col],
        at_row(small[6]),
        at_row(small[7]),
        at_row(small[8]),
        at_row(small[9]),
        small[10],
        small[11],
        small[12],
        small[13],
        small[14],
        small[15],
    )


MESH = pl.DeviceIdType.MESH
HBM = pl.BlockSpec(memory_space=pl.ANY)


def place():
    return lax.axis_index("dp"), lax.axis_index("row"), lax.axis_index("col")


def greet(peers, guarded=()):
    barrier = pltpu.get_barrier_semaphore()
    for peer in peers:
        pl.semaphore_signal(barrier, inc=1, device_id=peer, device_id_type=MESH)
    for there, peer in guarded:

        @pl.when(there)
        def _():
            pl.semaphore_signal(barrier, inc=1, device_id=peer, device_id_type=MESH)

    amount = len(peers)
    for there, _ in guarded:
        amount = amount + there.astype(jnp.int32)
    pl.semaphore_wait(barrier, amount)


def rcopy(src, dst, send, recv, peer):
    return pltpu.make_async_remote_copy(
        src_ref=src, dst_ref=dst, send_sem=send, recv_sem=recv, device_id=peer, device_id_type=MESH
    )


def take_copies(src, out, local, send, recv):
    d, r, c = place()
    own = out.shape[2]
    moves = []
    for i in range(2):
        for far in range(2):
            row, core = 2 * d + i, d ^ far
            piece = src.at[i, :, pl.ds(pl.multiple_of(core * own, own), own)]
            here = (row == r) if far == 0 else None

            def start(piece=piece, row=row, core=core, slot=2 * i + far, here=here):
                def away():
                    rcopy(piece, out.at[r], send.at[slot], recv.at[r], (core, row, c)).start()

                if here is None:
                    away()
                else:
                    pl.when(jnp.logical_not(here))(away)

                    @pl.when(here)
                    def _():
                        pltpu.make_async_copy(piece, out.at[r], local).start()

            def wait(piece=piece, row=row, core=core, slot=2 * i + far, here=here):
                def away():
                    rcopy(piece, out.at[r], send.at[slot], recv.at[r], (core, row, c)).wait_send()

                if here is None:
                    away()
                else:
                    pl.when(jnp.logical_not(here))(away)

                    @pl.when(here)
                    def _():
                        pltpu.make_async_copy(piece, out.at[r], local).wait()

            moves.append((start, wait))
    for row in range(4):

        def arrive(row=row):
            @pl.when(jnp.logical_not((row == r) & (r // 2 == d)))
            def _():
                piece = src.at[0, :, pl.ds(0, own)]
                rcopy(piece, out.at[row], send.at[0], recv.at[row], (d, r, c)).wait_recv()

        moves.append((lambda: None, arrive))
    return moves


VM = pl.BlockSpec(memory_space=pltpu.VMEM)


def head_kernel(scale, *refs):
    (w_qkv_ref, w_out_ref, w_in_ref, w_back_ref, tok, cot, ints), refs = refs[:7], refs[7:]
    (b_qkv_ref, b_in_ref, proj_ref), row_vecs, refs = refs[:3], refs[3:9], refs[9:]
    (a_out, b_out, c_out, tok_out, cot_out, ints_out, q_out, kv_out), refs = refs[:8], refs[8:]
    (wo_out, vec_all, b_in_all, proj_all, ctx_own, lse_ref, ctx_out), refs = refs[:7], refs[7:]
    (shard_a, shard_v, vec_out, x_nat, q_src, kv_src, kn, q3, s_scr, o_scr, kcol), refs = refs[:11], refs[11:]
    own_sem, zs, zr, xs, xr, ys, yr, cs, cr, ps, pr, tl, ts, tr, il, hs, hr, hps, hpr, xl, xs2, xr2, vs, vr = refs
    d, r, c = place()
    kinds = 4
    part = w_in_ref.shape[0] // 2
    mine = pl.ds(pl.multiple_of(d * part, 16), part)
    feats = tok_out.shape[1]
    shards = [shard_a.at[mine], shard_v.at[pl.ds(pl.multiple_of(d * 48, 8), 48)], w_in_ref.at[mine], w_back_ref.at[mine]]
    outs = [a_out, vec_out, b_out, c_out]
    cols = 4
    xn, yn, pn = (d, r ^ 1, c), (d, r ^ 2, c), (1 - d, r, c)
    up, down = (d, r, c + 1), (d, r, c - 1)
    has_up, has_down = c < cols - 1, c > 0
    columns = w_qkv_ref.shape[1]
    shard_a[:, :columns] = w_qkv_ref[...]
    shard_a[:, columns:] = w_out_ref[...]
    heads = columns // (3 * HD)
    pieces = []
    for h in range(heads):
        spot = slice(h * HD, (h + 1) * HD)
        pieces += [b_qkv_ref[0:1, spot], jnp.zeros((1, HD), f32), b_qkv_ref[1:2, spot]]
    bias_lanes = -(-columns // 128) * 128
    pieces.append(jnp.zeros((1, bias_lanes - columns), f32))
    line = jnp.concatenate(pieces, axis=1)
    at = 0
    for i in range(bias_lanes // 128):
        shard_v[at : at + 1] = line[:, i * 128 : (i + 1) * 128]
        at += 1
    for ref in row_vecs:
        line = jnp.concatenate([ref[...], jnp.zeros((1, 256 - feats), f32)], axis=1)
        for i in range(2):
            shard_v[at : at + 1] = line[:, i * 128 : (i + 1) * 128]
            at += 1
    for i in range(b_in_ref.shape[1] // 128):
        shard_v[at : at + 1] = b_in_ref[:, i * 128 : (i + 1) * 128]
        at += 1
    proj_at, proj_rows = 48, feats // 4
    for i in range(at, proj_at):
        shard_v[i : i + 1] = jnp.zeros((1, 128), f32)
    shard_v[proj_at:] = proj_ref[pl.ds(pl.multiple_of(c * proj_rows, 16), proj_rows)].astype(f32)

    greet(plane_peers() + [(d, r, c ^ j) for j in (1, 2, 3)])
    moves = take_copies(tok, tok_out, tl, ts, tr)
    for start, _ in moves:
        start()
    late_moves = take_copies(cot, cot_out, xl, xs2, xr2)
    pltpu.make_async_copy(ints, ints_out.at[d], il.at[0]).start()
    rcopy(ints, ints_out.at[d], il.at[1], il.at[2], pn).start()
    halves = [part // 2, 24, part // 2, part // 2]

    def z_send(k, at, way, hop):
        src = shards[k] if hop == 1 else outs[k].at[at, r, d]
        return rcopy(
            src, outs[k].at[at, r, d], zs.at[k, way, hop - 1], zr.at[k, way, hop - 1], up if way == 0 else down
        )

    def src_of(k, at, own):
        return shards[k] if own else outs[k].at[at, r, d]

    def to_x(k, at, own):
        return rcopy(src_of(k, at, own), outs[k].at[at, r, d], xs.at[k, at], xr.at[k, at], xn)

    def to_y(k, at, own):
        return rcopy(src_of(k, at, own), outs[k].at[at, r, d], ys.at[k, at], yr.at[k, at], yn)

    def to_p(k, at, own):
        return rcopy(src_of(k, at, own), outs[k].at[at, r, d], ps.at[k, at, 0], pr.at[k, at, 0], pn)

    def relay(k, at, which):
        row = r ^ 1 if which == 0 else r ^ 2
        ref = outs[k].at[at, row, d, pl.ds(which * halves[k], halves[k])]
        return rcopy(ref, ref, cs.at[k, at, which], cr.at[k, at, which], yn if which == 0 else xn)

    def pass_p(k, at, bit):
        ref = outs[k].at[at, r ^ bit, d]
        return rcopy(ref, ref, ps.at[k, at, bit], pr.at[k, at, bit], pn)

    def got_x(k, at):
        ref = outs[k].at[at, r ^ 1, d]
        rcopy(ref, ref, xs.at[k, at], xr.at[k, at], xn).wait_recv()

    def got_y(k, at):
        ref = outs[k].at[at, r ^ 2, d]
        rcopy(ref, ref, ys.at[k, at], yr.at[k, at], yn).wait_recv()

    def got_corner(k, at):
        for which in range(2):
            ref = outs[k].at[at, r ^ 3, d, pl.ds(which * halves[k], halves[k])]
            rcopy(ref, ref, cs.at[k, at, which], cr.at[k, at, which], xn).wait_recv()

    def got_p(k, at, bit):
        ref = outs[k].at[at, r ^ bit, 1 - d]
        rcopy(ref, ref, ps.at[k, at, bit], pr.at[k, at, bit], pn).wait_recv()

    def set_out(k):
        @pl.when(has_up)
        def _():
            z_send(k, c, 0, 1).start()

        @pl.when(has_down)
        def _():
            z_send(k, c, 1, 1).start()

    for k in range(kinds):
        pltpu.make_async_copy(shards[k], outs[k].at[c, r, d], own_sem.at[k]).start()
        if k < kinds - 1:
            set_out(k)

    def spread(k, at, own):
        to_x(k, at, own).start()
        to_y(k, at, own).start()
        to_p(k, at, own).start()

    def onward(k, at):
        got_x(k, at)
        relay(k, at, 0).start()
        pass_p(k, at, 1).start()
        got_y(k, at)
        relay(k, at, 1).start()
        pass_p(k, at, 2).start()

    steps = [(0, 0)] + [(way, hop) for hop in (1, 2, 3) for way in (0, 1)]
    jobs = [(k, way, hop) for k in range(kinds) for way, hop in steps]

    def at_of(way, hop):
        return c - hop if way == 0 else c + hop

    def valid(way, hop):
        return c >= hop if way == 0 else c + hop < cols

    def guard(way, hop, body):
        if hop == 0:
            body()
        else:
            pl.when(valid(way, hop))(body)

    def first(k, way, hop):
        def body():
            at = at_of(way, hop)
            if hop:
                z_send(k, at, way, hop).wait_recv()
                if hop < 3:
                    can = has_up if way == 0 else has_down

                    @pl.when(can)
                    def _():
                        z_send(k, at, way, hop + 1).start()

            spread(k, at, hop == 0)

        guard(way, hop, body)

    def second(k, way, hop):
        guard(way, hop, lambda: onward(k, at_of(way, hop)))

    def third(k, way, hop):
        def body():
            at = at_of(way, hop)
            got_corner(k, at)
            pass_p(k, at, 3).start()

        guard(way, hop, body)

    def settle(k):
        pltpu.make_async_copy(shards[k], outs[k].at[c, r, d], own_sem.at[k]).wait()
        for way, hop in steps:

            def body():
                for bit in range(4):
                    got_p(k, at_of(way, hop), bit)

            guard(way, hop, body)

    def kv(j):
        return rcopy(kv_src.at[c ^ j], kv_out.at[c, d], hs.at[0, j], hr.at[0, j], (d, r, c ^ j))

    def q(j):
        return rcopy(q_src.at[c ^ j], q_out.at[c], hs.at[1, j], hr.at[1, j], (d, r, c ^ j))

    def pair(j):
        src = kv_src.at[c] if j == 0 else kv_out.at[c ^ j, d]
        return rcopy(src, kv_out.at[c ^ j, d], hps.at[j], hpr.at[j], pn)

    lanes = bias_lanes

    def prepare():
        for _, wait in moves:
            wait()
        x_nat[...] = tok_out[...].reshape(4 * feats, -1).astype(f32).T.astype(bf16)

    def project(j):
        to = c ^ j
        weights = a_out[to, :, :, :, :lanes].reshape(-1, lanes)
        bias = vec_out[to, r, 0, pl.ds(0, 8)]
        bias = jnp.concatenate([bias[i : i + 1] for i in range(lanes // 128)], axis=1)
        made = jnp.dot(x_nat[...], weights, preferred_element_type=f32) + bias
        made = made.T.astype(bf16)
        for h in range(heads):
            rows = pl.ds(h * HD, HD)
            q_src[to, rows] = made[3 * h * HD : (3 * h + 1) * HD]
            kv_src[to, rows] = made[(3 * h + 1) * HD : (3 * h + 2) * HD]
            kv_src[to, pl.ds(wide + h * HD, HD)] = made[(3 * h + 2) * HD : (3 * h + 3) * HD]
        if j:
            kv(j).start()
            q(j).start()
        else:
            pair(0).start()
            kv_out[c, d] = kv_src[c]
            q_out[c] = q_src[c]

    def spread_out(at):
        for row in range(4):
            block = a_out[at, row, :, :, columns:].reshape(-1, feats)
            wo_out[pl.ds(at * wide, wide), row * feats : (row + 1) * feats] = block

    def unpack():
        first = bias_lanes // 128
        for i in range(6):
            for row in range(4):
                line = vec_out[0, row, 0, pl.ds(first + 2 * i, 2)]
                line = jnp.concatenate([line[0:1], line[1:2]], axis=1)
                vec_all[i : i + 1, row * feats : (row + 1) * feats] = line[:, :feats]
        vec_all[6:8] = jnp.zeros((2, 4 * feats), f32)
        first += 12
        for at in range(4):
            for i in range(b_in_all.shape[1] // 128):
                b_in_all[at : at + 1, i * 128 : (i + 1) * 128] = vec_out[at, 0, 0, pl.ds(first + i, 1)]
            for row in range(4):
                rows = pl.ds(row * feats + at * proj_rows, proj_rows)
                proj_all[rows] = vec_out[at, row, 1].astype(bf16)

    tiles = 8
    own = x_nat.shape[0]

    def segment(tile):
        return ints_out[r // 2, r % 2, pl.ds(tile, 1)].astype(f32)

    def collect():
        for j in (1, 2, 3):
            kv(j).wait_recv()
            pair(j).start()
        pltpu.make_async_copy(ints, ints_out.at[d], il.at[0]).wait()
        rcopy(ints, ints_out.at[1 - d], il.at[1], il.at[2], pn).wait()
        for tile in range(tiles):
            kcol[tile] = jnp.broadcast_to(segment(tile), (128, own)).T
        for j in (1, 2, 3):
            q(j).wait_recv()
        for j in range(4):
            pair(j).wait_recv()

        @pl.loop(0, 4)
        def _(at):
            for core in range(2):
                kn[2 * at + core] = kv_out[at, core, pl.ds(0, wide)].astype(f32).T.astype(bf16)

    def attend_block(block):
        block_rows(q_out.at[pl.ds(block, 1)], heads, scale, q3)
        here = 2 * block + d
        low, high = jnp.maximum(here - 4, 0), jnp.minimum(here + 5, tiles)
        qseg = jnp.concatenate([segment(here)] * heads, axis=1)

        def one(j, top):
            s = jnp.dot(kn[j], q3[...], preferred_element_type=f32)
            same = jnp.concatenate([kcol[j]] * (heads * own // 128), axis=1) == qseg
            s = jnp.where(same, s, masked_value)
            s_scr[j] = s
            return jnp.maximum(top, jnp.max(s, axis=0, keepdims=True))

        top = lax.fori_loop(low, high, one, jnp.full((1, heads * own), masked_value, f32))
        o_scr[...] = jnp.zeros_like(o_scr)

        def two(j, total):
            p = jnp.exp(s_scr[j] - top)
            low_p = p.astype(bf16)
            for h in range(heads):
                rows = pl.ds(h * HD, HD)
                v = kv_out[j // 2, j % 2, pl.ds(wide + h * HD, HD)]
                o_scr[rows] += jnp.dot(v, low_p[:, h * own : (h + 1) * own], preferred_element_type=f32)
            return total + jnp.sum(p, axis=0, keepdims=True)

        total = lax.fori_loop(low, high, two, jnp.zeros((1, heads * own), f32))
        for h in range(heads):
            rows = pl.ds(h * HD, HD)
            ctx_own[block, rows] = (o_scr[rows] / total[:, h * own : (h + 1) * own]).astype(bf16)
        lse_ref[block] = top + jnp.log(total)

    def back_copy(j):
        return rcopy(ctx_own.at[c ^ j], ctx_out.at[c], vs.at[j], vr.at[j], (d, r, c ^ j))

    def attend(j):
        attend_block(c ^ j)
        if j:
            back_copy(j).start()
        else:
            ctx_out[c] = ctx_own[c]

    wide = q_src.shape[1]
    lag = 3
    ready = 2 * len(steps) + 2 * lag

    def do(**stages):
        for stage, numbers in stages.items():
            for n in numbers:
                {"f": first, "s": second, "t": third}[stage](*jobs[n])

    for i in range(ready):
        do(f=[i], s=[i - lag] if i >= lag else [], t=[i - 2 * lag] if i >= 2 * lag else [])
    prepare()
    settle(0)
    settle(1)
    project(3)
    do(f=[20], s=[17], t=[14])
    project(2)
    do(f=[21], s=[18], t=[15])
    project(1)
    do(s=[19], t=[16])
    project(0)
    set_out(kinds - 1)
    do(s=[20], t=[17])
    for start, _ in late_moves:
        start()
    for at in range(3):
        spread_out(at)
        do(t=[18 + at])
    spread_out(3)
    do(s=[21])
    unpack()
    collect()
    attend(3)
    do(f=[22, 23])
    attend(2)
    do(f=[24, 25], s=[22])
    attend(1)
    do(f=[26, 27], s=[23], t=[21])
    attend(0)
    for n in (24, 25, 26, 27):
        do(s=[n], t=[n - 2])
    do(t=[26, 27])

    for k in range(kinds):
        if k > 1:
            settle(k)
        for way, hop in steps:

            def body():
                at = at_of(way, hop)
                own = hop == 0
                to_x(k, at, own).wait_send()
                to_y(k, at, own).wait_send()
                to_p(k, at, own).wait_send()
                for which in range(2):
                    relay(k, at, which).wait_send()
                for bit in (1, 2, 3):
                    pass_p(k, at, bit).wait_send()
                if hop < 3:
                    if own:

                        @pl.when(has_up)
                        def _():
                            z_send(k, c, 0, 1).wait_send()

                        @pl.when(has_down)
                        def _():
                            z_send(k, c, 1, 1).wait_send()
                    else:
                        can = has_up if way == 0 else has_down

                        @pl.when(can)
                        def _():
                            z_send(k, at, way, hop + 1).wait_send()

            guard(way, hop, body)
    for j in (1, 2, 3):
        q(j).wait_send()
        kv(j).wait_send()
        back_copy(j).wait()
    for j in range(4):
        pair(j).wait_send()
    for _, wait in late_moves:
        wait()


VM = pl.BlockSpec(memory_space=pltpu.VMEM)


def head_fast(weights, tokens, cotangent, ints, vectors, scale, cid):
    kinds = 4
    dma = pltpu.SemaphoreType.DMA
    _, feats, cols = tokens.shape
    own = cols // 2
    width = 4 * feats
    part = feats // 2
    wide = weights[0].shape[1] // 3
    full = 4 * wide
    heads = wide // HD
    shape = jax.ShapeDtypeStruct
    piece = shape((4, wide, own), bf16)
    taken = shape((4, feats, own), bf16)
    weight = shape((4, 4, 2, part, weights[2].shape[1]), bf16)
    hidden = weights[2].shape[1]
    student_width = vectors[2].shape[1]
    return pl.pallas_call(
        functools.partial(head_kernel, scale),
        out_shape=[
            shape((4, 4, 2, part, full), bf16), weight, weight, taken, taken, shape((2,) + ints.shape, ints.dtype),
            piece, shape((4, 2, 2 * wide, own), bf16), shape((4 * wide, width), bf16), shape((8, width), f32),
            shape((4, hidden), f32), shape((width, student_width), bf16), piece,
            shape((4, 1, heads * own), f32), piece,
        ],
        in_specs=[VM, VM] + [HBM] * 5 + [VM] * len(vectors),
        out_specs=[VM, HBM, HBM] + [VM] * 12,
        scratch_shapes=[
            pltpu.VMEM((feats, full), bf16),
            pltpu.VMEM((96, 128), f32),
            pltpu.VMEM((4, 4, 2, 48, 128), f32),
            pltpu.VMEM((own, width), bf16),
            pltpu.VMEM((4, wide, own), bf16),
            pltpu.VMEM((4, 2 * wide, own), bf16),
            pltpu.VMEM((8, own, wide), bf16),
            pltpu.VMEM((wide, heads * own), bf16),
            pltpu.VMEM((8, own, heads * own), f32),
            pltpu.VMEM((wide, own), f32),
            pltpu.VMEM((8, own, 128), f32),
            dma((kinds,)),
            dma((kinds, 2, 3)), dma((kinds, 2, 3)),
            dma((kinds, 4)), dma((kinds, 4)),
            dma((kinds, 4)), dma((kinds, 4)),
            dma((kinds, 4, 2)), dma((kinds, 4, 2)),
            dma((kinds, 4, 4)), dma((kinds, 4, 4)),
            dma, dma((4,)), dma((4,)), dma((3,)),
            dma((2, 4)), dma((2, 4)), dma((4,)), dma((4,)),
            dma, dma((4,)), dma((4,)), dma((4,)), dma((4,)),
        ],
        compiler_params=pltpu.CompilerParams(
            collective_id=cid, has_side_effects=True, vmem_limit_bytes=56 * 1024 * 1024
        ),
        name="head",
    )(*weights, tokens, cotangent, ints, *vectors)


def scatter_core(grads, outs, scratch, begin, during, late=0, gap=0):
    kinds = len(grads)
    (acc, precv, xr1, yr1, xr2, yr2, zup, zdn, fin) = scratch[:9]
    (ls, ps, pr, xs1, xm1, ys1, ym1, xs2, xm2, ys2, ym2, us, um, ds, dm, fs, fm, os) = scratch[9:]
    d, r, c = place()
    cols = 4
    chunks = kinds * cols
    xn, yn, pn = (d, r ^ 1, c), (d, r ^ 2, c), (1 - d, r, c)
    up, down = (d, r, c + 1), (d, r, c - 1)
    half = acc.shape[2] // 2
    first, last = pl.ds(0, half), pl.ds(half, half)

    def split(i):
        k = i // cols
        j = i - k * cols
        at = jnp.where(j == 0, 0, jnp.where(j == 1, 3, j - 1))
        return k, at

    def at_static(i):
        return i // cols, (0, 3, 1, 2)[i % cols]

    def load(i):
        k, at = at_static(i)
        return pltpu.make_async_copy(grads[k].at[at, :, d], acc.at[i], ls.at[i])

    def pair(i):
        k, at = at_static(i)
        return rcopy(grads[k].at[at, :, 1 - d], precv.at[i], ps.at[i], pr.at[i], pn)

    def launch(i):
        pair(i).start()
        load(i).start()

    for i in range((kinds - late) * cols):
        launch(i)
    begin()

    def x1(i, j):
        return rcopy(acc.at[i, r ^ 1 ^ (2 * j), first], xr1.at[i, j], xs1.at[i, j], xm1.at[i, j], xn)

    def y1(i, j):
        return rcopy(acc.at[i, r ^ 2 ^ j, last], yr1.at[i, j], ys1.at[i, j], ym1.at[i, j], yn)

    def y2(i):
        return rcopy(acc.at[i, r ^ 2, first], yr2.at[i], ys2.at[i], ym2.at[i], yn)

    def x2(i):
        return rcopy(acc.at[i, r ^ 1, last], xr2.at[i], xs2.at[i], xm2.at[i], xn)

    def to_up(i):
        return rcopy(acc.at[i, r], zup.at[i], us.at[i], um.at[i], up)

    def to_down(i):
        return rcopy(acc.at[i, r], zdn.at[i], ds.at[i], dm.at[i], down)

    def stage1(i):
        pltpu.make_async_copy(precv.at[i], acc.at[i], ls.at[i]).wait()
        rcopy(acc.at[i], precv.at[i], ps.at[i], pr.at[i], pn).wait_recv()

        @pl.loop(0, 4)
        def _(row):
            acc[i, row] = acc[i, row] + precv[i, row]

        x1(i, 1).start()
        y1(i, 1).start()
        x1(i, 0).start()
        y1(i, 0).start()

    def stage2(i):
        x1(i, 1).wait_recv()
        acc[i, r ^ 2, first] = acc[i, r ^ 2, first] + xr1[i, 1]
        y2(i).start()
        y1(i, 1).wait_recv()
        acc[i, r ^ 1, last] = acc[i, r ^ 1, last] + yr1[i, 1]
        x2(i).start()
        x1(i, 0).wait_recv()
        acc[i, r, first] = acc[i, r, first] + xr1[i, 0]
        y1(i, 0).wait_recv()
        acc[i, r, last] = acc[i, r, last] + yr1[i, 0]

    def stage3(i):
        y2(i).wait_recv()
        acc[i, r, first] = acc[i, r, first] + yr2[i]
        x2(i).wait_recv()
        acc[i, r, last] = acc[i, r, last] + xr2[i]

    def stage4(i, hops):
        k, at = split(i)

        @pl.when((at > c) & (c == hops))
        def _():
            @pl.when(c > 0)
            def _():
                to_up(i).wait_recv()
                acc[i, r] = acc[i, r] + zup[i]

            to_up(i).start()

        @pl.when((at < c) & (cols - 1 - c == hops))
        def _():
            @pl.when(c < cols - 1)
            def _():
                to_down(i).wait_recv()
                acc[i, r] = acc[i, r] + zdn[i]

            to_down(i).start()

        @pl.when((at == c) & (jnp.maximum(c, cols - 1 - c) == hops))
        def _():
            @pl.when(c > 0)
            def _():
                to_up(i).wait_recv()
                acc[i, r] = acc[i, r] + zup[i]

            @pl.when(c < cols - 1)
            def _():
                to_down(i).wait_recv()
                acc[i, r] = acc[i, r] + zdn[i]

            fin[k, d] = acc[i, r]
            rcopy(fin.at[k, d], fin.at[k, d], fs.at[k], fm.at[k], pn).start()

    stages = [(0, stage1), (2, stage2), (4, stage3)]
    stages += [(5 + h, functools.partial(lambda h, i: stage4(i, h), h)) for h in range(cols)]
    ending = stages[-1][0]

    assert len(during) <= chunks + gap + ending
    early = (kinds - late) * cols

    @pl.loop(0, chunks + gap + ending)
    def _(step):
        for i, extra in enumerate(during):
            pl.when(step == i)(functools.partial(extra, launch))

        for lag, stage in stages:

            spot = step - lag
            there = (spot >= 0) & (spot < early) | (spot >= early + gap) & (spot < chunks + gap)

            @pl.when(there)
            def _():
                stage(jnp.where(spot < early, spot, spot - gap))

    @pl.loop(0, chunks)
    def _(i):
        k, at = split(i)
        rcopy(acc.at[i], precv.at[i], ps.at[i], pr.at[i], pn).wait_send()
        for j in range(2):
            x1(i, j).wait_send()
            y1(i, j).wait_send()
        y2(i).wait_send()
        x2(i).wait_send()

        @pl.when(at > c)
        def _():
            to_up(i).wait_send()

        @pl.when(at < c)
        def _():
            to_down(i).wait_send()

    for k in range(kinds):
        rcopy(fin.at[k, 1 - d], fin.at[k, 1 - d], fs.at[k], fm.at[k], pn).wait()
        pltpu.make_async_copy(fin.at[k], outs[k], os.at[k]).start()
    for k in range(kinds):
        pltpu.make_async_copy(fin.at[k], outs[k], os.at[k]).wait()

def scatter_scratch(kinds, n, w, dt):
    dma = pltpu.SemaphoreType.DMA
    chunks = kinds * 4
    return [
        pltpu.VMEM((chunks, 4, n, w), dt),
        pltpu.VMEM((chunks, 4, n, w), dt),
        pltpu.VMEM((chunks, 2, n // 2, w), dt),
        pltpu.VMEM((chunks, 2, n // 2, w), dt),
        pltpu.VMEM((chunks, n // 2, w), dt),
        pltpu.VMEM((chunks, n // 2, w), dt),
        pltpu.VMEM((chunks, n, w), dt),
        pltpu.VMEM((chunks, n, w), dt),
        pltpu.VMEM((kinds, 2, n, w), dt),
        dma((chunks,)), dma((chunks,)), dma((chunks,)),
        dma((chunks, 2)), dma((chunks, 2)), dma((chunks, 2)), dma((chunks, 2)),
        dma((chunks,)), dma((chunks,)), dma((chunks,)), dma((chunks,)),
        dma((chunks,)), dma((chunks,)), dma((chunks,)), dma((chunks,)),
        dma((kinds,)), dma((kinds,)), dma((kinds,)),
    ]


def give_moves(src_ref, out_ref, local, send, recv):
    d, r, c = place()
    own = src_ref.shape[2]
    home = r // 2

    def slot(i, core):
        return out_ref.at[i, :, pl.ds(pl.multiple_of(core * own, own), own)]

    def move(row):
        return rcopy(src_ref.at[row], slot(r % 2, d), send.at[row], recv.at[r % 2, d], (home, row, c))

    def stay():
        return pltpu.make_async_copy(src_ref.at[r], slot(r % 2, d), local)

    def start():
        for row in range(4):

            @pl.when(jnp.logical_not((row == r) & (home == d)))
            def _():
                move(row).start()

        @pl.when(home == d)
        def _():
            stay().start()

    def finish():
        for row in range(4):

            @pl.when(jnp.logical_not((row == r) & (home == d)))
            def _():
                move(row).wait_send()

        @pl.when(home == d)
        def _():
            stay().wait()

        for i in range(2):
            for core in range(2):

                @pl.when(jnp.logical_not((2 * d + i == r) & (core == d)))
                def _():
                    rcopy(src_ref.at[0], slot(i, core), send.at[0], recv.at[i, core], (d, r, c)).wait_recv()

    return start, finish


def plane_peers():
    d, r, c = place()
    return [(d ^ (j // 4), r ^ (j % 4), c) for j in range(1, 8)]


def line_peers():
    d, r, c = place()
    return [(d ^ (j // 4), r, c ^ (j % 4)) for j in range(1, 8)]


def sum_steps(src, total, parts, sems):
    d, r, c = place()
    peers = [(1 - d, r, c), (d, r ^ 1, c), (d, r ^ 2, c), (d, r, c ^ 1), (d, r, c ^ 2)]
    bits = [d, r % 2, r // 2, c % 2, c // 2]
    rs, rr, gs, gr = sems
    count = len(peers)
    size = [src.shape[0] >> (i + 1) for i in range(count)]
    offset = [jnp.int32(0)]
    for i in range(count):
        offset.append(offset[i] + bits[i] * size[i])

    def rows(at, amount):
        return pl.ds(pl.multiple_of(at, 8), amount)

    def down(i):
        other = offset[i] + (1 - bits[i]) * size[i]
        held = src if i == 0 else parts[i - 1]
        at = other if i == 0 else other - offset[i]
        return rcopy(held.at[rows(at, size[i])], parts[count + i], rs.at[i], rr.at[i], peers[i])

    def fold(i):
        down(i).wait_recv()
        held = src if i == 0 else parts[i - 1]
        at = offset[i + 1] if i == 0 else offset[i + 1] - offset[i]
        parts[i][...] = held[rows(at, size[i])] + parts[count + i][...]

    def back(i):
        spot = total.at[rows(offset[i + 1], size[i])]
        return rcopy(spot, spot, gs.at[i], gr.at[i], peers[i])

    def back_recv(i):
        spot = total.at[rows(offset[i] + (1 - bits[i]) * size[i], size[i])]
        rcopy(spot, spot, gs.at[i], gr.at[i], peers[i]).wait_recv()

    steps = [lambda: down(0).start()]
    for i in range(1, count):

        def step(i=i):
            fold(i - 1)
            down(i).start()

        steps.append(step)

    def middle():
        fold(count - 1)
        total[rows(offset[count], size[-1])] = parts[count - 1][...]
        back(count - 1).start()

    steps.append(middle)
    for i in range(count - 2, -1, -1):

        def step(i=i):
            back_recv(i + 1)
            back(i).start()

        steps.append(step)

    def end():
        back_recv(0)
        for i in range(count):
            down(i).wait_send()
            back(i).wait_send()

    return steps, end


highest = lax.Precision.HIGHEST


def fine(a, b, contract=((1,), (0,))):
    return lax.dot_general(a, b, (contract, ((), ())), precision=highest, preferred_element_type=f32)


def same_head(size, part):
    one = lax.broadcasted_iota(jnp.int32, (size, size), 0) // part
    two = lax.broadcasted_iota(jnp.int32, (size, size), 1) // part
    return (one == two).astype(f32)


def student_stats(docs, scale, out_ref, seg_ref, proj_ref, vec_ref, hidden, logit, stats):
    width = hidden.shape[1]
    h = jnp.dot(out_ref[...], proj_ref[...], preferred_element_type=f32) + vec_ref[0:1]
    pool = fine(h * vec_ref[1:2], same_head(width, SHD)) * scale
    hidden[...] = h
    logit[...] = pool
    stats[0:8] = jnp.zeros((8, width), f32)
    stats[8:16] = jnp.zeros((8, width), f32)
    stats[16:24] = jnp.ones((8, width), f32)
    for doc in range(docs):
        mine = seg_ref[...] == doc
        top = jnp.max(jnp.where(mine, pool, masked_value), axis=0, keepdims=True)
        weight = jnp.where(mine, jnp.exp(pool - top), 0.0)
        stats[doc : doc + 1] = jnp.sum(weight * h, axis=0, keepdims=True)
        stats[8 + doc : 9 + doc] = top
        stats[16 + doc : 17 + doc] = jnp.sum(weight, axis=0, keepdims=True)


def student_grads(docs, classes, scale, once, row, out_ref, seg_ref, label_ref, vec_ref, mid_ref, cls_ref, hidden, logit, stats, small):
    width = hidden.shape[1]
    every = [stats[i, j] for i in range(stats.shape[0]) for j in range(stats.shape[1])]
    top = every[0][8:16]
    for one in every[1:]:
        top = jnp.maximum(top, one[8:16])
    total = jnp.zeros_like(top)
    pooled = jnp.zeros_like(top)
    for one in every:
        factor = jnp.exp(one[8:16] - top)
        total = total + one[16:24] * factor
        pooled = pooled + one[0:8] * factor
    pooled = pooled / total
    middle = jnp.tanh(fine(pooled, mid_ref[...]) + vec_ref[2:3])
    logits = fine(middle, cls_ref[...]) + vec_ref[3:4]
    lane = lax.broadcasted_iota(jnp.int32, logits.shape, 1)
    doc = lax.broadcasted_iota(jnp.int32, logits.shape, 0)
    real = lane < classes
    peak = jnp.max(jnp.where(real, logits, masked_value), axis=1, keepdims=True)
    share = jnp.where(real, jnp.exp(logits - peak), 0.0)
    share = share / jnp.sum(share, axis=1, keepdims=True)
    d_logits = jnp.where(doc < docs, share - (label_ref[...] == lane).astype(f32), 0.0)
    d_middle = fine(d_logits, cls_ref[...], ((1,), (1,))) * (1.0 - middle * middle)
    d_pooled = fine(d_middle, mid_ref[...], ((1,), (1,)))
    zeros = jnp.zeros((1, width), f32)
    small[768:896] = fine(pooled, d_middle, ((0,), (0,))) * once
    small[896:912] = fine(d_logits, middle, ((0,), (0,)))[0:16] * once
    small[912:913] = jnp.sum(d_middle, axis=0, keepdims=True) * once
    small[913:914] = jnp.sum(d_logits, axis=0, keepdims=True) * once
    for at in range(4):
        small[920 + 8 * at : 928 + 8 * at] = jnp.where(row == at, logits * once, 0.0)

    heads = same_head(width, SHD)
    base = fine(d_pooled * pooled, heads)
    h, pool = hidden[...], logit[...]
    top_t, total_t = jnp.zeros_like(h), jnp.ones_like(h)
    back_t, base_t = jnp.zeros_like(h), jnp.zeros_like(h)
    for doc in range(docs):
        mine = seg_ref[...] == doc
        top_t = jnp.where(mine, top[doc : doc + 1], top_t)
        total_t = jnp.where(mine, total[doc : doc + 1], total_t)
        back_t = jnp.where(mine, d_pooled[doc : doc + 1], back_t)
        base_t = jnp.where(mine, base[doc : doc + 1], base_t)
    share = jnp.exp(pool - top_t) / total_t
    d_pool = share * (fine(back_t * h, heads) - base_t)
    d_h = share * back_t + d_pool * vec_ref[1:2] * scale
    small[914:915] = jnp.sum(d_h, axis=0, keepdims=True)
    small[915:916] = jnp.sum(d_pool * h, axis=0, keepdims=True) * scale
    for i in range(916, 920):
        small[i : i + 1] = zeros
    small[0:768] = fine(out_ref[...].astype(f32), d_h, ((0,), (0,)))


def tail_kernel(docs, classes, scale, *refs):
    kinds = 2
    grads, refs = refs[:kinds], refs[kinds:]
    (q_ref, kv_ref, lse_ref, ctx_ref, dctx_ref, ints_ref), refs = refs[:6], refs[6:]
    (out_ref, seg_ref, label_ref, proj_ref, svec_ref, mid_ref, cls_ref), refs = refs[:7], refs[7:]
    vec_refs, refs = refs[:7], refs[7:]
    (x_ref, ctx_all_ref, resid_ref, out_t_ref, w_ref), refs = refs[:5], refs[5:]
    outs, refs = refs[: kinds + 1], refs[kinds + 1 :]
    (give_out, out_out, small_out), refs = refs[:3], refs[3:]
    (total, theirs, dqkv, own_grads, dpad, weights, resid_t, give_src), refs = refs[:8], refs[8:]
    (dctx, dq, dkv, kn, vn, q3, dc3, dq_scr, dkv_scr, bias_scr, landed, kcol, qsegs, deltas), refs = refs[:14], refs[14:]
    (hidden, logit, stats, stats_all, small), refs = refs[:5], refs[5:]
    parts, refs = refs[:10], refs[10:]
    (send, recv, psend, precv), sems, (wl, gl, gs, gr), refs = refs[:4], refs[4:8], refs[8:12], refs[12:]
    (dsend, drecv, ssend, srecv, ol, osend, orecv), scratch = refs[:7], refs[7:]
    d, r, c = place()
    pn = (1 - d, r, c)
    tiles, deep, tile = kv_ref.shape
    wide = deep // 2
    heads = wide // HD
    full = dqkv.shape[1]
    own = q_ref.shape[2]
    kv_rows, q_rows = pl.ds(0, deep), pl.ds(deep, wide)
    peers = line_peers()
    greet(plane_peers() + peers[:3] + peers[4:])

    def to_heads(j):
        return rcopy(dctx_ref.at[c ^ j], dctx.at[c], dsend.at[j], drecv.at[j], (d, r, c ^ j))

    for j in (3, 2, 1):
        to_heads(j).start()
    dctx[c] = dctx_ref[c]
    load_w = pltpu.make_async_copy(w_ref, weights, wl)
    load_w.start()

    def tell(j):
        return rcopy(stats, stats_all.at[d, c], ssend.at[j - 1], srecv.at[j - 1], peers[j - 1])

    out_start, out_finish = give_moves(out_t_ref, out_out, ol, osend, orecv)
    start, finish = give_moves(give_src, give_out, gl, gs, gr)
    steps, end = sum_steps(small, small_out, parts, sems)
    pool_scale = SHD ** (-0.5)

    def begin():
        out_start()
        student_stats(docs, pool_scale, out_ref, seg_ref, proj_ref, svec_ref, hidden, logit, stats)
        for j in range(1, 8):
            tell(j).start()
        stats_all[d, c] = stats[...]
        spare = full - deep - wide
        for at in range(4):
            dqkv[at, pl.ds(deep + wide, spare)] = jnp.zeros((spare, own), bf16)
        resid_t[...] = resid_ref[...].T
        feats = x_ref.shape[1]
        blank = dpad.shape[1] - feats
        for row in range(4):
            dpad[row, pl.ds(0, blank)] = jnp.zeros((blank, own), bf16)
            dpad[row, pl.ds(blank, feats)] = resid_t[pl.ds(row * feats, feats)].astype(bf16)
        at = 952
        for ref in vec_refs:
            for i in range(ref.shape[0]):
                for j in range(ref.shape[1] // 128):
                    small[at : at + 1] = ref[i : i + 1, j * 128 : (j + 1) * 128]
                    at += 1
        for i in range(at, small.shape[0]):
            small[i : i + 1] = jnp.zeros((1, 128), f32)

    def student(_):
        for j in range(1, 8):
            tell(j).wait_recv()
        once = 1.0 / 8
        student_grads(
            docs, classes, pool_scale, once, r, out_ref, seg_ref, label_ref, svec_ref, mid_ref, cls_ref, hidden, logit,
            stats_all, small,
        )

    def segment(at):
        return ints_ref[r // 2, r % 2, pl.ds(at, 1)].astype(f32)

    def prepare(_):
        @pl.loop(0, tiles)
        def _(j):
            kn[j] = kv_ref[j, pl.ds(0, wide)].astype(f32).T.astype(bf16)
            vn[j] = kv_ref[j, pl.ds(wide, wide)].astype(f32).T.astype(bf16)

        for j in range(tiles):
            kcol[j] = jnp.broadcast_to(segment(j), (128, own)).T
        bias_scr[...] = jnp.zeros_like(bias_scr)
        dq_scr[...] = jnp.zeros_like(dq_scr)
        for block in range(4):
            block_rows(q_ref.at[pl.ds(block, 1)], heads, scale, q3.at[block])
            qsegs[block] = jnp.concatenate([segment(2 * block + d)] * heads, axis=1)
        for j in (1, 2, 3):
            to_heads(j).wait_recv()
        for block in range(4):
            block_rows(dctx.at[pl.ds(block, 1)], heads, 1.0, dc3.at[block])
            product = ctx_ref[block].astype(f32) * dctx[block].astype(f32)
            deltas[block] = jnp.concatenate(
                [jnp.sum(product[h * HD : (h + 1) * HD], axis=0, keepdims=True) for h in range(heads)], axis=1
            )

    ones = jnp.ones((8, own), bf16)
    across = (((1,), (1,)), ((), ()))

    def attend(j, _):
        if j < 3:
            settle(j + 1)
        for core in range(2):
            tile_at = 2 * (c ^ j) + core
            k_nat, v_nat = kn.at[tile_at], vn.at[tile_at]
            k_t = kv_ref.at[tile_at]
            seen = jnp.concatenate([kcol[tile_at]] * (heads * own // 128), axis=1)
            dkv_scr[...] = jnp.zeros_like(dkv_scr)

            @pl.loop(jnp.maximum(tile_at - 3 - d, 0) // 2, jnp.minimum((tile_at + 4 - d) // 2 + 1, 4))
            def _(block):
                s = jnp.dot(k_nat[...], q3[block], preferred_element_type=f32)
                p = jnp.exp(jnp.where(seen == qsegs[block], s, masked_value) - lse_ref[block])
                d_p = jnp.dot(v_nat[...], dc3[block], preferred_element_type=f32)
                d_s = (p * (d_p - deltas[block])).astype(bf16)
                p = p.astype(bf16)
                for h in range(heads):
                    rows, lanes = pl.ds(h * HD, HD), slice(h * own, (h + 1) * own)
                    low = pl.ds(wide + h * HD, HD)
                    dq_scr[block, rows] += jnp.dot(k_t[rows], d_s[:, lanes], preferred_element_type=f32)
                    dkv_scr[rows] += lax.dot_general(
                        q3[block, rows, lanes], d_s[:, lanes], across, preferred_element_type=f32
                    )
                    dkv_scr[low] += lax.dot_general(dctx[block, rows], p[:, lanes], across, preferred_element_type=f32)

            made = dkv_scr[...].astype(bf16)
            dkv[c ^ j, core] = made
            bias_scr[:, wide:] += lax.dot_general(ones, made[wide:], across, preferred_element_type=f32)
        pair(j).start()

    def settle(j):
        pair(j).wait_recv()
        if j:
            total[c ^ j] = dkv[c ^ j, d] + theirs[c ^ j]
            kv(j).start()
        else:
            landed[c, kv_rows] = dkv[c, d] + theirs[c]

    def pair(j):
        return rcopy(dkv.at[c ^ j, 1 - d], theirs.at[c ^ j], psend.at[j], precv.at[j], pn)

    def kv(j):
        return rcopy(total.at[c ^ j], landed.at[c, kv_rows], send.at[0, j], recv.at[0, j], (d, r, c ^ j))

    def q(j):
        return rcopy(dq.at[c ^ j], landed.at[c, q_rows], send.at[1, j], recv.at[1, j], (d, r, c ^ j))

    def leave(_):
        for j in (3, 2, 1, 0):
            made = (dq_scr[c ^ j] * scale).astype(bf16)
            dq[c ^ j] = made
            bias_scr[:, :wide] += lax.dot_general(ones, made, across, preferred_element_type=f32)
            if j:
                q(j).start()
        landed[c, q_rows] = dq[c]
        settle(0)
        for i in range(3):
            small[pl.ds(1012 + 3 * c + i, 1)] = bias_scr[0:1, i * 128 : (i + 1) * 128]

    def make(at):
        lead = full - dpad.shape[1]

        @pl.loop(0, 4)
        def _(row):
            one = lax.dot_general(x_ref[row], dqkv[at], across, preferred_element_type=f32)
            two = lax.dot_general(ctx_all_ref[at], dpad[row], across, preferred_element_type=f32)
            shape = own_grads.shape[2:4] + (-1,)
            own_grads[at, row, :, :, :lead] = one[:, :lead].astype(bf16).reshape(shape)
            own_grads[at, row, :, :, lead:] = (one[:, lead:] + two).astype(bf16).reshape(shape)

    def make_chunk(j, launch):
        if j == 0:
            for far in (1, 2, 3):
                q(far).wait_recv()
                kv(far).wait_recv()

            @pl.loop(0, 4)
            def _(at):
                for h in range(heads):
                    for slot, spot in enumerate((deep, 0, wide)):
                        dqkv[at, pl.ds((3 * h + slot) * HD, HD)] = landed[at, pl.ds(spot + h * HD, HD)]

        make((0, 3, 1, 2)[j])
        launch(kinds * 4 + j)

    def input_grad(_):
        load_w.wait()
        feats = x_ref.shape[1]

        @pl.loop(0, 4)
        def _(row):
            part = resid_t[pl.ds(pl.multiple_of(row * feats, 8), feats)]
            for at in range(4):
                w = weights[at, row].reshape(feats, full)
                part = part + jnp.dot(w, dqkv[at], preferred_element_type=f32)
            give_src[row] = part.astype(bf16)

        start()

    gap = 3
    hooks = [[] for _ in range(max(8 + gap + 5, 8 + len(steps)))]
    hooks[0].append(prepare)
    for i, j in enumerate((3, 2, 1, 0)):
        hooks[1 + i].append(functools.partial(attend, j))
    hooks[5].append(leave)
    hooks[6].append(student)
    for i, step in enumerate(steps):
        hooks[8 + i].append(lambda launch, step=step: step())
    for j in range(4):
        hooks[7 + gap + j].append(functools.partial(make_chunk, j))
    hooks[11 + gap].append(input_grad)

    def run(todo, launch):
        for one in todo:
            one(launch)

    during = [functools.partial(run, todo) for todo in hooks]
    scatter_core(list(grads) + [own_grads], outs, scratch, begin, during, late=1, gap=gap)
    end()
    finish()
    out_finish()
    for j in range(1, 8):
        tell(j).wait_send()
    for j in range(4):
        pair(j).wait_send()
    for j in (1, 2, 3):
        to_heads(j).wait_send()
        q(j).wait_send()
        kv(j).wait_send()


def tail_fast(docs, classes, scale, grads, attention, student, vectors, rest, out_t, w_attn, cid):
    n, w = grads[0].shape[3:]
    q, kv = attention[:2]
    dma = pltpu.SemaphoreType.DMA
    tiles, deep, own = kv.shape
    wide = deep // 2
    cols = tiles // 2
    feats = rest[0].shape[1]
    student_width = student[3].shape[1]
    tall = 1024
    parts = [pltpu.VMEM((tall >> (i + 1), 128), f32) for i in range(5)]
    home = jax.ShapeDtypeStruct((2, feats, 2 * own), bf16)
    return pl.pallas_call(
        functools.partial(tail_kernel, docs, classes, scale),
        out_shape=[jax.ShapeDtypeStruct((2, n, w), bf16)] * 3 + [home, home, jax.ShapeDtypeStruct((tall, 128), f32)],
        in_specs=[HBM] * 2 + [VM] * (len(attention) + len(student) + len(vectors) + len(rest)) + [HBM] * 2,
        out_specs=[HBM] * 5 + [VM],
        scratch_shapes=[
            pltpu.VMEM((cols, deep, own), bf16),
            pltpu.VMEM((cols, deep, own), bf16),
            pltpu.VMEM((cols, w, own), bf16),
            pltpu.VMEM((4, 4, 2, n, w), bf16),
            pltpu.VMEM((4, 256, own), bf16),
            pltpu.VMEM((4, 4, 2, n, w), bf16),
            pltpu.VMEM((4 * feats, own), f32),
            pltpu.VMEM((4, feats, own), bf16),
            pltpu.VMEM((cols, wide, own), bf16),
            pltpu.VMEM((cols, wide, own), bf16),
            pltpu.VMEM((cols, 2, deep, own), bf16),
            pltpu.VMEM((tiles, own, wide), bf16),
            pltpu.VMEM((tiles, own, wide), bf16),
            pltpu.VMEM((4, wide, wide // HD * own), bf16),
            pltpu.VMEM((4, wide, wide // HD * own), bf16),
            pltpu.VMEM((4, wide, own), f32),
            pltpu.VMEM((deep, own), f32),
            pltpu.VMEM((8, deep), f32),
            pltpu.VMEM((cols, deep + wide, own), bf16),
            pltpu.VMEM((tiles, own, 128), f32),
            pltpu.VMEM((4, 1, wide // HD * own), f32),
            pltpu.VMEM((4, 1, wide // HD * own), f32),
            pltpu.VMEM((own, student_width), f32),
            pltpu.VMEM((own, student_width), f32),
            pltpu.VMEM((24, student_width), f32),
            pltpu.VMEM((2, 4, 24, student_width), f32),
            pltpu.VMEM((tall, 128), f32),
        ]
        + parts * 2
        + [dma((2, 4)), dma((2, 4)), dma((4,)), dma((4,)), dma((5,)), dma((5,)), dma((5,)), dma((5,))]
        + [dma, dma, dma((4,)), dma((2, 2))]
        + [dma((4,)), dma((4,)), dma((7,)), dma((7,)), dma, dma((4,)), dma((2, 2))]
        + scatter_scratch(3, n, w, bf16),
        compiler_params=pltpu.CompilerParams(
            collective_id=cid, has_side_effects=True, vmem_limit_bytes=60 * 1024 * 1024
        ),
        name="tail",
    )(*grads, *attention, *student, *vectors, *rest, out_t.reshape(4, feats, own), w_attn)


def finish_kernel(docs, classes, in_ref, back_ref, attn_ref, grad_ref, small_ref, *outs):
    d, r, c = place()
    w_qkv, w_out, w_in, w_back, tokens, proj, logits, b_qkv, b_in, singles = outs[:9] + (outs[9:],)
    rows = in_ref.shape[0] * in_ref.shape[1]
    w_in[...] = in_ref[...].reshape(rows, -1).astype(f32)
    w_back[...] = back_ref[...].reshape(rows, -1).astype(f32)
    columns = w_qkv.shape[1]
    w_qkv[...] = attn_ref[:, :, :columns].reshape(rows, -1).astype(f32)
    w_out[...] = attn_ref[:, :, columns:].reshape(rows, -1).astype(f32)
    tokens[...] = grad_ref[...].astype(f32)
    feats = proj.shape[0]
    proj[...] = small_ref[pl.ds(pl.multiple_of(r * feats, 8), feats)]
    for i in range(2):
        some = small_ref[pl.ds(pl.multiple_of(920 + 8 * (2 * d + i), 8), 8)]
        logits[i] = some[:docs, :classes]
    line = [small_ref[pl.ds(1012 + 3 * c + i, 1)] for i in range(3)]
    line = jnp.concatenate(line, axis=1)
    wide = b_qkv.shape[1]
    b_qkv[0:1] = line[:, :wide]
    b_qkv[1:2] = line[:, wide:]
    for i in range(b_in.shape[1] // 128):
        b_in[:, i * 128 : (i + 1) * 128] = small_ref[pl.ds(952 + 6 * c + i, 1)]
    for i in range(6):
        line = [small_ref[976 + 6 * i + j : 977 + 6 * i + j] for j in range(6)]
        line = jnp.concatenate(line, axis=1)
        for row in range(4):

            @pl.when(r == row)
            def _():
                singles[i][...] = line[:, row * feats : (row + 1) * feats]

    s_mid, s_cls, s_mid_bias, s_cls_bias, s_bias, s_query = singles[6:]
    s_mid[...] = small_ref[768:896]
    s_cls[...] = jnp.concatenate([small_ref[896:912]] + [jnp.zeros((112, 128), f32)], axis=0).T[:, :classes]
    s_mid_bias[...] = small_ref[912:913]
    s_cls_bias[...] = small_ref[913:914, :classes]
    s_bias[...] = small_ref[914:915]
    s_query[...] = small_ref[915:916]


def finish_fast(docs, classes, w_in, w_back, w_attn, grad, small, columns):
    _, part, hidden = w_in.shape
    feats = 2 * part
    width = small.shape[1]

    def shape(*dims):
        return jax.ShapeDtypeStruct(dims, f32)

    shapes = [
        shape(feats, columns), shape(w_attn.shape[2] - columns, feats), shape(feats, hidden), shape(feats, hidden),
        shape(*grad.shape), shape(feats, width), shape(2, docs, classes), shape(2, columns // 3), shape(1, hidden),
    ]
    shapes += [shape(1, feats)] * 6
    shapes += [shape(width, width), shape(width, classes), shape(1, width), shape(1, classes)] + [shape(1, width)] * 2
    return pl.pallas_call(
        functools.partial(finish_kernel, docs, classes),
        out_shape=shapes,
        in_specs=[VM] * 5,
        out_specs=[VM] * len(shapes),
        name="finish",
    )(w_in, w_back, w_attn, grad, small)


def dot(a, b, contract=((1,), (0,))):
    return lax.dot_general(a, b, (contract, ((), ())), preferred_element_type=f32)


def block_rows(ref, heads, scale, out):
    own = ref.shape[-1]
    for h in range(heads):
        for g in range(heads):
            spot = (pl.ds(h * HD, HD), pl.ds(g * own, own))
            if h == g:
                out[spot] = ref[0, pl.ds(h * HD, HD)] * jnp.asarray(scale, out.dtype)
            else:
                out[spot] = jnp.zeros((HD, own), out.dtype)


def spread_of(values):
    mean_v = jnp.mean(values, axis=1, keepdims=True)
    center = values - mean_v
    inv_std = lax.rsqrt(jnp.mean(center * center, axis=1, keepdims=True) + norm_eps)
    return center * inv_std, inv_std


def spread_back(grad_hat, normed, inv_std):
    return inv_std * (
        grad_hat
        - jnp.mean(grad_hat, axis=1, keepdims=True)
        - normed * jnp.mean(grad_hat * normed, axis=1, keepdims=True)
    )


def dense_kernel(
    ctx_ref, x_ref, cot_ref, wo_ref, vec_ref, b_in_ref, w_in_hbm, w_back_hbm,
    g_in_hbm, g_back_hbm, dctx_ref, out_ref, out_t_ref, resid_ref, gb_in_ref, gb_out_ref, g1_ref, b1_ref, gb_back_ref,
    g2_ref, b2_ref,
    w_in, w_back, g_in, g_back, slope, act, total, hidden, hat, low, low_t, in_sem, back_sem, gi_sem, gb_sem,
):
    cols = w_in.shape[0]
    across = (((1,), (1,)), ((), ()))

    def fetch(c):
        return (
            pltpu.make_async_copy(w_in_hbm.at[c], w_in.at[c], in_sem.at[c]),
            pltpu.make_async_copy(w_back_hbm.at[c], w_back.at[c], back_sem.at[c]),
        )

    def store(c):
        return (
            pltpu.make_async_copy(g_in.at[c], g_in_hbm.at[c], gi_sem.at[c]),
            pltpu.make_async_copy(g_back.at[c], g_back_hbm.at[c], gb_sem.at[c]),
        )

    for c in range(cols):
        for copy in fetch(c):
            copy.start()

    def natural(ref):
        return ref[...].reshape(-1, ref.shape[2]).astype(f32).T

    b_out, gain_one, bias_one, b_back, gain_two, bias_two = [vec_ref[i : i + 1] for i in range(6)]
    attn_out = jnp.dot(natural(ctx_ref).astype(bf16), wo_ref[...], preferred_element_type=f32) + b_out
    hat_one, inv_one = spread_of(natural(x_ref) + attn_out)
    hidden_one = hat_one * gain_one + bias_one
    hat[...] = hat_one
    hidden[...] = hidden_one
    low[...] = hidden_one.astype(bf16)
    low_t[...] = hidden_one.T.astype(bf16)
    total[...] = jnp.zeros_like(total)

    @pl.loop(0, cols)
    def _(c):
        into, out = fetch(c)
        into.wait()
        pre = jnp.dot(low[...], w_in[c], preferred_element_type=f32) + b_in_ref[pl.ds(c, 1)]
        share = 0.5 + 0.5 * lax.erf(pre * (0.5**0.5))
        slope[c] = share + pre * (jnp.exp(-0.5 * pre * pre) * (0.5 / math.pi) ** 0.5)
        made = (pre * share).astype(bf16)
        act[c] = made
        out.wait()
        total[...] += lax.dot_general(made, w_back[c], across, preferred_element_type=f32)

    hat_two, inv_two = spread_of(hidden[...] + total[...] + b_back)
    layer_out = hat_two * gain_two + bias_two
    out_ref[...] = layer_out.astype(bf16)
    out_t_ref[...] = layer_out.T.astype(bf16).reshape(out_t_ref.shape)
    cot = natural(cot_ref)
    g2_ref[...] = jnp.sum(cot * hat_two, axis=0, keepdims=True)
    b2_ref[...] = jnp.sum(cot, axis=0, keepdims=True)
    d_two = spread_back(cot * gain_two, hat_two, inv_two)
    d_ffn = d_two.astype(bf16)
    gb_back_ref[...] = jnp.sum(d_ffn.astype(f32), axis=0, keepdims=True)
    d_ffn_t = d_two.T.astype(bf16)
    total[...] = d_two

    @pl.loop(0, cols)
    def _(c):
        to_in, to_back = store(c)
        g_back[c] = jnp.dot(d_ffn_t, act[c], preferred_element_type=f32).astype(bf16)
        to_back.start()
        d_pre = (slope[c] * jnp.dot(d_ffn, w_back[c], preferred_element_type=f32)).astype(bf16)
        gb_in_ref[pl.ds(c, 1)] = jnp.sum(d_pre.astype(f32), axis=0, keepdims=True)
        total[...] += lax.dot_general(d_pre, w_in[c], across, preferred_element_type=f32)
        g_in[c] = jnp.dot(low_t[...], d_pre, preferred_element_type=f32).astype(bf16)
        to_in.start()

    d_hidden, hat_one = total[...], hat[...]
    g1_ref[...] = jnp.sum(d_hidden * hat_one, axis=0, keepdims=True)
    b1_ref[...] = jnp.sum(d_hidden, axis=0, keepdims=True)
    d_one = spread_back(d_hidden * gain_one, hat_one, inv_one)
    resid_ref[...] = d_one
    d_attn = d_one.astype(bf16)
    gb_out_ref[...] = jnp.sum(d_attn.astype(f32), axis=0, keepdims=True)
    d_ctx = lax.dot_general(wo_ref[...], d_attn, across, preferred_element_type=f32)
    dctx_ref[...] = d_ctx.astype(bf16).reshape(dctx_ref.shape)

    @pl.loop(0, cols)
    def _(c):
        for copy in store(c):
            copy.wait()


def dense_fast(ctx, x, cot, wo, vec, b_in, w_in, w_back):
    cols, width, hidden = w_in.shape
    own = x.shape[2]
    dma = pltpu.SemaphoreType.DMA
    shape = jax.ShapeDtypeStruct
    line = shape((1, width), f32)
    weight = shape(w_in.shape, bf16)
    return pl.pallas_call(
        dense_kernel,
        out_shape=[
            weight, weight, shape(ctx.shape, bf16), shape((own, width), bf16), shape(x.shape, bf16),
            shape((own, width), f32), shape((cols, hidden), f32),
        ]
        + [line] * 6,
        in_specs=[VM] * 6 + [HBM] * 2,
        out_specs=[HBM] * 2 + [VM] * 11,
        scratch_shapes=[
            pltpu.VMEM((cols, width, hidden), bf16),
            pltpu.VMEM((cols, width, hidden), bf16),
            pltpu.VMEM((cols, width, hidden), bf16),
            pltpu.VMEM((cols, width, hidden), bf16),
            pltpu.VMEM((cols, own, hidden), f32),
            pltpu.VMEM((cols, own, hidden), bf16),
            pltpu.VMEM((own, width), f32),
            pltpu.VMEM((own, width), f32),
            pltpu.VMEM((own, width), f32),
            pltpu.VMEM((own, width), bf16),
            pltpu.VMEM((width, own), bf16),
            dma((cols,)), dma((cols,)), dma((cols,)), dma((cols,)),
        ],
        compiler_params=pltpu.CompilerParams(vmem_limit_bytes=56 * 1024 * 1024),
        name="dense",
    )(ctx, x, cot, wo, vec, b_in, w_in, w_back)


def fast_local(
    tokens,
    segments,
    labels,
    cotangent,
    w_qkv,
    b_qkv,
    w_out,
    b_out,
    ln1_gain,
    ln1_bias,
    w_in,
    b_in,
    w_back,
    b_back,
    ln2_gain,
    ln2_bias,
    s_proj,
    s_bias,
    s_query,
    s_mid,
    s_mid_bias,
    s_cls,
    s_cls_bias,
):
    _, width_row, cols_local = tokens.shape
    parts, rows, cols, seqs, _ = sizes(tokens.shape[0])
    width = width_row * rows
    own = cols_local // parts
    width_col = b_qkv.shape[1]
    heads_dev = width_col // HD
    hidden_col = b_in.shape[0]
    docs_count = labels.shape[1]
    class_count = s_cls.shape[1]
    student_width = s_proj.shape[1]
    seq_len = segments.shape[1]
    row_index = lax.axis_index("row")
    col_index = lax.axis_index("col")
    dp_index = lax.axis_index("dp")
    score_scale = HD ** (-0.5)
    pool_scale = SHD ** (-0.5)
    query_heads = s_query.reshape(SH, SHD)
    doc_ids = jnp.arange(docs_count, dtype=jnp.int32)
    class_ids = jnp.arange(class_count, dtype=jnp.int32)

    ints = jnp.pad(labels, ((0, 0), (0, own - docs_count)))[:, None]
    ints = jnp.concatenate([segments.reshape(-1, seq_len // own, own), ints], axis=1)
    ints = jnp.pad(ints, ((0, 0), (0, 16 - ints.shape[1]), (0, 0)))
    row_vectors = [b_out, ln1_gain, ln1_bias, b_back, ln2_gain, ln2_bias]
    (
        w_attn, w_in_all, w_back_all, x_parts, c_parts, ints, queries, kv, w_out_all, row_vectors, b_in_all,
        s_proj_all, context, lse, ctx_parts,
    ) = head_fast(
        [w_qkv, w_out, w_in, w_back],
        tokens,
        cotangent,
        ints,
        [b_qkv, b_in[None], s_proj] + [v[None] for v in row_vectors],
        score_scale,
        1,
    )
    w_in_all = w_in_all.reshape(cols, width, hidden_col)
    w_back_all = w_back_all.reshape(cols, width, hidden_col)
    kv = kv.reshape(cols * parts, 2 * width_col, own)
    own_ints = lax.dynamic_index_in_dim(ints.reshape(seqs, 16, own), row_index, 0, False)
    seg_own = lax.dynamic_index_in_dim(own_ints, 2 * col_index + dp_index, 0, False)
    label_seq = own_ints[seq_len // own, :docs_count]

    (
        g_in, g_back, d_ctx, layer_out, out_t, d_resid_one, g_in_bias, g_out_bias, g_ln1_gain, g_ln1_bias, g_back_bias,
        g_ln2_gain, g_ln2_bias,
    ) = dense_fast(ctx_parts, x_parts, c_parts, w_out_all, row_vectors, b_in_all, w_in_all, w_back_all)

    blocked = (cols, rows, parts, width_row // parts, -1)
    lane_pad = ((0, 0), (0, 128 - class_count))
    student_vectors = jnp.stack([s_bias, s_query, s_mid_bias, jnp.pad(s_cls_bias, (0, 128 - class_count))])
    student_vectors = jnp.pad(student_vectors, ((0, 4), (0, 0)))
    g_in, g_back, g_attn, grad_tokens, out, small = tail_fast(
        docs_count,
        class_count,
        score_scale,
        [g_in.reshape(blocked), g_back.reshape(blocked)],
        [queries, kv, lse, context, d_ctx, ints],
        [
            layer_out,
            seg_own[:, None],
            jnp.pad(label_seq, (0, 8 - docs_count))[:, None],
            s_proj_all,
            student_vectors,
            s_mid,
            jnp.pad(s_cls, lane_pad),
        ],
        [g_in_bias, g_out_bias, g_ln1_gain, g_ln1_bias, g_back_bias, g_ln2_gain, g_ln2_bias],
        [x_parts, ctx_parts, d_resid_one],
        out_t.reshape(width, own),
        w_attn,
        4,
    )
    (
        g_qkv, g_out, g_in, g_back, grad_tokens, g_sproj, logits, g_qkv_bias, g_in_bias, g_out_bias, g_ln1_gain,
        g_ln1_bias, g_back_bias, g_ln2_gain, g_ln2_bias, g_mid, g_cls, g_mid_bias, g_cls_bias, g_sbias, g_query,
    ) = finish_fast(docs_count, class_count, g_in, g_back, g_attn, grad_tokens, small, 3 * width_col)
    return (
        out,
        logits,
        grad_tokens,
        g_qkv,
        g_qkv_bias,
        g_out,
        g_out_bias[0],
        g_ln1_gain[0],
        g_ln1_bias[0],
        g_in,
        g_in_bias[0],
        g_back,
        g_back_bias[0],
        g_ln2_gain[0],
        g_ln2_bias[0],
        g_sproj,
        g_sbias[0],
        g_query[0],
        g_mid,
        g_mid_bias[0],
        g_cls,
        g_cls_bias[0],
    )


def solution(mesh):
    row, col = P("row"), P("col")
    grid, whole = P("row", "col"), P("dp", "row", "col")
    placed = (
        (whole, P("dp", None), P("dp", None), whole, grid, P(None, "col"), P("col", "row"))
        + (row, row, row, grid, col, grid, row, row, row, P("row", None))
        + (P(),) * 6
    )
    results = (
        (whole, P("dp", None, None), whole, grid, P(None, "col"), P("col", "row"))
        + (row, row, row, grid, col, grid, row, row, row, P("row", None))
        + (P(),) * 6
    )
    quick = dict(mesh.shape) == {"dp": 2, "row": 4, "col": 4}
    local = fast_local if quick else general_local
    return jax.shard_map(local, mesh=mesh, in_specs=placed, out_specs=results, check_vma=False)
```

```python
import functools
import math
import jax
import jax.numpy as jnp
from jax import lax
from jax.experimental import pallas as pl
from jax.experimental.pallas import tpu as pltpu
from jax.sharding import PartitionSpec as P

HD = 64
SH = 2
SHD = 64

norm_eps = 1e-06
masked_value = -1e30
highest = lax.Precision.HIGHEST
f32 = jnp.float32
bf16 = jnp.bfloat16
WORLD = ("col", "row", "dp")


def sizes(seqs_local):
    parts = lax.axis_size("dp")
    rows = lax.axis_size("row")
    seqs = seqs_local * parts
    return parts, rows, lax.axis_size("col"), seqs, rows // seqs


def row_groups(rows, sub):
    return [list(range(at, at + sub)) for at in range(0, rows, sub)]


def take_in(values):
    parts, rows, _, seqs, sub = sizes(values.shape[0])
    held = lax.all_to_all(values, "dp", 2, 0, tiled=True)
    feats, half = held.shape[1:]
    held = held.reshape(seqs, feats, sub, half // sub).transpose(0, 2, 1, 3)
    held = held.reshape(rows, feats, half // sub)
    held = lax.all_to_all(held, "row", 0, 0, tiled=True)
    return held.reshape(rows * feats, half // sub)


def give_back(values, seqs_local):
    parts, rows, _, seqs, sub = sizes(seqs_local)
    width, own = values.shape
    feats = width // rows
    held = lax.all_to_all(values.reshape(rows, feats, own), "row", 0, 0, tiled=True)
    held = held.reshape(seqs, sub, feats, own).transpose(0, 2, 1, 3).reshape(seqs, feats, sub * own)
    return lax.all_to_all(held, "dp", 0, 2, tiled=True)


def gather_world(shard):
    cols, rows = lax.axis_size("col"), lax.axis_size("row")
    out = lax.all_gather(shard, WORLD, axis=0, tiled=True)
    return out.reshape(cols, rows, -1, shard.shape[1])


def own_half(block):
    parts = lax.axis_size("dp")
    amount = block.shape[0] // parts
    return lax.dynamic_slice_in_dim(block, lax.axis_index("dp") * amount, amount)


def scatter_world(full):
    flat = full.reshape(-1, full.shape[-1])
    mine = lax.psum_scatter(flat, WORLD, scatter_dimension=0, tiled=True)
    return lax.all_gather(mine, "dp", axis=0, tiled=True)


def swap_cols(values):
    return lax.all_to_all(values, "col", 0, 0, tiled=True)


def gather_sequence(values, sub):
    cols, own, width = values.shape
    held = values[:, None]
    if sub > 1:
        groups = row_groups(lax.axis_size("row"), sub)
        held = lax.all_gather(held, "row", axis=1, tiled=True, axis_index_groups=groups)
    held = lax.all_gather(held[:, None], "dp", axis=1, tiled=True)
    return held.reshape(-1, width)


def scatter_sequence(values, cols, sub):
    parts = lax.axis_size("dp")
    width = values.shape[-1]
    held = values.reshape(cols, parts, sub, -1, width)
    held = lax.psum_scatter(held, "dp", scatter_dimension=1, tiled=True)[:, 0]
    if sub > 1:
        groups = row_groups(lax.axis_size("row"), sub)
        held = lax.psum_scatter(
            held, "row", scatter_dimension=1, tiled=True, axis_index_groups=groups
        )
    return held[:, 0]


def normalize(values):
    mean_v = jnp.mean(values, axis=-1, keepdims=True)
    center = values - mean_v
    inv_std = lax.rsqrt(jnp.mean(center * center, axis=-1, keepdims=True) + norm_eps)
    return center * inv_std, inv_std


def normalize_back(grad_hat, normed, inv_std):
    return inv_std * (
        grad_hat
        - jnp.mean(grad_hat, axis=-1, keepdims=True)
        - normed * jnp.mean(grad_hat * normed, axis=-1, keepdims=True)
    )


def gelu_exact(values):
    return jax.nn.gelu(values, approximate=False)


def mm(a, b, contract):
    return lax.dot_general(a, b, (contract, ((), ())), preferred_element_type=f32)


def combine_pool(part_one, part_two):
    top_a, total_a, sum_a = part_one
    top_b, total_b, sum_b = part_two
    row_top = jnp.maximum(top_a, top_b)
    factor_a = jnp.exp(top_a - row_top)
    factor_b = jnp.exp(top_b - row_top)
    return (
        row_top,
        total_a * factor_a + total_b * factor_b,
        sum_a * factor_a[:, :, None] + sum_b * factor_b[:, :, None],
    )


def attend(q, k, v, q_seg, k_seg, scale):
    scores = jnp.einsum("qhd,khd->hqk", q, k, preferred_element_type=f32) * scale
    scores = jnp.where((q_seg[:, None] == k_seg[None, :])[None], scores, masked_value)
    top = jnp.max(scores, axis=-1, keepdims=True)
    exp_scores = jnp.exp(scores - top)
    total = jnp.sum(exp_scores, axis=-1, keepdims=True)
    probs = exp_scores / total
    context = jnp.einsum("hqk,khd->qhd", probs.astype(bf16), v, preferred_element_type=f32)
    return context.astype(bf16), probs


def attend_back(q, k, v, probs, d_ctx, scale):
    d_probs = jnp.einsum("qhd,khd->hqk", d_ctx, v, preferred_element_type=f32)
    delta = jnp.sum(probs * d_probs, axis=-1, keepdims=True)
    d_scores = (probs * (d_probs - delta)).astype(bf16)
    d_q = jnp.einsum("hqk,khd->qhd", d_scores, k, preferred_element_type=f32) * scale
    d_k = jnp.einsum("hqk,qhd->khd", d_scores, q, preferred_element_type=f32) * scale
    d_v = jnp.einsum("hqk,qhd->khd", probs.astype(bf16), d_ctx, preferred_element_type=f32)
    return d_q, d_k, d_v


def general_local(
    tokens,
    segments,
    labels,
    cotangent,
    w_qkv,
    b_qkv,
    w_out,
    b_out,
    ln1_gain,
    ln1_bias,
    w_in,
    b_in,
    w_back,
    b_back,
    ln2_gain,
    ln2_bias,
    s_proj,
    s_bias,
    s_query,
    s_mid,
    s_mid_bias,
    s_cls,
    s_cls_bias,
):
    seqs_local, width_row, cols_local = tokens.shape
    parts, rows, cols, seqs, sub = sizes(seqs_local)
    width = width_row * rows
    own = cols_local // (parts * sub)
    width_col = b_qkv.shape[1]
    heads_dev = width_col // HD
    hidden_col = b_in.shape[0]
    docs_count = labels.shape[1]
    class_count = s_cls.shape[1]
    student_width = s_proj.shape[1]
    row_index = lax.axis_index("row")
    col_index = lax.axis_index("col")
    dp_index = lax.axis_index("dp")
    seq_index = row_index // sub
    sub_index = row_index % sub
    score_scale = HD ** (-0.5)
    pool_scale = SHD ** (-0.5)
    query_heads = s_query.reshape(SH, SHD)
    doc_ids = jnp.arange(docs_count, dtype=jnp.int32)
    class_ids = jnp.arange(class_count, dtype=jnp.int32)

    w_qkv_all = gather_world(own_half(w_qkv)).reshape(cols, width, 3 * width_col)
    x_t = take_in(tokens)
    rest = jnp.concatenate([own_half(w_in), own_half(w_back), own_half(w_out).reshape(-1, width_col)], axis=1)
    rest_all = gather_world(rest)
    w_in_all = rest_all[..., :hidden_col].reshape(cols, width, hidden_col)
    w_back_all = rest_all[..., hidden_col : 2 * hidden_col].reshape(cols, width, hidden_col)
    w_out_all = rest_all[..., 2 * hidden_col :].reshape(cols, rows, width_col, width_row)
    w_out_all = w_out_all.transpose(0, 2, 1, 3).reshape(width, width)
    row_vectors = lax.all_gather(
        jnp.stack([b_out, ln1_gain, ln1_bias, b_back, ln2_gain, ln2_bias]), "row", axis=1, tiled=True
    )
    b_out_a, gain_one, bias_one, b_back_a, gain_two, bias_two = [row_vectors[i] for i in range(6)]
    b_qkv_all = lax.all_gather(b_qkv, "col")
    b_in_all = lax.all_gather(b_in, "col")
    s_proj_all = lax.all_gather(s_proj, "row", axis=0, tiled=True)
    whole_ints = lax.all_gather(jnp.concatenate([segments, labels], axis=1), "dp", axis=0, tiled=True)
    ints = lax.dynamic_index_in_dim(whole_ints, seq_index, 0, False)
    seq_len = segments.shape[1]
    seg_all, label_seq = ints[:seq_len], ints[seq_len:]
    seg_blocks = seg_all.reshape(cols, parts, sub, own)
    seg_q = lax.dynamic_index_in_dim(seg_blocks, dp_index, 1, False)
    seg_q = lax.dynamic_index_in_dim(seg_q, sub_index, 1, False)
    seg_own = lax.dynamic_index_in_dim(seg_q, col_index, 0, False)
    seg_q = seg_q.reshape(-1)

    x = x_t.T
    offsets = jnp.stack([b_qkv_all[:, 0], jnp.zeros_like(b_qkv_all[:, 0]), b_qkv_all[:, 1]], axis=1)
    offsets = offsets.reshape(cols, 3, heads_dev, HD).transpose(0, 2, 1, 3).reshape(cols, 1, -1)
    qkv = jnp.einsum("td,cdn->ctn", x, w_qkv_all, preferred_element_type=f32) + offsets
    qkv = swap_cols(qkv.astype(bf16)).reshape(cols, own, heads_dev, 3, HD)
    queries = qkv[:, :, :, 0].reshape(cols * own, heads_dev, HD)
    kv = gather_sequence(qkv[:, :, :, 1:].reshape(cols, own, -1), sub)
    kv = kv.reshape(seq_len, heads_dev, 2, HD)
    key_rows, value_rows = kv[:, :, 0], kv[:, :, 1]
    context, probs = attend(queries, key_rows, value_rows, seg_q, seg_all, score_scale)
    ctx = swap_cols(context.reshape(cols, own, width_col))
    ctx = ctx.transpose(1, 0, 2).reshape(own, width)

    attn_out = mm(ctx, w_out_all, ((1,), (0,))) + b_out_a
    normed_one, inv_one = normalize(x.astype(f32) + attn_out)
    hidden_one = normed_one * gain_one + bias_one
    hidden_low = hidden_one.astype(bf16)
    pre_act = jnp.einsum("td,cdn->ctn", hidden_low, w_in_all, preferred_element_type=f32)
    pre_act = pre_act + b_in_all[:, None, :]
    act = gelu_exact(pre_act).astype(bf16)
    ffn_out = jnp.einsum("ctn,cdn->td", act, w_back_all, preferred_element_type=f32) + b_back_a
    normed_two, inv_two = normalize(hidden_one + ffn_out)
    layer_out = (normed_two * gain_two + bias_two).astype(bf16)
    out = give_back(layer_out.T, seqs_local)

    student_h = mm(layer_out, s_proj_all, ((1,), (0,))) + s_bias
    head_parts = student_h.reshape(own, SH, SHD)
    pool_logit = jnp.sum(head_parts * query_heads, axis=-1) * pool_scale
    member = (seg_own[:, None] == doc_ids[None, :])[:, :, None]
    masked = jnp.where(member, pool_logit[:, None, :], masked_value)
    local_top = jnp.max(masked, axis=0)
    local_exp = jnp.where(member, jnp.exp(masked - local_top[None]), 0.0)
    local_total = jnp.sum(local_exp, axis=0)
    local_sum = jnp.einsum("tdh,thk->dhk", local_exp, head_parts, precision=highest)
    stats = jnp.concatenate([local_top[..., None], local_total[..., None], local_sum], axis=-1)
    stats = lax.all_gather(stats, ("dp", "col"))
    if sub > 1:
        stats = lax.all_gather(stats, "row", axis=0, tiled=True, axis_index_groups=row_groups(rows, sub))
    tops, totals, sums = stats[..., 0], stats[..., 1], stats[..., 2:]
    doc_top = jnp.max(tops, axis=0)
    factors = jnp.exp(tops - doc_top[None])
    doc_total = jnp.sum(totals * factors, axis=0)
    pooled_heads = jnp.sum(sums * factors[..., None], axis=0) / doc_total[:, :, None]
    pooled = pooled_heads.reshape(docs_count, student_width)
    middle = jnp.tanh(jnp.dot(pooled, s_mid, precision=highest) + s_mid_bias)
    logit_rows = jnp.dot(middle, s_cls, precision=highest) + s_cls_bias
    logits = lax.all_gather(logit_rows, "row")[::sub]
    logits = lax.dynamic_slice_in_dim(logits, dp_index * seqs_local, seqs_local)
    logit_top = jnp.max(logit_rows, axis=-1, keepdims=True)
    logit_exp = jnp.exp(logit_rows - logit_top)
    one_hot = (label_seq[:, None] == class_ids[None, :]).astype(f32)
    d_logits = logit_exp / jnp.sum(logit_exp, axis=-1, keepdims=True) - one_hot
    g_cls = jnp.dot(middle.T, d_logits, precision=highest)
    g_cls_bias = jnp.sum(d_logits, axis=0)
    d_middle = jnp.dot(d_logits, s_cls.T, precision=highest) * (1.0 - middle * middle)
    g_mid = jnp.dot(pooled.T, d_middle, precision=highest)
    g_mid_bias = jnp.sum(d_middle, axis=0)
    d_pooled = jnp.dot(d_middle, s_mid.T, precision=highest).reshape(docs_count, SH, SHD)
    shares = jnp.where(member, jnp.exp(masked - doc_top[None]), 0.0) / doc_total[None]
    d_share = jnp.einsum("dhk,thk->tdh", d_pooled, head_parts, precision=highest)
    base_term = jnp.sum(d_pooled * pooled_heads, axis=-1)
    d_pool_logit = jnp.sum(shares * (d_share - base_term[None]), axis=1)
    d_heads = jnp.einsum("tdh,dhk->thk", shares, d_pooled, precision=highest)
    d_heads = d_heads + d_pool_logit[:, :, None] * query_heads[None] * pool_scale
    g_query = (jnp.sum(d_pool_logit[:, :, None] * head_parts, axis=0) * pool_scale).reshape(-1)
    d_student = d_heads.reshape(own, student_width)
    g_sbias = jnp.sum(d_student, axis=0)
    g_sproj = jnp.dot(layer_out.astype(f32).T, d_student, precision=highest)

    d_out = take_in(cotangent).T.astype(f32)
    g_ln2_gain = jnp.sum(d_out * normed_two, axis=0)
    g_ln2_bias = jnp.sum(d_out, axis=0)
    d_resid_two = normalize_back(d_out * gain_two, normed_two, inv_two)
    d_ffn = d_resid_two.astype(bf16)
    g_back_bias = jnp.sum(d_ffn.astype(f32), axis=0)
    g_back = jnp.einsum("td,ctn->cdn", d_ffn, act, preferred_element_type=f32)
    d_act = jnp.einsum("td,cdn->ctn", d_ffn, w_back_all, preferred_element_type=f32)
    _, gelu_fn = jax.vjp(gelu_exact, pre_act)
    d_pre = gelu_fn(d_act)[0].astype(bf16)
    g_in_bias = jnp.sum(d_pre.astype(f32), axis=1)
    g_in = jnp.einsum("td,ctn->cdn", hidden_low, d_pre, preferred_element_type=f32)
    d_hidden_one = d_resid_two + jnp.einsum(
        "ctn,cdn->td", d_pre, w_in_all, preferred_element_type=f32
    )
    g_ln1_gain = jnp.sum(d_hidden_one * normed_one, axis=0)
    g_ln1_bias = jnp.sum(d_hidden_one, axis=0)
    d_resid_one = normalize_back(d_hidden_one * gain_one, normed_one, inv_one)
    d_attn = d_resid_one.astype(bf16)
    g_out_bias = jnp.sum(d_attn.astype(f32), axis=0)
    g_out = mm(ctx, d_attn, ((0,), (0,)))
    d_ctx = mm(d_attn, w_out_all, ((1,), (1,))).astype(bf16)
    d_ctx = swap_cols(d_ctx.reshape(own, cols, width_col).transpose(1, 0, 2))
    d_ctx = d_ctx.reshape(cols * own, heads_dev, HD)
    d_q, d_k, d_v = attend_back(queries, key_rows, value_rows, probs, d_ctx, score_scale)
    d_kv = jnp.stack([d_k, d_v], axis=2).astype(bf16).reshape(seq_len, -1)
    d_kv = scatter_sequence(d_kv, cols, sub).reshape(cols, own, heads_dev, 2, HD)
    d_q = d_q.astype(bf16).reshape(cols, own, heads_dev, 1, HD)
    d_qkv = jnp.concatenate([d_q, d_kv], axis=3).reshape(cols, own, 3 * width_col)
    d_qkv = swap_cols(d_qkv)
    g_qkv_bias = jnp.sum(d_qkv.astype(f32), axis=1).reshape(cols, heads_dev, 3, HD)
    g_qkv = jnp.einsum("td,ctn->cdn", x, d_qkv, preferred_element_type=f32)
    d_tokens = d_resid_one + jnp.einsum("ctn,cdn->td", d_qkv, w_qkv_all, preferred_element_type=f32)
    grad_tokens = give_back(d_tokens.astype(bf16).T, seqs_local).astype(f32)

    g_out = g_out.reshape(cols, width_col, rows, width_row).transpose(0, 2, 1, 3)
    g_out = g_out.reshape(cols, rows, width_row, width_col)
    model = jnp.concatenate(
        [
            g_in.reshape(cols, rows, width_row, hidden_col).astype(bf16),
            g_back.reshape(cols, rows, width_row, hidden_col).astype(bf16),
            g_out.astype(bf16),
        ],
        axis=-1,
    )
    model = scatter_world(model).astype(f32)
    g_qkv = scatter_world(g_qkv.reshape(cols, rows, width_row, 3 * width_col).astype(bf16)).astype(f32)
    once = 1.0 / (parts * cols * sub)
    small = (
        g_qkv_bias[:, :, 0].reshape(cols, width_col),
        g_qkv_bias[:, :, 2].reshape(cols, width_col),
        g_in_bias,
        g_out_bias,
        g_ln1_gain,
        g_ln1_bias,
        g_back_bias,
        g_ln2_gain,
        g_ln2_bias,
        g_sproj,
        g_sbias,
        g_query,
        g_mid * once,
        g_mid_bias * once,
        g_cls * once,
        g_cls_bias * once,
    )
    small = lax.psum(small, WORLD)

    def at_col(part):
        return lax.dynamic_index_in_dim(part, col_index, 0, False)

    def at_row(part):
        return lax.dynamic_slice_in_dim(part, row_index * width_row, width_row)

    return (
        out,
        logits,
        grad_tokens,
        g_qkv,
        jnp.stack([at_col(small[0]), at_col(small[1])]),
        model[:, 2 * hidden_col :].reshape(width_col, width_row),
        at_row(small[3]),
        at_row(small[4]),
        at_row(small[5]),
        model[:, :hidden_col],
        at_col(small[2]),
        model[:, hidden_col : 2 * hidden_col],
        at_row(small[6]),
        at_row(small[7]),
        at_row(small[8]),
        at_row(small[9]),
        small[10],
        small[11],
        small[12],
        small[13],
        small[14],
        small[15],
    )


MESH = pl.DeviceIdType.MESH
HBM = pl.BlockSpec(memory_space=pl.ANY)


def place():
    return lax.axis_index("dp"), lax.axis_index("row"), lax.axis_index("col")


def greet(peers, guarded=()):
    barrier = pltpu.get_barrier_semaphore()
    for peer in peers:
        pl.semaphore_signal(barrier, inc=1, device_id=peer, device_id_type=MESH)
    for there, peer in guarded:

        @pl.when(there)
        def _():
            pl.semaphore_signal(barrier, inc=1, device_id=peer, device_id_type=MESH)

    amount = len(peers)
    for there, _ in guarded:
        amount = amount + there.astype(jnp.int32)
    pl.semaphore_wait(barrier, amount)


def rcopy(src, dst, send, recv, peer):
    return pltpu.make_async_remote_copy(
        src_ref=src, dst_ref=dst, send_sem=send, recv_sem=recv, device_id=peer, device_id_type=MESH
    )


def take_copies(src, out, local, send, recv):
    d, r, c = place()
    own = out.shape[2]
    moves = []
    for i in range(2):
        for far in range(2):
            row, core = 2 * d + i, d ^ far
            piece = src.at[i, :, pl.ds(pl.multiple_of(core * own, own), own)]
            here = (row == r) if far == 0 else None

            def start(piece=piece, row=row, core=core, slot=2 * i + far, here=here):
                def away():
                    rcopy(piece, out.at[r], send.at[slot], recv.at[r], (core, row, c)).start()

                if here is None:
                    away()
                else:
                    pl.when(jnp.logical_not(here))(away)

                    @pl.when(here)
                    def _():
                        pltpu.make_async_copy(piece, out.at[r], local).start()

            def wait(piece=piece, row=row, core=core, slot=2 * i + far, here=here):
                def away():
                    rcopy(piece, out.at[r], send.at[slot], recv.at[r], (core, row, c)).wait_send()

                if here is None:
                    away()
                else:
                    pl.when(jnp.logical_not(here))(away)

                    @pl.when(here)
                    def _():
                        pltpu.make_async_copy(piece, out.at[r], local).wait()

            moves.append((start, wait))
    for row in range(4):

        def arrive(row=row):
            @pl.when(jnp.logical_not((row == r) & (r // 2 == d)))
            def _():
                piece = src.at[0, :, pl.ds(0, own)]
                rcopy(piece, out.at[row], send.at[0], recv.at[row], (d, r, c)).wait_recv()

        moves.append((lambda: None, arrive))
    return moves


VM = pl.BlockSpec(memory_space=pltpu.VMEM)


def head_kernel(scale, *refs):
    (w_qkv_ref, w_out_ref, w_in_ref, w_back_ref, tok, cot, ints), refs = refs[:7], refs[7:]
    (b_qkv_ref, b_in_ref, proj_ref), row_vecs, refs = refs[:3], refs[3:9], refs[9:]
    (a_out, b_out, c_out, tok_out, cot_out, ints_out, q_out, kv_out), refs = refs[:8], refs[8:]
    (wo_out, vec_all, b_in_all, proj_all, ctx_own, lse_ref, ctx_out), refs = refs[:7], refs[7:]
    (shard_a, shard_v, vec_out, x_nat, q_src, kv_src, kn, q3, s_scr, o_scr, kcol), refs = refs[:11], refs[11:]
    own_sem, zs, zr, xs, xr, ys, yr, cs, cr, ps, pr, tl, ts, tr, il, hs, hr, hps, hpr, xl, xs2, xr2, vs, vr = refs
    d, r, c = place()
    kinds = 4
    part = w_in_ref.shape[0] // 2
    mine = pl.ds(pl.multiple_of(d * part, 16), part)
    feats = tok_out.shape[1]
    shards = [shard_a.at[mine], shard_v.at[pl.ds(pl.multiple_of(d * 48, 8), 48)], w_in_ref.at[mine], w_back_ref.at[mine]]
    outs = [a_out, vec_out, b_out, c_out]
    cols = 4
    xn, yn, pn = (d, r ^ 1, c), (d, r ^ 2, c), (1 - d, r, c)
    up, down = (d, r, c + 1), (d, r, c - 1)
    has_up, has_down = c < cols - 1, c > 0
    columns = w_qkv_ref.shape[1]
    shard_a[:, :columns] = w_qkv_ref[...]
    shard_a[:, columns:] = w_out_ref[...]
    heads = columns // (3 * HD)
    pieces = []
    for h in range(heads):
        spot = slice(h * HD, (h + 1) * HD)
        pieces += [b_qkv_ref[0:1, spot], jnp.zeros((1, HD), f32), b_qkv_ref[1:2, spot]]
    bias_lanes = -(-columns // 128) * 128
    pieces.append(jnp.zeros((1, bias_lanes - columns), f32))
    line = jnp.concatenate(pieces, axis=1)
    at = 0
    for i in range(bias_lanes // 128):
        shard_v[at : at + 1] = line[:, i * 128 : (i + 1) * 128]
        at += 1
    for ref in row_vecs:
        line = jnp.concatenate([ref[...], jnp.zeros((1, 256 - feats), f32)], axis=1)
        for i in range(2):
            shard_v[at : at + 1] = line[:, i * 128 : (i + 1) * 128]
            at += 1
    for i in range(b_in_ref.shape[1] // 128):
        shard_v[at : at + 1] = b_in_ref[:, i * 128 : (i + 1) * 128]
        at += 1
    proj_at, proj_rows = 48, feats // 4
    for i in range(at, proj_at):
        shard_v[i : i + 1] = jnp.zeros((1, 128), f32)
    shard_v[proj_at:] = proj_ref[pl.ds(pl.multiple_of(c * proj_rows, 16), proj_rows)].astype(f32)

    greet(plane_peers() + [(d, r, c ^ j) for j in (1, 2, 3)])
    moves = take_copies(tok, tok_out, tl, ts, tr)
    for start, _ in moves:
        start()
    late_moves = take_copies(cot, cot_out, xl, xs2, xr2)
    pltpu.make_async_copy(ints, ints_out.at[d], il.at[0]).start()
    rcopy(ints, ints_out.at[d], il.at[1], il.at[2], pn).start()
    halves = [part // 2, 24, part // 2, part // 2]

    def z_send(k, at, way, hop):
        src = shards[k] if hop == 1 else outs[k].at[at, r, d]
        return rcopy(
            src, outs[k].at[at, r, d], zs.at[k, way, hop - 1], zr.at[k, way, hop - 1], up if way == 0 else down
        )

    def src_of(k, at, own):
        return shards[k] if own else outs[k].at[at, r, d]

    def to_x(k, at, own):
        return rcopy(src_of(k, at, own), outs[k].at[at, r, d], xs.at[k, at], xr.at[k, at], xn)

    def to_y(k, at, own):
        return rcopy(src_of(k, at, own), outs[k].at[at, r, d], ys.at[k, at], yr.at[k, at], yn)

    def to_p(k, at, own):
        return rcopy(src_of(k, at, own), outs[k].at[at, r, d], ps.at[k, at, 0], pr.at[k, at, 0], pn)

    def relay(k, at, which):
        row = r ^ 1 if which == 0 else r ^ 2
        ref = outs[k].at[at, row, d, pl.ds(which * halves[k], halves[k])]
        return rcopy(ref, ref, cs.at[k, at, which], cr.at[k, at, which], yn if which == 0 else xn)

    def pass_p(k, at, bit):
        ref = outs[k].at[at, r ^ bit, d]
        return rcopy(ref, ref, ps.at[k, at, bit], pr.at[k, at, bit], pn)

    def got_x(k, at):
        ref = outs[k].at[at, r ^ 1, d]
        rcopy(ref, ref, xs.at[k, at], xr.at[k, at], xn).wait_recv()

    def got_y(k, at):
        ref = outs[k].at[at, r ^ 2, d]
        rcopy(ref, ref, ys.at[k, at], yr.at[k, at], yn).wait_recv()

    def got_corner(k, at):
        for which in range(2):
            ref = outs[k].at[at, r ^ 3, d, pl.ds(which * halves[k], halves[k])]
            rcopy(ref, ref, cs.at[k, at, which], cr.at[k, at, which], xn).wait_recv()

    def got_p(k, at, bit):
        ref = outs[k].at[at, r ^ bit, 1 - d]
        rcopy(ref, ref, ps.at[k, at, bit], pr.at[k, at, bit], pn).wait_recv()

    def set_out(k):
        @pl.when(has_up)
        def _():
            z_send(k, c, 0, 1).start()

        @pl.when(has_down)
        def _():
            z_send(k, c, 1, 1).start()

    for k in range(kinds):
        pltpu.make_async_copy(shards[k], outs[k].at[c, r, d], own_sem.at[k]).start()
        if k < kinds - 1:
            set_out(k)

    def spread(k, at, own):
        to_x(k, at, own).start()
        to_y(k, at, own).start()
        to_p(k, at, own).start()

    def onward(k, at):
        got_x(k, at)
        relay(k, at, 0).start()
        pass_p(k, at, 1).start()
        got_y(k, at)
        relay(k, at, 1).start()
        pass_p(k, at, 2).start()

    steps = [(0, 0)] + [(way, hop) for hop in (1, 2, 3) for way in (0, 1)]
    jobs = [(group, way, hop) for group in ((0, 1), (2,), (3,)) for way, hop in steps]

    def at_of(way, hop):
        return c - hop if way == 0 else c + hop

    def valid(way, hop):
        return c >= hop if way == 0 else c + hop < cols

    def guard(way, hop, body):
        if hop == 0:
            body()
        else:
            pl.when(valid(way, hop))(body)

    def first(group, way, hop):
        def body():
            at = at_of(way, hop)
            for k in group:
                if hop:
                    z_send(k, at, way, hop).wait_recv()
                    if hop < 3:
                        can = has_up if way == 0 else has_down

                        @pl.when(can)
                        def _():
                            z_send(k, at, way, hop + 1).start()

                spread(k, at, hop == 0)

        guard(way, hop, body)

    def second(group, way, hop):
        def body():
            for k in group:
                onward(k, at_of(way, hop))

        guard(way, hop, body)

    def third(group, way, hop):
        def body():
            at = at_of(way, hop)
            for k in group:
                got_corner(k, at)
                pass_p(k, at, 3).start()

        guard(way, hop, body)

    def settle(k):
        pltpu.make_async_copy(shards[k], outs[k].at[c, r, d], own_sem.at[k]).wait()
        for way, hop in steps:

            def body():
                for bit in range(4):
                    got_p(k, at_of(way, hop), bit)

            guard(way, hop, body)

    def kv(j):
        return rcopy(kv_src.at[c ^ j], kv_out.at[c, d], hs.at[0, j], hr.at[0, j], (d, r, c ^ j))

    def q(j):
        return rcopy(q_src.at[c ^ j], q_out.at[c], hs.at[1, j], hr.at[1, j], (d, r, c ^ j))

    def pair(j):
        src = kv_src.at[c] if j == 0 else kv_out.at[c ^ j, d]
        return rcopy(src, kv_out.at[c ^ j, d], hps.at[j], hpr.at[j], pn)

    lanes = bias_lanes

    def prepare():
        for _, wait in moves:
            wait()
        x_nat[...] = tok_out[...].reshape(4 * feats, -1).astype(f32).T.astype(bf16)

    def project(j):
        to = c ^ j
        weights = a_out[to, :, :, :, :lanes].reshape(-1, lanes)
        bias = vec_out[to, r, 0, pl.ds(0, 8)]
        bias = jnp.concatenate([bias[i : i + 1] for i in range(lanes // 128)], axis=1)
        made = jnp.dot(x_nat[...], weights, preferred_element_type=f32) + bias
        made = made.T.astype(bf16)
        for h in range(heads):
            rows = pl.ds(h * HD, HD)
            q_src[to, rows] = made[3 * h * HD : (3 * h + 1) * HD]
            kv_src[to, rows] = made[(3 * h + 1) * HD : (3 * h + 2) * HD]
            kv_src[to, pl.ds(wide + h * HD, HD)] = made[(3 * h + 2) * HD : (3 * h + 3) * HD]
        if j:
            kv(j).start()
            q(j).start()
        else:
            pair(0).start()
            kv_out[c, d] = kv_src[c]
            q_out[c] = q_src[c]

    def spread_out(at):
        for row in range(4):
            block = a_out[at, row, :, :, columns:].reshape(-1, feats)
            wo_out[pl.ds(at * wide, wide), row * feats : (row + 1) * feats] = block

    def unpack():
        first = bias_lanes // 128
        for i in range(6):
            for row in range(4):
                line = vec_out[0, row, 0, pl.ds(first + 2 * i, 2)]
                line = jnp.concatenate([line[0:1], line[1:2]], axis=1)
                vec_all[i : i + 1, row * feats : (row + 1) * feats] = line[:, :feats]
        vec_all[6:8] = jnp.zeros((2, 4 * feats), f32)
        first += 12
        for at in range(4):
            for i in range(b_in_all.shape[1] // 128):
                b_in_all[at : at + 1, i * 128 : (i + 1) * 128] = vec_out[at, 0, 0, pl.ds(first + i, 1)]
            for row in range(4):
                rows = pl.ds(row * feats + at * proj_rows, proj_rows)
                proj_all[rows] = vec_out[at, row, 1].astype(bf16)

    tiles = 8
    own = x_nat.shape[0]

    def segment(tile):
        return ints_out[r // 2, r % 2, pl.ds(tile, 1)].astype(f32)

    def collect():
        for j in (1, 2, 3):
            kv(j).wait_recv()
            pair(j).start()
        pltpu.make_async_copy(ints, ints_out.at[d], il.at[0]).wait()
        rcopy(ints, ints_out.at[1 - d], il.at[1], il.at[2], pn).wait()
        for tile in range(tiles):
            kcol[tile] = jnp.broadcast_to(segment(tile), (128, own)).T
        for j in (1, 2, 3):
            q(j).wait_recv()
        for j in range(4):
            pair(j).wait_recv()

        @pl.loop(0, 4)
        def _(at):
            for core in range(2):
                kn[2 * at + core] = kv_out[at, core, pl.ds(0, wide)].astype(f32).T.astype(bf16)

    def attend_block(block):
        block_rows(q_out.at[pl.ds(block, 1)], heads, scale, q3)
        here = 2 * block + d
        low, high = jnp.maximum(here - 4, 0), jnp.minimum(here + 5, tiles)
        qseg = jnp.concatenate([segment(here)] * heads, axis=1)

        def one(j, top):
            s = jnp.dot(kn[j], q3[...], preferred_element_type=f32)
            same = jnp.concatenate([kcol[j]] * (heads * own // 128), axis=1) == qseg
            s = jnp.where(same, s, masked_value)
            s_scr[j] = s
            return jnp.maximum(top, jnp.max(s, axis=0, keepdims=True))

        top = lax.fori_loop(low, high, one, jnp.full((1, heads * own), masked_value, f32))
        o_scr[...] = jnp.zeros_like(o_scr)

        def two(j, total):
            p = jnp.exp(s_scr[j] - top)
            low_p = p.astype(bf16)
            for h in range(heads):
                rows = pl.ds(h * HD, HD)
                v = kv_out[j // 2, j % 2, pl.ds(wide + h * HD, HD)]
                o_scr[rows] += jnp.dot(v, low_p[:, h * own : (h + 1) * own], preferred_element_type=f32)
            return total + jnp.sum(p, axis=0, keepdims=True)

        total = lax.fori_loop(low, high, two, jnp.zeros((1, heads * own), f32))
        for h in range(heads):
            rows = pl.ds(h * HD, HD)
            ctx_own[block, rows] = (o_scr[rows] / total[:, h * own : (h + 1) * own]).astype(bf16)
        lse_ref[block] = top + jnp.log(total)

    def back_copy(j):
        return rcopy(ctx_own.at[c ^ j], ctx_out.at[c], vs.at[j], vr.at[j], (d, r, c ^ j))

    def attend(j):
        attend_block(c ^ j)
        if j:
            back_copy(j).start()
        else:
            ctx_out[c] = ctx_own[c]

    wide = q_src.shape[1]
    lag = 3
    ready = len(steps) + 2 * lag

    def do(**stages):
        for stage, numbers in stages.items():
            for n in numbers:
                {"f": first, "s": second, "t": third}[stage](*jobs[n])

    for i in range(ready):
        if i == ready - 4:
            set_out(kinds - 1)
        do(f=[i], s=[i - lag] if i >= lag else [], t=[i - 2 * lag] if i >= 2 * lag else [])
    prepare()
    settle(0)
    settle(1)
    project(3)
    do(f=[13], s=[10], t=[7])
    project(2)
    do(f=[14], s=[11], t=[8])
    project(1)
    do(s=[12], t=[9])
    project(0)
    do(s=[13], t=[10])
    for start, _ in late_moves:
        start()
    for at in range(3):
        spread_out(at)
        do(t=[11 + at])
    spread_out(3)
    do(s=[14])
    unpack()
    collect()
    attend(3)
    do(f=[15, 16])
    attend(2)
    do(f=[17, 18], s=[15])
    attend(1)
    do(f=[19, 20], s=[16], t=[14])
    attend(0)
    for n in (17, 18, 19, 20):
        do(s=[n], t=[n - 2])
    do(t=[19, 20])

    for k in range(kinds):
        if k > 1:
            settle(k)
        for way, hop in steps:

            def body():
                at = at_of(way, hop)
                own = hop == 0
                to_x(k, at, own).wait_send()
                to_y(k, at, own).wait_send()
                to_p(k, at, own).wait_send()
                for which in range(2):
                    relay(k, at, which).wait_send()
                for bit in (1, 2, 3):
                    pass_p(k, at, bit).wait_send()
                if hop < 3:
                    if own:

                        @pl.when(has_up)
                        def _():
                            z_send(k, c, 0, 1).wait_send()

                        @pl.when(has_down)
                        def _():
                            z_send(k, c, 1, 1).wait_send()
                    else:
                        can = has_up if way == 0 else has_down

                        @pl.when(can)
                        def _():
                            z_send(k, at, way, hop + 1).wait_send()

            guard(way, hop, body)
    for j in (1, 2, 3):
        q(j).wait_send()
        kv(j).wait_send()
        back_copy(j).wait()
    for j in range(4):
        pair(j).wait_send()
    for _, wait in late_moves:
        wait()


VM = pl.BlockSpec(memory_space=pltpu.VMEM)


def head_fast(weights, tokens, cotangent, ints, vectors, scale, cid):
    kinds = 4
    dma = pltpu.SemaphoreType.DMA
    _, feats, cols = tokens.shape
    own = cols // 2
    width = 4 * feats
    part = feats // 2
    wide = weights[0].shape[1] // 3
    full = 4 * wide
    heads = wide // HD
    shape = jax.ShapeDtypeStruct
    piece = shape((4, wide, own), bf16)
    taken = shape((4, feats, own), bf16)
    weight = shape((4, 4, 2, part, weights[2].shape[1]), bf16)
    hidden = weights[2].shape[1]
    student_width = vectors[2].shape[1]
    return pl.pallas_call(
        functools.partial(head_kernel, scale),
        out_shape=[
            shape((4, 4, 2, part, full), bf16), weight, weight, taken, taken, shape((2,) + ints.shape, ints.dtype),
            piece, shape((4, 2, 2 * wide, own), bf16), shape((4 * wide, width), bf16), shape((8, width), f32),
            shape((4, hidden), f32), shape((width, student_width), bf16), piece,
            shape((4, 1, heads * own), f32), piece,
        ],
        in_specs=[VM, VM] + [HBM] * 5 + [VM] * len(vectors),
        out_specs=[VM, HBM, HBM] + [VM] * 12,
        scratch_shapes=[
            pltpu.VMEM((feats, full), bf16),
            pltpu.VMEM((96, 128), f32),
            pltpu.VMEM((4, 4, 2, 48, 128), f32),
            pltpu.VMEM((own, width), bf16),
            pltpu.VMEM((4, wide, own), bf16),
            pltpu.VMEM((4, 2 * wide, own), bf16),
            pltpu.VMEM((8, own, wide), bf16),
            pltpu.VMEM((wide, heads * own), bf16),
            pltpu.VMEM((8, own, heads * own), f32),
            pltpu.VMEM((wide, own), f32),
            pltpu.VMEM((8, own, 128), f32),
            dma((kinds,)),
            dma((kinds, 2, 3)), dma((kinds, 2, 3)),
            dma((kinds, 4)), dma((kinds, 4)),
            dma((kinds, 4)), dma((kinds, 4)),
            dma((kinds, 4, 2)), dma((kinds, 4, 2)),
            dma((kinds, 4, 4)), dma((kinds, 4, 4)),
            dma, dma((4,)), dma((4,)), dma((3,)),
            dma((2, 4)), dma((2, 4)), dma((4,)), dma((4,)),
            dma, dma((4,)), dma((4,)), dma((4,)), dma((4,)),
        ],
        compiler_params=pltpu.CompilerParams(
            collective_id=cid, has_side_effects=True, vmem_limit_bytes=56 * 1024 * 1024
        ),
        name="head",
    )(*weights, tokens, cotangent, ints, *vectors)


def scatter_core(grads, outs, scratch, begin, during, late=0, gap=0):
    kinds = len(grads)
    (acc, precv, xr1, yr1, xr2, yr2, zup, zdn, fin) = scratch[:9]
    (ls, ps, pr, xs1, xm1, ys1, ym1, xs2, xm2, ys2, ym2, us, um, ds, dm, fs, fm, os) = scratch[9:]
    d, r, c = place()
    cols = 4
    chunks = kinds * cols
    xn, yn, pn = (d, r ^ 1, c), (d, r ^ 2, c), (1 - d, r, c)
    up, down = (d, r, c + 1), (d, r, c - 1)
    half = acc.shape[2] // 2
    first, last = pl.ds(0, half), pl.ds(half, half)

    def split(i):
        k = i // cols
        j = i - k * cols
        at = jnp.where(j == 0, 0, jnp.where(j == 1, 3, j - 1))
        return k, at

    def at_static(i):
        return i // cols, (0, 3, 1, 2)[i % cols]

    def load(i):
        k, at = at_static(i)
        return pltpu.make_async_copy(grads[k].at[at, :, d], acc.at[i], ls.at[i])

    def pair(i):
        k, at = at_static(i)
        return rcopy(grads[k].at[at, :, 1 - d], precv.at[i], ps.at[i], pr.at[i], pn)

    def launch(i):
        pair(i).start()
        load(i).start()

    for i in range((kinds - late) * cols):
        launch(i)
    begin()

    def x1(i, j):
        return rcopy(acc.at[i, r ^ 1 ^ (2 * j), first], xr1.at[i, j], xs1.at[i, j], xm1.at[i, j], xn)

    def y1(i, j):
        return rcopy(acc.at[i, r ^ 2 ^ j, last], yr1.at[i, j], ys1.at[i, j], ym1.at[i, j], yn)

    def y2(i):
        return rcopy(acc.at[i, r ^ 2, first], yr2.at[i], ys2.at[i], ym2.at[i], yn)

    def x2(i):
        return rcopy(acc.at[i, r ^ 1, last], xr2.at[i], xs2.at[i], xm2.at[i], xn)

    def to_up(i):
        return rcopy(acc.at[i, r], zup.at[i], us.at[i], um.at[i], up)

    def to_down(i):
        return rcopy(acc.at[i, r], zdn.at[i], ds.at[i], dm.at[i], down)

    def stage1(i):
        pltpu.make_async_copy(precv.at[i], acc.at[i], ls.at[i]).wait()
        rcopy(acc.at[i], precv.at[i], ps.at[i], pr.at[i], pn).wait_recv()

        @pl.loop(0, 4)
        def _(row):
            acc[i, row] = acc[i, row] + precv[i, row]

        x1(i, 1).start()
        y1(i, 1).start()
        x1(i, 0).start()
        y1(i, 0).start()

    def stage2(i):
        x1(i, 1).wait_recv()
        acc[i, r ^ 2, first] = acc[i, r ^ 2, first] + xr1[i, 1]
        y2(i).start()
        y1(i, 1).wait_recv()
        acc[i, r ^ 1, last] = acc[i, r ^ 1, last] + yr1[i, 1]
        x2(i).start()
        x1(i, 0).wait_recv()
        acc[i, r, first] = acc[i, r, first] + xr1[i, 0]
        y1(i, 0).wait_recv()
        acc[i, r, last] = acc[i, r, last] + yr1[i, 0]

    def stage3(i):
        y2(i).wait_recv()
        acc[i, r, first] = acc[i, r, first] + yr2[i]
        x2(i).wait_recv()
        acc[i, r, last] = acc[i, r, last] + xr2[i]

    def stage4(i, hops):
        k, at = split(i)

        @pl.when((at > c) & (c == hops))
        def _():
            @pl.when(c > 0)
            def _():
                to_up(i).wait_recv()
                acc[i, r] = acc[i, r] + zup[i]

            to_up(i).start()

        @pl.when((at < c) & (cols - 1 - c == hops))
        def _():
            @pl.when(c < cols - 1)
            def _():
                to_down(i).wait_recv()
                acc[i, r] = acc[i, r] + zdn[i]

            to_down(i).start()

        @pl.when((at == c) & (jnp.maximum(c, cols - 1 - c) == hops))
        def _():
            @pl.when(c > 0)
            def _():
                to_up(i).wait_recv()
                acc[i, r] = acc[i, r] + zup[i]

            @pl.when(c < cols - 1)
            def _():
                to_down(i).wait_recv()
                acc[i, r] = acc[i, r] + zdn[i]

            fin[k, d] = acc[i, r]
            rcopy(fin.at[k, d], fin.at[k, d], fs.at[k], fm.at[k], pn).start()

    stages = [(0, stage1), (2, stage2), (4, stage3)]
    stages += [(5 + h, functools.partial(lambda h, i: stage4(i, h), h)) for h in range(cols)]
    ending = stages[-1][0]

    assert len(during) <= chunks + gap + ending
    early = (kinds - late) * cols

    @pl.loop(0, chunks + gap + ending)
    def _(step):
        for i, extra in enumerate(during):
            pl.when(step == i)(functools.partial(extra, launch))

        for lag, stage in stages:

            spot = step - lag
            there = (spot >= 0) & (spot < early) | (spot >= early + gap) & (spot < chunks + gap)

            @pl.when(there)
            def _():
                stage(jnp.where(spot < early, spot, spot - gap))

    @pl.loop(0, chunks)
    def _(i):
        k, at = split(i)
        rcopy(acc.at[i], precv.at[i], ps.at[i], pr.at[i], pn).wait_send()
        for j in range(2):
            x1(i, j).wait_send()
            y1(i, j).wait_send()
        y2(i).wait_send()
        x2(i).wait_send()

        @pl.when(at > c)
        def _():
            to_up(i).wait_send()

        @pl.when(at < c)
        def _():
            to_down(i).wait_send()

    for k in range(kinds):
        rcopy(fin.at[k, 1 - d], fin.at[k, 1 - d], fs.at[k], fm.at[k], pn).wait()
        pltpu.make_async_copy(fin.at[k], outs[k], os.at[k]).start()
    for k in range(kinds):
        pltpu.make_async_copy(fin.at[k], outs[k], os.at[k]).wait()

def scatter_scratch(kinds, n, w, dt):
    dma = pltpu.SemaphoreType.DMA
    chunks = kinds * 4
    return [
        pltpu.VMEM((chunks, 4, n, w), dt),
        pltpu.VMEM((chunks, 4, n, w), dt),
        pltpu.VMEM((chunks, 2, n // 2, w), dt),
        pltpu.VMEM((chunks, 2, n // 2, w), dt),
        pltpu.VMEM((chunks, n // 2, w), dt),
        pltpu.VMEM((chunks, n // 2, w), dt),
        pltpu.VMEM((chunks, n, w), dt),
        pltpu.VMEM((chunks, n, w), dt),
        pltpu.VMEM((kinds, 2, n, w), dt),
        dma((chunks,)), dma((chunks,)), dma((chunks,)),
        dma((chunks, 2)), dma((chunks, 2)), dma((chunks, 2)), dma((chunks, 2)),
        dma((chunks,)), dma((chunks,)), dma((chunks,)), dma((chunks,)),
        dma((chunks,)), dma((chunks,)), dma((chunks,)), dma((chunks,)),
        dma((kinds,)), dma((kinds,)), dma((kinds,)),
    ]


def give_moves(src_ref, out_ref, local, send, recv):
    d, r, c = place()
    own = src_ref.shape[2]
    home = r // 2

    def slot(i, core):
        return out_ref.at[i, :, pl.ds(pl.multiple_of(core * own, own), own)]

    def move(row):
        return rcopy(src_ref.at[row], slot(r % 2, d), send.at[row], recv.at[r % 2, d], (home, row, c))

    def stay():
        return pltpu.make_async_copy(src_ref.at[r], slot(r % 2, d), local)

    def start():
        for row in range(4):

            @pl.when(jnp.logical_not((row == r) & (home == d)))
            def _():
                move(row).start()

        @pl.when(home == d)
        def _():
            stay().start()

    def finish():
        for row in range(4):

            @pl.when(jnp.logical_not((row == r) & (home == d)))
            def _():
                move(row).wait_send()

        @pl.when(home == d)
        def _():
            stay().wait()

        for i in range(2):
            for core in range(2):

                @pl.when(jnp.logical_not((2 * d + i == r) & (core == d)))
                def _():
                    rcopy(src_ref.at[0], slot(i, core), send.at[0], recv.at[i, core], (d, r, c)).wait_recv()

    return start, finish


def plane_peers():
    d, r, c = place()
    return [(d ^ (j // 4), r ^ (j % 4), c) for j in range(1, 8)]


def line_peers():
    d, r, c = place()
    return [(d ^ (j // 4), r, c ^ (j % 4)) for j in range(1, 8)]


def sum_steps(src, total, parts, sems):
    d, r, c = place()
    peers = [(1 - d, r, c), (d, r ^ 1, c), (d, r ^ 2, c), (d, r, c ^ 1), (d, r, c ^ 2)]
    bits = [d, r % 2, r // 2, c % 2, c // 2]
    rs, rr, gs, gr = sems
    count = len(peers)
    size = [src.shape[0] >> (i + 1) for i in range(count)]
    offset = [jnp.int32(0)]
    for i in range(count):
        offset.append(offset[i] + bits[i] * size[i])

    def rows(at, amount):
        return pl.ds(pl.multiple_of(at, 8), amount)

    def down(i):
        other = offset[i] + (1 - bits[i]) * size[i]
        held = src if i == 0 else parts[i - 1]
        at = other if i == 0 else other - offset[i]
        return rcopy(held.at[rows(at, size[i])], parts[count + i], rs.at[i], rr.at[i], peers[i])

    def fold(i):
        down(i).wait_recv()
        held = src if i == 0 else parts[i - 1]
        at = offset[i + 1] if i == 0 else offset[i + 1] - offset[i]
        parts[i][...] = held[rows(at, size[i])] + parts[count + i][...]

    def back(i):
        spot = total.at[rows(offset[i + 1], size[i])]
        return rcopy(spot, spot, gs.at[i], gr.at[i], peers[i])

    def back_recv(i):
        spot = total.at[rows(offset[i] + (1 - bits[i]) * size[i], size[i])]
        rcopy(spot, spot, gs.at[i], gr.at[i], peers[i]).wait_recv()

    steps = [lambda: down(0).start()]
    for i in range(1, count):

        def step(i=i):
            fold(i - 1)
            down(i).start()

        steps.append(step)

    def middle():
        fold(count - 1)
        total[rows(offset[count], size[-1])] = parts[count - 1][...]
        back(count - 1).start()

    steps.append(middle)
    for i in range(count - 2, -1, -1):

        def step(i=i):
            back_recv(i + 1)
            back(i).start()

        steps.append(step)

    def end():
        back_recv(0)
        for i in range(count):
            down(i).wait_send()
            back(i).wait_send()

    return steps, end


highest = lax.Precision.HIGHEST


def fine(a, b, contract=((1,), (0,))):
    return lax.dot_general(a, b, (contract, ((), ())), precision=highest, preferred_element_type=f32)


def same_head(size, part):
    one = lax.broadcasted_iota(jnp.int32, (size, size), 0) // part
    two = lax.broadcasted_iota(jnp.int32, (size, size), 1) // part
    return (one == two).astype(f32)


def student_stats(docs, scale, out_ref, seg_ref, proj_ref, vec_ref, hidden, logit, stats):
    width = hidden.shape[1]
    h = jnp.dot(out_ref[...], proj_ref[...], preferred_element_type=f32) + vec_ref[0:1]
    pool = fine(h * vec_ref[1:2], same_head(width, SHD)) * scale
    hidden[...] = h
    logit[...] = pool
    stats[0:8] = jnp.zeros((8, width), f32)
    stats[8:16] = jnp.zeros((8, width), f32)
    stats[16:24] = jnp.ones((8, width), f32)
    for doc in range(docs):
        mine = seg_ref[...] == doc
        top = jnp.max(jnp.where(mine, pool, masked_value), axis=0, keepdims=True)
        weight = jnp.where(mine, jnp.exp(pool - top), 0.0)
        stats[doc : doc + 1] = jnp.sum(weight * h, axis=0, keepdims=True)
        stats[8 + doc : 9 + doc] = top
        stats[16 + doc : 17 + doc] = jnp.sum(weight, axis=0, keepdims=True)


def student_grads(docs, classes, scale, once, row, out_ref, seg_ref, label_ref, vec_ref, mid_ref, cls_ref, hidden, logit, stats, small):
    width = hidden.shape[1]
    every = [stats[i, j] for i in range(stats.shape[0]) for j in range(stats.shape[1])]
    top = every[0][8:16]
    for one in every[1:]:
        top = jnp.maximum(top, one[8:16])
    total = jnp.zeros_like(top)
    pooled = jnp.zeros_like(top)
    for one in every:
        factor = jnp.exp(one[8:16] - top)
        total = total + one[16:24] * factor
        pooled = pooled + one[0:8] * factor
    pooled = pooled / total
    middle = jnp.tanh(fine(pooled, mid_ref[...]) + vec_ref[2:3])
    logits = fine(middle, cls_ref[...]) + vec_ref[3:4]
    lane = lax.broadcasted_iota(jnp.int32, logits.shape, 1)
    doc = lax.broadcasted_iota(jnp.int32, logits.shape, 0)
    real = lane < classes
    peak = jnp.max(jnp.where(real, logits, masked_value), axis=1, keepdims=True)
    share = jnp.where(real, jnp.exp(logits - peak), 0.0)
    share = share / jnp.sum(share, axis=1, keepdims=True)
    d_logits = jnp.where(doc < docs, share - (label_ref[...] == lane).astype(f32), 0.0)
    d_middle = fine(d_logits, cls_ref[...], ((1,), (1,))) * (1.0 - middle * middle)
    d_pooled = fine(d_middle, mid_ref[...], ((1,), (1,)))
    zeros = jnp.zeros((1, width), f32)
    small[768:896] = fine(pooled, d_middle, ((0,), (0,))) * once
    small[896:912] = fine(d_logits, middle, ((0,), (0,)))[0:16] * once
    small[912:913] = jnp.sum(d_middle, axis=0, keepdims=True) * once
    small[913:914] = jnp.sum(d_logits, axis=0, keepdims=True) * once
    for at in range(4):
        small[920 + 8 * at : 928 + 8 * at] = jnp.where(row == at, logits * once, 0.0)

    heads = same_head(width, SHD)
    base = fine(d_pooled * pooled, heads)
    h, pool = hidden[...], logit[...]
    top_t, total_t = jnp.zeros_like(h), jnp.ones_like(h)
    back_t, base_t = jnp.zeros_like(h), jnp.zeros_like(h)
    for doc in range(docs):
        mine = seg_ref[...] == doc
        top_t = jnp.where(mine, top[doc : doc + 1], top_t)
        total_t = jnp.where(mine, total[doc : doc + 1], total_t)
        back_t = jnp.where(mine, d_pooled[doc : doc + 1], back_t)
        base_t = jnp.where(mine, base[doc : doc + 1], base_t)
    share = jnp.exp(pool - top_t) / total_t
    d_pool = share * (fine(back_t * h, heads) - base_t)
    d_h = share * back_t + d_pool * vec_ref[1:2] * scale
    small[914:915] = jnp.sum(d_h, axis=0, keepdims=True)
    small[915:916] = jnp.sum(d_pool * h, axis=0, keepdims=True) * scale
    for i in range(916, 920):
        small[i : i + 1] = zeros
    small[0:768] = fine(out_ref[...].astype(f32), d_h, ((0,), (0,)))


def tail_kernel(docs, classes, scale, *refs):
    kinds = 2
    grads, refs = refs[:kinds], refs[kinds:]
    (q_ref, kv_ref, lse_ref, ctx_ref, dctx_ref, ints_ref), refs = refs[:6], refs[6:]
    (out_ref, seg_ref, label_ref, proj_ref, svec_ref, mid_ref, cls_ref), refs = refs[:7], refs[7:]
    vec_refs, refs = refs[:7], refs[7:]
    (x_ref, ctx_all_ref, resid_ref, out_t_ref, w_ref), refs = refs[:5], refs[5:]
    outs, refs = refs[: kinds + 1], refs[kinds + 1 :]
    (give_out, out_out, small_out), refs = refs[:3], refs[3:]
    (total, theirs, dqkv, own_grads, dpad, weights, resid_t, give_src), refs = refs[:8], refs[8:]
    (dctx, dq, dkv, kn, vn, q3, dc3, dq_scr, dkv_scr, bias_scr, landed, kcol, qsegs, deltas), refs = refs[:14], refs[14:]
    (hidden, logit, stats, stats_all, small), refs = refs[:5], refs[5:]
    parts, refs = refs[:10], refs[10:]
    (send, recv, psend, precv), sems, (wl, gl, gs, gr), refs = refs[:4], refs[4:8], refs[8:12], refs[12:]
    (dsend, drecv, ssend, srecv, ol, osend, orecv), scratch = refs[:7], refs[7:]
    d, r, c = place()
    pn = (1 - d, r, c)
    tiles, deep, tile = kv_ref.shape
    wide = deep // 2
    heads = wide // HD
    full = dqkv.shape[1]
    own = q_ref.shape[2]
    kv_rows, q_rows = pl.ds(0, deep), pl.ds(deep, wide)
    peers = line_peers()
    greet(plane_peers() + peers[:3] + peers[4:])

    def to_heads(j):
        return rcopy(dctx_ref.at[c ^ j], dctx.at[c], dsend.at[j], drecv.at[j], (d, r, c ^ j))

    for j in (3, 2, 1):
        to_heads(j).start()
    dctx[c] = dctx_ref[c]
    load_w = pltpu.make_async_copy(w_ref, weights, wl)
    load_w.start()

    def tell(j):
        return rcopy(stats, stats_all.at[d, c], ssend.at[j - 1], srecv.at[j - 1], peers[j - 1])

    out_start, out_finish = give_moves(out_t_ref, out_out, ol, osend, orecv)
    start, finish = give_moves(give_src, give_out, gl, gs, gr)
    steps, end = sum_steps(small, small_out, parts, sems)
    pool_scale = SHD ** (-0.5)

    def begin():
        out_start()
        student_stats(docs, pool_scale, out_ref, seg_ref, proj_ref, svec_ref, hidden, logit, stats)
        for j in range(1, 8):
            tell(j).start()
        stats_all[d, c] = stats[...]
        spare = full - deep - wide
        for at in range(4):
            dqkv[at, pl.ds(deep + wide, spare)] = jnp.zeros((spare, own), bf16)
        resid_t[...] = resid_ref[...].T
        feats = x_ref.shape[1]
        blank = dpad.shape[1] - feats
        for row in range(4):
            dpad[row, pl.ds(0, blank)] = jnp.zeros((blank, own), bf16)
            dpad[row, pl.ds(blank, feats)] = resid_t[pl.ds(row * feats, feats)].astype(bf16)
        at = 952
        for ref in vec_refs:
            for i in range(ref.shape[0]):
                for j in range(ref.shape[1] // 128):
                    small[at : at + 1] = ref[i : i + 1, j * 128 : (j + 1) * 128]
                    at += 1
        for i in range(at, small.shape[0]):
            small[i : i + 1] = jnp.zeros((1, 128), f32)

    def student(_):
        for j in range(1, 8):
            tell(j).wait_recv()
        once = 1.0 / 8
        student_grads(
            docs, classes, pool_scale, once, r, out_ref, seg_ref, label_ref, svec_ref, mid_ref, cls_ref, hidden, logit,
            stats_all, small,
        )

    def segment(at):
        return ints_ref[r // 2, r % 2, pl.ds(at, 1)].astype(f32)

    def prepare(_):
        @pl.loop(0, tiles)
        def _(j):
            kn[j] = kv_ref[j, pl.ds(0, wide)].astype(f32).T.astype(bf16)
            vn[j] = kv_ref[j, pl.ds(wide, wide)].astype(f32).T.astype(bf16)

        for j in range(tiles):
            kcol[j] = jnp.broadcast_to(segment(j), (128, own)).T
        bias_scr[...] = jnp.zeros_like(bias_scr)
        dq_scr[...] = jnp.zeros_like(dq_scr)
        for block in range(4):
            block_rows(q_ref.at[pl.ds(block, 1)], heads, scale, q3.at[block])
            qsegs[block] = jnp.concatenate([segment(2 * block + d)] * heads, axis=1)
        for j in (1, 2, 3):
            to_heads(j).wait_recv()
        for block in range(4):
            block_rows(dctx.at[pl.ds(block, 1)], heads, 1.0, dc3.at[block])
            product = ctx_ref[block].astype(f32) * dctx[block].astype(f32)
            deltas[block] = jnp.concatenate(
                [jnp.sum(product[h * HD : (h + 1) * HD], axis=0, keepdims=True) for h in range(heads)], axis=1
            )

    ones = jnp.ones((8, own), bf16)
    across = (((1,), (1,)), ((), ()))

    def attend(j, _):
        if j < 3:
            settle(j + 1)
        for core in range(2):
            tile_at = 2 * (c ^ j) + core
            k_nat, v_nat = kn.at[tile_at], vn.at[tile_at]
            k_t = kv_ref.at[tile_at]
            seen = jnp.concatenate([kcol[tile_at]] * (heads * own // 128), axis=1)
            dkv_scr[...] = jnp.zeros_like(dkv_scr)

            @pl.loop(jnp.maximum(tile_at - 3 - d, 0) // 2, jnp.minimum((tile_at + 4 - d) // 2 + 1, 4))
            def _(block):
                s = jnp.dot(k_nat[...], q3[block], preferred_element_type=f32)
                p = jnp.exp(jnp.where(seen == qsegs[block], s, masked_value) - lse_ref[block])
                d_p = jnp.dot(v_nat[...], dc3[block], preferred_element_type=f32)
                d_s = (p * (d_p - deltas[block])).astype(bf16)
                p = p.astype(bf16)
                for h in range(heads):
                    rows, lanes = pl.ds(h * HD, HD), slice(h * own, (h + 1) * own)
                    low = pl.ds(wide + h * HD, HD)
                    dq_scr[block, rows] += jnp.dot(k_t[rows], d_s[:, lanes], preferred_element_type=f32)
                    dkv_scr[rows] += lax.dot_general(
                        q3[block, rows, lanes], d_s[:, lanes], across, preferred_element_type=f32
                    )
                    dkv_scr[low] += lax.dot_general(dctx[block, rows], p[:, lanes], across, preferred_element_type=f32)

            made = dkv_scr[...].astype(bf16)
            dkv[c ^ j, core] = made
            bias_scr[:, wide:] += lax.dot_general(ones, made[wide:], across, preferred_element_type=f32)
        pair(j).start()

    def settle(j):
        pair(j).wait_recv()
        if j:
            total[c ^ j] = dkv[c ^ j, d] + theirs[c ^ j]
            kv(j).start()
        else:
            landed[c, kv_rows] = dkv[c, d] + theirs[c]

    def pair(j):
        return rcopy(dkv.at[c ^ j, 1 - d], theirs.at[c ^ j], psend.at[j], precv.at[j], pn)

    def kv(j):
        return rcopy(total.at[c ^ j], landed.at[c, kv_rows], send.at[0, j], recv.at[0, j], (d, r, c ^ j))

    def q(j):
        return rcopy(dq.at[c ^ j], landed.at[c, q_rows], send.at[1, j], recv.at[1, j], (d, r, c ^ j))

    def leave(_):
        for j in (3, 2, 1, 0):
            made = (dq_scr[c ^ j] * scale).astype(bf16)
            dq[c ^ j] = made
            bias_scr[:, :wide] += lax.dot_general(ones, made, across, preferred_element_type=f32)
            if j:
                q(j).start()
        landed[c, q_rows] = dq[c]
        settle(0)
        for i in range(3):
            small[pl.ds(1012 + 3 * c + i, 1)] = bias_scr[0:1, i * 128 : (i + 1) * 128]

    def make(at):
        lead = full - dpad.shape[1]

        @pl.loop(0, 4)
        def _(row):
            one = lax.dot_general(x_ref[row], dqkv[at], across, preferred_element_type=f32)
            two = lax.dot_general(ctx_all_ref[at], dpad[row], across, preferred_element_type=f32)
            shape = own_grads.shape[2:4] + (-1,)
            own_grads[at, row, :, :, :lead] = one[:, :lead].astype(bf16).reshape(shape)
            own_grads[at, row, :, :, lead:] = (one[:, lead:] + two).astype(bf16).reshape(shape)

    def make_chunk(j, launch):
        if j == 0:
            for far in (1, 2, 3):
                q(far).wait_recv()
                kv(far).wait_recv()

            @pl.loop(0, 4)
            def _(at):
                for h in range(heads):
                    for slot, spot in enumerate((deep, 0, wide)):
                        dqkv[at, pl.ds((3 * h + slot) * HD, HD)] = landed[at, pl.ds(spot + h * HD, HD)]

        make((0, 3, 1, 2)[j])
        launch(kinds * 4 + j)

    def input_grad(_):
        load_w.wait()
        feats = x_ref.shape[1]

        @pl.loop(0, 4)
        def _(row):
            part = resid_t[pl.ds(pl.multiple_of(row * feats, 8), feats)]
            for at in range(4):
                w = weights[at, row].reshape(feats, full)
                part = part + jnp.dot(w, dqkv[at], preferred_element_type=f32)
            give_src[row] = part.astype(bf16)

        start()

    gap = 1
    hooks = [[] for _ in range(max(8 + gap + 5, 8 + len(steps)))]
    hooks[0].append(prepare)
    for i, j in enumerate((3, 2, 1, 0)):
        hooks[1 + i].append(functools.partial(attend, j))
    hooks[5].append(leave)
    hooks[6].append(student)
    for i, step in enumerate(steps):
        hooks[8 + i].append(lambda launch, step=step: step())
    for j in range(4):
        hooks[7 + gap + j].append(functools.partial(make_chunk, j))
    hooks[11 + gap].append(input_grad)

    def run(todo, launch):
        for one in todo:
            one(launch)

    during = [functools.partial(run, todo) for todo in hooks]
    scatter_core(list(grads) + [own_grads], outs, scratch, begin, during, late=1, gap=gap)
    end()
    finish()
    out_finish()
    for j in range(1, 8):
        tell(j).wait_send()
    for j in range(4):
        pair(j).wait_send()
    for j in (1, 2, 3):
        to_heads(j).wait_send()
        q(j).wait_send()
        kv(j).wait_send()


def tail_fast(docs, classes, scale, grads, attention, student, vectors, rest, out_t, w_attn, cid):
    n, w = grads[0].shape[3:]
    q, kv = attention[:2]
    dma = pltpu.SemaphoreType.DMA
    tiles, deep, own = kv.shape
    wide = deep // 2
    cols = tiles // 2
    feats = rest[0].shape[1]
    student_width = student[3].shape[1]
    tall = 1024
    parts = [pltpu.VMEM((tall >> (i + 1), 128), f32) for i in range(5)]
    home = jax.ShapeDtypeStruct((2, feats, 2 * own), bf16)
    return pl.pallas_call(
        functools.partial(tail_kernel, docs, classes, scale),
        out_shape=[jax.ShapeDtypeStruct((2, n, w), bf16)] * 3 + [home, home, jax.ShapeDtypeStruct((tall, 128), f32)],
        in_specs=[HBM] * 2 + [VM] * (len(attention) + len(student) + len(vectors) + len(rest)) + [HBM] * 2,
        out_specs=[HBM] * 5 + [VM],
        scratch_shapes=[
            pltpu.VMEM((cols, deep, own), bf16),
            pltpu.VMEM((cols, deep, own), bf16),
            pltpu.VMEM((cols, w, own), bf16),
            pltpu.VMEM((4, 4, 2, n, w), bf16),
            pltpu.VMEM((4, 256, own), bf16),
            pltpu.VMEM((4, 4, 2, n, w), bf16),
            pltpu.VMEM((4 * feats, own), f32),
            pltpu.VMEM((4, feats, own), bf16),
            pltpu.VMEM((cols, wide, own), bf16),
            pltpu.VMEM((cols, wide, own), bf16),
            pltpu.VMEM((cols, 2, deep, own), bf16),
            pltpu.VMEM((tiles, own, wide), bf16),
            pltpu.VMEM((tiles, own, wide), bf16),
            pltpu.VMEM((4, wide, wide // HD * own), bf16),
            pltpu.VMEM((4, wide, wide // HD * own), bf16),
            pltpu.VMEM((4, wide, own), f32),
            pltpu.VMEM((deep, own), f32),
            pltpu.VMEM((8, deep), f32),
            pltpu.VMEM((cols, deep + wide, own), bf16),
            pltpu.VMEM((tiles, own, 128), f32),
            pltpu.VMEM((4, 1, wide // HD * own), f32),
            pltpu.VMEM((4, 1, wide // HD * own), f32),
            pltpu.VMEM((own, student_width), f32),
            pltpu.VMEM((own, student_width), f32),
            pltpu.VMEM((24, student_width), f32),
            pltpu.VMEM((2, 4, 24, student_width), f32),
            pltpu.VMEM((tall, 128), f32),
        ]
        + parts * 2
        + [dma((2, 4)), dma((2, 4)), dma((4,)), dma((4,)), dma((5,)), dma((5,)), dma((5,)), dma((5,))]
        + [dma, dma, dma((4,)), dma((2, 2))]
        + [dma((4,)), dma((4,)), dma((7,)), dma((7,)), dma, dma((4,)), dma((2, 2))]
        + scatter_scratch(3, n, w, bf16),
        compiler_params=pltpu.CompilerParams(
            collective_id=cid, has_side_effects=True, vmem_limit_bytes=60 * 1024 * 1024
        ),
        name="tail",
    )(*grads, *attention, *student, *vectors, *rest, out_t.reshape(4, feats, own), w_attn)


def finish_kernel(docs, classes, in_ref, back_ref, attn_ref, grad_ref, small_ref, *outs):
    d, r, c = place()
    w_qkv, w_out, w_in, w_back, tokens, proj, logits, b_qkv, b_in, singles = outs[:9] + (outs[9:],)
    rows = in_ref.shape[0] * in_ref.shape[1]
    w_in[...] = in_ref[...].reshape(rows, -1).astype(f32)
    w_back[...] = back_ref[...].reshape(rows, -1).astype(f32)
    columns = w_qkv.shape[1]
    w_qkv[...] = attn_ref[:, :, :columns].reshape(rows, -1).astype(f32)
    w_out[...] = attn_ref[:, :, columns:].reshape(rows, -1).astype(f32)
    tokens[...] = grad_ref[...].astype(f32)
    feats = proj.shape[0]
    proj[...] = small_ref[pl.ds(pl.multiple_of(r * feats, 8), feats)]
    for i in range(2):
        some = small_ref[pl.ds(pl.multiple_of(920 + 8 * (2 * d + i), 8), 8)]
        logits[i] = some[:docs, :classes]
    line = [small_ref[pl.ds(1012 + 3 * c + i, 1)] for i in range(3)]
    line = jnp.concatenate(line, axis=1)
    wide = b_qkv.shape[1]
    b_qkv[0:1] = line[:, :wide]
    b_qkv[1:2] = line[:, wide:]
    for i in range(b_in.shape[1] // 128):
        b_in[:, i * 128 : (i + 1) * 128] = small_ref[pl.ds(952 + 6 * c + i, 1)]
    for i in range(6):
        line = [small_ref[976 + 6 * i + j : 977 + 6 * i + j] for j in range(6)]
        line = jnp.concatenate(line, axis=1)
        for row in range(4):

            @pl.when(r == row)
            def _():
                singles[i][...] = line[:, row * feats : (row + 1) * feats]

    s_mid, s_cls, s_mid_bias, s_cls_bias, s_bias, s_query = singles[6:]
    s_mid[...] = small_ref[768:896]
    s_cls[...] = jnp.concatenate([small_ref[896:912]] + [jnp.zeros((112, 128), f32)], axis=0).T[:, :classes]
    s_mid_bias[...] = small_ref[912:913]
    s_cls_bias[...] = small_ref[913:914, :classes]
    s_bias[...] = small_ref[914:915]
    s_query[...] = small_ref[915:916]


def finish_fast(docs, classes, w_in, w_back, w_attn, grad, small, columns):
    _, part, hidden = w_in.shape
    feats = 2 * part
    width = small.shape[1]

    def shape(*dims):
        return jax.ShapeDtypeStruct(dims, f32)

    shapes = [
        shape(feats, columns), shape(w_attn.shape[2] - columns, feats), shape(feats, hidden), shape(feats, hidden),
        shape(*grad.shape), shape(feats, width), shape(2, docs, classes), shape(2, columns // 3), shape(1, hidden),
    ]
    shapes += [shape(1, feats)] * 6
    shapes += [shape(width, width), shape(width, classes), shape(1, width), shape(1, classes)] + [shape(1, width)] * 2
    return pl.pallas_call(
        functools.partial(finish_kernel, docs, classes),
        out_shape=shapes,
        in_specs=[VM] * 5,
        out_specs=[VM] * len(shapes),
        name="finish",
    )(w_in, w_back, w_attn, grad, small)


def dot(a, b, contract=((1,), (0,))):
    return lax.dot_general(a, b, (contract, ((), ())), preferred_element_type=f32)


def block_rows(ref, heads, scale, out):
    own = ref.shape[-1]
    for h in range(heads):
        for g in range(heads):
            spot = (pl.ds(h * HD, HD), pl.ds(g * own, own))
            if h == g:
                out[spot] = ref[0, pl.ds(h * HD, HD)] * jnp.asarray(scale, out.dtype)
            else:
                out[spot] = jnp.zeros((HD, own), out.dtype)


def spread_of(values):
    mean_v = jnp.mean(values, axis=1, keepdims=True)
    center = values - mean_v
    inv_std = lax.rsqrt(jnp.mean(center * center, axis=1, keepdims=True) + norm_eps)
    return center * inv_std, inv_std


def spread_back(grad_hat, normed, inv_std):
    return inv_std * (
        grad_hat
        - jnp.mean(grad_hat, axis=1, keepdims=True)
        - normed * jnp.mean(grad_hat * normed, axis=1, keepdims=True)
    )


def dense_kernel(
    ctx_ref, x_ref, cot_ref, wo_ref, vec_ref, b_in_ref, w_in_hbm, w_back_hbm,
    g_in_hbm, g_back_hbm, dctx_ref, out_ref, out_t_ref, resid_ref, gb_in_ref, gb_out_ref, g1_ref, b1_ref, gb_back_ref,
    g2_ref, b2_ref,
    w_in, w_back, g_in, g_back, slope, act, total, hidden, hat, low, low_t, in_sem, back_sem, gi_sem, gb_sem,
):
    cols = w_in.shape[0]
    across = (((1,), (1,)), ((), ()))

    def fetch(c):
        return (
            pltpu.make_async_copy(w_in_hbm.at[c], w_in.at[c], in_sem.at[c]),
            pltpu.make_async_copy(w_back_hbm.at[c], w_back.at[c], back_sem.at[c]),
        )

    def store(c):
        return (
            pltpu.make_async_copy(g_in.at[c], g_in_hbm.at[c], gi_sem.at[c]),
            pltpu.make_async_copy(g_back.at[c], g_back_hbm.at[c], gb_sem.at[c]),
        )

    for c in range(cols):
        for copy in fetch(c):
            copy.start()

    def natural(ref):
        return ref[...].reshape(-1, ref.shape[2]).astype(f32).T

    b_out, gain_one, bias_one, b_back, gain_two, bias_two = [vec_ref[i : i + 1] for i in range(6)]
    attn_out = jnp.dot(natural(ctx_ref).astype(bf16), wo_ref[...], preferred_element_type=f32) + b_out
    hat_one, inv_one = spread_of(natural(x_ref) + attn_out)
    hidden_one = hat_one * gain_one + bias_one
    hat[...] = hat_one
    hidden[...] = hidden_one
    low[...] = hidden_one.astype(bf16)
    low_t[...] = hidden_one.T.astype(bf16)
    total[...] = jnp.zeros_like(total)

    @pl.loop(0, cols)
    def _(c):
        into, out = fetch(c)
        into.wait()
        pre = jnp.dot(low[...], w_in[c], preferred_element_type=f32) + b_in_ref[pl.ds(c, 1)]
        share = 0.5 + 0.5 * lax.erf(pre * (0.5**0.5))
        slope[c] = share + pre * (jnp.exp(-0.5 * pre * pre) * (0.5 / math.pi) ** 0.5)
        made = (pre * share).astype(bf16)
        act[c] = made
        out.wait()
        total[...] += lax.dot_general(made, w_back[c], across, preferred_element_type=f32)

    hat_two, inv_two = spread_of(hidden[...] + total[...] + b_back)
    layer_out = hat_two * gain_two + bias_two
    out_ref[...] = layer_out.astype(bf16)
    out_t_ref[...] = layer_out.T.astype(bf16).reshape(out_t_ref.shape)
    cot = natural(cot_ref)
    g2_ref[...] = jnp.sum(cot * hat_two, axis=0, keepdims=True)
    b2_ref[...] = jnp.sum(cot, axis=0, keepdims=True)
    d_two = spread_back(cot * gain_two, hat_two, inv_two)
    d_ffn = d_two.astype(bf16)
    gb_back_ref[...] = jnp.sum(d_ffn.astype(f32), axis=0, keepdims=True)
    d_ffn_t = d_two.T.astype(bf16)
    total[...] = d_two

    @pl.loop(0, cols)
    def _(c):
        to_in, to_back = store(c)
        g_back[c] = jnp.dot(d_ffn_t, act[c], preferred_element_type=f32).astype(bf16)
        to_back.start()
        d_pre = (slope[c] * jnp.dot(d_ffn, w_back[c], preferred_element_type=f32)).astype(bf16)
        gb_in_ref[pl.ds(c, 1)] = jnp.sum(d_pre.astype(f32), axis=0, keepdims=True)
        total[...] += lax.dot_general(d_pre, w_in[c], across, preferred_element_type=f32)
        g_in[c] = jnp.dot(low_t[...], d_pre, preferred_element_type=f32).astype(bf16)
        to_in.start()

    d_hidden, hat_one = total[...], hat[...]
    g1_ref[...] = jnp.sum(d_hidden * hat_one, axis=0, keepdims=True)
    b1_ref[...] = jnp.sum(d_hidden, axis=0, keepdims=True)
    d_one = spread_back(d_hidden * gain_one, hat_one, inv_one)
    resid_ref[...] = d_one
    d_attn = d_one.astype(bf16)
    gb_out_ref[...] = jnp.sum(d_attn.astype(f32), axis=0, keepdims=True)
    d_ctx = lax.dot_general(wo_ref[...], d_attn, across, preferred_element_type=f32)
    dctx_ref[...] = d_ctx.astype(bf16).reshape(dctx_ref.shape)

    @pl.loop(0, cols)
    def _(c):
        for copy in store(c):
            copy.wait()


def dense_fast(ctx, x, cot, wo, vec, b_in, w_in, w_back):
    cols, width, hidden = w_in.shape
    own = x.shape[2]
    dma = pltpu.SemaphoreType.DMA
    shape = jax.ShapeDtypeStruct
    line = shape((1, width), f32)
    weight = shape(w_in.shape, bf16)
    return pl.pallas_call(
        dense_kernel,
        out_shape=[
            weight, weight, shape(ctx.shape, bf16), shape((own, width), bf16), shape(x.shape, bf16),
            shape((own, width), f32), shape((cols, hidden), f32),
        ]
        + [line] * 6,
        in_specs=[VM] * 6 + [HBM] * 2,
        out_specs=[HBM] * 2 + [VM] * 11,
        scratch_shapes=[
            pltpu.VMEM((cols, width, hidden), bf16),
            pltpu.VMEM((cols, width, hidden), bf16),
            pltpu.VMEM((cols, width, hidden), bf16),
            pltpu.VMEM((cols, width, hidden), bf16),
            pltpu.VMEM((cols, own, hidden), f32),
            pltpu.VMEM((cols, own, hidden), bf16),
            pltpu.VMEM((own, width), f32),
            pltpu.VMEM((own, width), f32),
            pltpu.VMEM((own, width), f32),
            pltpu.VMEM((own, width), bf16),
            pltpu.VMEM((width, own), bf16),
            dma((cols,)), dma((cols,)), dma((cols,)), dma((cols,)),
        ],
        compiler_params=pltpu.CompilerParams(vmem_limit_bytes=56 * 1024 * 1024),
        name="dense",
    )(ctx, x, cot, wo, vec, b_in, w_in, w_back)


def fast_local(
    tokens,
    segments,
    labels,
    cotangent,
    w_qkv,
    b_qkv,
    w_out,
    b_out,
    ln1_gain,
    ln1_bias,
    w_in,
    b_in,
    w_back,
    b_back,
    ln2_gain,
    ln2_bias,
    s_proj,
    s_bias,
    s_query,
    s_mid,
    s_mid_bias,
    s_cls,
    s_cls_bias,
):
    _, width_row, cols_local = tokens.shape
    parts, rows, cols, seqs, _ = sizes(tokens.shape[0])
    width = width_row * rows
    own = cols_local // parts
    width_col = b_qkv.shape[1]
    heads_dev = width_col // HD
    hidden_col = b_in.shape[0]
    docs_count = labels.shape[1]
    class_count = s_cls.shape[1]
    student_width = s_proj.shape[1]
    seq_len = segments.shape[1]
    row_index = lax.axis_index("row")
    col_index = lax.axis_index("col")
    dp_index = lax.axis_index("dp")
    score_scale = HD ** (-0.5)
    pool_scale = SHD ** (-0.5)
    query_heads = s_query.reshape(SH, SHD)
    doc_ids = jnp.arange(docs_count, dtype=jnp.int32)
    class_ids = jnp.arange(class_count, dtype=jnp.int32)

    ints = jnp.pad(labels, ((0, 0), (0, own - docs_count)))[:, None]
    ints = jnp.concatenate([segments.reshape(-1, seq_len // own, own), ints], axis=1)
    ints = jnp.pad(ints, ((0, 0), (0, 16 - ints.shape[1]), (0, 0)))
    row_vectors = [b_out, ln1_gain, ln1_bias, b_back, ln2_gain, ln2_bias]
    (
        w_attn, w_in_all, w_back_all, x_parts, c_parts, ints, queries, kv, w_out_all, row_vectors, b_in_all,
        s_proj_all, context, lse, ctx_parts,
    ) = head_fast(
        [w_qkv, w_out, w_in, w_back],
        tokens,
        cotangent,
        ints,
        [b_qkv, b_in[None], s_proj] + [v[None] for v in row_vectors],
        score_scale,
        1,
    )
    w_in_all = w_in_all.reshape(cols, width, hidden_col)
    w_back_all = w_back_all.reshape(cols, width, hidden_col)
    kv = kv.reshape(cols * parts, 2 * width_col, own)
    own_ints = lax.dynamic_index_in_dim(ints.reshape(seqs, 16, own), row_index, 0, False)
    seg_own = lax.dynamic_index_in_dim(own_ints, 2 * col_index + dp_index, 0, False)
    label_seq = own_ints[seq_len // own, :docs_count]

    (
        g_in, g_back, d_ctx, layer_out, out_t, d_resid_one, g_in_bias, g_out_bias, g_ln1_gain, g_ln1_bias, g_back_bias,
        g_ln2_gain, g_ln2_bias,
    ) = dense_fast(ctx_parts, x_parts, c_parts, w_out_all, row_vectors, b_in_all, w_in_all, w_back_all)

    blocked = (cols, rows, parts, width_row // parts, -1)
    lane_pad = ((0, 0), (0, 128 - class_count))
    student_vectors = jnp.stack([s_bias, s_query, s_mid_bias, jnp.pad(s_cls_bias, (0, 128 - class_count))])
    student_vectors = jnp.pad(student_vectors, ((0, 4), (0, 0)))
    g_in, g_back, g_attn, grad_tokens, out, small = tail_fast(
        docs_count,
        class_count,
        score_scale,
        [g_in.reshape(blocked), g_back.reshape(blocked)],
        [queries, kv, lse, context, d_ctx, ints],
        [
            layer_out,
            seg_own[:, None],
            jnp.pad(label_seq, (0, 8 - docs_count))[:, None],
            s_proj_all,
            student_vectors,
            s_mid,
            jnp.pad(s_cls, lane_pad),
        ],
        [g_in_bias, g_out_bias, g_ln1_gain, g_ln1_bias, g_back_bias, g_ln2_gain, g_ln2_bias],
        [x_parts, ctx_parts, d_resid_one],
        out_t.reshape(width, own),
        w_attn,
        4,
    )
    (
        g_qkv, g_out, g_in, g_back, grad_tokens, g_sproj, logits, g_qkv_bias, g_in_bias, g_out_bias, g_ln1_gain,
        g_ln1_bias, g_back_bias, g_ln2_gain, g_ln2_bias, g_mid, g_cls, g_mid_bias, g_cls_bias, g_sbias, g_query,
    ) = finish_fast(docs_count, class_count, g_in, g_back, g_attn, grad_tokens, small, 3 * width_col)
    return (
        out,
        logits,
        grad_tokens,
        g_qkv,
        g_qkv_bias,
        g_out,
        g_out_bias[0],
        g_ln1_gain[0],
        g_ln1_bias[0],
        g_in,
        g_in_bias[0],
        g_back,
        g_back_bias[0],
        g_ln2_gain[0],
        g_ln2_bias[0],
        g_sproj,
        g_sbias[0],
        g_query[0],
        g_mid,
        g_mid_bias[0],
        g_cls,
        g_cls_bias[0],
    )


def solution(mesh):
    row, col = P("row"), P("col")
    grid, whole = P("row", "col"), P("dp", "row", "col")
    placed = (
        (whole, P("dp", None), P("dp", None), whole, grid, P(None, "col"), P("col", "row"))
        + (row, row, row, grid, col, grid, row, row, row, P("row", None))
        + (P(),) * 6
    )
    results = (
        (whole, P("dp", None, None), whole, grid, P(None, "col"), P("col", "row"))
        + (row, row, row, grid, col, grid, row, row, row, P("row", None))
        + (P(),) * 6
    )
    quick = dict(mesh.shape) == {"dp": 2, "row": 4, "col": 4}
    local = fast_local if quick else general_local
    return jax.shard_map(local, mesh=mesh, in_specs=placed, out_specs=results, check_vma=False)
```
